32 devices in a mesh: dp: 1 (over z), cp: 32 (over y, x, core).
Axes of the slice: x: 4, y: 4, z: 1, core: 2. Of those that a mesh axis runs over, the one named last changes fastest.
The devices are a block of a 4x4x8 slice.
Arguments:
- x_act: bfloat16 [1, 4096, 3072], P('dp', 'cp')
- d_out: bfloat16 [1, 4096, 3072], P('dp', 'cp')
- positions: int32 [1, 4096], P('dp', 'cp')
- ln_gain: float32 [3072], replicated
- ln_bias: float32 [3072], replicated
- w_query: bfloat16 [3072, 32, 128], replicated
- w_key: bfloat16 [3072, 8, 128], replicated
- w_value: bfloat16 [3072, 8, 128], replicated
- w_out: bfloat16 [4096, 3072], replicated
Outputs:
- output 1: bfloat16 [1, 4096, 3072], P('dp', 'cp')
- output 2: bfloat16 [1, 4096, 3072], P('dp', 'cp')
- output 3: float32 [3072, 32, 128], P(('dp', 'cp'))
- output 4: float32 [3072, 8, 128], P(('dp', 'cp'))
- output 5: float32 [3072, 8, 128], P(('dp', 'cp'))
- output 6: float32 [4096, 3072], P(('dp', 'cp'))
- output 7: float32 [3072], P('dp')
- output 8: float32 [3072], P('dp')
All inputs are finite; a program needn't handle non-finite values.
Results may differ from the reference program's by a relative error of at most 0.00603942.
Values are sent between devices in bfloat16 or wider.
A program may use at most 768 MiB of HBM per device.

```python
import math
import jax
import jax.numpy as jnp
from jax import lax

BATCH = 1
SEQ = 4096
WIDTH = 3072
Q_HEADS = 32
KV_HEADS = 8
HEAD_DIM = 128
Q_TILE = 128
TOKEN_KINDS = 64
DOC_SPAN = 128
GROUPS = Q_HEADS // KV_HEADS
EPS = 1e-5
ROPE_BASE = 10000.0


def setup_inputs(seed: int = 0, part: int = 0) -> dict:
    part_keys = jax.random.split(jax.random.fold_in(jax.random.key(seed), part), 5)
    shared_keys = jax.random.split(jax.random.key(seed + 1), 6)
    tokens = jax.random.randint(part_keys[0], (BATCH, SEQ), 0, TOKEN_KINDS)
    token_table = jax.random.normal(part_keys[1], (TOKEN_KINDS, WIDTH), jnp.float32)
    noise_draw = jax.random.normal(part_keys[2], (BATCH, SEQ, WIDTH), jnp.float32)
    x_act = (token_table[tokens] + 0.5 * noise_draw).astype(jnp.bfloat16)
    d_out = jax.random.normal(part_keys[3], (BATCH, SEQ, WIDTH), jnp.float32).astype(jnp.bfloat16)
    doc_flags = jax.random.randint(part_keys[4], (BATCH, SEQ), 0, DOC_SPAN) == 0
    seq_index = jnp.arange(SEQ, dtype=jnp.int32)
    starts = jnp.where(doc_flags, seq_index[None, :], 0)
    positions = (seq_index[None, :] - lax.cummax(starts, axis=1)).astype(jnp.int32)
    fan_in = WIDTH ** -0.5
    w_query = jax.random.normal(shared_keys[0], (WIDTH, Q_HEADS, HEAD_DIM), jnp.float32) * fan_in
    key_noise = jax.random.normal(shared_keys[1], (WIDTH, KV_HEADS, HEAD_DIM), jnp.float32) * fan_in
    w_key = 0.8 * w_query[:, ::GROUPS, :] + 0.6 * key_noise
    w_value = jax.random.normal(shared_keys[2], (WIDTH, KV_HEADS, HEAD_DIM), jnp.float32) * fan_in
    w_out = jax.random.normal(shared_keys[3], (Q_HEADS * HEAD_DIM, WIDTH), jnp.float32) * (Q_HEADS * HEAD_DIM) ** -0.5
    ln_gain = 0.3 * jax.random.normal(shared_keys[4], (WIDTH,), jnp.float32)
    ln_bias = 0.3 * jax.random.normal(shared_keys[5], (WIDTH,), jnp.float32)
    return {'x_act': x_act, 'd_out': d_out, 'positions': positions, 'ln_gain': ln_gain, 'ln_bias': ln_bias, 'w_query': w_query.astype(jnp.bfloat16), 'w_key': w_key.astype(jnp.bfloat16), 'w_value': w_value.astype(jnp.bfloat16), 'w_out': w_out.astype(jnp.bfloat16)}


def norm_forward(x_act, ln_gain, ln_bias):
    x_f32 = x_act.astype(jnp.float32)
    centered = x_f32 - jnp.mean(x_f32, axis=-1, keepdims=True)
    inv_std = lax.rsqrt(jnp.mean(centered * centered, axis=-1, keepdims=True) + EPS)
    x_hat = centered * inv_std
    return (x_hat * (1.0 + ln_gain) + ln_bias).astype(jnp.bfloat16), x_hat, inv_std


def norm_backward(grad_h, x_hat, inv_std, ln_gain):
    grad_hat = grad_h * (1.0 + ln_gain)
    mean_one = jnp.mean(grad_hat, axis=-1, keepdims=True)
    mean_two = jnp.mean(grad_hat * x_hat, axis=-1, keepdims=True)
    return inv_std * (grad_hat - mean_one - x_hat * mean_two)


def rope_tables(positions):
    quarter = HEAD_DIM // 4
    freq_tab = jnp.exp(jnp.arange(quarter, dtype=jnp.float32) * (-2.0 * math.log(ROPE_BASE) / (HEAD_DIM // 2)))
    angles = positions.astype(jnp.float32)[..., None] * freq_tab
    return jnp.cos(angles)[..., None, :], jnp.sin(angles)[..., None, :]


def rope_rotate(values, cos_tab, sin_tab):
    quarter = cos_tab.shape[-1]
    first_half = values[..., :quarter]
    second_half = values[..., quarter:2 * quarter]
    return jnp.concatenate([first_half * cos_tab - second_half * sin_tab, second_half * cos_tab + first_half * sin_tab, values[..., 2 * quarter:]], axis=-1)


def tile_probs(q_tile, key_f, q_first):
    scores = jnp.einsum('bqkgd,blkd->bkgql', q_tile, key_f) * (HEAD_DIM ** -0.5)
    q_index = q_first + jnp.arange(Q_TILE)
    k_index = jnp.arange(SEQ)
    scores = jnp.where(k_index[None, :] <= q_index[:, None], scores, -1e30)
    shifted = jnp.exp(scores - jnp.max(scores, axis=-1, keepdims=True))
    return shifted / jnp.sum(shifted, axis=-1, keepdims=True)


def attention_forward(q_grouped, key_f, value_f):
    def one_tile(tile_idx):
        q_first = tile_idx * Q_TILE
        q_tile = lax.dynamic_slice_in_dim(q_grouped, q_first, Q_TILE, axis=1)
        tile_prob = tile_probs(q_tile, key_f, q_first)
        prob_bf16 = tile_prob.astype(jnp.bfloat16).astype(jnp.float32)
        return jnp.einsum('bkgql,blkd->bqkgd', prob_bf16, value_f).astype(jnp.bfloat16)
    out_tiles = lax.map(one_tile, jnp.arange(SEQ // Q_TILE))
    return jnp.moveaxis(out_tiles, 0, 1).reshape(BATCH * SEQ, Q_HEADS * HEAD_DIM)


def attention_backward(q_grouped, key_f, value_f, grad_attn):
    def one_tile(acc_pair, tile_idx):
        grad_k, grad_v = acc_pair
        q_first = tile_idx * Q_TILE
        q_tile = lax.dynamic_slice_in_dim(q_grouped, q_first, Q_TILE, axis=1)
        ga_tile = lax.dynamic_slice_in_dim(grad_attn, q_first, Q_TILE, axis=1)
        tile_prob = tile_probs(q_tile, key_f, q_first)
        grad_prob = jnp.einsum('bqkgd,blkd->bkgql', ga_tile, value_f)
        row_dot = jnp.sum(tile_prob * grad_prob, axis=-1, keepdims=True)
        grad_score = (tile_prob * (grad_prob - row_dot) * (HEAD_DIM ** -0.5)).astype(jnp.bfloat16).astype(jnp.float32)
        grad_q = jnp.einsum('bkgql,blkd->bqkgd', grad_score, key_f)
        grad_k = grad_k + jnp.einsum('bkgql,bqkgd->blkd', grad_score, q_tile)
        prob_bf16 = tile_prob.astype(jnp.bfloat16).astype(jnp.float32)
        grad_v = grad_v + jnp.einsum('bkgql,bqkgd->blkd', prob_bf16, ga_tile)
        return (grad_k, grad_v), grad_q
    zero_acc = jnp.zeros((BATCH, SEQ, KV_HEADS, HEAD_DIM), jnp.float32)
    (grad_k, grad_v), q_tiles = lax.scan(one_tile, (zero_acc, zero_acc), jnp.arange(SEQ // Q_TILE))
    grad_q = jnp.moveaxis(q_tiles, 0, 1).reshape(BATCH, SEQ, Q_HEADS, HEAD_DIM)
    return grad_q, grad_k, grad_v


def reference(x_act, d_out, positions, ln_gain, ln_bias, w_query, w_key, w_value, w_out):
    n_tokens = BATCH * SEQ
    wq_flat = w_query.reshape(WIDTH, Q_HEADS * HEAD_DIM)
    wk_flat = w_key.reshape(WIDTH, KV_HEADS * HEAD_DIM)
    wv_flat = w_value.reshape(WIDTH, KV_HEADS * HEAD_DIM)
    normed, x_hat, inv_std = norm_forward(x_act, ln_gain, ln_bias)
    flat_h = normed.reshape(n_tokens, WIDTH)
    cos_tab, sin_tab = rope_tables(positions)
    q_act = rope_rotate(jnp.dot(flat_h, wq_flat, preferred_element_type=jnp.float32).reshape(BATCH, SEQ, Q_HEADS, HEAD_DIM), cos_tab, sin_tab).astype(jnp.bfloat16)
    k_act = rope_rotate(jnp.dot(flat_h, wk_flat, preferred_element_type=jnp.float32).reshape(BATCH, SEQ, KV_HEADS, HEAD_DIM), cos_tab, sin_tab).astype(jnp.bfloat16)
    v_act = jnp.dot(flat_h, wv_flat, preferred_element_type=jnp.float32).astype(jnp.bfloat16).reshape(BATCH, SEQ, KV_HEADS, HEAD_DIM)
    q_grouped = q_act.reshape(BATCH, SEQ, KV_HEADS, GROUPS, HEAD_DIM).astype(jnp.float32)
    key_f = k_act.astype(jnp.float32)
    value_f = v_act.astype(jnp.float32)
    attn_act = attention_forward(q_grouped, key_f, value_f)
    block_out = (x_act.astype(jnp.float32) + jnp.dot(attn_act, w_out, preferred_element_type=jnp.float32).reshape(BATCH, SEQ, WIDTH)).astype(jnp.bfloat16)
    grad_flat = d_out.reshape(n_tokens, WIDTH)
    grad_wo = jnp.dot(attn_act.T, grad_flat, preferred_element_type=jnp.float32)
    grad_attn = jnp.dot(grad_flat, w_out.T, preferred_element_type=jnp.float32).astype(jnp.bfloat16)
    grad_q, grad_k, grad_v = attention_backward(q_grouped, key_f, value_f, grad_attn.reshape(BATCH, SEQ, KV_HEADS, GROUPS, HEAD_DIM).astype(jnp.float32))
    grad_q_pre = rope_rotate(grad_q, cos_tab, -sin_tab).astype(jnp.bfloat16).reshape(n_tokens, Q_HEADS * HEAD_DIM)
    grad_k_pre = rope_rotate(grad_k, cos_tab, -sin_tab).astype(jnp.bfloat16).reshape(n_tokens, KV_HEADS * HEAD_DIM)
    grad_v_pre = grad_v.astype(jnp.bfloat16).reshape(n_tokens, KV_HEADS * HEAD_DIM)
    grad_h = (jnp.dot(grad_q_pre, wq_flat.T, preferred_element_type=jnp.float32) + jnp.dot(grad_k_pre, wk_flat.T, preferred_element_type=jnp.float32) + jnp.dot(grad_v_pre, wv_flat.T, preferred_element_type=jnp.float32)).reshape(BATCH, SEQ, WIDTH)
    grad_wq = jnp.dot(flat_h.T, grad_q_pre, preferred_element_type=jnp.float32).reshape(WIDTH, Q_HEADS, HEAD_DIM)
    grad_wk = jnp.dot(flat_h.T, grad_k_pre, preferred_element_type=jnp.float32).reshape(WIDTH, KV_HEADS, HEAD_DIM)
    grad_wv = jnp.dot(flat_h.T, grad_v_pre, preferred_element_type=jnp.float32).reshape(WIDTH, KV_HEADS, HEAD_DIM)
    grad_x = (d_out.astype(jnp.float32) + norm_backward(grad_h, x_hat, inv_std, ln_gain)).astype(jnp.bfloat16)
    grad_gain = jnp.sum(grad_h * x_hat, axis=(0, 1))
    grad_bias = jnp.sum(grad_h, axis=(0, 1))
    return (block_out, grad_x, grad_wq, grad_wk, grad_wv, grad_wo, grad_gain, grad_bias)
```

```python
import functools
import math

import jax
import jax.numpy as jnp
from jax import lax
from jax.experimental import pallas as pl
from jax.experimental.pallas import tpu as pltpu
from jax.sharding import PartitionSpec as P

EPS = 1e-5
ROPE_BASE = 10000.0
BLOCK = 512
AXIS = "cp"
BF16, F32 = jnp.bfloat16, jnp.float32
VMEM_LIMIT = 60 * 1024 * 1024


def norm_forward(x_act, ln_gain, ln_bias):
    x_f32 = x_act.astype(F32)
    centered = x_f32 - jnp.mean(x_f32, axis=-1, keepdims=True)
    inv_std = lax.rsqrt(jnp.mean(centered * centered, axis=-1, keepdims=True) + EPS)
    x_hat = centered * inv_std
    return (x_hat * (1.0 + ln_gain) + ln_bias).astype(BF16), x_hat, inv_std


def norm_backward(grad_h, x_hat, inv_std, ln_gain):
    grad_hat = grad_h * (1.0 + ln_gain)
    mean_one = jnp.mean(grad_hat, axis=-1, keepdims=True)
    mean_two = jnp.mean(grad_hat * x_hat, axis=-1, keepdims=True)
    return inv_std * (grad_hat - mean_one - x_hat * mean_two)


def rope_tables(positions, head_dim):
    quarter = head_dim // 4
    freq_tab = jnp.exp(jnp.arange(quarter, dtype=F32) * (-2.0 * math.log(ROPE_BASE) / (head_dim // 2)))
    angles = positions.astype(F32)[:, None] * freq_tab
    cos, sin = jnp.cos(angles), jnp.sin(angles)
    rest = jnp.zeros((positions.shape[0], head_dim - 2 * quarter), F32)
    return jnp.concatenate([cos, cos, rest + 1.0], axis=1), jnp.concatenate([-sin, sin, rest], axis=1)


def rotate(values, cos_tab, sin_tab):
    head_dim = values.shape[-1]
    quarter = head_dim // 4
    lane = lax.broadcasted_iota(jnp.int32, values.shape, 1)
    partner = jnp.where(lane < quarter, pltpu.roll(values, head_dim - quarter, 1), pltpu.roll(values, quarter, 1))
    return values * cos_tab + partner * sin_tab


def rows_of(index, size):
    return pl.ds(pl.multiple_of(index * size, size), size)


def dot(lhs, rhs):
    return jnp.dot(lhs, rhs, preferred_element_type=F32)


def full_barrier(n_dev):
    me = lax.axis_index(AXIS)
    barrier = pltpu.get_barrier_semaphore()

    def tell(step, carry):
        pl.semaphore_signal(barrier, inc=1, device_id={AXIS: lax.rem(me + step, n_dev)}, device_id_type=pl.DeviceIdType.MESH)
        return carry

    lax.fori_loop(1, n_dev, tell, 0)
    pl.semaphore_wait(barrier, n_dev - 1)


def remote(src, dst, send_sem, recv_sem, peer):
    return pltpu.make_async_remote_copy(src_ref=src, dst_ref=dst, send_sem=send_sem, recv_sem=recv_sem, device_id={AXIS: peer}, device_id_type=pl.DeviceIdType.MESH)


def each(lower, upper, body):
    def step(index, carry):
        body(index)
        return carry

    lax.fori_loop(lower, upper, step, 0)


def project_kernel(h_ref, w_ref, cos_ref, sin_ref, q_ref, k_ref, v_ref):
    head_dim = q_ref.shape[1]
    out = dot(h_ref[...], w_ref[...])
    cos, sin = cos_ref[...], sin_ref[...]
    q_ref[...] = rotate(out[:, :head_dim], cos, sin).astype(BF16)
    k_ref[...] = rotate(out[:, head_dim : 2 * head_dim], cos, sin).astype(BF16)
    v_ref[...] = out[:, 2 * head_dim :].astype(BF16)


def project(h_all, w_head, cos_tab, sin_tab):
    seq, width = h_all.shape
    head_dim = cos_tab.shape[1]
    block = min(BLOCK, seq)
    head_spec = pl.BlockSpec((block, head_dim), lambda i: (i, 0))
    return pl.pallas_call(
        project_kernel,
        grid=(seq // block,),
        out_shape=[jax.ShapeDtypeStruct((seq, head_dim), BF16)] * 3,
        in_specs=[pl.BlockSpec((block, width), lambda i: (i, 0)), pl.BlockSpec(w_head.shape, lambda i: (0, 0)), head_spec, head_spec],
        out_specs=[head_spec] * 3,
        compiler_params=pltpu.CompilerParams(vmem_limit_bytes=VMEM_LIMIT),
        cost_estimate=pl.CostEstimate(flops=2 * seq * width * w_head.shape[1], bytes_accessed=2 * seq * width, transcendentals=0),
        name="project",
    )(h_all, w_head, cos_tab, sin_tab)


def attention_kernel(scale, q_ref, k_ref, v_ref, da_ref, cos_ref, sin_ref, a_ref, dq_ref, dkv_ref, e_ref, dp_ref, m_ref, kt_ref, vt_ref, qt_ref, dat_ref, at_ref, dqt_ref):
    seq, head_dim = q_ref.shape
    block = e_ref.shape[1]
    n_block = seq // block
    fold = scale * math.log2(math.e)

    def prepare(j):
        rows = rows_of(j, block)
        kt_ref[:, rows] = k_ref[rows, :].T
        vt_ref[:, rows] = v_ref[rows, :].T
        dkv_ref[rows, :] = jnp.zeros((block, 2 * head_dim), F32)

    each(0, n_block, prepare)

    def part_sum(values):
        return jnp.sum(values.reshape(block // 8, 8, block), axis=0)

    def one_block(i):
        own = rows_of(i, block)
        qt_ref[...] = q_ref[own, :].T
        dat_ref[...] = da_ref[own, :].T
        at_ref[...] = jnp.zeros_like(at_ref)
        dqt_ref[...] = jnp.zeros_like(dqt_ref)

        def scores(j, carry, diagonal):
            peak, total, mix = carry
            rows = rows_of(j, block)
            s = dot(k_ref[rows, :], qt_ref[...])
            if diagonal:
                key = lax.broadcasted_iota(jnp.int32, (block, block), 0)
                query = lax.broadcasted_iota(jnp.int32, (block, block), 1)
                s = jnp.where(key <= query, s, -1e30)
            top = jnp.maximum(peak, jnp.max(s, axis=0, keepdims=True))
            e = jnp.exp2((s - top) * fold)
            dp = dot(v_ref[rows, :], dat_ref[...])
            fade = jnp.exp2((peak - top) * fold)
            e_ref[rows, :] = e
            dp_ref[rows, :] = dp
            m_ref[j] = top
            return top, total * fade + part_sum(e), mix * fade + part_sum(e * dp)

        start = (jnp.full((1, block), -jnp.inf, F32), jnp.zeros((8, block), F32), jnp.zeros((8, block), F32))
        carry = lax.fori_loop(0, i, functools.partial(scores, diagonal=False), start)
        peak, total, mix = scores(i, carry, True)
        inv = 1.0 / jnp.sum(total, axis=0, keepdims=True)
        row_dot = jnp.sum(mix, axis=0, keepdims=True) * inv
        q_own, da_own = q_ref[own, :], da_ref[own, :]

        def grads(j):
            rows = rows_of(j, block)
            p = e_ref[rows, :] * (jnp.exp2((m_ref[j] - peak) * fold) * inv)
            pb = p.astype(BF16)
            ds = ((dp_ref[rows, :] - row_dot) * (p * scale)).astype(BF16)
            dkv_ref[rows, :head_dim] += dot(ds, q_own)
            dkv_ref[rows, head_dim:] += dot(pb, da_own)
            at_ref[...] += dot(vt_ref[:, rows], pb)
            dqt_ref[...] += dot(kt_ref[:, rows], ds)

        each(0, i + 1, grads)
        a_ref[own, :] = at_ref[...].T.astype(BF16)
        dq_ref[own, :] = rotate(dqt_ref[...].T, cos_ref[own, :], -sin_ref[own, :]).astype(BF16)

    each(0, n_block, one_block)


def attention(q, k, v, da, cos_tab, sin_tab):
    seq, head_dim = q.shape
    block = min(BLOCK, seq)
    whole = pl.BlockSpec(memory_space=pltpu.VMEM)
    return pl.pallas_call(
        functools.partial(attention_kernel, head_dim**-0.5),
        out_shape=[jax.ShapeDtypeStruct((seq, head_dim), BF16), jax.ShapeDtypeStruct((seq, head_dim), BF16), jax.ShapeDtypeStruct((seq, 2 * head_dim), F32)],
        in_specs=[whole] * 6,
        out_specs=[whole] * 3,
        scratch_shapes=[
            pltpu.VMEM((seq, block), F32),
            pltpu.VMEM((seq, block), F32),
            pltpu.VMEM((seq // block, 1, block), F32),
            pltpu.VMEM((head_dim, seq), BF16),
            pltpu.VMEM((head_dim, seq), BF16),
            pltpu.VMEM((head_dim, block), BF16),
            pltpu.VMEM((head_dim, block), BF16),
            pltpu.VMEM((head_dim, block), F32),
            pltpu.VMEM((head_dim, block), F32),
        ],
        compiler_params=pltpu.CompilerParams(vmem_limit_bytes=VMEM_LIMIT),
        cost_estimate=pl.CostEstimate(flops=6 * seq * seq * head_dim * 2, bytes_accessed=16 * seq * head_dim, transcendentals=seq * seq // 2),
        name="attention",
    )(q, k, v, da, cos_tab, sin_tab)


def comm_call(kernel, name, collective_id, operands, outs, scratch):
    anywhere = pl.BlockSpec(memory_space=pl.ANY)
    return pl.pallas_call(
        kernel,
        out_shape=[jax.ShapeDtypeStruct(shape, dtype) for shape, dtype in outs],
        in_specs=[anywhere] * len(operands),
        out_specs=[anywhere] * len(outs),
        scratch_shapes=scratch,
        compiler_params=pltpu.CompilerParams(collective_id=collective_id, has_side_effects=True, vmem_limit_bytes=VMEM_LIMIT),
        name=name,
    )(*operands)


def to_heads_kernel(n_dev, da_ref, pos_ref, out_ref, pos_out_ref, send, recv, pos_send, pos_recv, local):
    me = lax.axis_index(AXIS)
    tokens = da_ref.shape[0]
    head_dim = out_ref.shape[1]
    full_barrier(n_dev)

    def copies(step, peer, origin):
        piece = remote(da_ref.at[:, rows_of(peer, head_dim)], out_ref.at[rows_of(origin, tokens)], send.at[step], recv.at[step], peer)
        where = remote(pos_ref, pos_out_ref.at[origin], pos_send.at[step], pos_recv.at[step], peer)
        return piece, where

    def start(step):
        for copy in copies(step, lax.rem(me + step, n_dev), me):
            copy.start()

    def finish(step):
        for copy in copies(step, lax.rem(me + step, n_dev), lax.rem(me - step + n_dev, n_dev)):
            copy.wait_send()
            copy.wait_recv()

    each(1, n_dev, start)
    own = pltpu.make_async_copy(da_ref.at[:, rows_of(me, head_dim)], out_ref.at[rows_of(me, tokens)], local.at[0])
    own_pos = pltpu.make_async_copy(pos_ref, pos_out_ref.at[me], local.at[1])
    own.start()
    own_pos.start()
    own.wait()
    own_pos.wait()
    each(1, n_dev, finish)


def to_tokens_kernel(n_dev, n_group, q_heads, kv_heads, a_ref, dq_ref, dkv_ref, cos_ref, sin_ref, a_out, grad_out, kv_out, acc, half_in, quarter_in, kv_mine, cos_v, sin_v, a_send, a_recv, q_send, q_recv, kv_send, kv_recv, grp_send, grp_recv, red_send, red_recv, local):
    me = lax.axis_index(AXIS)
    tokens = a_out.shape[0]
    head_dim = a_ref.shape[1]
    half, quarter = half_in.shape[0], quarter_in.shape[0]
    core, side = lax.rem(me, 2), lax.rem(me // 2, 2)
    group = me // n_group
    n_piece = quarter // tokens
    full_barrier(n_dev)

    def sends(step, peer, origin):
        rows, cols = rows_of(peer, tokens), rows_of(origin, head_dim)
        return (
            remote(a_ref.at[rows], a_out.at[:, cols], a_send.at[step], a_recv.at[step], peer),
            remote(dq_ref.at[rows], grad_out.at[:, cols], q_send.at[step], q_recv.at[step], peer),
        )

    def start(step):
        for copy in sends(step, lax.rem(me + step, n_dev), me):
            copy.start()

    def finish(step):
        for copy in sends(step, lax.rem(me + step, n_dev), lax.rem(me - step + n_dev, n_dev)):
            copy.wait_send()
            copy.wait_recv()

    first = remote(dkv_ref.at[rows_of(1 - core, half)], half_in, red_send.at[0], red_recv.at[0], me + 1 - 2 * core)
    first.start()
    mine = pltpu.make_async_copy(dkv_ref.at[rows_of(core, half)], acc, local.at[0])
    mine.start()
    table_row = core * 2 + side
    cos_copy = pltpu.make_async_copy(cos_ref.at[rows_of(table_row, quarter)], cos_v, local.at[1])
    sin_copy = pltpu.make_async_copy(sin_ref.at[rows_of(table_row, quarter)], sin_v, local.at[2])
    cos_copy.start()
    sin_copy.start()
    mine.wait()
    first.wait()

    chunk = quarter // 4

    def add_half(part):
        def body(t):
            rows = pl.ds(pl.multiple_of(part * quarter + t * chunk, chunk), chunk)
            acc[rows, :] += half_in[rows, :]

        each(0, 4, body)

    add_half(1 - side)
    add_half(side)
    second = remote(acc.at[rows_of(1 - side, quarter)], quarter_in, red_send.at[1], red_recv.at[1], me + 2 - 4 * side)
    second.start()
    each(1, n_dev, start)
    own_a = pltpu.make_async_copy(a_ref.at[rows_of(me, tokens)], a_out.at[:, rows_of(me, head_dim)], local.at[3])
    own_q = pltpu.make_async_copy(dq_ref.at[rows_of(me, tokens)], grad_out.at[:, rows_of(me, head_dim)], local.at[4])
    own_a.start()
    own_q.start()
    cos_copy.wait()
    sin_copy.wait()
    second.wait()

    def close(t):
        rows = rows_of(t, chunk)
        full_rows = pl.ds(pl.multiple_of(side * quarter + t * chunk, chunk), chunk)
        total = acc[full_rows, :] + quarter_in[rows, :]
        kv_mine[rows, :head_dim] = rotate(total[:, :head_dim], cos_v[rows, :], -sin_v[rows, :]).astype(BF16)
        kv_mine[rows, head_dim:] = total[:, head_dim:].astype(BF16)

    each(0, 4, close)

    def group_copy(step, place):
        return remote(kv_mine, kv_out.at[rows_of(place, quarter)], grp_send.at[step], grp_recv.at[step], peer_in_group(step))

    def peer_in_group(step):
        return group * n_group + lax.rem(lax.rem(me, n_group) + step, n_group)

    def place_of(member):
        return lax.rem(member, 2) * 2 + lax.rem(member // 2, 2)

    for step in range(1, n_group):
        group_copy(step, table_row).start()
    own_kv = pltpu.make_async_copy(kv_mine, kv_out.at[rows_of(table_row, quarter)], local.at[5])
    own_kv.start()

    def piece_copies(index, kv_head, slot, peer):
        rows = rows_of(index, tokens)
        return (
            remote(kv_mine.at[rows, pl.ds(0, head_dim)], grad_out.at[:, rows_of(q_heads + kv_head, head_dim)], kv_send.at[0, index], kv_recv.at[0, slot], peer),
            remote(kv_mine.at[rows, pl.ds(head_dim, head_dim)], grad_out.at[:, rows_of(q_heads + kv_heads + kv_head, head_dim)], kv_send.at[1, index], kv_recv.at[1, slot], peer),
        )

    def piece_start(index):
        peer = table_row * n_piece + index

        @pl.when(peer != me)
        def _():
            for copy in piece_copies(index, group, group, peer):
                copy.start()

        @pl.when(peer == me)
        def _():
            for which, copy in enumerate(piece_copies(index, group, group, peer)):
                own = pltpu.make_async_copy(copy.src_ref, copy.dst_ref, kv_recv.at[which, group])
                own.start()

    each(0, n_piece, piece_start)

    def piece_sent(index):
        @pl.when(table_row * n_piece + index != me)
        def _():
            for copy in piece_copies(index, group, group, me):
                copy.wait_send()

    def piece_got(kv_head):
        for copy in piece_copies(0, kv_head, kv_head, me):
            copy.wait_recv()

    own_a.wait()
    own_q.wait()
    own_kv.wait()
    each(1, n_dev, finish)
    for step in range(1, n_group):
        sender = lax.rem(lax.rem(me, n_group) - step + n_group, n_group)
        copy = group_copy(step, place_of(sender))
        copy.wait_send()
        copy.wait_recv()
    each(0, n_piece, piece_sent)
    each(0, kv_heads, piece_got)


def to_rows_kernel(n_dev, n_group, wq_ref, wkv_ref, gc_ref, q_out, kv_out, gc_out, q_send, q_recv, gc_send, gc_recv, kv_send, kv_recv, local):
    me = lax.axis_index(AXIS)
    depth = q_out.shape[1]
    n_piece = n_dev // n_group
    member, group = lax.rem(me, n_group), me // n_group
    full_barrier(n_dev)

    def kv_copy(index, slot, peer):
        return remote(wkv_ref.at[rows_of(index, depth)], kv_out.at[slot], kv_send.at[index], kv_recv.at[slot], peer)

    def kv_start(index):
        peer = member * n_piece + index

        @pl.when(peer != me)
        def _():
            kv_copy(index, group, peer).start()

        @pl.when(peer == me)
        def _():
            pltpu.make_async_copy(wkv_ref.at[rows_of(index, depth)], kv_out.at[group], kv_recv.at[group]).start()

    def copies(step, peer, origin):
        return (
            remote(wq_ref.at[rows_of(peer, depth)], q_out.at[origin], q_send.at[step], q_recv.at[step], peer),
            remote(gc_ref, gc_out.at[origin], gc_send.at[step], gc_recv.at[step], peer),
        )

    def start(step):
        for copy in copies(step, lax.rem(me + step, n_dev), me):
            copy.start()

    def finish(step):
        for copy in copies(step, lax.rem(me + step, n_dev), lax.rem(me - step + n_dev, n_dev)):
            copy.wait_send()
            copy.wait_recv()

    each(1, n_dev, start)
    each(0, n_piece, kv_start)
    own_q = pltpu.make_async_copy(wq_ref.at[rows_of(me, depth)], q_out.at[me], local.at[0])
    own_gc = pltpu.make_async_copy(gc_ref, gc_out.at[me], local.at[1])
    own_q.start()
    own_gc.start()
    own_q.wait()
    own_gc.wait()
    each(1, n_dev, finish)

    def kv_sent(index):
        @pl.when(member * n_piece + index != me)
        def _():
            kv_copy(index, group, me).wait_send()

    def kv_got(slot):
        kv_copy(0, slot, me).wait_recv()

    each(0, n_piece, kv_sent)
    each(0, kv_out.shape[0], kv_got)


def solution(mesh):
    n_dev = mesh.shape[AXIS]
    dma = pltpu.SemaphoreType.DMA

    def device_step(x_act, d_out, positions, ln_gain, ln_bias, w_query, w_key, w_value, w_out):
        n_batch, piece, width = x_act.shape
        q_heads, head_dim = w_query.shape[1:]
        kv_heads = w_key.shape[1]
        n_group = q_heads // kv_heads
        tokens = n_batch * piece
        seq = tokens * n_dev
        depth = width // n_dev
        me = lax.axis_index(AXIS)
        kv_head, member = me // n_group, lax.rem(me, n_group)

        normed, x_hat, inv_std = norm_forward(x_act.reshape(tokens, width), ln_gain, ln_bias)
        grad_flat = d_out.reshape(tokens, width)
        h_all = lax.all_gather(normed, AXIS, axis=0, tiled=True)
        dy_all = lax.all_gather(lax.optimization_barrier((grad_flat, normed))[0], AXIS, axis=0, tiled=True)

        grad_attn = lax.dot_general(grad_flat, w_out, (((1,), (1,)), ((), ())), preferred_element_type=F32).astype(BF16)
        pos_tile = jnp.broadcast_to(positions.reshape(1, tokens), (8, tokens))
        da_head, pos_all = comm_call(
            functools.partial(to_heads_kernel, n_dev), "to_heads", 1, (grad_attn, pos_tile),
            [((seq, head_dim), BF16), ((n_dev, 8, tokens), jnp.int32)],
            [dma((n_dev,)), dma((n_dev,)), dma((n_dev,)), dma((n_dev,)), dma((2,))],
        )
        cos_tab, sin_tab = rope_tables(pos_all[:, 0, :].reshape(seq), head_dim)
        w_head = jnp.concatenate([lax.dynamic_index_in_dim(w, i, 1, keepdims=False) for w, i in ((w_query, me), (w_key, kv_head), (w_value, kv_head))], axis=1)
        q, k, v = project(h_all, w_head, cos_tab, sin_tab)
        a_head, dq_head, dkv_part = attention(q, k, v, da_head, cos_tab, sin_tab)

        quarter = seq // n_group
        a_own, grads_own, dkv_head = comm_call(
            functools.partial(to_tokens_kernel, n_dev, n_group, q_heads, kv_heads), "to_tokens", 2, (a_head, dq_head, dkv_part, cos_tab, sin_tab),
            [((tokens, q_heads * head_dim), BF16), ((tokens, (q_heads + 2 * kv_heads) * head_dim), BF16), ((seq, 2 * head_dim), BF16)],
            [
                pltpu.VMEM((2 * quarter, 2 * head_dim), F32), pltpu.VMEM((2 * quarter, 2 * head_dim), F32), pltpu.VMEM((quarter, 2 * head_dim), F32),
                pltpu.VMEM((quarter, 2 * head_dim), BF16), pltpu.VMEM((quarter, head_dim), F32), pltpu.VMEM((quarter, head_dim), F32),
                dma((n_dev,)), dma((n_dev,)), dma((n_dev,)), dma((n_dev,)), dma((2, quarter // tokens)), dma((2, kv_heads)),
                dma((n_group,)), dma((n_group,)), dma((2,)), dma((2,)), dma((6,)),
            ],
        )

        grad_wo = lax.dot_general(a_head, dy_all, (((0,), (0,)), ((), ())), preferred_element_type=F32)
        col_wq = lax.dot_general(h_all, dq_head, (((0,), (0,)), ((), ())), preferred_element_type=F32)
        h_part = lax.dynamic_slice_in_dim(h_all, member * (width // n_group), width // n_group, axis=1)
        col_wkv = lax.dot_general(h_part, dkv_head, (((0,), (0,)), ((), ())), preferred_element_type=F32)

        block_out = (x_act.reshape(tokens, width).astype(F32) + dot(a_own, w_out)).astype(BF16)
        heads = grads_own.reshape(tokens, q_heads + 2 * kv_heads, head_dim)

        def back(first, weight):
            return jnp.einsum("tnh,dnh->td", heads[:, first : first + weight.shape[1]], weight, preferred_element_type=F32)

        grad_h = back(0, w_query) + back(q_heads, w_key) + back(q_heads + kv_heads, w_value)
        grad_x = (grad_flat.astype(F32) + norm_backward(grad_h, x_hat, inv_std, ln_gain)).astype(BF16)
        sums = jnp.concatenate([jnp.sum(grad_h * x_hat, axis=0), jnp.sum(grad_h, axis=0)]).reshape(2 * width // 128, 128)
        rows_wq, rows_wkv, sums_all = comm_call(
            functools.partial(to_rows_kernel, n_dev, n_group), "to_rows", 3, (col_wq, col_wkv, sums),
            [((q_heads, depth, head_dim), F32), ((kv_heads, depth, 2 * head_dim), F32), ((n_dev,) + sums.shape, F32)],
            [dma((n_dev,)), dma((n_dev,)), dma((n_dev,)), dma((n_dev,)), dma((n_dev // n_group,)), dma((kv_heads,)), dma((2,))],
        )
        grad_wq = jnp.swapaxes(rows_wq, 0, 1)
        grad_wk = jnp.swapaxes(rows_wkv[:, :, :head_dim], 0, 1)
        grad_wv = jnp.swapaxes(rows_wkv[:, :, head_dim:], 0, 1)
        grad_gain, grad_bias = jnp.sum(sums_all, axis=0).reshape(2, width)
        return (block_out.reshape(x_act.shape), grad_x.reshape(x_act.shape), grad_wq, grad_wk, grad_wv, grad_wo, grad_gain, grad_bias)

    return jax.shard_map(device_step, mesh=mesh, in_specs=(P("dp", AXIS, None), P("dp", AXIS, None), P("dp", AXIS), P(None), P(None), P(None, None, None), P(None, None, None), P(None, None, None), P(None, None)), out_specs=(P("dp", AXIS, None), P("dp", AXIS, None), P(("dp", AXIS), None, None), P(("dp", AXIS), None, None), P(("dp", AXIS), None, None), P(("dp", AXIS), None), P("dp"), P("dp")), check_vma=False)
```

```python
import functools
import math

import jax
import jax.numpy as jnp
from jax import lax
from jax.experimental import pallas as pl
from jax.experimental.pallas import tpu as pltpu
from jax.sharding import PartitionSpec as P

EPS = 1e-5
ROPE_BASE = 10000.0
BLOCK = 512
AXIS = "cp"
BF16, F32 = jnp.bfloat16, jnp.float32
VMEM_LIMIT = 60 * 1024 * 1024


def norm_forward(x_act, ln_gain, ln_bias):
    x_f32 = x_act.astype(F32)
    centered = x_f32 - jnp.mean(x_f32, axis=-1, keepdims=True)
    inv_std = lax.rsqrt(jnp.mean(centered * centered, axis=-1, keepdims=True) + EPS)
    x_hat = centered * inv_std
    return (x_hat * (1.0 + ln_gain) + ln_bias).astype(BF16), x_hat, inv_std


def rope_tables(positions, head_dim):
    quarter = head_dim // 4
    freq_tab = jnp.exp(jnp.arange(quarter, dtype=F32) * (-2.0 * math.log(ROPE_BASE) / (head_dim // 2)))
    angles = freq_tab[:, None] * positions.astype(F32)[None, :]
    return jnp.cos(angles), jnp.sin(angles)


def rotate(values, cos, sin):
    quarter = cos.shape[0]
    first, second = values[:quarter], values[quarter : 2 * quarter]
    return jnp.concatenate([first * cos - second * sin, second * cos + first * sin, values[2 * quarter :]], axis=0)


def rows_of(index, size):
    return pl.ds(pl.multiple_of(index * size, size), size)


def dot(lhs, rhs):
    return jnp.dot(lhs, rhs, preferred_element_type=F32)


def full_barrier(n_dev):
    me = lax.axis_index(AXIS)
    barrier = pltpu.get_barrier_semaphore()

    def tell(step):
        pl.semaphore_signal(barrier, inc=1, device_id={AXIS: lax.rem(me + step, n_dev)}, device_id_type=pl.DeviceIdType.MESH)

    each(1, n_dev, tell)
    pl.semaphore_wait(barrier, n_dev - 1)


def remote(src, dst, send_sem, recv_sem, peer):
    return pltpu.make_async_remote_copy(src_ref=src, dst_ref=dst, send_sem=send_sem, recv_sem=recv_sem, device_id={AXIS: peer}, device_id_type=pl.DeviceIdType.MESH)


def each(lower, upper, body):
    def step(index, carry):
        body(index)
        return carry

    lax.fori_loop(lower, upper, step, 0)


class Exchange:
    def __init__(self, src, dst, send, recv):
        self.src, self.dst, self.send, self.recv = src, dst, send, recv

    def start(self, index, slot, peer):
        me = lax.axis_index(AXIS)
        src, dst, recv = self.src(index), self.dst(slot), self.recv(slot)

        @pl.when(peer != me)
        def _():
            remote(src, dst, self.send(index), recv, peer).start()

        @pl.when(peer == me)
        def _():
            pltpu.make_async_copy(src, dst, recv).start()

    def sent(self, index, peer):
        me = lax.axis_index(AXIS)

        @pl.when(peer != me)
        def _():
            remote(self.src(index), self.src(index), self.send(index), self.send(index), me).wait_send()

    def got(self, slot):
        dst = self.dst(slot)
        remote(dst, dst, self.recv(slot), self.recv(slot), lax.axis_index(AXIS)).wait_recv()


def project_kernel(h_ref, w_ref, cos_ref, sin_ref, q_ref, k_ref, v_ref, qt_ref, kt_ref, vt_ref):
    head_dim = q_ref.shape[1]
    out = dot(h_ref[...], w_ref[...])
    cos, sin = cos_ref[...], sin_ref[...]
    qt = rotate(out[:, :head_dim].T, cos, sin).astype(BF16)
    kt = rotate(out[:, head_dim : 2 * head_dim].T, cos, sin).astype(BF16)
    v = out[:, 2 * head_dim :].astype(BF16)
    qt_ref[...], kt_ref[...], vt_ref[...] = qt, kt, v.T
    q_ref[...], k_ref[...], v_ref[...] = qt.T, kt.T, v


def project(h_all, w_head, cos_tab, sin_tab, head_dim):
    seq, width = h_all.shape
    block = min(BLOCK, seq)
    by_rows = pl.BlockSpec((block, head_dim), lambda i: (i, 0))
    by_cols = pl.BlockSpec((head_dim, block), lambda i: (0, i))
    table = pl.BlockSpec((head_dim // 4, block), lambda i: (0, i))
    return pl.pallas_call(
        project_kernel,
        grid=(seq // block,),
        out_shape=[jax.ShapeDtypeStruct((seq, head_dim), BF16)] * 3 + [jax.ShapeDtypeStruct((head_dim, seq), BF16)] * 3,
        in_specs=[pl.BlockSpec((block, width), lambda i: (i, 0)), pl.BlockSpec(w_head.shape, lambda i: (0, 0)), table, table],
        out_specs=[by_rows] * 3 + [by_cols] * 3,
        compiler_params=pltpu.CompilerParams(vmem_limit_bytes=VMEM_LIMIT),
        cost_estimate=pl.CostEstimate(flops=2 * seq * width * w_head.shape[1], bytes_accessed=2 * seq * width, transcendentals=0),
        name="project",
    )(h_all, w_head, cos_tab, sin_tab)


def causal(block):
    key = lax.broadcasted_iota(jnp.int32, (block, block), 0)
    query = lax.broadcasted_iota(jnp.int32, (block, block), 1)
    return key <= query


def part_sum(values):
    return jnp.sum(values.reshape(values.shape[0] // 8, 8, values.shape[1]), axis=0)


def forward_kernel(fold, qt_ref, k_ref, vt_ref, a_ref, at_ref, stat_ref, e_ref, m_ref, acc_ref):
    seq = k_ref.shape[0]
    block = e_ref.shape[1]

    def one_block(i):
        own = rows_of(i, block)

        def scores(j, carry, diagonal):
            peak, total = carry
            rows = rows_of(j, block)
            s = dot(k_ref[rows, :], qt_ref[:, own])
            if diagonal:
                s = jnp.where(causal(block), s, -1e30)
            top = jnp.maximum(peak, jnp.max(s, axis=0, keepdims=True))
            e = jnp.exp2((s - top) * fold)
            e_ref[rows, :] = e
            m_ref[j] = top
            return top, total * jnp.exp2((peak - top) * fold) + part_sum(e)

        start = (jnp.full((1, block), -jnp.inf, F32), jnp.zeros((8, block), F32))
        peak, total = scores(i, lax.fori_loop(0, i, functools.partial(scores, diagonal=False), start), True)
        total = jnp.sum(total, axis=0, keepdims=True)
        inv = 1.0 / total
        stat_ref[:, own] = peak * fold + jnp.log2(total)
        acc_ref[...] = jnp.zeros_like(acc_ref)

        def mix(j):
            rows = rows_of(j, block)
            p = e_ref[rows, :] * (jnp.exp2((m_ref[j] - peak) * fold) * inv)
            acc_ref[...] += dot(vt_ref[:, rows], p.astype(BF16))

        each(0, i + 1, mix)
        at = acc_ref[...].astype(BF16)
        at_ref[:, own] = at
        a_ref[own, :] = at.T

    each(0, seq // block, one_block)


def attention_forward(qt, k, vt):
    seq, head_dim = k.shape
    block = min(BLOCK, seq)
    whole = pl.BlockSpec(memory_space=pltpu.VMEM)
    return pl.pallas_call(
        functools.partial(forward_kernel, head_dim**-0.5 * math.log2(math.e)),
        out_shape=[jax.ShapeDtypeStruct((seq, head_dim), BF16), jax.ShapeDtypeStruct((head_dim, seq), BF16), jax.ShapeDtypeStruct((1, seq), F32)],
        in_specs=[whole] * 3,
        out_specs=[whole] * 3,
        scratch_shapes=[pltpu.VMEM((seq, block), F32), pltpu.VMEM((seq // block, 1, block), F32), pltpu.VMEM((head_dim, block), F32)],
        compiler_params=pltpu.CompilerParams(vmem_limit_bytes=VMEM_LIMIT),
        cost_estimate=pl.CostEstimate(flops=2 * seq * seq * head_dim, bytes_accessed=10 * seq * head_dim, transcendentals=seq * seq // 2),
        name="attention_forward",
    )(qt, k, vt)


def backward_kernel(
    n_dev, n_group, q_heads, kv_heads, scale,
    dy_ref, a_ref, wo_ref, q_ref, k_ref, v_ref, qt_ref, kt_ref, stat_ref, cos_ref, sin_ref,
    dqt_ref, dkvt_ref, a_out, grad_out,
    dy_buf, da_ref, dq_ref, dkv_ref, p_ref, dp_ref, dat_ref, acc_ref, land_one, land_two, kv_ref, kvt_ref,
    dy_sem, a_send, a_recv, q_send, q_recv, one_send, one_recv, two_send, two_recv, kv_send, kv_recv, near_send, near_recv, far_send, far_recv, fwd_send, fwd_recv, local,
):
    me = lax.axis_index(AXIS)
    seq, head_dim = q_ref.shape
    block = p_ref.shape[1]
    n_block = seq // block
    tokens = seq // n_dev
    half = block // 2
    fold = scale * math.log2(math.e)
    core, side = lax.rem(me, 2), lax.rem(me // 2, 2)
    group = me // n_group
    partner, across = me + 1 - 2 * core, me + 2 - 4 * side
    place, place_across = core * 2 + side, core * 2 + 1 - side
    place_partner, place_last = (1 - core) * 2 + side, (1 - core) * 2 + 1 - side

    def piece(index):
        return rows_of(index, tokens)

    def column(head):
        return rows_of(head, head_dim)

    a_copy = Exchange(lambda peer: a_ref.at[piece(peer)], lambda head: a_out.at[:, column(head)], lambda peer: a_send.at[peer], lambda head: a_recv.at[head])
    q_copy = Exchange(lambda peer: dq_ref.at[piece(peer)], lambda head: grad_out.at[:, column(head)], lambda peer: q_send.at[peer], lambda head: q_recv.at[head])
    kv_copy = [
        Exchange(
            lambda i, w=w: kv_ref.at[i, w],
            lambda head, w=w: grad_out.at[:, column(q_heads + w * kv_heads + head)],
            lambda i, w=w: kv_send.at[w, i],
            lambda head, w=w: kv_recv.at[w, head],
        )
        for w in range(2)
    ]

    def one_copy(i):
        return remote(dkv_ref.at[rows_of(i * 2 + 1 - core, half)], land_one.at[i], one_send.at[i], one_recv.at[i], partner)

    def two_copy(i):
        return remote(dkv_ref.at[piece(i * n_group + core * 2 + 1 - side)], land_two.at[i], two_send.at[i], two_recv.at[i], across)

    def near_copy(i, where):
        return remote(kvt_ref.at[i], dkvt_ref.at[:, piece(i * n_group + where)], near_send.at[i], near_recv.at[i], partner)

    def far_copy(i, where):
        return remote(kvt_ref.at[i], dkvt_ref.at[:, piece(i * n_group + where)], far_send.at[i], far_recv.at[i], across)

    def fwd_copy(i, where):
        view = dkvt_ref.at[:, piece(i * n_group + where)]
        return remote(view, view, fwd_send.at[i], fwd_recv.at[i], partner)

    def own_copy(i):
        return pltpu.make_async_copy(kvt_ref.at[i], dkvt_ref.at[:, piece(i * n_group + place)], local.at[i])

    def first(i):
        def send(u):
            q_copy.start(i * n_group + u, me, i * n_group + u)

        one_copy(i).start()
        each(0, n_group, send)

    def second(i):
        one_copy(i).wait_recv()
        for part in (1 - side, side):
            rows = piece(i * n_group + core * 2 + part)
            dkv_ref[rows, :] += land_one[i, pl.ds(pl.multiple_of(part * tokens, tokens), tokens), :]
        two_copy(i).start()

    def close(i):
        two_copy(i).wait_recv()
        rows = piece(i * n_group + place)
        total = dkv_ref[rows, :] + land_two[i]
        dkt = rotate(total[:, :head_dim].T, cos_ref[:, rows], -sin_ref[:, rows]).astype(BF16)
        dv = total[:, head_dim:].astype(BF16)
        kvt_ref[i, :head_dim, :], kvt_ref[i, head_dim:, :] = dkt, dv.T
        kv_ref[i, 0], kv_ref[i, 1] = dkt.T, dv

    def spread(i):
        near_copy(i, place).start()
        far_copy(i, place).start()
        own_copy(i).start()
        for copy in kv_copy:
            copy.start(i, group, i * n_group + place)

    def forward(i):
        far_copy(i, place_across).wait_recv()
        fwd_copy(i, place_across).start()

    def stages(t):
        for late, stage in ((5, forward), (4, spread), (3, close), (2, second), (1, first)):
            @pl.when((t >= late) & (t < n_block + late))
            def _():
                stage(n_block - 1 - (t - late))

    def dy_copy(t):
        slot = lax.rem(t, 2)
        return pltpu.make_async_copy(dy_ref.at[rows_of(t, block)], dy_buf.at[slot], dy_sem.at[slot])

    full_barrier(n_dev)
    dy_copy(0).start()

    def send_a(step):
        peer = lax.rem(me + step, n_dev)
        a_copy.start(peer, me, peer)

    each(0, n_dev, send_a)

    def make_da(t):
        @pl.when(t + 1 < n_block)
        def _():
            dy_copy(t + 1).start()

        dy_copy(t).wait()
        da = dot(dy_buf[lax.rem(t, 2)], wo_ref[...])
        da_ref[rows_of(t, block), :] = da.astype(BF16)
        dkv_ref[rows_of(t, block), :] = jnp.zeros((block, 2 * head_dim), F32)

    each(0, n_block, make_da)

    def compute(i):
        own = rows_of(i, block)
        dat_ref[...] = da_ref[own, :].T
        acc_ref[...] = jnp.zeros_like(acc_ref)
        stat = stat_ref[:, own]
        q_own, da_own = q_ref[own, :], da_ref[own, :]

        def probs(j, mixed, diagonal):
            rows = rows_of(j, block)
            s = dot(k_ref[rows, :], qt_ref[:, own])
            if diagonal:
                s = jnp.where(causal(block), s, -1e30)
            p = jnp.exp2(s * fold - stat)
            dp = dot(v_ref[rows, :], dat_ref[...])
            dkv_ref[rows, head_dim:] += dot(p.astype(BF16), da_own)
            p_ref[rows, :] = p * scale
            dp_ref[rows, :] = dp
            return mixed + part_sum(p * dp)

        mixed = lax.fori_loop(0, i, functools.partial(probs, diagonal=False), jnp.zeros((8, block), F32))
        row_dot = jnp.sum(probs(i, mixed, True), axis=0, keepdims=True)

        def grads(j):
            rows = rows_of(j, block)
            ds = ((dp_ref[rows, :] - row_dot) * p_ref[rows, :]).astype(BF16)
            dkv_ref[rows, :head_dim] += dot(ds, q_own)
            acc_ref[...] += dot(kt_ref[:, rows], ds)

        each(0, i + 1, grads)
        dqt = rotate(acc_ref[...], cos_ref[:, own], -sin_ref[:, own]).astype(BF16)
        dqt_ref[:, own] = dqt
        dq_ref[own, :] = dqt.T

    def iteration(t):
        stages(t)

        @pl.when(t < n_block)
        def _():
            compute(n_block - 1 - t)

    each(0, n_block + 5, iteration)

    def drain(i):
        one_copy(i).wait_send()
        two_copy(i).wait_send()
        near_copy(i, place).wait_send()
        near_copy(i, place_partner).wait_recv()
        far_copy(i, place).wait_send()
        fwd_copy(i, place_across).wait_send()
        fwd_copy(i, place_last).wait_recv()
        own_copy(i).wait()
        for copy in kv_copy:
            copy.sent(i, i * n_group + place)

    each(0, n_block, drain)

    def drain_heads(index):
        for copy in (a_copy, q_copy):
            copy.sent(index, index)
            copy.got(index)

    each(0, n_dev, drain_heads)

    def drain_kv(head):
        for copy in kv_copy:
            copy.got(head)

    each(0, kv_heads, drain_kv)


def attention_backward(n_dev, kv_heads, dy_all, a, wo_head, q, k, v, qt, kt, stat, cos_tab, sin_tab):
    seq, head_dim = q.shape
    width = dy_all.shape[1]
    q_heads = n_dev
    n_group = q_heads // kv_heads
    tokens = seq // n_dev
    block = tokens * n_group
    n_block = seq // block
    whole, anywhere = pl.BlockSpec(memory_space=pltpu.VMEM), pl.BlockSpec(memory_space=pl.ANY)
    dma = pltpu.SemaphoreType.DMA
    return pl.pallas_call(
        functools.partial(backward_kernel, n_dev, n_group, q_heads, kv_heads, head_dim**-0.5),
        out_shape=[
            jax.ShapeDtypeStruct((head_dim, seq), BF16),
            jax.ShapeDtypeStruct((2 * head_dim, seq), BF16),
            jax.ShapeDtypeStruct((tokens, q_heads * head_dim), BF16),
            jax.ShapeDtypeStruct((tokens, (q_heads + 2 * kv_heads) * head_dim), BF16),
        ],
        in_specs=[anywhere] * 2 + [whole] * 9,
        out_specs=[whole] + [anywhere] * 3,
        scratch_shapes=[
            pltpu.VMEM((2, block, width), BF16),
            pltpu.VMEM((seq, head_dim), BF16),
            pltpu.VMEM((seq, head_dim), BF16),
            pltpu.VMEM((seq, 2 * head_dim), F32),
            pltpu.VMEM((seq, block), F32),
            pltpu.VMEM((seq, block), F32),
            pltpu.VMEM((head_dim, block), BF16),
            pltpu.VMEM((head_dim, block), F32),
            pltpu.VMEM((n_block, block // 2, 2 * head_dim), F32),
            pltpu.VMEM((n_block, tokens, 2 * head_dim), F32),
            pltpu.VMEM((n_block, 2, tokens, head_dim), BF16),
            pltpu.VMEM((n_block, 2 * head_dim, tokens), BF16),
            dma((2,)), dma((n_dev,)), dma((n_dev,)), dma((n_dev,)), dma((n_dev,)),
            dma((n_block,)), dma((n_block,)), dma((n_block,)), dma((n_block,)), dma((2, n_block)), dma((2, kv_heads)),
            dma((n_block,)), dma((n_block,)), dma((n_block,)), dma((n_block,)), dma((n_block,)), dma((n_block,)), dma((n_block,)),
        ],
        compiler_params=pltpu.CompilerParams(collective_id=1, has_side_effects=True, vmem_limit_bytes=VMEM_LIMIT),
        cost_estimate=pl.CostEstimate(flops=6 * seq * seq * head_dim, bytes_accessed=2 * seq * width, transcendentals=seq * seq // 2),
        name="attention_backward",
    )(dy_all, a, wo_head, q, k, v, qt, kt, stat, cos_tab, sin_tab)


def finish_kernel(
    n_dev, n_group, n_buf,
    h_ref, dy_ref, wq_ref, wk_ref, wv_ref, wo_ref, dqt_ref, dkvt_ref, at_ref, a_ref, g_ref, x_ref, dy_own_ref, x_hat_ref, inv_ref, gain_ref,
    out_ref, gx_ref, gwo_ref, q_rows, kv_rows, sum_ref,
    buf, wq_out, wkv_out, dh_ref, part_ref, own_sum, all_sum,
    load_sem, q_send, q_recv, kv_send, kv_recv, s_send, s_recv,
):
    me = lax.axis_index(AXIS)
    seq, width = h_ref.shape
    span = buf.shape[2]
    head_dim = dqt_ref.shape[0]
    depth = width // n_dev
    n_col = width // span
    per_col = span // depth
    member, group = lax.rem(me, n_group), me // n_group
    col_member = n_col // n_group
    per_member = n_dev // n_group
    kv_rows_n = wk_ref.shape[0]
    q_rows_n = wq_ref.shape[0]

    def cols(j):
        return rows_of(j, span)

    def loads(phase, j, slot):
        def whole(ref):
            return pltpu.make_async_copy(ref.at[:, cols(j)], buf.at[slot, pl.ds(0, ref.shape[0])], load_sem.at[slot, 0])

        if phase == 2:
            second = pltpu.make_async_copy(wv_ref.at[:, cols(j)], buf.at[slot, pl.ds(kv_rows_n, kv_rows_n)], load_sem.at[slot, 1])
            return (whole(wk_ref), second)
        return (whole((h_ref, wq_ref, None, wo_ref, dy_ref)[phase]),)

    def load(step):
        slot = lax.rem(step, n_buf)
        for phase in range(5):
            @pl.when((step >= phase * n_col) & (step < (phase + 1) * n_col))
            def _():
                for copy in loads(phase, step - phase * n_col, slot):
                    copy.start()

    q_copy = Exchange(lambda peer: wq_out.at[rows_of(peer, depth)], lambda head: q_rows.at[head], lambda peer: q_send.at[peer], lambda head: q_recv.at[head])
    kv_copy = Exchange(lambda i: wkv_out.at[rows_of(i, depth)], lambda head: kv_rows.at[head], lambda i: kv_send.at[i], lambda head: kv_recv.at[head])
    s_copy = Exchange(lambda peer: own_sum, lambda origin: all_sum.at[origin], lambda peer: s_send.at[peer], lambda origin: s_recv.at[origin])

    def send_q(j):
        def send(u):
            peer = j * per_col + u
            q_copy.start(peer, me, peer)

        each(0, per_col, send)

    def run(phase, body):
        def step(j):
            number = phase * n_col + j
            slot = lax.rem(number, n_buf)
            for copy in loads(phase, j, slot):
                copy.wait()
            body(j, slot)
            load(number + n_buf)

        each(0, n_col, step)

    full_barrier(n_dev)
    each(0, n_buf, load)

    def weight_columns(j, slot):
        @pl.when(j > 0)
        def _():
            send_q(j - 1)

        block = buf[slot]
        wq_out[cols(j), :] = dot(dqt_ref[...], block).T

        @pl.when(j // col_member == member)
        def _():
            wkv_out[cols(j - member * col_member), :] = dot(dkvt_ref[...], buf[slot]).T

    run(0, weight_columns)

    def send_kv(index):
        kv_copy.start(index, group, member * per_member + index)

    def back_query(j, slot):
        dh_ref[:, cols(j)] = dot(g_ref[:, :q_rows_n], buf[slot])

        @pl.when(j == 0)
        def _():
            send_q(n_col - 1)
            each(0, per_member, send_kv)

    run(1, back_query)

    def back_key(j, slot):
        dh_ref[:, cols(j)] += dot(g_ref[:, q_rows_n:], buf[slot, : 2 * kv_rows_n])

    run(2, back_key)

    part_ref[...] = jnp.zeros_like(part_ref)
    gain = 1.0 + gain_ref[...]

    def norm(t):
        rows = rows_of(t, 16)
        grad_h, x_hat = dh_ref[rows, :], x_hat_ref[rows, :]
        grad_hat = grad_h * gain
        one = jnp.sum(grad_hat, axis=1, keepdims=True) * (1.0 / width)
        two = jnp.sum(grad_hat * x_hat, axis=1, keepdims=True) * (1.0 / width)
        back = inv_ref[rows, :] * (grad_hat - one - x_hat * two)
        gx_ref[rows, :] = (dy_own_ref[rows, :].astype(F32) + back).astype(BF16)
        part_ref[0] += part_sum(grad_h * x_hat)
        part_ref[1] += part_sum(grad_h)

    each(0, dh_ref.shape[0] // 16, norm)
    n_lane = width // 128
    for which in range(2):
        total = jnp.sum(part_ref[which], axis=0, keepdims=True)
        for c in range(n_lane):
            own_sum[pl.ds(which * n_lane + c, 1), :] = total[:, c * 128 : (c + 1) * 128]

    def send_sum(step):
        peer = lax.rem(me + step, n_dev)
        s_copy.start(peer, me, peer)

    def output(j, slot):
        @pl.when(j == 0)
        def _():
            each(0, n_dev, send_sum)

        out_ref[:, cols(j)] = (x_ref[:, cols(j)].astype(F32) + dot(a_ref[...], buf[slot])).astype(BF16)

    run(3, output)

    def weight_out(j, slot):
        gwo_ref[:, cols(j)] = dot(at_ref[...], buf[slot])

    run(4, weight_out)

    def drain(index):
        s_copy.sent(index, index)
        s_copy.got(index)
        q_copy.sent(index, index)
        q_copy.got(index)

    def drain_kv(index):
        kv_copy.sent(index, member * per_member + index)

    each(0, n_dev, drain)
    each(0, per_member, drain_kv)
    each(0, kv_rows.shape[0], kv_copy.got)
    sum_ref[...] = jnp.zeros_like(sum_ref)

    def add(origin):
        sum_ref[...] += all_sum[origin]

    each(0, n_dev, add)


def finish(n_dev, kv_heads, h_all, dy_all, wq, wk, wv, wo, dqt, dkvt, at, a_own, g_own, x_own, dy_own, x_hat, inv_std, gain):
    seq, width = h_all.shape
    tokens = seq // n_dev
    head_dim = dqt.shape[0]
    q_heads = n_dev
    n_group = q_heads // kv_heads
    depth = width // n_dev
    span = math.lcm(depth, 128)
    n_buf = 4
    sums = (2 * width // 128, 128)
    whole, anywhere = pl.BlockSpec(memory_space=pltpu.VMEM), pl.BlockSpec(memory_space=pl.ANY)
    dma = pltpu.SemaphoreType.DMA
    return pl.pallas_call(
        functools.partial(finish_kernel, n_dev, n_group, n_buf),
        out_shape=[
            jax.ShapeDtypeStruct((tokens, width), BF16),
            jax.ShapeDtypeStruct((tokens, width), BF16),
            jax.ShapeDtypeStruct((head_dim, width), F32),
            jax.ShapeDtypeStruct((q_heads, depth, head_dim), F32),
            jax.ShapeDtypeStruct((kv_heads, depth, 2 * head_dim), F32),
            jax.ShapeDtypeStruct(sums, F32),
        ],
        in_specs=[anywhere] * 6 + [whole] * 10,
        out_specs=[whole] * 3 + [anywhere] * 2 + [whole],
        scratch_shapes=[
            pltpu.VMEM((n_buf, seq, span), BF16),
            pltpu.VMEM((width, head_dim), F32),
            pltpu.VMEM((width // n_group, 2 * head_dim), F32),
            pltpu.VMEM((tokens, width), F32),
            pltpu.VMEM((2, 8, width), F32),
            pltpu.VMEM(sums, F32),
            pltpu.VMEM((n_dev,) + sums, F32),
            dma((n_buf, 2)), dma((n_dev,)), dma((n_dev,)), dma((n_dev // n_group,)), dma((kv_heads,)), dma((n_dev,)), dma((n_dev,)),
        ],
        compiler_params=pltpu.CompilerParams(collective_id=2, has_side_effects=True, vmem_limit_bytes=VMEM_LIMIT),
        cost_estimate=pl.CostEstimate(flops=10 * seq * width * head_dim, bytes_accessed=10 * seq * width, transcendentals=0),
        name="finish",
    )(h_all, dy_all, wq, wk, wv, wo, dqt, dkvt, at, a_own, g_own, x_own, dy_own, x_hat, inv_std, gain)


def solution(mesh):
    n_dev = mesh.shape[AXIS]

    def device_step(x_act, d_out, positions, ln_gain, ln_bias, w_query, w_key, w_value, w_out):
        n_batch, piece, width = x_act.shape
        q_heads, head_dim = w_query.shape[1:]
        kv_heads = w_key.shape[1]
        n_group = q_heads // kv_heads
        tokens = n_batch * piece
        me = lax.axis_index(AXIS)
        kv_head = me // n_group

        x_own, dy_own = x_act.reshape(tokens, width), d_out.reshape(tokens, width)
        normed, x_hat, inv_std = norm_forward(x_own, ln_gain, ln_bias)
        h_all = lax.all_gather(normed, AXIS, axis=0, tiled=True)
        dy_all = lax.all_gather(lax.optimization_barrier((dy_own, normed))[0], AXIS, axis=0, tiled=True)
        pos_all = lax.all_gather(positions.reshape(tokens), AXIS, axis=0, tiled=True)
        cos_tab, sin_tab = rope_tables(pos_all, head_dim)

        w_head = jnp.concatenate([lax.dynamic_index_in_dim(w, i, 1, keepdims=False) for w, i in ((w_query, me), (w_key, kv_head), (w_value, kv_head))], axis=1)
        wo_head = lax.dynamic_slice_in_dim(w_out, me * head_dim, head_dim, axis=0).T
        wq_rows, wk_rows, wv_rows = (jnp.transpose(w, (1, 2, 0)).reshape(-1, width) for w in (w_query, w_key, w_value))

        q, k, v, qt, kt, vt = project(h_all, w_head, cos_tab, sin_tab, head_dim)
        a, at, stat = attention_forward(qt, k, vt)
        dqt, dkvt, a_own, g_own = attention_backward(n_dev, kv_heads, dy_all, a, wo_head, q, k, v, qt, kt, stat, cos_tab, sin_tab)
        block_out, grad_x, grad_wo, rows_wq, rows_wkv, sums = finish(
            n_dev, kv_heads, h_all, dy_all, wq_rows, wk_rows, wv_rows, w_out, dqt, dkvt, at, a_own, g_own, x_own, dy_own, x_hat, inv_std, ln_gain.reshape(1, width)
        )
        grad_wq = jnp.swapaxes(rows_wq, 0, 1)
        grad_wk = jnp.swapaxes(rows_wkv[:, :, :head_dim], 0, 1)
        grad_wv = jnp.swapaxes(rows_wkv[:, :, head_dim:], 0, 1)
        grad_gain, grad_bias = sums.reshape(2, width)
        return (block_out.reshape(x_act.shape), grad_x.reshape(x_act.shape), grad_wq, grad_wk, grad_wv, grad_wo, grad_gain, grad_bias)

    return jax.shard_map(device_step, mesh=mesh, in_specs=(P("dp", AXIS, None), P("dp", AXIS, None), P("dp", AXIS), P(None), P(None), P(None, None, None), P(None, None, None), P(None, None, None), P(None, None)), out_specs=(P("dp", AXIS, None), P("dp", AXIS, None), P(("dp", AXIS), None, None), P(("dp", AXIS), None, None), P(("dp", AXIS), None, None), P(("dp", AXIS), None), P("dp"), P("dp")), check_vma=False)
```

```python
import functools
import math

import jax
import jax.numpy as jnp
from jax import lax
from jax.experimental import pallas as pl
from jax.experimental.pallas import tpu as pltpu
from jax.sharding import PartitionSpec as P

EPS = 1e-5
ROPE_BASE = 10000.0
BLOCK = 512
AXIS = "cp"
BF16, F32 = jnp.bfloat16, jnp.float32
VMEM_LIMIT = 60 * 1024 * 1024


def norm_forward(x_act, ln_gain, ln_bias):
    x_f32 = x_act.astype(F32)
    centered = x_f32 - jnp.mean(x_f32, axis=-1, keepdims=True)
    inv_std = lax.rsqrt(jnp.mean(centered * centered, axis=-1, keepdims=True) + EPS)
    x_hat = centered * inv_std
    return (x_hat * (1.0 + ln_gain) + ln_bias).astype(BF16), x_hat, inv_std


def rope_tables(positions, head_dim):
    quarter = head_dim // 4
    freq_tab = jnp.exp(jnp.arange(quarter, dtype=F32) * (-2.0 * math.log(ROPE_BASE) / (head_dim // 2)))
    angles = freq_tab[:, None] * positions.astype(F32)[None, :]
    return jnp.cos(angles), jnp.sin(angles)


def rotate(values, cos, sin):
    quarter = cos.shape[0]
    first, second = values[:quarter], values[quarter : 2 * quarter]
    return jnp.concatenate([first * cos - second * sin, second * cos + first * sin, values[2 * quarter :]], axis=0)


def rows_of(index, size):
    return pl.ds(pl.multiple_of(index * size, size), size)


def dot(lhs, rhs):
    return jnp.dot(lhs, rhs, preferred_element_type=F32)


def dot_t(lhs, rhs):
    return lax.dot_general(lhs, rhs, (((1,), (1,)), ((), ())), preferred_element_type=F32)


def full_barrier(n_dev):
    me = lax.axis_index(AXIS)
    barrier = pltpu.get_barrier_semaphore()

    def tell(step):
        pl.semaphore_signal(barrier, inc=1, device_id={AXIS: lax.rem(me + step, n_dev)}, device_id_type=pl.DeviceIdType.MESH)

    each(1, n_dev, tell)
    pl.semaphore_wait(barrier, n_dev - 1)


def remote(src, dst, send_sem, recv_sem, peer):
    return pltpu.make_async_remote_copy(src_ref=src, dst_ref=dst, send_sem=send_sem, recv_sem=recv_sem, device_id={AXIS: peer}, device_id_type=pl.DeviceIdType.MESH)


def each(lower, upper, body):
    def step(index, carry):
        body(index)
        return carry

    lax.fori_loop(lower, upper, step, 0)


class Exchange:
    def __init__(self, src, dst, send, recv):
        self.src, self.dst, self.send, self.recv = src, dst, send, recv

    def start(self, index, slot, peer):
        me = lax.axis_index(AXIS)
        src, dst, recv = self.src(index), self.dst(slot), self.recv(slot)

        @pl.when(peer != me)
        def _():
            remote(src, dst, self.send(index), recv, peer).start()

        @pl.when(peer == me)
        def _():
            pltpu.make_async_copy(src, dst, recv).start()

    def sent(self, index, peer):
        me = lax.axis_index(AXIS)

        @pl.when(peer != me)
        def _():
            remote(self.src(index), self.src(index), self.send(index), self.send(index), me).wait_send()

    def got(self, slot):
        dst = self.dst(slot)
        remote(dst, dst, self.recv(slot), self.recv(slot), lax.axis_index(AXIS)).wait_recv()


def heads_in_kernel(n_dev, n_buf, dy_ref, pos_ref, wo_ref, da_ref, pos_out, buf, da_buf, load_sem, send, recv, pos_send, pos_recv):
    me = lax.axis_index(AXIS)
    tokens = dy_ref.shape[0]
    head_dim = da_ref.shape[1]
    span = buf.shape[1]
    n_step = wo_ref.shape[0] // span
    per_step = span // head_dim
    piece = Exchange(lambda peer: da_buf.at[peer], lambda origin: da_ref.at[rows_of(origin, tokens)], lambda peer: send.at[peer], lambda origin: recv.at[origin])
    where = Exchange(lambda peer: pos_ref, lambda origin: pos_out.at[origin], lambda peer: pos_send.at[peer], lambda origin: pos_recv.at[origin])

    def load(step):
        slot = lax.rem(step, n_buf)
        return pltpu.make_async_copy(wo_ref.at[rows_of(step, span)], buf.at[slot], load_sem.at[slot])

    for step in range(n_buf):
        load(step).start()
    full_barrier(n_dev)

    def send_pos(step):
        peer = lax.rem(me + step, n_dev)
        where.start(peer, me, peer)

    each(0, n_dev, send_pos)

    def send_heads(step):
        def one(u):
            peer = step * per_step + u
            piece.start(peer, me, peer)

        each(0, per_step, one)

    def product(step):
        @pl.when(step > 0)
        def _():
            send_heads(step - 1)

        load(step).wait()
        da = dot_t(dy_ref[...], buf[lax.rem(step, n_buf)]).astype(BF16)
        for u in range(per_step):
            da_buf[step * per_step + u] = da[:, u * head_dim : (u + 1) * head_dim]

        @pl.when(step + n_buf < n_step)
        def _():
            load(step + n_buf).start()

    each(0, n_step, product)
    send_heads(n_step - 1)

    def drain(index):
        for copy in (piece, where):
            copy.sent(index, index)
            copy.got(index)

    each(0, n_dev, drain)


def heads_in(n_dev, dy_own, positions, w_out, head_dim):
    tokens, width = dy_own.shape
    span = min(BLOCK, w_out.shape[0])
    n_buf = min(3, w_out.shape[0] // span)
    whole, anywhere = pl.BlockSpec(memory_space=pltpu.VMEM), pl.BlockSpec(memory_space=pl.ANY)
    dma = pltpu.SemaphoreType.DMA
    return pl.pallas_call(
        functools.partial(heads_in_kernel, n_dev, n_buf),
        out_shape=[jax.ShapeDtypeStruct((tokens * n_dev, head_dim), BF16), jax.ShapeDtypeStruct((n_dev,) + positions.shape, jnp.int32)],
        in_specs=[whole, whole, anywhere],
        out_specs=[anywhere] * 2,
        scratch_shapes=[
            pltpu.VMEM((n_buf, span, width), BF16),
            pltpu.VMEM((n_dev, tokens, head_dim), BF16),
            dma((n_buf,)), dma((n_dev,)), dma((n_dev,)), dma((n_dev,)), dma((n_dev,)),
        ],
        compiler_params=pltpu.CompilerParams(collective_id=3, has_side_effects=True, vmem_limit_bytes=VMEM_LIMIT),
        cost_estimate=pl.CostEstimate(flops=2 * tokens * width * w_out.shape[0], bytes_accessed=2 * width * w_out.shape[0], transcendentals=0),
        name="heads_in",
    )(dy_own, positions, w_out)


def project_kernel(h_ref, w_ref, cos_ref, sin_ref, q_ref, k_ref, v_ref, qt_ref, kt_ref, vt_ref):
    head_dim = q_ref.shape[1]
    out = dot_t(h_ref[...], w_ref[...])
    cos, sin = cos_ref[...], sin_ref[...]
    qt = rotate(out[:, :head_dim].T, cos, sin).astype(BF16)
    kt = rotate(out[:, head_dim : 2 * head_dim].T, cos, sin).astype(BF16)
    v = out[:, 2 * head_dim :].astype(BF16)
    qt_ref[...], kt_ref[...], vt_ref[...] = qt, kt, v.T
    q_ref[...], k_ref[...], v_ref[...] = qt.T, kt.T, v


def project(h_all, w_head, cos_tab, sin_tab, head_dim):
    seq, width = h_all.shape
    block = min(BLOCK, seq)
    by_rows = pl.BlockSpec((block, head_dim), lambda i: (i, 0))
    by_cols = pl.BlockSpec((head_dim, block), lambda i: (0, i))
    table = pl.BlockSpec((head_dim // 4, block), lambda i: (0, i))
    return pl.pallas_call(
        project_kernel,
        grid=(seq // block,),
        out_shape=[jax.ShapeDtypeStruct((seq, head_dim), BF16)] * 3 + [jax.ShapeDtypeStruct((head_dim, seq), BF16)] * 3,
        in_specs=[pl.BlockSpec((block, width), lambda i: (i, 0)), pl.BlockSpec(w_head.shape, lambda i: (0, 0)), table, table],
        out_specs=[by_rows] * 3 + [by_cols] * 3,
        compiler_params=pltpu.CompilerParams(vmem_limit_bytes=VMEM_LIMIT),
        cost_estimate=pl.CostEstimate(flops=2 * seq * width * w_head.shape[0], bytes_accessed=2 * seq * width, transcendentals=0),
        name="project",
    )(h_all, w_head, cos_tab, sin_tab)


def causal(block):
    key = lax.broadcasted_iota(jnp.int32, (block, block), 0)
    query = lax.broadcasted_iota(jnp.int32, (block, block), 1)
    return key <= query


def part_sum(values):
    return jnp.sum(values.reshape(values.shape[0] // 8, 8, values.shape[1]), axis=0)


def attention_kernel(
    n_dev, n_group, q_heads, kv_heads, scale,
    q_ref, k_ref, v_ref, da_ref, qt_ref, kt_ref, vt_ref, cos_ref, sin_ref,
    at_ref, dqt_ref, dkvt_ref, a_out, grad_out,
    a_ref, dq_ref, dkv_ref, e_ref, dp_ref, peak_ref, dat_ref, mix_ref, acc_ref, land_one, land_two, kv_ref, kvt_ref,
    a_send, a_recv, q_send, q_recv, one_send, one_recv, two_send, two_recv, kv_send, kv_recv, near_send, near_recv, far_send, far_recv, fwd_send, fwd_recv, local,
):
    me = lax.axis_index(AXIS)
    seq, head_dim = q_ref.shape
    block = e_ref.shape[1]
    n_block = seq // block
    tokens = seq // n_dev
    half = block // 2
    fold = scale * math.log2(math.e)
    core, side = lax.rem(me, 2), lax.rem(me // 2, 2)
    group = me // n_group
    partner, across = me + 1 - 2 * core, me + 2 - 4 * side
    place, place_across = core * 2 + side, core * 2 + 1 - side
    place_partner, place_last = (1 - core) * 2 + side, (1 - core) * 2 + 1 - side

    def piece(index):
        return rows_of(index, tokens)

    def column(head):
        return rows_of(head, head_dim)

    a_copy = Exchange(lambda peer: a_ref.at[piece(peer)], lambda head: a_out.at[:, column(head)], lambda peer: a_send.at[peer], lambda head: a_recv.at[head])
    q_copy = Exchange(lambda peer: dq_ref.at[piece(peer)], lambda head: grad_out.at[:, column(head)], lambda peer: q_send.at[peer], lambda head: q_recv.at[head])
    kv_copy = [
        Exchange(
            lambda i, w=w: kv_ref.at[i, w],
            lambda head, w=w: grad_out.at[:, column(q_heads + w * kv_heads + head)],
            lambda i, w=w: kv_send.at[w, i],
            lambda head, w=w: kv_recv.at[w, head],
        )
        for w in range(2)
    ]

    def one_copy(i):
        return remote(dkv_ref.at[rows_of(i * 2 + 1 - core, half)], land_one.at[i], one_send.at[i], one_recv.at[i], partner)

    def two_copy(i):
        return remote(dkv_ref.at[piece(i * n_group + core * 2 + 1 - side)], land_two.at[i], two_send.at[i], two_recv.at[i], across)

    def near_copy(i, where):
        return remote(kvt_ref.at[i], dkvt_ref.at[:, piece(i * n_group + where)], near_send.at[i], near_recv.at[i], partner)

    def far_copy(i, where):
        return remote(kvt_ref.at[i], dkvt_ref.at[:, piece(i * n_group + where)], far_send.at[i], far_recv.at[i], across)

    def fwd_copy(i, where):
        view = dkvt_ref.at[:, piece(i * n_group + where)]
        return remote(view, view, fwd_send.at[i], fwd_recv.at[i], partner)

    def own_copy(i):
        return pltpu.make_async_copy(kvt_ref.at[i], dkvt_ref.at[:, piece(i * n_group + place)], local.at[i])

    def first(i):
        def send(u):
            peer = i * n_group + u
            a_copy.start(peer, me, peer)
            q_copy.start(peer, me, peer)

        one_copy(i).start()
        each(0, n_group, send)

    def second(i):
        one_copy(i).wait_recv()
        for part in (1 - side, side):
            rows = piece(i * n_group + core * 2 + part)
            dkv_ref[rows, :] += land_one[i, pl.ds(pl.multiple_of(part * tokens, tokens), tokens), :]
        two_copy(i).start()

    def close(i):
        two_copy(i).wait_recv()
        rows = piece(i * n_group + place)
        total = dkv_ref[rows, :] + land_two[i]
        dkt = rotate(total[:, :head_dim].T, cos_ref[:, rows], -sin_ref[:, rows]).astype(BF16)
        dv = total[:, head_dim:].astype(BF16)
        kvt_ref[i, :head_dim, :], kvt_ref[i, head_dim:, :] = dkt, dv.T
        kv_ref[i, 0], kv_ref[i, 1] = dkt.T, dv

    def spread(i):
        near_copy(i, place).start()
        far_copy(i, place).start()
        own_copy(i).start()
        for copy in kv_copy:
            copy.start(i, group, i * n_group + place)

    def forward(i):
        far_copy(i, place_across).wait_recv()
        fwd_copy(i, place_across).start()

    def stages(t):
        for late, stage in ((5, forward), (4, spread), (3, close), (2, second), (1, first)):
            @pl.when((t >= late) & (t < n_block + late))
            def _():
                stage(n_block - 1 - (t - late))

    full_barrier(n_dev)

    def clear(i):
        dkv_ref[rows_of(i, block), :] = jnp.zeros((block, 2 * head_dim), F32)

    each(0, n_block, clear)

    def compute(i):
        own = rows_of(i, block)
        dat_ref[...] = da_ref[own, :].T
        mix_ref[...] = jnp.zeros_like(mix_ref)
        acc_ref[...] = jnp.zeros_like(acc_ref)

        def scores(j, carry, diagonal):
            peak, total, mixed = carry
            rows = rows_of(j, block)
            s = dot(k_ref[rows, :], qt_ref[:, own])
            if diagonal:
                s = jnp.where(causal(block), s, -1e30)
            top = jnp.maximum(peak, jnp.max(s, axis=0, keepdims=True))
            e = jnp.exp2((s - top) * fold)
            dp = dot(v_ref[rows, :], dat_ref[...])
            fade = jnp.exp2((peak - top) * fold)
            e_ref[rows, :] = e
            dp_ref[rows, :] = dp
            peak_ref[j] = top
            return top, total * fade + part_sum(e), mixed * fade + part_sum(e * dp)

        start = (jnp.full((1, block), -jnp.inf, F32), jnp.zeros((8, block), F32), jnp.zeros((8, block), F32))
        carry = lax.fori_loop(0, i, functools.partial(scores, diagonal=False), start)
        peak, total, mixed = scores(i, carry, True)
        inv = 1.0 / jnp.sum(total, axis=0, keepdims=True)
        row_dot = jnp.sum(mixed, axis=0, keepdims=True) * inv
        q_own, da_own = q_ref[own, :], da_ref[own, :]

        def grads(j):
            rows = rows_of(j, block)
            p = e_ref[rows, :] * (jnp.exp2((peak_ref[j] - peak) * fold) * inv)
            pb = p.astype(BF16)
            ds = ((dp_ref[rows, :] - row_dot) * (p * scale)).astype(BF16)
            dkv_ref[rows, :head_dim] += dot(ds, q_own)
            dkv_ref[rows, head_dim:] += dot(pb, da_own)
            mix_ref[...] += dot(vt_ref[:, rows], pb)
            acc_ref[...] += dot(kt_ref[:, rows], ds)

        each(0, i + 1, grads)
        at = mix_ref[...].astype(BF16)
        at_ref[:, own] = at
        a_ref[own, :] = at.T
        dqt = rotate(acc_ref[...], cos_ref[:, own], -sin_ref[:, own]).astype(BF16)
        dqt_ref[:, own] = dqt
        dq_ref[own, :] = dqt.T

    def iteration(t):
        stages(t)

        @pl.when(t < n_block)
        def _():
            compute(n_block - 1 - t)

    each(0, n_block + 5, iteration)

    def drain(i):
        one_copy(i).wait_send()
        two_copy(i).wait_send()
        near_copy(i, place).wait_send()
        near_copy(i, place_partner).wait_recv()
        far_copy(i, place).wait_send()
        fwd_copy(i, place_across).wait_send()
        fwd_copy(i, place_last).wait_recv()
        own_copy(i).wait()
        for copy in kv_copy:
            copy.sent(i, i * n_group + place)

    each(0, n_block, drain)

    def drain_heads(index):
        for copy in (a_copy, q_copy):
            copy.sent(index, index)
            copy.got(index)

    each(0, n_dev, drain_heads)

    def drain_kv(head):
        for copy in kv_copy:
            copy.got(head)

    each(0, kv_heads, drain_kv)


def attention(n_dev, kv_heads, q, k, v, da, qt, kt, vt, cos_tab, sin_tab):
    seq, head_dim = q.shape
    q_heads = n_dev
    n_group = q_heads // kv_heads
    tokens = seq // n_dev
    block = tokens * n_group
    n_block = seq // block
    whole, anywhere = pl.BlockSpec(memory_space=pltpu.VMEM), pl.BlockSpec(memory_space=pl.ANY)
    dma = pltpu.SemaphoreType.DMA
    return pl.pallas_call(
        functools.partial(attention_kernel, n_dev, n_group, q_heads, kv_heads, head_dim**-0.5),
        out_shape=[
            jax.ShapeDtypeStruct((head_dim, seq), BF16),
            jax.ShapeDtypeStruct((head_dim, seq), BF16),
            jax.ShapeDtypeStruct((2 * head_dim, seq), BF16),
            jax.ShapeDtypeStruct((tokens, q_heads * head_dim), BF16),
            jax.ShapeDtypeStruct((tokens, (q_heads + 2 * kv_heads) * head_dim), BF16),
        ],
        in_specs=[whole] * 9,
        out_specs=[whole] * 2 + [anywhere] * 3,
        scratch_shapes=[
            pltpu.VMEM((seq, head_dim), BF16),
            pltpu.VMEM((seq, head_dim), BF16),
            pltpu.VMEM((seq, 2 * head_dim), F32),
            pltpu.VMEM((seq, block), F32),
            pltpu.VMEM((seq, block), F32),
            pltpu.VMEM((n_block, 1, block), F32),
            pltpu.VMEM((head_dim, block), BF16),
            pltpu.VMEM((head_dim, block), F32),
            pltpu.VMEM((head_dim, block), F32),
            pltpu.VMEM((n_block, block // 2, 2 * head_dim), F32),
            pltpu.VMEM((n_block, tokens, 2 * head_dim), F32),
            pltpu.VMEM((n_block, 2, tokens, head_dim), BF16),
            pltpu.VMEM((n_block, 2 * head_dim, tokens), BF16),
            dma((n_dev,)), dma((n_dev,)), dma((n_dev,)), dma((n_dev,)),
            dma((n_block,)), dma((n_block,)), dma((n_block,)), dma((n_block,)), dma((2, n_block)), dma((2, kv_heads)),
            dma((n_block,)), dma((n_block,)), dma((n_block,)), dma((n_block,)), dma((n_block,)), dma((n_block,)), dma((n_block,)),
        ],
        compiler_params=pltpu.CompilerParams(collective_id=1, has_side_effects=True, vmem_limit_bytes=VMEM_LIMIT),
        cost_estimate=pl.CostEstimate(flops=6 * seq * seq * head_dim, bytes_accessed=18 * seq * head_dim, transcendentals=seq * seq // 2),
        name="attention",
    )(q, k, v, da, qt, kt, vt, cos_tab, sin_tab)


def finish_kernel(
    n_dev, n_group, n_buf,
    h_ref, wq_ref, wk_ref, wv_ref, wo_ref, dqt_ref, dkvt_ref, a_ref, g_ref, x_ref, dy_own_ref, x_hat_ref, inv_ref, gain_ref,
    out_ref, gx_ref, q_rows, kv_rows, sum_ref,
    buf, wq_out, wkv_out, dh_ref, part_ref, own_sum, sum_in, sum_mine,
    load_sem, q_send, q_recv, kv_send, kv_recv, s_send, s_recv, t_send, t_recv,
):
    me = lax.axis_index(AXIS)
    seq, width = h_ref.shape
    span = buf.shape[2]
    head_dim = dqt_ref.shape[0]
    depth = width // n_dev
    n_col = width // span
    per_col = span // depth
    member, group = lax.rem(me, n_group), me // n_group
    col_member = n_col // n_group
    per_member = n_dev // n_group
    kv_rows_n = wk_ref.shape[0]
    n_sum = sum_mine.shape[0]
    q_rows_n = wq_ref.shape[0]

    def cols(j):
        return rows_of(j, span)

    def loads(phase, j, slot):
        def whole(ref):
            return pltpu.make_async_copy(ref.at[:, cols(j)], buf.at[slot, pl.ds(0, ref.shape[0])], load_sem.at[slot, 0])

        if phase == 2:
            second = pltpu.make_async_copy(wv_ref.at[:, cols(j)], buf.at[slot, pl.ds(kv_rows_n, kv_rows_n)], load_sem.at[slot, 1])
            return (whole(wk_ref), second)
        return (whole((h_ref, wq_ref, None, wo_ref)[phase]),)

    def load(step):
        slot = lax.rem(step, n_buf)
        for phase in range(4):
            @pl.when((step >= phase * n_col) & (step < (phase + 1) * n_col))
            def _():
                for copy in loads(phase, step - phase * n_col, slot):
                    copy.start()

    q_copy = Exchange(lambda peer: wq_out.at[rows_of(peer, depth)], lambda head: q_rows.at[head], lambda peer: q_send.at[peer], lambda head: q_recv.at[head])
    kv_copy = Exchange(lambda i: wkv_out.at[rows_of(i, depth)], lambda head: kv_rows.at[head], lambda i: kv_send.at[i], lambda head: kv_recv.at[head])
    s_copy = Exchange(lambda peer: own_sum.at[pl.ds(peer * n_sum, n_sum)], lambda origin: sum_in.at[origin], lambda peer: s_send.at[peer], lambda origin: s_recv.at[origin])
    t_copy = Exchange(lambda peer: sum_mine, lambda origin: sum_ref.at[pl.ds(origin * n_sum, n_sum)], lambda peer: t_send.at[peer], lambda origin: t_recv.at[origin])

    def send_q(j):
        def send(u):
            peer = j * per_col + u
            q_copy.start(peer, me, peer)

        each(0, per_col, send)

    def run(phase, body):
        def step(j):
            number = phase * n_col + j
            slot = lax.rem(number, n_buf)
            for copy in loads(phase, j, slot):
                copy.wait()
            body(j, slot)
            load(number + n_buf)

        each(0, n_col, step)

    full_barrier(n_dev)
    each(0, n_buf, load)

    def weight_columns(j, slot):
        @pl.when(j > 0)
        def _():
            send_q(j - 1)

        block = buf[slot]
        wq_out[cols(j), :] = dot(dqt_ref[...], block).T

        @pl.when(j // col_member == member)
        def _():
            wkv_out[cols(j - member * col_member), :] = dot(dkvt_ref[...], buf[slot]).T

    run(0, weight_columns)

    def send_kv(index):
        kv_copy.start(index, group, member * per_member + index)

    def back_query(j, slot):
        dh_ref[:, cols(j)] = dot(g_ref[:, :q_rows_n], buf[slot])

        @pl.when(j == 0)
        def _():
            send_q(n_col - 1)
            each(0, per_member, send_kv)

    run(1, back_query)

    def back_key(j, slot):
        dh_ref[:, cols(j)] += dot(g_ref[:, q_rows_n:], buf[slot, : 2 * kv_rows_n])

    run(2, back_key)

    part_ref[...] = jnp.zeros_like(part_ref)
    gain = 1.0 + gain_ref[...]

    def norm(t):
        rows = rows_of(t, 16)
        grad_h, x_hat = dh_ref[rows, :], x_hat_ref[rows, :]
        grad_hat = grad_h * gain
        one = jnp.sum(grad_hat, axis=1, keepdims=True) * (1.0 / width)
        two = jnp.sum(grad_hat * x_hat, axis=1, keepdims=True) * (1.0 / width)
        back = inv_ref[rows, :] * (grad_hat - one - x_hat * two)
        gx_ref[rows, :] = (dy_own_ref[rows, :].astype(F32) + back).astype(BF16)
        part_ref[0] += part_sum(grad_h * x_hat)
        part_ref[1] += part_sum(grad_h)

    each(0, dh_ref.shape[0] // 16, norm)
    own_sum[...] = jnp.zeros_like(own_sum)
    for which in range(2):
        total = jnp.sum(part_ref[which], axis=0, keepdims=True)
        for c in range(width // 128):
            own_sum[c, pl.ds(which, 1), :] = total[:, c * 128 : (c + 1) * 128]

    def to_all(copy):
        def send(step):
            peer = lax.rem(me + step, n_dev)
            copy.start(peer, me, peer)

        each(0, n_dev, send)

    def add(origin):
        sum_mine[...] += sum_in[origin]

    def output(j, slot):
        @pl.when(j == 0)
        def _():
            to_all(s_copy)

        @pl.when(j == n_col // 2)
        def _():
            each(0, n_dev, s_copy.got)
            sum_mine[...] = jnp.zeros_like(sum_mine)
            each(0, n_dev, add)

        out_ref[:, cols(j)] = (x_ref[:, cols(j)].astype(F32) + dot(a_ref[...], buf[slot])).astype(BF16)

        @pl.when(j == n_col // 2)
        def _():
            to_all(t_copy)

    run(3, output)

    def drain(index):
        s_copy.sent(index, index)
        t_copy.sent(index, index)
        t_copy.got(index)
        q_copy.sent(index, index)
        q_copy.got(index)

    def drain_kv(index):
        kv_copy.sent(index, member * per_member + index)

    each(0, n_dev, drain)
    each(0, per_member, drain_kv)
    each(0, kv_rows.shape[0], kv_copy.got)


def finish(n_dev, kv_heads, h_all, wq, wk, wv, wo, dqt, dkvt, a_own, g_own, x_own, dy_own, x_hat, inv_std, gain):
    seq, width = h_all.shape
    tokens = seq // n_dev
    head_dim = dqt.shape[0]
    q_heads = n_dev
    n_group = q_heads // kv_heads
    depth = width // n_dev
    span = math.lcm(depth, 128)
    n_buf = 4
    n_sum = -(-width // (128 * n_dev))
    sums = (n_sum * n_dev, 8, 128)
    whole, anywhere = pl.BlockSpec(memory_space=pltpu.VMEM), pl.BlockSpec(memory_space=pl.ANY)
    dma = pltpu.SemaphoreType.DMA
    return pl.pallas_call(
        functools.partial(finish_kernel, n_dev, n_group, n_buf),
        out_shape=[
            jax.ShapeDtypeStruct((tokens, width), BF16),
            jax.ShapeDtypeStruct((tokens, width), BF16),
            jax.ShapeDtypeStruct((q_heads, depth, head_dim), F32),
            jax.ShapeDtypeStruct((kv_heads, depth, 2 * head_dim), F32),
            jax.ShapeDtypeStruct(sums, F32),
        ],
        in_specs=[anywhere] * 5 + [whole] * 9,
        out_specs=[whole] * 2 + [anywhere] * 2 + [whole],
        scratch_shapes=[
            pltpu.VMEM((n_buf, seq, span), BF16),
            pltpu.VMEM((width, head_dim), F32),
            pltpu.VMEM((width // n_group, 2 * head_dim), F32),
            pltpu.VMEM((tokens, width), F32),
            pltpu.VMEM((2, 8, width), F32),
            pltpu.VMEM(sums, F32),
            pltpu.VMEM((n_dev, n_sum, 8, 128), F32),
            pltpu.VMEM((n_sum, 8, 128), F32),
            dma((n_buf, 2)), dma((n_dev,)), dma((n_dev,)), dma((n_dev // n_group,)), dma((kv_heads,)), dma((n_dev,)), dma((n_dev,)), dma((n_dev,)), dma((n_dev,)),
        ],
        compiler_params=pltpu.CompilerParams(collective_id=2, has_side_effects=True, vmem_limit_bytes=VMEM_LIMIT),
        cost_estimate=pl.CostEstimate(flops=8 * seq * width * head_dim, bytes_accessed=8 * seq * width, transcendentals=0),
        name="finish",
    )(h_all, wq, wk, wv, wo, dqt, dkvt, a_own, g_own, x_own, dy_own, x_hat, inv_std, gain)


def solution(mesh):
    n_dev = mesh.shape[AXIS]

    def device_step(x_act, d_out, positions, ln_gain, ln_bias, w_query, w_key, w_value, w_out):
        n_batch, piece, width = x_act.shape
        q_heads, head_dim = w_query.shape[1:]
        kv_heads = w_key.shape[1]
        n_group = q_heads // kv_heads
        tokens = n_batch * piece
        me = lax.axis_index(AXIS)
        kv_head = me // n_group

        x_own, dy_own = x_act.reshape(tokens, width), d_out.reshape(tokens, width)
        normed, x_hat, inv_std = norm_forward(x_own, ln_gain, ln_bias)
        h_all = lax.all_gather(normed, AXIS, axis=0, tiled=True)
        dy_all = lax.all_gather(lax.optimization_barrier((dy_own, normed))[0], AXIS, axis=0, tiled=True)
        da, pos_all = heads_in(n_dev, dy_own, jnp.broadcast_to(positions.reshape(1, tokens), (8, tokens)), w_out, head_dim)
        cos_tab, sin_tab = rope_tables(pos_all[:, 0, :].reshape(-1), head_dim)
        wq_rows, wk_rows, wv_rows = (jnp.transpose(w, (1, 2, 0)).reshape(-1, width) for w in (w_query, w_key, w_value))
        w_head = jnp.concatenate([lax.dynamic_slice_in_dim(w, i * head_dim, head_dim, axis=0) for w, i in ((wq_rows, me), (wk_rows, kv_head), (wv_rows, kv_head))], axis=0)

        q, k, v, qt, kt, vt = project(h_all, w_head, cos_tab, sin_tab, head_dim)
        at, dqt, dkvt, a_own, g_own = attention(n_dev, kv_heads, q, k, v, da, qt, kt, vt, cos_tab, sin_tab)
        block_out, grad_x, rows_wq, rows_wkv, sums = finish(
            n_dev, kv_heads, h_all, wq_rows, wk_rows, wv_rows, w_out, dqt, dkvt, a_own, g_own, x_own, dy_own, x_hat, inv_std, ln_gain.reshape(1, width)
        )
        grad_wo = dot(at, lax.optimization_barrier((dy_all, sums))[0])
        grad_wq = jnp.swapaxes(rows_wq, 0, 1)
        grad_wk = jnp.swapaxes(rows_wkv[:, :, :head_dim], 0, 1)
        grad_wv = jnp.swapaxes(rows_wkv[:, :, head_dim:], 0, 1)
        n_lane = width // 128
        grad_gain, grad_bias = sums[:n_lane, 0].reshape(width), sums[:n_lane, 1].reshape(width)
        return (block_out.reshape(x_act.shape), grad_x.reshape(x_act.shape), grad_wq, grad_wk, grad_wv, grad_wo, grad_gain, grad_bias)

    return jax.shard_map(device_step, mesh=mesh, in_specs=(P("dp", AXIS, None), P("dp", AXIS, None), P("dp", AXIS), P(None), P(None), P(None, None, None), P(None, None, None), P(None, None, None), P(None, None)), out_specs=(P("dp", AXIS, None), P("dp", AXIS, None), P(("dp", AXIS), None, None), P(("dp", AXIS), None, None), P(("dp", AXIS), None, None), P(("dp", AXIS), None), P("dp"), P("dp")), check_vma=False)
```

```python
import functools
import math

import jax
import jax.numpy as jnp
from jax import lax
from jax.experimental import pallas as pl
from jax.experimental.pallas import tpu as pltpu
from jax.sharding import PartitionSpec as P

EPS = 1e-5
ROPE_BASE = 10000.0
BLOCK = 512
AXIS = "cp"
BF16, F32 = jnp.bfloat16, jnp.float32
VMEM_LIMIT = 60 * 1024 * 1024


def norm_forward(x_act, ln_gain, ln_bias):
    x_f32 = x_act.astype(F32)
    centered = x_f32 - jnp.mean(x_f32, axis=-1, keepdims=True)
    inv_std = lax.rsqrt(jnp.mean(centered * centered, axis=-1, keepdims=True) + EPS)
    x_hat = centered * inv_std
    return (x_hat * (1.0 + ln_gain) + ln_bias).astype(BF16), x_hat, inv_std


def rope_tables(positions, head_dim):
    quarter = head_dim // 4
    freq_tab = jnp.exp(jnp.arange(quarter, dtype=F32) * (-2.0 * math.log(ROPE_BASE) / (head_dim // 2)))
    angles = freq_tab[:, None] * positions.astype(F32)[None, :]
    return jnp.cos(angles), jnp.sin(angles)


def rotate(values, cos, sin):
    quarter = cos.shape[0]
    first, second = values[:quarter], values[quarter : 2 * quarter]
    return jnp.concatenate([first * cos - second * sin, second * cos + first * sin, values[2 * quarter :]], axis=0)


def rows_of(index, size):
    return pl.ds(pl.multiple_of(index * size, size), size)


def dot(lhs, rhs):
    return jnp.dot(lhs, rhs, preferred_element_type=F32)


def dot_t(lhs, rhs):
    return lax.dot_general(lhs, rhs, (((1,), (1,)), ((), ())), preferred_element_type=F32)


def full_barrier(n_dev):
    me = lax.axis_index(AXIS)
    barrier = pltpu.get_barrier_semaphore()

    def tell(step):
        pl.semaphore_signal(barrier, inc=1, device_id={AXIS: lax.rem(me + step, n_dev)}, device_id_type=pl.DeviceIdType.MESH)

    each(1, n_dev, tell)
    pl.semaphore_wait(barrier, n_dev - 1)


def remote(src, dst, send_sem, recv_sem, peer):
    return pltpu.make_async_remote_copy(src_ref=src, dst_ref=dst, send_sem=send_sem, recv_sem=recv_sem, device_id={AXIS: peer}, device_id_type=pl.DeviceIdType.MESH)


def each(lower, upper, body):
    def step(index, carry):
        body(index)
        return carry

    lax.fori_loop(lower, upper, step, 0)


class Exchange:
    def __init__(self, src, dst, send, recv):
        self.src, self.dst, self.send, self.recv = src, dst, send, recv

    def start(self, index, slot, peer):
        me = lax.axis_index(AXIS)
        src, dst, recv = self.src(index), self.dst(slot), self.recv(slot)

        @pl.when(peer != me)
        def _():
            remote(src, dst, self.send(index), recv, peer).start()

        @pl.when(peer == me)
        def _():
            pltpu.make_async_copy(src, dst, recv).start()

    def sent(self, index, peer):
        me = lax.axis_index(AXIS)

        @pl.when(peer != me)
        def _():
            remote(self.src(index), self.src(index), self.send(index), self.send(index), me).wait_send()

    def got(self, slot):
        dst = self.dst(slot)
        remote(dst, dst, self.recv(slot), self.recv(slot), lax.axis_index(AXIS)).wait_recv()


def heads_in_kernel(n_dev, n_buf, dy_ref, pos_ref, wo_ref, da_ref, pos_out, buf, da_buf, load_sem, send, recv, pos_send, pos_recv):
    me = lax.axis_index(AXIS)
    tokens = dy_ref.shape[0]
    head_dim = da_ref.shape[1]
    span = buf.shape[1]
    n_step = wo_ref.shape[0] // span
    per_step = span // head_dim
    piece = Exchange(lambda peer: da_buf.at[peer], lambda origin: da_ref.at[rows_of(origin, tokens)], lambda peer: send.at[peer], lambda origin: recv.at[origin])
    where = Exchange(lambda peer: pos_ref, lambda origin: pos_out.at[origin], lambda peer: pos_send.at[peer], lambda origin: pos_recv.at[origin])

    def turn(step):
        return lax.rem(step + me // per_step, n_step)

    def load(step):
        slot = lax.rem(step, n_buf)
        return pltpu.make_async_copy(wo_ref.at[rows_of(turn(step), span)], buf.at[slot], load_sem.at[slot])

    for step in range(n_buf):
        load(step).start()
    full_barrier(n_dev)

    def send_pos(step):
        peer = lax.rem(me + step, n_dev)
        where.start(peer, me, peer)

    each(0, n_dev, send_pos)

    def send_heads(step):
        def one(u):
            peer = turn(step) * per_step + lax.rem(u + me, per_step)
            piece.start(peer, me, peer)

        each(0, per_step, one)

    def product(step):
        @pl.when(step > 0)
        def _():
            send_heads(step - 1)

        load(step).wait()
        da = dot_t(dy_ref[...], buf[lax.rem(step, n_buf)]).astype(BF16)
        for u in range(per_step):
            da_buf[turn(step) * per_step + u] = da[:, u * head_dim : (u + 1) * head_dim]

        @pl.when(step + n_buf < n_step)
        def _():
            load(step + n_buf).start()

    each(0, n_step, product)
    send_heads(n_step - 1)

    def drain(index):
        for copy in (piece, where):
            copy.sent(index, index)
            copy.got(index)

    each(0, n_dev, drain)


def heads_in(n_dev, dy_own, positions, w_out, head_dim):
    tokens, width = dy_own.shape
    span = min(BLOCK, w_out.shape[0])
    n_buf = min(3, w_out.shape[0] // span)
    whole, anywhere = pl.BlockSpec(memory_space=pltpu.VMEM), pl.BlockSpec(memory_space=pl.ANY)
    dma = pltpu.SemaphoreType.DMA
    return pl.pallas_call(
        functools.partial(heads_in_kernel, n_dev, n_buf),
        out_shape=[jax.ShapeDtypeStruct((tokens * n_dev, head_dim), BF16), jax.ShapeDtypeStruct((n_dev,) + positions.shape, jnp.int32)],
        in_specs=[whole, whole, anywhere],
        out_specs=[anywhere] * 2,
        scratch_shapes=[
            pltpu.VMEM((n_buf, span, width), BF16),
            pltpu.VMEM((n_dev, tokens, head_dim), BF16),
            dma((n_buf,)), dma((n_dev,)), dma((n_dev,)), dma((n_dev,)), dma((n_dev,)),
        ],
        compiler_params=pltpu.CompilerParams(collective_id=3, has_side_effects=True, vmem_limit_bytes=VMEM_LIMIT),
        cost_estimate=pl.CostEstimate(flops=2 * tokens * width * w_out.shape[0], bytes_accessed=2 * width * w_out.shape[0], transcendentals=0),
        name="heads_in",
    )(dy_own, positions, w_out)


def project_kernel(h_ref, w_ref, cos_ref, sin_ref, q_ref, k_ref, v_ref, qt_ref, kt_ref, vt_ref):
    head_dim = q_ref.shape[1]
    out = dot_t(h_ref[...], w_ref[...])
    cos, sin = cos_ref[...], sin_ref[...]
    qt = rotate(out[:, :head_dim].T, cos, sin).astype(BF16)
    kt = rotate(out[:, head_dim : 2 * head_dim].T, cos, sin).astype(BF16)
    v = out[:, 2 * head_dim :].astype(BF16)
    qt_ref[...], kt_ref[...], vt_ref[...] = qt, kt, v.T
    q_ref[...], k_ref[...], v_ref[...] = qt.T, kt.T, v


def project(h_all, w_head, cos_tab, sin_tab, head_dim):
    seq, width = h_all.shape
    block = min(BLOCK, seq)
    by_rows = pl.BlockSpec((block, head_dim), lambda i: (i, 0))
    by_cols = pl.BlockSpec((head_dim, block), lambda i: (0, i))
    table = pl.BlockSpec((head_dim // 4, block), lambda i: (0, i))
    return pl.pallas_call(
        project_kernel,
        grid=(seq // block,),
        out_shape=[jax.ShapeDtypeStruct((seq, head_dim), BF16)] * 3 + [jax.ShapeDtypeStruct((head_dim, seq), BF16)] * 3,
        in_specs=[pl.BlockSpec((block, width), lambda i: (i, 0)), pl.BlockSpec(w_head.shape, lambda i: (0, 0)), table, table],
        out_specs=[by_rows] * 3 + [by_cols] * 3,
        compiler_params=pltpu.CompilerParams(vmem_limit_bytes=VMEM_LIMIT),
        cost_estimate=pl.CostEstimate(flops=2 * seq * width * w_head.shape[0], bytes_accessed=2 * seq * width, transcendentals=0),
        name="project",
    )(h_all, w_head, cos_tab, sin_tab)


def causal(block):
    key = lax.broadcasted_iota(jnp.int32, (block, block), 0)
    query = lax.broadcasted_iota(jnp.int32, (block, block), 1)
    return key <= query


def part_sum(values):
    return jnp.sum(values.reshape(values.shape[0] // 8, 8, values.shape[1]), axis=0)


def attention_kernel(
    n_dev, n_group, q_heads, kv_heads, scale,
    q_ref, k_ref, v_ref, da_ref, qt_ref, kt_ref, vt_ref, cos_ref, sin_ref,
    at_ref, dqt_ref, a_ref, dq_ref, dkvt_ref, a_out, grad_out,
    dkv_ref, e_ref, dp_ref, peak_ref, dat_ref, mix_ref, acc_ref, land_one, land_two, kv_ref, kvt_ref,
    a_send, a_recv, q_send, q_recv, one_send, one_recv, two_send, two_recv, kv_send, kv_recv, near_send, near_recv, far_send, far_recv, fwd_send, fwd_recv, local,
):
    me = lax.axis_index(AXIS)
    seq, head_dim = q_ref.shape
    block = e_ref.shape[1]
    n_block = seq // block
    tokens = seq // n_dev
    half = block // 2
    fold = scale * math.log2(math.e)
    core, side = lax.rem(me, 2), lax.rem(me // 2, 2)
    group = me // n_group
    partner, across = me + 1 - 2 * core, me + 2 - 4 * side
    place, place_across = core * 2 + side, core * 2 + 1 - side
    place_partner, place_last = (1 - core) * 2 + side, (1 - core) * 2 + 1 - side

    def piece(index):
        return rows_of(index, tokens)

    def column(head):
        return rows_of(head, head_dim)

    a_copy = Exchange(lambda peer: a_ref.at[piece(peer)], lambda head: a_out.at[:, column(head)], lambda peer: a_send.at[peer], lambda head: a_recv.at[head])
    q_copy = Exchange(lambda peer: dq_ref.at[piece(peer)], lambda head: grad_out.at[:, column(head)], lambda peer: q_send.at[peer], lambda head: q_recv.at[head])
    kv_copy = [
        Exchange(
            lambda i, w=w: kv_ref.at[i, w],
            lambda head, w=w: grad_out.at[:, column(q_heads + w * kv_heads + head)],
            lambda i, w=w: kv_send.at[w, i],
            lambda head, w=w: kv_recv.at[w, head],
        )
        for w in range(2)
    ]

    def one_copy(i):
        return remote(dkv_ref.at[rows_of(i * 2 + 1 - core, half)], land_one.at[i], one_send.at[i], one_recv.at[i], partner)

    def two_copy(i):
        return remote(dkv_ref.at[piece(i * n_group + core * 2 + 1 - side)], land_two.at[i], two_send.at[i], two_recv.at[i], across)

    def near_copy(i, where):
        return remote(kvt_ref.at[i], dkvt_ref.at[:, piece(i * n_group + where)], near_send.at[i], near_recv.at[i], partner)

    def far_copy(i, where):
        return remote(kvt_ref.at[i], dkvt_ref.at[:, piece(i * n_group + where)], far_send.at[i], far_recv.at[i], across)

    def fwd_copy(i, where):
        view = dkvt_ref.at[:, piece(i * n_group + where)]
        return remote(view, view, fwd_send.at[i], fwd_recv.at[i], partner)

    def own_copy(i):
        return pltpu.make_async_copy(kvt_ref.at[i], dkvt_ref.at[:, piece(i * n_group + place)], local.at[i])

    def first(i):
        def send(u):
            peer = i * n_group + lax.rem(u + me, n_group)
            a_copy.start(peer, me, peer)
            q_copy.start(peer, me, peer)

        one_copy(i).start()

        @pl.when(i >= n_block // 2)
        def _():
            each(0, n_group, send)

    def second(i):
        one_copy(i).wait_recv()
        for part in (1 - side, side):
            rows = piece(i * n_group + core * 2 + part)
            dkv_ref[rows, :] += land_one[i, pl.ds(pl.multiple_of(part * tokens, tokens), tokens), :]
        two_copy(i).start()

    def close(i):
        two_copy(i).wait_recv()
        rows = piece(i * n_group + place)
        total = dkv_ref[rows, :] + land_two[i]
        dkt = rotate(total[:, :head_dim].T, cos_ref[:, rows], -sin_ref[:, rows]).astype(BF16)
        dv = total[:, head_dim:].astype(BF16)
        kvt_ref[i, :head_dim, :], kvt_ref[i, head_dim:, :] = dkt, dv.T
        kv_ref[i, 0], kv_ref[i, 1] = dkt.T, dv

    def spread(i):
        near_copy(i, place).start()
        far_copy(i, place).start()
        own_copy(i).start()
        for copy in kv_copy:
            copy.start(i, group, i * n_group + place)

    def forward(i):
        far_copy(i, place_across).wait_recv()
        fwd_copy(i, place_across).start()

    def stages(t):
        for late, stage in ((5, forward), (4, spread), (3, close), (2, second), (1, first)):
            @pl.when((t >= late) & (t < n_block + late))
            def _():
                stage(n_block - 1 - (t - late))

    full_barrier(n_dev)

    def clear(i):
        dkv_ref[rows_of(i, block), :] = jnp.zeros((block, 2 * head_dim), F32)

    each(0, n_block, clear)

    def compute(i):
        own = rows_of(i, block)
        dat_ref[...] = da_ref[own, :].T
        mix_ref[...] = jnp.zeros_like(mix_ref)
        acc_ref[...] = jnp.zeros_like(acc_ref)

        def scores(j, carry, diagonal):
            peak, total, mixed = carry
            rows = rows_of(j, block)
            s = dot(k_ref[rows, :], qt_ref[:, own])
            if diagonal:
                s = jnp.where(causal(block), s, -1e30)
            top = jnp.maximum(peak, jnp.max(s, axis=0, keepdims=True))
            e = jnp.exp2((s - top) * fold)
            dp = dot(v_ref[rows, :], dat_ref[...])
            fade = jnp.exp2((peak - top) * fold)
            e_ref[rows, :] = e
            dp_ref[rows, :] = dp
            peak_ref[j] = top
            return top, total * fade + part_sum(e), mixed * fade + part_sum(e * dp)

        start = (jnp.full((1, block), -jnp.inf, F32), jnp.zeros((8, block), F32), jnp.zeros((8, block), F32))
        carry = lax.fori_loop(0, i, functools.partial(scores, diagonal=False), start)
        peak, total, mixed = scores(i, carry, True)
        inv = 1.0 / jnp.sum(total, axis=0, keepdims=True)
        row_dot = jnp.sum(mixed, axis=0, keepdims=True) * inv
        q_own, da_own = q_ref[own, :], da_ref[own, :]

        def grads(j):
            rows = rows_of(j, block)
            p = e_ref[rows, :] * (jnp.exp2((peak_ref[j] - peak) * fold) * inv)
            pb = p.astype(BF16)
            ds = ((dp_ref[rows, :] - row_dot) * (p * scale)).astype(BF16)
            dkv_ref[rows, :head_dim] += dot(ds, q_own)
            dkv_ref[rows, head_dim:] += dot(pb, da_own)
            mix_ref[...] += dot(vt_ref[:, rows], pb)
            acc_ref[...] += dot(kt_ref[:, rows], ds)

        each(0, i + 1, grads)
        at = mix_ref[...].astype(BF16)
        at_ref[:, own] = at
        a_ref[own, :] = at.T
        dqt = rotate(acc_ref[...], cos_ref[:, own], -sin_ref[:, own]).astype(BF16)
        dqt_ref[:, own] = dqt
        dq_ref[own, :] = dqt.T

    def iteration(t):
        stages(t)

        @pl.when(t < n_block)
        def _():
            compute(n_block - 1 - t)

    each(0, n_block + 5, iteration)

    def drain(i):
        one_copy(i).wait_send()
        two_copy(i).wait_send()
        near_copy(i, place).wait_send()
        near_copy(i, place_partner).wait_recv()
        far_copy(i, place).wait_send()
        fwd_copy(i, place_across).wait_send()
        fwd_copy(i, place_last).wait_recv()
        own_copy(i).wait()
        for copy in kv_copy:
            copy.sent(i, i * n_group + place)

    each(0, n_block, drain)

    def drain_sent(peer):
        for copy in (a_copy, q_copy):
            copy.sent(peer, peer)

    def drain_got(head):
        for copy in (a_copy, q_copy):
            copy.got(head)

    low = n_block // 2 * n_group
    each(low, n_dev, drain_sent)

    @pl.when(me >= low)
    def _():
        each(0, n_dev, drain_got)

    def drain_kv(head):
        for copy in kv_copy:
            copy.got(head)

    each(0, kv_heads, drain_kv)


def attention(n_dev, kv_heads, q, k, v, da, qt, kt, vt, cos_tab, sin_tab):
    seq, head_dim = q.shape
    q_heads = n_dev
    n_group = q_heads // kv_heads
    tokens = seq // n_dev
    block = tokens * n_group
    n_block = seq // block
    whole, anywhere = pl.BlockSpec(memory_space=pltpu.VMEM), pl.BlockSpec(memory_space=pl.ANY)
    dma = pltpu.SemaphoreType.DMA
    return pl.pallas_call(
        functools.partial(attention_kernel, n_dev, n_group, q_heads, kv_heads, head_dim**-0.5),
        out_shape=[
            jax.ShapeDtypeStruct((head_dim, seq), BF16),
            jax.ShapeDtypeStruct((head_dim, seq), BF16),
            jax.ShapeDtypeStruct((seq, head_dim), BF16),
            jax.ShapeDtypeStruct((seq, head_dim), BF16),
            jax.ShapeDtypeStruct((2 * head_dim, seq), BF16),
            jax.ShapeDtypeStruct((tokens, q_heads * head_dim), BF16),
            jax.ShapeDtypeStruct((tokens, (q_heads + 2 * kv_heads) * head_dim), BF16),
        ],
        in_specs=[whole] * 9,
        out_specs=[whole] * 4 + [anywhere] * 3,
        scratch_shapes=[
            pltpu.VMEM((seq, 2 * head_dim), F32),
            pltpu.VMEM((seq, block), F32),
            pltpu.VMEM((seq, block), F32),
            pltpu.VMEM((n_block, 1, block), F32),
            pltpu.VMEM((head_dim, block), BF16),
            pltpu.VMEM((head_dim, block), F32),
            pltpu.VMEM((head_dim, block), F32),
            pltpu.VMEM((n_block, block // 2, 2 * head_dim), F32),
            pltpu.VMEM((n_block, tokens, 2 * head_dim), F32),
            pltpu.VMEM((n_block, 2, tokens, head_dim), BF16),
            pltpu.VMEM((n_block, 2 * head_dim, tokens), BF16),
            dma((n_dev,)), dma((n_dev,)), dma((n_dev,)), dma((n_dev,)),
            dma((n_block,)), dma((n_block,)), dma((n_block,)), dma((n_block,)), dma((2, n_block)), dma((2, kv_heads)),
            dma((n_block,)), dma((n_block,)), dma((n_block,)), dma((n_block,)), dma((n_block,)), dma((n_block,)), dma((n_block,)),
        ],
        compiler_params=pltpu.CompilerParams(collective_id=1, has_side_effects=True, vmem_limit_bytes=VMEM_LIMIT),
        cost_estimate=pl.CostEstimate(flops=6 * seq * seq * head_dim, bytes_accessed=18 * seq * head_dim, transcendentals=seq * seq // 2),
        name="attention",
    )(q, k, v, da, qt, kt, vt, cos_tab, sin_tab)


def finish_kernel(
    n_dev, n_group, n_buf,
    h_ref, dy_ref, wq_ref, wk_ref, wv_ref, wo_ref, a_in, g_in, a_head, dq_head, dqt_ref, dkvt_ref, at_ref, x_ref, dy_own_ref, x_hat_ref, inv_ref, gain_ref,
    out_ref, gx_ref, gwo_ref, q_rows, kv_rows, sum_ref,
    a_ref, g_ref, buf, wq_out, wkv_out, dh_ref, part_ref, own_sum, sum_in, sum_mine,
    load_sem, q_send, q_recv, kv_send, kv_recv, s_send, s_recv, t_send, t_recv, a_send, a_recv, dq_send, dq_recv, local,
):
    me = lax.axis_index(AXIS)
    seq, width = h_ref.shape
    span = buf.shape[2]
    head_dim = dqt_ref.shape[0]
    depth = width // n_dev
    n_col = width // span
    per_col = span // depth
    member, group = lax.rem(me, n_group), me // n_group
    col_member = n_col // n_group
    per_member = n_dev // n_group
    kv_rows_n = wk_ref.shape[0]
    n_sum = sum_mine.shape[0]
    q_rows_n = wq_ref.shape[0]

    tokens = x_ref.shape[0]
    low = n_dev // n_group // 2 * n_group

    def cols(j):
        return rows_of(j, span)

    def turn(phase, j):
        return lax.rem(j + me // per_col, n_col) if phase == 0 else j

    def loads(phase, j, slot):
        def whole(ref):
            return pltpu.make_async_copy(ref.at[:, cols(turn(phase, j))], buf.at[slot, pl.ds(0, ref.shape[0])], load_sem.at[slot, 0])

        if phase == 3:
            second = pltpu.make_async_copy(wv_ref.at[:, cols(j)], buf.at[slot, pl.ds(kv_rows_n, kv_rows_n)], load_sem.at[slot, 1])
            return (whole(wk_ref), second)
        return (whole((h_ref, dy_ref, wq_ref, None, wo_ref)[phase]),)

    def load(step):
        slot = lax.rem(step, n_buf)
        for phase in range(5):
            @pl.when((step >= phase * n_col) & (step < (phase + 1) * n_col))
            def _():
                for copy in loads(phase, step - phase * n_col, slot):
                    copy.start()

    q_copy = Exchange(lambda peer: wq_out.at[rows_of(peer, depth)], lambda head: q_rows.at[head], lambda peer: q_send.at[peer], lambda head: q_recv.at[head])
    kv_copy = Exchange(lambda i: wkv_out.at[rows_of(i, depth)], lambda head: kv_rows.at[head], lambda i: kv_send.at[i], lambda head: kv_recv.at[head])
    s_copy = Exchange(lambda peer: own_sum.at[pl.ds(peer * n_sum, n_sum)], lambda origin: sum_in.at[origin], lambda peer: s_send.at[peer], lambda origin: s_recv.at[origin])
    t_copy = Exchange(lambda peer: sum_mine, lambda origin: sum_ref.at[pl.ds(origin * n_sum, n_sum)], lambda peer: t_send.at[peer], lambda origin: t_recv.at[origin])

    def column(head):
        return rows_of(head, head_dim)

    a_copy = Exchange(lambda peer: a_head.at[rows_of(peer, tokens)], lambda head: a_ref.at[:, column(head)], lambda peer: a_send.at[peer], lambda head: a_recv.at[head])
    dq_copy = Exchange(lambda peer: dq_head.at[rows_of(peer, tokens)], lambda head: g_ref.at[:, column(head)], lambda peer: dq_send.at[peer], lambda head: dq_recv.at[head])

    def send_heads(step):
        peer = lax.rem(me + step, low)
        a_copy.start(peer, me, peer)
        dq_copy.start(peer, me, peer)

    own_kv = pltpu.make_async_copy(g_in.at[:, pl.ds(q_rows_n, 2 * kv_rows_n)], g_ref.at[:, pl.ds(q_rows_n, 2 * kv_rows_n)], local.at[0])
    own_a = pltpu.make_async_copy(a_in, a_ref, local.at[1])
    own_dq = pltpu.make_async_copy(g_in.at[:, pl.ds(0, q_rows_n)], g_ref.at[:, pl.ds(0, q_rows_n)], local.at[2])

    def send_q(j):
        def send(u):
            peer = turn(0, j) * per_col + lax.rem(u + me, per_col)
            q_copy.start(peer, me, peer)

        each(0, per_col, send)

    def run(phase, body):
        def step(j):
            number = phase * n_col + j
            slot = lax.rem(number, n_buf)
            for copy in loads(phase, j, slot):
                copy.wait()
            body(j, slot)
            load(number + n_buf)

        each(0, n_col, step)

    each(0, n_buf, load)
    own_kv.start()

    @pl.when(me >= low)
    def _():
        own_a.start()
        own_dq.start()

    full_barrier(n_dev)
    each(0, low, send_heads)

    def weight_columns(j, slot):
        @pl.when(j > 0)
        def _():
            send_q(j - 1)

        col = turn(0, j)
        wq_out[cols(col), :] = dot(dqt_ref[...], buf[slot]).T

        @pl.when(col // col_member == member)
        def _():
            wkv_out[cols(col - member * col_member), :] = dot(dkvt_ref[...], buf[slot]).T

    run(0, weight_columns)

    def send_kv(step):
        index = lax.rem(step + group, per_member)
        kv_copy.start(index, group, member * per_member + index)

    def weight_out(j, slot):
        gwo_ref[:, cols(j)] = dot(at_ref[...], buf[slot])

        @pl.when(j == 0)
        def _():
            send_q(n_col - 1)
            each(0, per_member, send_kv)

    run(1, weight_out)
    own_kv.wait()

    @pl.when(me >= low)
    def _():
        own_a.wait()
        own_dq.wait()

    def got_heads(head):
        a_copy.got(head)
        dq_copy.got(head)

    @pl.when(me < low)
    def _():
        each(0, n_dev, got_heads)

    def back_query(j, slot):
        dh_ref[:, cols(j)] = dot(g_ref[:, :q_rows_n], buf[slot])

    run(2, back_query)

    def back_key(j, slot):
        dh_ref[:, cols(j)] += dot(g_ref[:, q_rows_n:], buf[slot, : 2 * kv_rows_n])

    run(3, back_key)

    part_ref[...] = jnp.zeros_like(part_ref)
    gain = 1.0 + gain_ref[...]

    def norm(t):
        rows = rows_of(t, 16)
        grad_h, x_hat = dh_ref[rows, :], x_hat_ref[rows, :]
        grad_hat = grad_h * gain
        one = jnp.sum(grad_hat, axis=1, keepdims=True) * (1.0 / width)
        two = jnp.sum(grad_hat * x_hat, axis=1, keepdims=True) * (1.0 / width)
        back = inv_ref[rows, :] * (grad_hat - one - x_hat * two)
        gx_ref[rows, :] = (dy_own_ref[rows, :].astype(F32) + back).astype(BF16)
        part_ref[0] += part_sum(grad_h * x_hat)
        part_ref[1] += part_sum(grad_h)

    each(0, dh_ref.shape[0] // 16, norm)
    own_sum[...] = jnp.zeros_like(own_sum)
    for which in range(2):
        total = jnp.sum(part_ref[which], axis=0, keepdims=True)
        for c in range(width // 128):
            own_sum[c, pl.ds(which, 1), :] = total[:, c * 128 : (c + 1) * 128]

    def to_all(copy):
        def send(step):
            peer = lax.rem(me + step, n_dev)
            copy.start(peer, me, peer)

        each(0, n_dev, send)

    def add(origin):
        sum_mine[...] += sum_in[origin]

    def output(j, slot):
        @pl.when(j == 0)
        def _():
            to_all(s_copy)

        @pl.when(j == n_col // 2)
        def _():
            each(0, n_dev, s_copy.got)
            sum_mine[...] = jnp.zeros_like(sum_mine)
            each(0, n_dev, add)

        out_ref[:, cols(j)] = (x_ref[:, cols(j)].astype(F32) + dot(a_ref[...], buf[slot])).astype(BF16)

        @pl.when(j == n_col // 2)
        def _():
            to_all(t_copy)

    run(4, output)

    def drain(index):
        s_copy.sent(index, index)
        t_copy.sent(index, index)
        t_copy.got(index)
        q_copy.sent(index, index)
        q_copy.got(index)

    def drain_kv(index):
        kv_copy.sent(index, member * per_member + index)

    def drain_heads(peer):
        a_copy.sent(peer, peer)
        dq_copy.sent(peer, peer)

    each(0, n_dev, drain)
    each(0, low, drain_heads)
    each(0, per_member, drain_kv)
    each(0, kv_rows.shape[0], kv_copy.got)


def finish(n_dev, kv_heads, h_all, dy_all, wq, wk, wv, wo, a_in, g_in, a_head, dq_head, dqt, dkvt, at, x_own, dy_own, x_hat, inv_std, gain):
    seq, width = h_all.shape
    tokens = seq // n_dev
    head_dim = dqt.shape[0]
    q_heads = n_dev
    n_group = q_heads // kv_heads
    depth = width // n_dev
    span = math.lcm(depth, 128)
    n_buf = 4
    n_sum = -(-width // (128 * n_dev))
    sums = (n_sum * n_dev, 8, 128)
    whole, anywhere = pl.BlockSpec(memory_space=pltpu.VMEM), pl.BlockSpec(memory_space=pl.ANY)
    dma = pltpu.SemaphoreType.DMA
    return pl.pallas_call(
        functools.partial(finish_kernel, n_dev, n_group, n_buf),
        out_shape=[
            jax.ShapeDtypeStruct((tokens, width), BF16),
            jax.ShapeDtypeStruct((tokens, width), BF16),
            jax.ShapeDtypeStruct((head_dim, width), F32),
            jax.ShapeDtypeStruct((q_heads, depth, head_dim), F32),
            jax.ShapeDtypeStruct((kv_heads, depth, 2 * head_dim), F32),
            jax.ShapeDtypeStruct(sums, F32),
        ],
        in_specs=[anywhere] * 10 + [whole] * 8,
        out_specs=[whole] * 3 + [anywhere] * 2 + [whole],
        scratch_shapes=[
            pltpu.VMEM(a_in.shape, BF16),
            pltpu.VMEM(g_in.shape, BF16),
            pltpu.VMEM((n_buf, seq, span), BF16),
            pltpu.VMEM((width, head_dim), F32),
            pltpu.VMEM((width // n_group, 2 * head_dim), F32),
            pltpu.VMEM((tokens, width), F32),
            pltpu.VMEM((2, 8, width), F32),
            pltpu.VMEM(sums, F32),
            pltpu.VMEM((n_dev, n_sum, 8, 128), F32),
            pltpu.VMEM((n_sum, 8, 128), F32),
            dma((n_buf, 2)), dma((n_dev,)), dma((n_dev,)), dma((n_dev // n_group,)), dma((kv_heads,)), dma((n_dev,)), dma((n_dev,)), dma((n_dev,)), dma((n_dev,)),
            dma((n_dev,)), dma((n_dev,)), dma((n_dev,)), dma((n_dev,)), dma((3,)),
        ],
        compiler_params=pltpu.CompilerParams(collective_id=2, has_side_effects=True, vmem_limit_bytes=VMEM_LIMIT),
        cost_estimate=pl.CostEstimate(flops=8 * seq * width * head_dim, bytes_accessed=8 * seq * width, transcendentals=0),
        name="finish",
    )(h_all, dy_all, wq, wk, wv, wo, a_in, g_in, a_head, dq_head, dqt, dkvt, at, x_own, dy_own, x_hat, inv_std, gain)


def solution(mesh):
    n_dev = mesh.shape[AXIS]

    def device_step(x_act, d_out, positions, ln_gain, ln_bias, w_query, w_key, w_value, w_out):
        n_batch, piece, width = x_act.shape
        q_heads, head_dim = w_query.shape[1:]
        kv_heads = w_key.shape[1]
        n_group = q_heads // kv_heads
        tokens = n_batch * piece
        me = lax.axis_index(AXIS)
        kv_head = me // n_group

        x_own, dy_own = x_act.reshape(tokens, width), d_out.reshape(tokens, width)
        normed, x_hat, inv_std = norm_forward(x_own, ln_gain, ln_bias)
        h_all = lax.all_gather(normed, AXIS, axis=0, tiled=True)
        dy_all = lax.all_gather(lax.optimization_barrier((dy_own, normed))[0], AXIS, axis=0, tiled=True)
        da, pos_all = heads_in(n_dev, dy_own, jnp.broadcast_to(positions.reshape(1, tokens), (8, tokens)), w_out, head_dim)
        cos_tab, sin_tab = rope_tables(pos_all[:, 0, :].reshape(-1), head_dim)
        wq_rows, wk_rows, wv_rows = (jnp.transpose(w, (1, 2, 0)).reshape(-1, width) for w in (w_query, w_key, w_value))
        w_head = jnp.concatenate([lax.dynamic_slice_in_dim(w, i * head_dim, head_dim, axis=0) for w, i in ((wq_rows, me), (wk_rows, kv_head), (wv_rows, kv_head))], axis=0)

        q, k, v, qt, kt, vt = project(h_all, w_head, cos_tab, sin_tab, head_dim)
        at, dqt, a_head, dq_head, dkvt, a_own, g_own = attention(n_dev, kv_heads, q, k, v, da, qt, kt, vt, cos_tab, sin_tab)
        block_out, grad_x, grad_wo, rows_wq, rows_wkv, sums = finish(
            n_dev, kv_heads, h_all, dy_all, wq_rows, wk_rows, wv_rows, w_out, a_own, g_own, a_head, dq_head, dqt, dkvt, at, x_own, dy_own, x_hat, inv_std, ln_gain.reshape(1, width)
        )
        grad_wq = jnp.swapaxes(rows_wq, 0, 1)
        grad_wk = jnp.swapaxes(rows_wkv[:, :, :head_dim], 0, 1)
        grad_wv = jnp.swapaxes(rows_wkv[:, :, head_dim:], 0, 1)
        n_lane = width // 128
        grad_gain, grad_bias = sums[:n_lane, 0].reshape(width), sums[:n_lane, 1].reshape(width)
        return (block_out.reshape(x_act.shape), grad_x.reshape(x_act.shape), grad_wq, grad_wk, grad_wv, grad_wo, grad_gain, grad_bias)

    return jax.shard_map(device_step, mesh=mesh, in_specs=(P("dp", AXIS, None), P("dp", AXIS, None), P("dp", AXIS), P(None), P(None), P(None, None, None), P(None, None, None), P(None, None, None), P(None, None)), out_specs=(P("dp", AXIS, None), P("dp", AXIS, None), P(("dp", AXIS), None, None), P(("dp", AXIS), None, None), P(("dp", AXIS), None, None), P(("dp", AXIS), None), P("dp"), P("dp")), check_vma=False)
```

```python
import functools
import math

import jax
import jax.numpy as jnp
from jax import lax
from jax.experimental import pallas as pl
from jax.experimental.pallas import tpu as pltpu
from jax.sharding import PartitionSpec as P

EPS = 1e-5
ROPE_BASE = 10000.0
BLOCK = 512
AXIS = "cp"
BF16, F32 = jnp.bfloat16, jnp.float32
VMEM_LIMIT = 60 * 1024 * 1024


def norm_forward(x_act, ln_gain, ln_bias):
    x_f32 = x_act.astype(F32)
    centered = x_f32 - jnp.mean(x_f32, axis=-1, keepdims=True)
    inv_std = lax.rsqrt(jnp.mean(centered * centered, axis=-1, keepdims=True) + EPS)
    x_hat = centered * inv_std
    return (x_hat * (1.0 + ln_gain) + ln_bias).astype(BF16), x_hat, inv_std


def frequencies(head_dim):
    quarter = head_dim // 4
    return jnp.exp(jnp.arange(quarter, dtype=F32) * (-2.0 * math.log(ROPE_BASE) / (head_dim // 2)))


def rotate(values, cos, sin):
    quarter = cos.shape[0]
    first, second = values[:quarter], values[quarter : 2 * quarter]
    return jnp.concatenate([first * cos - second * sin, second * cos + first * sin, values[2 * quarter :]], axis=0)


def rows_of(index, size):
    return pl.ds(pl.multiple_of(index * size, size), size)


def dot(lhs, rhs):
    return jnp.dot(lhs, rhs, preferred_element_type=F32)


def dot_t(lhs, rhs):
    return lax.dot_general(lhs, rhs, (((1,), (1,)), ((), ())), preferred_element_type=F32)


def full_barrier(n_dev):
    me = lax.axis_index(AXIS)
    barrier = pltpu.get_barrier_semaphore()

    def tell(step):
        pl.semaphore_signal(barrier, inc=1, device_id={AXIS: lax.rem(me + step, n_dev)}, device_id_type=pl.DeviceIdType.MESH)

    each(1, n_dev, tell)
    pl.semaphore_wait(barrier, n_dev - 1)


def remote(src, dst, send_sem, recv_sem, peer):
    return pltpu.make_async_remote_copy(src_ref=src, dst_ref=dst, send_sem=send_sem, recv_sem=recv_sem, device_id={AXIS: peer}, device_id_type=pl.DeviceIdType.MESH)


def each(lower, upper, body):
    def step(index, carry):
        body(index)
        return carry

    lax.fori_loop(lower, upper, step, 0)


class Exchange:
    def __init__(self, src, dst, send, recv):
        self.src, self.dst, self.send, self.recv = src, dst, send, recv

    def start(self, index, slot, peer):
        me = lax.axis_index(AXIS)
        src, dst, recv = self.src(index), self.dst(slot), self.recv(slot)

        @pl.when(peer != me)
        def _():
            remote(src, dst, self.send(index), recv, peer).start()

        @pl.when(peer == me)
        def _():
            pltpu.make_async_copy(src, dst, recv).start()

    def sent(self, index, peer):
        me = lax.axis_index(AXIS)

        @pl.when(peer != me)
        def _():
            remote(self.src(index), self.src(index), self.send(index), self.send(index), me).wait_send()

    def got(self, slot):
        dst = self.dst(slot)
        remote(dst, dst, self.recv(slot), self.recv(slot), lax.axis_index(AXIS)).wait_recv()


def ring_plan(side):
    first = [(True, s, 0) for s in range(side - 1)]
    second = sorted(((s, h) for s in range(side) for h in range(side - 1)), key=lambda p: (p[0] + p[1], p[1]))
    second = [(False, s, h) for s, h in second]
    sends = []
    while first or second:
        if first and len(sends) % 2 == 0:
            sends.append(first.pop(0))
        else:
            sends.append((second or first).pop(0))
    sent_at = {(s + 1, 0) if along else (s, h + 1): slot for slot, (along, s, h) in enumerate(sends)}
    used_at = {}
    for slot, (_, s, h) in enumerate(sends):
        used_at.setdefault((s, h), slot)
    waits = {piece: used_at.get(piece, slot + 2) for piece, slot in sent_at.items()}
    return sends, waits


def lookup(table, index):
    out = jnp.int32(table[0])
    for key, value in enumerate(table[1:], 1):
        out = jnp.where(index == key, jnp.int32(value), out)
    return out


class Ring:
    def __init__(self, n_dev, own, everything, ring_send, ring_recv, core_send, core_recv):
        self.own, self.all = own, everything
        self.ring_send, self.ring_recv, self.core_send, self.core_recv = ring_send, ring_recv, core_send, core_recv
        self.side = math.isqrt(n_dev // 2)
        self.tokens = own.shape[0]
        self.rows = self.tokens // 4
        me = lax.axis_index(AXIS)
        self.core = lax.rem(me, 2)
        self.x, self.y = lax.rem(me // 2, self.side), me // (2 * self.side)
        self.sends, waits = ring_plan(self.side)
        self.n_send = len(self.sends)
        by_slot = {}
        for piece, slot in sorted(waits.items(), key=lambda item: (item[1], item[0])):
            while len(by_slot.setdefault(slot, [])) == 2:
                slot += 1
            by_slot[slot].append(piece)
        self.by_slot = by_slot
        self.n_slot = max(by_slot) + 1
        self.order = [(0, (0, 0))] + [(slot, piece) for slot in range(self.n_slot) for piece in by_slot.get(slot, [])]

    def device(self, colour, along, across, core):
        side = self.side
        x_first = 1 - colour // 2
        sign = 1 - 2 * lax.rem(colour, 2)
        dx = x_first * along + (1 - x_first) * across
        dy = x_first * across + (1 - x_first) * along
        x = lax.rem(self.x - sign * dx + 2 * side, side)
        y = lax.rem(self.y - sign * dy + 2 * side, side)
        return (y * side + x) * 2 + core

    def place(self, colour, s, h, core):
        return pl.ds(pl.multiple_of(self.device(colour, s, h, core) * self.tokens + colour * self.rows, self.rows), self.rows)

    def piece(self, colour, s, h):
        return self.all.at[self.place(colour, s, h, self.core)]

    def ring_copy(self, colour, s, h, along):
        number = (s + along) * self.side + h + 1 - along
        peer = self.device(colour, -along, along - 1, self.core)
        src = self.piece(colour, s, h)
        return remote(src, src, self.ring_send.at[colour, number], self.ring_recv.at[colour, number], peer)

    def arrival(self, colour, s, h):
        number = s * self.side + h
        dst = self.piece(colour, s, h)
        return remote(dst, dst, self.ring_send.at[colour, number], self.ring_recv.at[colour, number], lax.axis_index(AXIS))

    def core_copy(self, colour, s, h):
        number = s * self.side + h
        src = self.piece(colour, s, h)
        me = lax.axis_index(AXIS)
        return remote(src, src, self.core_send.at[colour, number], self.core_recv.at[colour, number], me + 1 - 2 * self.core)

    def core_arrival(self, colour, s, h):
        number = s * self.side + h
        dst = self.all.at[self.place(colour, s, h, 1 - self.core)]
        return remote(dst, dst, self.core_send.at[colour, number], self.core_recv.at[colour, number], lax.axis_index(AXIS))

    def begin(self):
        each(0, 4, lambda colour: self.core_copy(colour, 0, 0).start())

    def step(self, slot):
        for turn in range(2):
            known = [self.by_slot.get(k, [])[turn] if len(self.by_slot.get(k, [])) > turn else None for k in range(self.n_slot)]
            due = lookup([int(p is not None) for p in known], slot)
            s, h = lookup([p[0] if p else 0 for p in known], slot), lookup([p[1] if p else 0 for p in known], slot)

            @pl.when((due == 1) & (slot < self.n_slot))
            def _():
                def one(colour):
                    self.arrival(colour, s, h).wait_recv()
                    self.core_copy(colour, s, h).start()

                each(0, 4, one)

        along, s, h = (lookup([int(send[k]) for send in self.sends], slot) for k in range(3))

        @pl.when(slot < self.n_send)
        def _():
            each(0, 4, lambda colour: self.ring_copy(colour, s, h, along).start())

    def end(self):
        def sent(slot):
            along, s, h = (lookup([int(send[k]) for send in self.sends], slot) for k in range(3))
            each(0, 4, lambda colour: self.ring_copy(colour, s, h, along).wait_send())

        each(0, self.n_send, sent)

        def core_sent(number):
            each(0, 4, lambda colour: self.core_copy(colour, number // self.side, lax.rem(number, self.side)).wait_send())

        each(0, self.side * self.side, core_sent)


def front_kernel(
    n_dev, n_group, h_ref, dy_ref, pos_ref, freq_ref, wo_ref, wq_ref, wk_ref, wv_ref,
    h_out, q_ref, k_ref, v_ref, cos_ref, sin_ref, da_ref,
    h_all, w_ref, pick_ref, w_buf, wo_buf, da_buf, pos_in,
    ring_send, ring_recv, core_send, core_recv, w_sem, wo_sem, send, recv, pos_send, pos_recv, local,
):
    me = lax.axis_index(AXIS)
    tokens, width = h_ref.shape
    head_dim = v_ref.shape[1]
    heads_tile = w_buf.shape[2]
    d_block = w_buf.shape[1]
    span = wo_buf.shape[1]
    n_wo = wo_ref.shape[0] // span
    per_wo = span // head_dim
    ring = Ring(n_dev, h_ref, h_all, ring_send, ring_recv, core_send, core_recv)
    piece = Exchange(lambda peer: da_buf.at[peer], lambda origin: da_ref.at[rows_of(origin, tokens)], lambda peer: send.at[peer], lambda origin: recv.at[origin])
    where = Exchange(lambda peer: pos_ref, lambda origin: pos_in.at[origin], lambda peer: pos_send.at[peer], lambda origin: pos_recv.at[origin])

    own_rows = pltpu.make_async_copy(h_ref, h_all.at[rows_of(me, tokens)], local.at[0])
    own_rows.start()

    n_d = width // d_block
    kv_head = me // n_group
    n_load = 3 * n_d

    def w_load(t, which):
        rows = rows_of(t, d_block)
        if which == 0:
            return pltpu.make_async_copy(wq_ref.at[rows, rows_of(me // heads_tile, heads_tile)], w_buf.at[lax.rem(t, 2)], w_sem.at[lax.rem(t, 2)])
        ref = (wk_ref, wv_ref)[which - 1]
        return pltpu.make_async_copy(ref.at[rows, rows_of(kv_head // heads_tile, heads_tile)], w_buf.at[lax.rem(t, 2)], w_sem.at[lax.rem(t, 2)])

    def wo_turn(t):
        return lax.rem(t + me // per_wo, n_wo)

    def wo_load(t):
        slot = lax.rem(t, 2)
        return pltpu.make_async_copy(wo_ref.at[rows_of(wo_turn(t), span)], wo_buf.at[slot], wo_sem.at[slot])

    w_load(0, 0).start()
    wo_load(0).start()
    wo_load(1).start()
    own_rows.wait()
    full_barrier(n_dev)

    def send_pos(step):
        peer = lax.rem(me + step, n_dev)
        where.start(peer, me, peer)

    ring.begin()
    ring.step(jnp.int32(0))
    ring.step(jnp.int32(1))
    each(0, n_dev, send_pos)

    for which in range(3):
        head = me if which == 0 else kv_head

        def pick(t):
            @pl.when(t + 1 < n_d)
            def _():
                w_load(t + 1, which).start()

            w_load(t, which).wait()
            pick_ref[...] = jnp.swapaxes(w_buf[lax.rem(t, 2)], 0, 1)
            w_ref[rows_of(t, d_block), which * head_dim : (which + 1) * head_dim] = pick_ref[lax.rem(head, heads_tile)]

        each(0, n_d, pick)
        if which < 2:
            w_load(0, which + 1).start()

    def send_da(t):
        def one(u):
            peer = wo_turn(t) * per_wo + lax.rem(u + me, per_wo)
            piece.start(peer, me, peer)

        each(0, per_wo, one)

    def make_da(t):
        @pl.when((t > 0) & (t <= n_wo))
        def _():
            send_da(t - 1)

        @pl.when(t < n_wo)
        def _():
            wo_load(t).wait()
            da = dot_t(dy_ref[...], wo_buf[lax.rem(t, 2)]).astype(BF16)
            for u in range(per_wo):
                da_buf[wo_turn(t) * per_wo + u] = da[:, u * head_dim : (u + 1) * head_dim]

            @pl.when(t + 2 < n_wo)
            def _():
                wo_load(t + 2).start()

    def tables(origin):
        where.got(origin)
        angles = freq_ref[...] * pos_in[origin, 0:1, :].astype(F32)
        cos_ref[:, rows_of(origin, tokens)] = jnp.cos(angles)
        sin_ref[:, rows_of(origin, tokens)] = jnp.sin(angles)

    ready = []
    for slot, found in ring.order:
        ready.append((max(slot + 1, ready[-1][0] + 1 if ready else 1), found))
    use = dict(ready)
    n_step = max(use) + 1
    rows_n = ring.rows

    def keep(place):
        return pltpu.make_async_copy(h_all.at[place], h_out.at[place], local.at[1])

    def project(s, h):
        def arrived(colour):
            ring.core_arrival(colour, s, h).wait_recv()

        each(0, 4, arrived)
        places = [ring.place(jnp.int32(colour), s, h, core) for colour in range(4) for core in range(2)]
        for place in places:
            keep(place).start()
        out = dot(jnp.concatenate([h_all[place, :] for place in places], axis=0), w_ref[...])
        for n, place in enumerate(places):
            part = out[n * rows_n : (n + 1) * rows_n]
            q_ref[place, :] = part[:, :head_dim]
            k_ref[place, :] = part[:, head_dim : 2 * head_dim]
            v_ref[place, :] = part[:, 2 * head_dim :].astype(BF16)

    def step(slot):
        @pl.when(slot >= 2)
        def _():
            ring.step(slot)

        make_da(slot - 1)
        s = lookup([use.get(k, (0, 0))[0] for k in range(n_step)], slot)
        h = lookup([use.get(k, (0, 0))[1] for k in range(n_step)], slot)
        due = lookup([int(k in use) for k in range(n_step)], slot)

        @pl.when(due == 1)
        def _():
            project(s, h)

        @pl.when(slot == 2)
        def _():
            each(0, n_dev, tables)

    each(1, max(n_step, n_wo + 3), step)
    ring.end()
    pltpu.make_async_copy(h_all, h_out, local.at[1]).wait()

    def drain(index):
        where.sent(index, index)
        piece.sent(index, index)
        piece.got(index)

    each(0, n_dev, drain)


def front(n_dev, n_group, h_own, dy_own, positions, freq, w_out, w_query, w_key, w_value):
    tokens, width = h_own.shape
    head_dim = w_query.shape[2]
    seq = tokens * n_dev
    heads_tile = min(8, w_key.shape[1])
    d_block = 384
    span = min(BLOCK, w_out.shape[0] // 2)
    side = math.isqrt(n_dev // 2)
    whole, anywhere = pl.BlockSpec(memory_space=pltpu.VMEM), pl.BlockSpec(memory_space=pl.ANY)
    dma = pltpu.SemaphoreType.DMA
    return pl.pallas_call(
        functools.partial(front_kernel, n_dev, n_group),
        out_shape=[
            jax.ShapeDtypeStruct((seq, width), BF16),
            jax.ShapeDtypeStruct((seq, head_dim), F32),
            jax.ShapeDtypeStruct((seq, head_dim), F32),
            jax.ShapeDtypeStruct((seq, head_dim), BF16),
            jax.ShapeDtypeStruct((head_dim // 4, seq), F32),
            jax.ShapeDtypeStruct((head_dim // 4, seq), F32),
            jax.ShapeDtypeStruct((seq, head_dim), BF16),
        ],
        in_specs=[whole] * 4 + [anywhere] * 4,
        out_specs=[anywhere] + [whole] * 5 + [anywhere],
        scratch_shapes=[
            pltpu.VMEM((seq, width), BF16),
            pltpu.VMEM((width, 3 * head_dim), BF16),
            pltpu.VMEM((heads_tile, d_block, head_dim), BF16),
            pltpu.VMEM((2, d_block, heads_tile, head_dim), BF16),
            pltpu.VMEM((2, span, width), BF16),
            pltpu.VMEM((n_dev, tokens, head_dim), BF16),
            pltpu.VMEM((n_dev,) + positions.shape, jnp.int32),
            dma((4, side * side)), dma((4, side * side)), dma((4, side * side)), dma((4, side * side)),
            dma((2,)), dma((2,)), dma((n_dev,)), dma((n_dev,)), dma((n_dev,)), dma((n_dev,)), dma((2,)),
        ],
        compiler_params=pltpu.CompilerParams(collective_id=3, has_side_effects=True, vmem_limit_bytes=VMEM_LIMIT),
        cost_estimate=pl.CostEstimate(flops=6 * seq * width * head_dim, bytes_accessed=4 * width * w_out.shape[0], transcendentals=0),
        name="front",
    )(h_own, dy_own, positions, freq, w_out, w_query, w_key, w_value)


def causal(block):
    key = lax.broadcasted_iota(jnp.int32, (block, block), 0)
    query = lax.broadcasted_iota(jnp.int32, (block, block), 1)
    return key <= query


def part_sum(values):
    return jnp.sum(values.reshape(values.shape[0] // 8, 8, values.shape[1]), axis=0)


def attention_kernel(
    n_dev, n_group, q_heads, kv_heads, scale,
    q_raw, k_raw, v_ref, da_ref, cos_ref, sin_ref,
    at_ref, dqt_ref, a_ref, dq_ref, dkvt_ref, a_out, grad_out,
    q_ref, k_ref, qt_ref, kt_ref, vt_ref, dkv_ref, e_ref, dp_ref, peak_ref, dat_ref, mix_ref, acc_ref, land_one, land_two, kv_ref, kvt_ref,
    a_send, a_recv, q_send, q_recv, one_send, one_recv, two_send, two_recv, kv_send, kv_recv, near_send, near_recv, far_send, far_recv, fwd_send, fwd_recv, local,
):
    me = lax.axis_index(AXIS)
    seq, head_dim = v_ref.shape
    block = e_ref.shape[1]
    n_block = seq // block
    tokens = seq // n_dev
    half = block // 2
    fold = scale * math.log2(math.e)
    core, side = lax.rem(me, 2), lax.rem(me // 2, 2)
    group = me // n_group
    partner, across = me + 1 - 2 * core, me + 2 - 4 * side
    place, place_across = core * 2 + side, core * 2 + 1 - side
    place_partner, place_last = (1 - core) * 2 + side, (1 - core) * 2 + 1 - side

    def piece(index):
        return rows_of(index, tokens)

    def column(head):
        return rows_of(head, head_dim)

    a_copy = Exchange(lambda peer: a_ref.at[piece(peer)], lambda head: a_out.at[:, column(head)], lambda peer: a_send.at[peer], lambda head: a_recv.at[head])
    q_copy = Exchange(lambda peer: dq_ref.at[piece(peer)], lambda head: grad_out.at[:, column(head)], lambda peer: q_send.at[peer], lambda head: q_recv.at[head])
    kv_copy = [
        Exchange(
            lambda i, w=w: kv_ref.at[i, w],
            lambda head, w=w: grad_out.at[:, column(q_heads + w * kv_heads + head)],
            lambda i, w=w: kv_send.at[w, i],
            lambda head, w=w: kv_recv.at[w, head],
        )
        for w in range(2)
    ]

    def one_copy(i):
        return remote(dkv_ref.at[rows_of(i * 2 + 1 - core, half)], land_one.at[i], one_send.at[i], one_recv.at[i], partner)

    def two_copy(i):
        return remote(dkv_ref.at[piece(i * n_group + core * 2 + 1 - side)], land_two.at[i], two_send.at[i], two_recv.at[i], across)

    def near_copy(i, where):
        return remote(kvt_ref.at[i], dkvt_ref.at[:, piece(i * n_group + where)], near_send.at[i], near_recv.at[i], partner)

    def far_copy(i, where):
        return remote(kvt_ref.at[i], dkvt_ref.at[:, piece(i * n_group + where)], far_send.at[i], far_recv.at[i], across)

    def fwd_copy(i, where):
        view = dkvt_ref.at[:, piece(i * n_group + where)]
        return remote(view, view, fwd_send.at[i], fwd_recv.at[i], partner)

    def own_copy(i):
        return pltpu.make_async_copy(kvt_ref.at[i], dkvt_ref.at[:, piece(i * n_group + place)], local.at[i])

    def first(i):
        def send(u):
            peer = i * n_group + lax.rem(u + me, n_group)
            a_copy.start(peer, me, peer)
            q_copy.start(peer, me, peer)

        one_copy(i).start()

        @pl.when(i >= n_block // 2)
        def _():
            each(0, n_group, send)

    def second(i):
        one_copy(i).wait_recv()
        for part in (1 - side, side):
            rows = piece(i * n_group + core * 2 + part)
            dkv_ref[rows, :] += land_one[i, pl.ds(pl.multiple_of(part * tokens, tokens), tokens), :]
        two_copy(i).start()

    def close(i):
        two_copy(i).wait_recv()
        rows = piece(i * n_group + place)
        total = dkv_ref[rows, :] + land_two[i]
        dkt = rotate(total[:, :head_dim].T, cos_ref[:, rows], -sin_ref[:, rows]).astype(BF16)
        dv = total[:, head_dim:].astype(BF16)
        kvt_ref[i, :head_dim, :], kvt_ref[i, head_dim:, :] = dkt, dv.T
        kv_ref[i, 0], kv_ref[i, 1] = dkt.T, dv

    def spread(i):
        near_copy(i, place).start()
        far_copy(i, place).start()
        own_copy(i).start()
        for copy in kv_copy:
            copy.start(i, group, i * n_group + place)

    def forward(i):
        far_copy(i, place_across).wait_recv()
        fwd_copy(i, place_across).start()

    def stages(t):
        for late, stage in ((5, forward), (4, spread), (3, close), (2, second), (1, first)):
            @pl.when((t >= late) & (t < n_block + late))
            def _():
                stage(n_block - 1 - (t - late))

    full_barrier(n_dev)

    def prepare(i):
        rows = rows_of(i, block)
        for raw, turned, plain in ((q_raw, qt_ref, q_ref), (k_raw, kt_ref, k_ref)):
            t = rotate(raw[rows, :].T, cos_ref[:, rows], sin_ref[:, rows]).astype(BF16)
            turned[:, rows] = t
            plain[rows, :] = t.T
        vt_ref[:, rows] = v_ref[rows, :].T
        dkv_ref[rows, :] = jnp.zeros((block, 2 * head_dim), F32)

    each(0, n_block, prepare)

    def compute(i):
        own = rows_of(i, block)
        dat_ref[...] = da_ref[own, :].T
        mix_ref[...] = jnp.zeros_like(mix_ref)
        acc_ref[...] = jnp.zeros_like(acc_ref)

        def scores(j, carry, diagonal):
            peak, total, mixed = carry
            rows = rows_of(j, block)
            s = dot(k_ref[rows, :], qt_ref[:, own])
            if diagonal:
                s = jnp.where(causal(block), s, -1e30)
            top = jnp.maximum(peak, jnp.max(s, axis=0, keepdims=True))
            e = jnp.exp2((s - top) * fold)
            dp = dot(v_ref[rows, :], dat_ref[...])
            fade = jnp.exp2((peak - top) * fold)
            e_ref[rows, :] = e
            dp_ref[rows, :] = dp
            peak_ref[j] = top
            return top, total * fade + part_sum(e), mixed * fade + part_sum(e * dp)

        start = (jnp.full((1, block), -jnp.inf, F32), jnp.zeros((8, block), F32), jnp.zeros((8, block), F32))
        carry = lax.fori_loop(0, i, functools.partial(scores, diagonal=False), start)
        peak, total, mixed = scores(i, carry, True)
        inv = 1.0 / jnp.sum(total, axis=0, keepdims=True)
        row_dot = jnp.sum(mixed, axis=0, keepdims=True) * inv
        q_own, da_own = q_ref[own, :], da_ref[own, :]

        def grads(j):
            rows = rows_of(j, block)
            p = e_ref[rows, :] * (jnp.exp2((peak_ref[j] - peak) * fold) * inv)
            pb = p.astype(BF16)
            ds = ((dp_ref[rows, :] - row_dot) * (p * scale)).astype(BF16)
            dkv_ref[rows, :head_dim] += dot(ds, q_own)
            dkv_ref[rows, head_dim:] += dot(pb, da_own)
            mix_ref[...] += dot(vt_ref[:, rows], pb)
            acc_ref[...] += dot(kt_ref[:, rows], ds)

        each(0, i + 1, grads)
        at = mix_ref[...].astype(BF16)
        at_ref[:, own] = at
        a_ref[own, :] = at.T
        dqt = rotate(acc_ref[...], cos_ref[:, own], -sin_ref[:, own]).astype(BF16)
        dqt_ref[:, own] = dqt
        dq_ref[own, :] = dqt.T

    def iteration(t):
        stages(t)

        @pl.when(t < n_block)
        def _():
            compute(n_block - 1 - t)

    each(0, n_block + 5, iteration)

    def drain(i):
        one_copy(i).wait_send()
        two_copy(i).wait_send()
        near_copy(i, place).wait_send()
        near_copy(i, place_partner).wait_recv()
        far_copy(i, place).wait_send()
        fwd_copy(i, place_across).wait_send()
        fwd_copy(i, place_last).wait_recv()
        own_copy(i).wait()
        for copy in kv_copy:
            copy.sent(i, i * n_group + place)

    each(0, n_block, drain)

    def drain_sent(peer):
        for copy in (a_copy, q_copy):
            copy.sent(peer, peer)

    def drain_got(head):
        for copy in (a_copy, q_copy):
            copy.got(head)

    low = n_block // 2 * n_group
    each(low, n_dev, drain_sent)

    @pl.when(me >= low)
    def _():
        each(0, n_dev, drain_got)

    def drain_kv(head):
        for copy in kv_copy:
            copy.got(head)

    each(0, kv_heads, drain_kv)


def attention(n_dev, kv_heads, q, k, v, da, cos_tab, sin_tab):
    seq, head_dim = q.shape
    q_heads = n_dev
    n_group = q_heads // kv_heads
    tokens = seq // n_dev
    block = tokens * n_group
    n_block = seq // block
    whole, anywhere = pl.BlockSpec(memory_space=pltpu.VMEM), pl.BlockSpec(memory_space=pl.ANY)
    dma = pltpu.SemaphoreType.DMA
    return pl.pallas_call(
        functools.partial(attention_kernel, n_dev, n_group, q_heads, kv_heads, head_dim**-0.5),
        out_shape=[
            jax.ShapeDtypeStruct((head_dim, seq), BF16),
            jax.ShapeDtypeStruct((head_dim, seq), BF16),
            jax.ShapeDtypeStruct((seq, head_dim), BF16),
            jax.ShapeDtypeStruct((seq, head_dim), BF16),
            jax.ShapeDtypeStruct((2 * head_dim, seq), BF16),
            jax.ShapeDtypeStruct((tokens, q_heads * head_dim), BF16),
            jax.ShapeDtypeStruct((tokens, (q_heads + 2 * kv_heads) * head_dim), BF16),
        ],
        in_specs=[whole] * 6,
        out_specs=[whole] * 4 + [anywhere] * 3,
        scratch_shapes=[
            pltpu.VMEM((seq, head_dim), BF16),
            pltpu.VMEM((seq, head_dim), BF16),
            pltpu.VMEM((head_dim, seq), BF16),
            pltpu.VMEM((head_dim, seq), BF16),
            pltpu.VMEM((head_dim, seq), BF16),
            pltpu.VMEM((seq, 2 * head_dim), F32),
            pltpu.VMEM((seq, block), F32),
            pltpu.VMEM((seq, block), F32),
            pltpu.VMEM((n_block, 1, block), F32),
            pltpu.VMEM((head_dim, block), BF16),
            pltpu.VMEM((head_dim, block), F32),
            pltpu.VMEM((head_dim, block), F32),
            pltpu.VMEM((n_block, block // 2, 2 * head_dim), F32),
            pltpu.VMEM((n_block, tokens, 2 * head_dim), F32),
            pltpu.VMEM((n_block, 2, tokens, head_dim), BF16),
            pltpu.VMEM((n_block, 2 * head_dim, tokens), BF16),
            dma((n_dev,)), dma((n_dev,)), dma((n_dev,)), dma((n_dev,)),
            dma((n_block,)), dma((n_block,)), dma((n_block,)), dma((n_block,)), dma((2, n_block)), dma((2, kv_heads)),
            dma((n_block,)), dma((n_block,)), dma((n_block,)), dma((n_block,)), dma((n_block,)), dma((n_block,)), dma((n_block,)),
        ],
        compiler_params=pltpu.CompilerParams(collective_id=1, has_side_effects=True, vmem_limit_bytes=VMEM_LIMIT),
        cost_estimate=pl.CostEstimate(flops=6 * seq * seq * head_dim, bytes_accessed=18 * seq * head_dim, transcendentals=seq * seq // 2),
        name="attention",
    )(q, k, v, da, cos_tab, sin_tab)


def finish_kernel(
    n_dev, n_group, n_buf,
    h_ref, dy_ref, wq_ref, wk_ref, wv_ref, wo_ref, a_in, g_in, a_head, dq_head, dqt_ref, dkvt_ref, at_ref, x_ref, dy_own_ref, x_hat_ref, inv_ref, gain_ref,
    out_ref, gx_ref, gwo_ref, q_rows, kv_rows, sum_ref,
    a_ref, g_ref, buf, wq_buf, wk_buf, wv_buf, wq_out, wkv_out, dh_ref, part_ref, own_sum, sum_in, sum_mine,
    load_sem, q_send, q_recv, kv_send, kv_recv, s_send, s_recv, t_send, t_recv, a_send, a_recv, dq_send, dq_recv, local,
):
    me = lax.axis_index(AXIS)
    seq, width = h_ref.shape
    span = buf.shape[2]
    head_dim = dqt_ref.shape[0]
    depth = width // n_dev
    n_col = width // span
    per_col = span // depth
    member, group = lax.rem(me, n_group), me // n_group
    col_member = n_col // n_group
    per_member = n_dev // n_group
    n_sum = sum_mine.shape[0]
    q_rows_n = a_ref.shape[1]
    kv_rows_n = (g_ref.shape[1] - q_rows_n) // 2

    tokens = x_ref.shape[0]
    low = n_dev // n_group // 2 * n_group

    def cols(j):
        return rows_of(j, span)

    def turn(phase, j):
        return lax.rem(j + me // per_col, n_col) if phase == 0 else j

    def loads(phase, j, slot):
        if phase == 2:
            pairs = ((wq_ref, wq_buf), (wk_ref, wk_buf), (wv_ref, wv_buf))
            return [pltpu.make_async_copy(ref.at[cols(j)], to.at[slot], load_sem.at[slot, n]) for n, (ref, to) in enumerate(pairs)]
        ref = (h_ref, dy_ref, None, wo_ref)[phase]
        return [pltpu.make_async_copy(ref.at[:, cols(turn(phase, j))], buf.at[slot], load_sem.at[slot, 0])]

    def load(step):
        slot = lax.rem(step, n_buf)
        for phase in range(4):
            @pl.when((step >= phase * n_col) & (step < (phase + 1) * n_col))
            def _():
                for copy in loads(phase, step - phase * n_col, slot):
                    copy.start()

    q_copy = Exchange(lambda peer: wq_out.at[rows_of(peer, depth)], lambda head: q_rows.at[head], lambda peer: q_send.at[peer], lambda head: q_recv.at[head])
    kv_copy = Exchange(lambda i: wkv_out.at[rows_of(i, depth)], lambda head: kv_rows.at[head], lambda i: kv_send.at[i], lambda head: kv_recv.at[head])
    s_copy = Exchange(lambda peer: own_sum.at[pl.ds(peer * n_sum, n_sum)], lambda origin: sum_in.at[origin], lambda peer: s_send.at[peer], lambda origin: s_recv.at[origin])
    t_copy = Exchange(lambda peer: sum_mine, lambda origin: sum_ref.at[pl.ds(origin * n_sum, n_sum)], lambda peer: t_send.at[peer], lambda origin: t_recv.at[origin])

    def column(head):
        return rows_of(head, head_dim)

    a_copy = Exchange(lambda peer: a_head.at[rows_of(peer, tokens)], lambda head: a_ref.at[:, column(head)], lambda peer: a_send.at[peer], lambda head: a_recv.at[head])
    dq_copy = Exchange(lambda peer: dq_head.at[rows_of(peer, tokens)], lambda head: g_ref.at[:, column(head)], lambda peer: dq_send.at[peer], lambda head: dq_recv.at[head])

    def send_heads(step):
        peer = lax.rem(me + step, low)
        a_copy.start(peer, me, peer)
        dq_copy.start(peer, me, peer)

    own_kv = pltpu.make_async_copy(g_in.at[:, pl.ds(q_rows_n, 2 * kv_rows_n)], g_ref.at[:, pl.ds(q_rows_n, 2 * kv_rows_n)], local.at[0])
    own_a = pltpu.make_async_copy(a_in, a_ref, local.at[1])
    own_dq = pltpu.make_async_copy(g_in.at[:, pl.ds(0, q_rows_n)], g_ref.at[:, pl.ds(0, q_rows_n)], local.at[2])

    def send_q(j):
        def send(u):
            peer = turn(0, j) * per_col + lax.rem(u + me, per_col)
            q_copy.start(peer, me, peer)

        each(0, per_col, send)

    def run(phase, body):
        def step(j):
            number = phase * n_col + j
            slot = lax.rem(number, n_buf)
            for copy in loads(phase, j, slot):
                copy.wait()
            body(j, slot)
            load(number + n_buf)

        each(0, n_col, step)

    each(0, n_buf, load)
    own_kv.start()

    @pl.when(me >= low)
    def _():
        own_a.start()
        own_dq.start()

    full_barrier(n_dev)
    each(0, low, send_heads)

    def weight_columns(j, slot):
        @pl.when(j > 0)
        def _():
            send_q(j - 1)

        col = turn(0, j)
        wq_out[cols(col), :] = dot(dqt_ref[...], buf[slot]).T

        @pl.when(col // col_member == member)
        def _():
            wkv_out[cols(col - member * col_member), :] = dot(dkvt_ref[...], buf[slot]).T

    run(0, weight_columns)

    def send_kv(step):
        index = lax.rem(step + group, per_member)
        kv_copy.start(index, group, member * per_member + index)

    def weight_out(j, slot):
        gwo_ref[:, cols(j)] = dot(at_ref[...], buf[slot])

        @pl.when(j == 0)
        def _():
            send_q(n_col - 1)
            each(0, per_member, send_kv)

    run(1, weight_out)
    own_kv.wait()

    @pl.when(me >= low)
    def _():
        own_a.wait()
        own_dq.wait()

    def got_heads(head):
        a_copy.got(head)
        dq_copy.got(head)

    @pl.when(me < low)
    def _():
        each(0, n_dev, got_heads)

    def back(j, slot):
        def flat(ref):
            block = ref[slot]
            return block.reshape(block.shape[0], block.shape[1] * block.shape[2])

        grad_h = dot_t(g_ref[:, :q_rows_n], flat(wq_buf))
        grad_h += dot_t(g_ref[:, q_rows_n : q_rows_n + kv_rows_n], flat(wk_buf))
        dh_ref[:, cols(j)] = grad_h + dot_t(g_ref[:, q_rows_n + kv_rows_n :], flat(wv_buf))

    run(2, back)

    part_ref[...] = jnp.zeros_like(part_ref)
    gain = 1.0 + gain_ref[...]

    def norm(t):
        rows = rows_of(t, 16)
        grad_h, x_hat = dh_ref[rows, :], x_hat_ref[rows, :]
        grad_hat = grad_h * gain
        one = jnp.sum(grad_hat, axis=1, keepdims=True) * (1.0 / width)
        two = jnp.sum(grad_hat * x_hat, axis=1, keepdims=True) * (1.0 / width)
        back = inv_ref[rows, :] * (grad_hat - one - x_hat * two)
        gx_ref[rows, :] = (dy_own_ref[rows, :].astype(F32) + back).astype(BF16)
        part_ref[0] += part_sum(grad_h * x_hat)
        part_ref[1] += part_sum(grad_h)

    each(0, dh_ref.shape[0] // 16, norm)
    own_sum[...] = jnp.zeros_like(own_sum)
    for which in range(2):
        total = jnp.sum(part_ref[which], axis=0, keepdims=True)
        for c in range(width // 128):
            own_sum[c, pl.ds(which, 1), :] = total[:, c * 128 : (c + 1) * 128]

    def to_all(copy):
        def send(step):
            peer = lax.rem(me + step, n_dev)
            copy.start(peer, me, peer)

        each(0, n_dev, send)

    def add(origin):
        sum_mine[...] += sum_in[origin]

    def output(j, slot):
        @pl.when(j == 0)
        def _():
            to_all(s_copy)

        @pl.when(j == n_col // 2)
        def _():
            each(0, n_dev, s_copy.got)
            sum_mine[...] = jnp.zeros_like(sum_mine)
            each(0, n_dev, add)

        out_ref[:, cols(j)] = (x_ref[:, cols(j)].astype(F32) + dot(a_ref[...], buf[slot])).astype(BF16)

        @pl.when(j == n_col // 2)
        def _():
            to_all(t_copy)

    run(3, output)

    def drain(index):
        s_copy.sent(index, index)
        t_copy.sent(index, index)
        t_copy.got(index)
        q_copy.sent(index, index)
        q_copy.got(index)

    def drain_kv(index):
        kv_copy.sent(index, member * per_member + index)

    def drain_heads(peer):
        a_copy.sent(peer, peer)
        dq_copy.sent(peer, peer)

    each(0, n_dev, drain)
    each(0, low, drain_heads)
    each(0, per_member, drain_kv)
    each(0, kv_rows.shape[0], kv_copy.got)


def finish(n_dev, kv_heads, h_all, dy_all, wq, wk, wv, wo, a_in, g_in, a_head, dq_head, dqt, dkvt, at, x_own, dy_own, x_hat, inv_std, gain):
    seq, width = h_all.shape
    tokens = seq // n_dev
    head_dim = dqt.shape[0]
    q_heads = n_dev
    n_group = q_heads // kv_heads
    depth = width // n_dev
    span = math.lcm(depth, 128)
    n_buf = 3
    n_sum = -(-width // (128 * n_dev))
    sums = (n_sum * n_dev, 8, 128)
    whole, anywhere = pl.BlockSpec(memory_space=pltpu.VMEM), pl.BlockSpec(memory_space=pl.ANY)
    dma = pltpu.SemaphoreType.DMA
    return pl.pallas_call(
        functools.partial(finish_kernel, n_dev, n_group, n_buf),
        out_shape=[
            jax.ShapeDtypeStruct((tokens, width), BF16),
            jax.ShapeDtypeStruct((tokens, width), BF16),
            jax.ShapeDtypeStruct((head_dim, width), F32),
            jax.ShapeDtypeStruct((q_heads, depth, head_dim), F32),
            jax.ShapeDtypeStruct((kv_heads, depth, 2 * head_dim), F32),
            jax.ShapeDtypeStruct(sums, F32),
        ],
        in_specs=[anywhere] * 10 + [whole] * 8,
        out_specs=[whole] * 3 + [anywhere] * 2 + [whole],
        scratch_shapes=[
            pltpu.VMEM(a_in.shape, BF16),
            pltpu.VMEM(g_in.shape, BF16),
            pltpu.VMEM((n_buf, seq, span), BF16),
            pltpu.VMEM((n_buf, span) + wq.shape[1:], BF16),
            pltpu.VMEM((n_buf, span) + wk.shape[1:], BF16),
            pltpu.VMEM((n_buf, span) + wv.shape[1:], BF16),
            pltpu.VMEM((width, head_dim), F32),
            pltpu.VMEM((width // n_group, 2 * head_dim), F32),
            pltpu.VMEM((tokens, width), F32),
            pltpu.VMEM((2, 8, width), F32),
            pltpu.VMEM(sums, F32),
            pltpu.VMEM((n_dev, n_sum, 8, 128), F32),
            pltpu.VMEM((n_sum, 8, 128), F32),
            dma((n_buf, 3)), dma((n_dev,)), dma((n_dev,)), dma((n_dev // n_group,)), dma((kv_heads,)), dma((n_dev,)), dma((n_dev,)), dma((n_dev,)), dma((n_dev,)),
            dma((n_dev,)), dma((n_dev,)), dma((n_dev,)), dma((n_dev,)), dma((3,)),
        ],
        compiler_params=pltpu.CompilerParams(collective_id=2, has_side_effects=True, vmem_limit_bytes=VMEM_LIMIT),
        cost_estimate=pl.CostEstimate(flops=8 * seq * width * head_dim, bytes_accessed=8 * seq * width, transcendentals=0),
        name="finish",
    )(h_all, dy_all, wq, wk, wv, wo, a_in, g_in, a_head, dq_head, dqt, dkvt, at, x_own, dy_own, x_hat, inv_std, gain)


def solution(mesh):
    n_dev = mesh.shape[AXIS]

    def device_step(x_act, d_out, positions, ln_gain, ln_bias, w_query, w_key, w_value, w_out):
        n_batch, piece, width = x_act.shape
        q_heads, head_dim = w_query.shape[1:]
        kv_heads = w_key.shape[1]
        n_group = q_heads // kv_heads
        tokens = n_batch * piece

        x_own, dy_own = x_act.reshape(tokens, width), d_out.reshape(tokens, width)
        normed, x_hat, inv_std = norm_forward(x_own, ln_gain, ln_bias)
        pos_tile = jnp.broadcast_to(positions.reshape(1, tokens), (8, tokens))
        freq = jnp.broadcast_to(frequencies(head_dim)[:, None], (head_dim // 4, tokens))
        h_all, q, k, v, cos_tab, sin_tab, da = front(n_dev, n_group, normed, dy_own, pos_tile, freq, w_out, w_query, w_key, w_value)
        dy_all = lax.all_gather(lax.optimization_barrier((dy_own, v))[0], AXIS, axis=0, tiled=True)
        at, dqt, a_head, dq_head, dkvt, a_own, g_own = attention(n_dev, kv_heads, q, k, v, da, cos_tab, sin_tab)
        block_out, grad_x, grad_wo, rows_wq, rows_wkv, sums = finish(
            n_dev, kv_heads, h_all, dy_all, w_query, w_key, w_value, w_out, a_own, g_own, a_head, dq_head, dqt, dkvt, at, x_own, dy_own, x_hat, inv_std, ln_gain.reshape(1, width)
        )
        grad_wq = jnp.swapaxes(rows_wq, 0, 1)
        grad_wk = jnp.swapaxes(rows_wkv[:, :, :head_dim], 0, 1)
        grad_wv = jnp.swapaxes(rows_wkv[:, :, head_dim:], 0, 1)
        n_lane = width // 128
        grad_gain, grad_bias = sums[:n_lane, 0].reshape(width), sums[:n_lane, 1].reshape(width)
        return (block_out.reshape(x_act.shape), grad_x.reshape(x_act.shape), grad_wq, grad_wk, grad_wv, grad_wo, grad_gain, grad_bias)

    return jax.shard_map(device_step, mesh=mesh, in_specs=(P("dp", AXIS, None), P("dp", AXIS, None), P("dp", AXIS), P(None), P(None), P(None, None, None), P(None, None, None), P(None, None, None), P(None, None)), out_specs=(P("dp", AXIS, None), P("dp", AXIS, None), P(("dp", AXIS), None, None), P(("dp", AXIS), None, None), P(("dp", AXIS), None, None), P(("dp", AXIS), None), P("dp"), P("dp")), check_vma=False)
```

```python
import functools
import math

import jax
import jax.numpy as jnp
from jax import lax
from jax.experimental import pallas as pl
from jax.experimental.pallas import tpu as pltpu
from jax.sharding import PartitionSpec as P

EPS = 1e-5
ROPE_BASE = 10000.0
BLOCK = 512
AXIS = "cp"
BF16, F32 = jnp.bfloat16, jnp.float32
VMEM_LIMIT = 60 * 1024 * 1024


def frequencies(head_dim):
    quarter = head_dim // 4
    return jnp.exp(jnp.arange(quarter, dtype=F32) * (-2.0 * math.log(ROPE_BASE) / (head_dim // 2)))


def rotate(values, cos, sin):
    quarter = cos.shape[0]
    first, second = values[:quarter], values[quarter : 2 * quarter]
    return jnp.concatenate([first * cos - second * sin, second * cos + first * sin, values[2 * quarter :]], axis=0)


def rows_of(index, size):
    return pl.ds(pl.multiple_of(index * size, size), size)


def dot(lhs, rhs):
    return jnp.dot(lhs, rhs, preferred_element_type=F32)


def dot_t(lhs, rhs):
    return lax.dot_general(lhs, rhs, (((1,), (1,)), ((), ())), preferred_element_type=F32)


def full_barrier(n_dev):
    me = lax.axis_index(AXIS)
    barrier = pltpu.get_barrier_semaphore()

    def tell(step):
        pl.semaphore_signal(barrier, inc=1, device_id={AXIS: lax.rem(me + step, n_dev)}, device_id_type=pl.DeviceIdType.MESH)

    each(1, n_dev, tell)
    pl.semaphore_wait(barrier, n_dev - 1)


def remote(src, dst, send_sem, recv_sem, peer):
    return pltpu.make_async_remote_copy(src_ref=src, dst_ref=dst, send_sem=send_sem, recv_sem=recv_sem, device_id={AXIS: peer}, device_id_type=pl.DeviceIdType.MESH)


def each(lower, upper, body):
    def step(index, carry):
        body(index)
        return carry

    lax.fori_loop(lower, upper, step, 0)


class Exchange:
    def __init__(self, src, dst, send, recv):
        self.src, self.dst, self.send, self.recv = src, dst, send, recv

    def start(self, index, slot, peer):
        me = lax.axis_index(AXIS)
        src, dst, recv = self.src(index), self.dst(slot), self.recv(slot)

        @pl.when(peer != me)
        def _():
            remote(src, dst, self.send(index), recv, peer).start()

        @pl.when(peer == me)
        def _():
            pltpu.make_async_copy(src, dst, recv).start()

    def sent(self, index, peer):
        me = lax.axis_index(AXIS)

        @pl.when(peer != me)
        def _():
            remote(self.src(index), self.src(index), self.send(index), self.send(index), me).wait_send()

    def got(self, slot):
        dst = self.dst(slot)
        remote(dst, dst, self.recv(slot), self.recv(slot), lax.axis_index(AXIS)).wait_recv()


def ring_order(side):
    queue, free, order = [(0.0, True, 0, 0), (0.0, False, 0, 0)], 0.0, []
    waiting = []
    while queue or waiting:
        if queue and (not waiting or free <= waiting[0][0]):
            at, along, s, h = queue.pop(0)
            free = max(free, at) + 1.0
            waiting.append((free + 0.5, (s + along, h + 1 - along)))
        else:
            at, (s, h) = waiting.pop(0)
            order.append((s, h))
            if h == 0 and s < side - 1:
                queue.append((at, True, s, h))
            if h < side - 1:
                queue.append((at, False, s, h))
    return order


def lookup(table, index):
    out = jnp.int32(table[0])
    for key, value in enumerate(table[1:], 1):
        out = jnp.where(index == key, jnp.int32(value), out)
    return out


class Ring:
    def __init__(self, n_dev, own, everything, ring_send, ring_recv, core_send, core_recv):
        self.own, self.all = own, everything
        self.ring_send, self.ring_recv, self.core_send, self.core_recv = ring_send, ring_recv, core_send, core_recv
        self.side = math.isqrt(n_dev // 2)
        self.tokens = own.shape[0]
        self.rows = self.tokens // 4
        self.me = lax.axis_index(AXIS)
        self.core = lax.rem(self.me, 2)
        self.x, self.y = lax.rem(self.me // 2, self.side), self.me // (2 * self.side)

    def device(self, colour, along, across, core):
        side = self.side
        x_first = 1 - colour // 2
        sign = 1 - 2 * lax.rem(colour, 2)
        dx = x_first * along + (1 - x_first) * across
        dy = x_first * across + (1 - x_first) * along
        x = lax.rem(self.x - sign * dx + 2 * side, side)
        y = lax.rem(self.y - sign * dy + 2 * side, side)
        return (y * side + x) * 2 + core

    def place(self, colour, s, h, core):
        return pl.ds(pl.multiple_of(self.device(colour, s, h, core) * self.tokens + colour * self.rows, self.rows), self.rows)

    def piece(self, colour, s, h):
        return self.all.at[self.place(colour, s, h, self.core)]

    def number(self, s, h):
        return s * self.side + h

    def ring_copy(self, colour, s, h, along, src=None):
        number = self.number(s + along, h + 1 - along)
        dst = self.piece(colour, s, h)
        peer = self.device(colour, -along, along - 1, self.core)
        return remote(dst if src is None else src, dst, self.ring_send.at[colour, number], self.ring_recv.at[colour, number], peer)

    def core_copy(self, colour, s, h, src=None):
        number = self.number(s, h)
        dst = self.piece(colour, s, h)
        return remote(dst if src is None else src, dst, self.core_send.at[colour, number], self.core_recv.at[colour, number], self.me + 1 - 2 * self.core)

    def arrival(self, colour, s, h):
        number = self.number(s, h)
        dst = self.piece(colour, s, h)
        return remote(dst, dst, self.ring_send.at[colour, number], self.ring_recv.at[colour, number], self.me)

    def core_arrival(self, colour, s, h):
        number = self.number(s, h)
        dst = self.all.at[self.place(colour, s, h, 1 - self.core)]
        return remote(dst, dst, self.core_send.at[colour, number], self.core_recv.at[colour, number], self.me)

    def begin(self):
        def one(colour):
            src = self.own.at[rows_of(colour, self.rows)]
            self.ring_copy(colour, 0, 0, 1, src).start()
            self.ring_copy(colour, 0, 0, 0, src).start()

        def other(colour):
            self.core_copy(colour, 0, 0, self.own.at[rows_of(colour, self.rows)]).start()

        each(0, 4, one)
        each(0, 4, other)

    def pass_on(self, s, h):
        def one(colour):
            self.arrival(colour, s, h).wait_recv()

            @pl.when((h == 0) & (s < self.side - 1))
            def _():
                self.ring_copy(colour, s, h, 1).start()

            @pl.when(h < self.side - 1)
            def _():
                self.ring_copy(colour, s, h, 0).start()

            self.core_copy(colour, s, h).start()

        each(0, 4, one)

    def got_core(self, s, h):
        each(0, 4, lambda colour: self.core_arrival(colour, s, h).wait_recv())

    def end(self):
        def sent(number):
            s, h = number // self.side, lax.rem(number, self.side)

            def one(colour):
                @pl.when((s > 0) | (h > 0))
                def _():
                    self.arrival(colour, s, h).wait_send()

                self.core_copy(colour, s, h).wait_send()

            each(0, 4, one)

        each(0, self.side * self.side, sent)


def front_kernel(
    n_dev, n_group, x_ref, dy_ref, pos_ref, freq_ref, gain_ref, bias_ref, wo_ref, wq_ref, wk_ref, wv_ref,
    h_all, dy_all, q_ref, k_ref, v_ref, da_ref, cos_ref, sin_ref, x_hat_ref, inv_ref,
    h_own, w_ref, wo_own, pick_ref, w_buf, h_buf, dy_buf, pos_in,
    h_send, h_recv, h_core_send, h_core_recv, dy_send, dy_recv, dy_core_send, dy_core_recv, w_sem, h_sem, dy_sem, pos_send, pos_recv, local,
):
    me = lax.axis_index(AXIS)
    tokens, width = x_ref.shape
    head_dim = v_ref.shape[1]
    heads_tile = w_buf.shape[2]
    d_block = w_buf.shape[1]
    h_ring = Ring(n_dev, h_own, h_all, h_send, h_recv, h_core_send, h_core_recv)
    dy_ring = Ring(n_dev, dy_ref, dy_all, dy_send, dy_recv, dy_core_send, dy_core_recv)
    rows_n = h_ring.rows
    order = [(0, 0)] + ring_order(h_ring.side)
    n_event = len(order)
    where = Exchange(lambda peer: pos_ref, lambda origin: pos_in.at[origin], lambda peer: pos_send.at[peer], lambda origin: pos_recv.at[origin])

    n_d = width // d_block
    kv_head = me // n_group

    def w_load(t, which):
        ref, head = ((wq_ref, me), (wk_ref, kv_head), (wv_ref, kv_head))[which]
        slot = lax.rem(t, 2)
        return pltpu.make_async_copy(ref.at[rows_of(t, d_block), rows_of(head // heads_tile, heads_tile)], w_buf.at[slot], w_sem.at[slot])

    own_dy = pltpu.make_async_copy(dy_ref, dy_all.at[rows_of(me, tokens)], local.at[0])
    own_h = pltpu.make_async_copy(h_own, h_all.at[rows_of(me, tokens)], local.at[1])
    own_wo = pltpu.make_async_copy(wo_ref.at[rows_of(me, head_dim)], wo_own, local.at[2])
    own_dy.start()
    own_wo.start()
    w_load(0, 0).start()
    full_barrier(n_dev)
    dy_ring.begin()

    gain, bias = 1.0 + gain_ref[...], bias_ref[...]

    def norm(t):
        rows = rows_of(t, 16)
        x = x_ref[rows, :].astype(F32)
        centered = x - jnp.sum(x, axis=1, keepdims=True) * (1.0 / width)
        inv = lax.rsqrt(jnp.sum(centered * centered, axis=1, keepdims=True) * (1.0 / width) + EPS)
        x_hat = centered * inv
        x_hat_ref[rows, :] = x_hat
        inv_ref[rows, :] = inv
        h_own[rows, :] = (x_hat * gain + bias).astype(BF16)

    each(0, tokens // 16, norm)

    def send_pos(step):
        peer = lax.rem(me + step, n_dev)
        where.start(peer, me, peer)

    each(0, n_dev, send_pos)
    h_ring.begin()
    own_h.start()

    for which in range(3):
        head = me if which == 0 else kv_head

        def pick(t):
            @pl.when(t + 1 < n_d)
            def _():
                w_load(t + 1, which).start()

            w_load(t, which).wait()
            pick_ref[...] = jnp.swapaxes(w_buf[lax.rem(t, 2)], 0, 1)
            w_ref[rows_of(t, d_block), which * head_dim : (which + 1) * head_dim] = pick_ref[lax.rem(head, heads_tile)]

        each(0, n_d, pick)
        if which < 2:
            w_load(0, which + 1).start()
        if which == 0:
            dy_ring.pass_on(*(jnp.int32(v) for v in order[1]))
        if which == 1:
            h_ring.pass_on(*(jnp.int32(v) for v in order[1]))
    own_wo.wait()
    own_dy.wait()
    own_h.wait()

    def tables(origin):
        where.got(origin)
        angles = freq_ref[...] * pos_in[origin, 0:1, :].astype(F32)
        cos_ref[:, rows_of(origin, tokens)] = jnp.cos(angles)
        sin_ref[:, rows_of(origin, tokens)] = jnp.sin(angles)

    def event(e):
        return lookup([p[0] for p in order], e), lookup([p[1] for p in order], e)

    def places_of(ring, s, h):
        return [ring.place(jnp.int32(colour), s, h, core) for colour in range(4) for core in range(2)]

    def fetch(ring, buf, sem, e):
        slot = lax.rem(e, 2)
        s, h = event(e)
        ring.got_core(s, h)
        for n, place in enumerate(places_of(ring, s, h)):
            pltpu.make_async_copy(ring.all.at[place], buf.at[slot, pl.ds(n * rows_n, rows_n)], sem.at[slot]).start()

    def fetched(ring, buf, sem, e):
        slot = lax.rem(e, 2)
        pltpu.make_async_copy(ring.all.at[pl.ds(0, 8 * rows_n)], buf.at[slot], sem.at[slot]).wait()
        return buf[slot]

    def gradient_rows(e):
        s, h = event(e)
        da = dot_t(fetched(dy_ring, dy_buf, dy_sem, e), wo_own[...]).astype(BF16)
        for n, place in enumerate(places_of(dy_ring, s, h)):
            da_ref[place, :] = da[n * rows_n : (n + 1) * rows_n]

    def project_rows(e):
        s, h = event(e)
        out = dot(fetched(h_ring, h_buf, h_sem, e), w_ref[...])
        for n, place in enumerate(places_of(h_ring, s, h)):
            part = out[n * rows_n : (n + 1) * rows_n]
            q_ref[place, :] = part[:, :head_dim]
            k_ref[place, :] = part[:, head_dim : 2 * head_dim]
            v_ref[place, :] = part[:, 2 * head_dim :].astype(BF16)

    def step(e):
        for ring, buf, sem, rows in ((dy_ring, dy_buf, dy_sem, gradient_rows), (h_ring, h_buf, h_sem, project_rows)):
            @pl.when((e > 1) & (e < n_event))
            def _():
                ring.pass_on(*event(e))

            @pl.when((e > 0) & (e <= n_event))
            def _():
                fetch(ring, buf, sem, e - 1)

            @pl.when(e > 1)
            def _():
                rows(e - 2)

        @pl.when(e == 3)
        def _():
            each(0, n_dev, tables)

    each(1, n_event + 2, step)
    h_ring.end()
    dy_ring.end()
    each(0, n_dev, lambda index: where.sent(index, index))


def front(n_dev, n_group, x_own, dy_own, positions, freq, gain, bias, w_out, w_query, w_key, w_value):
    tokens, width = x_own.shape
    head_dim = w_query.shape[2]
    seq = tokens * n_dev
    heads_tile = min(8, w_key.shape[1])
    d_block = 384
    pieces = math.isqrt(n_dev // 2) ** 2
    whole, anywhere = pl.BlockSpec(memory_space=pltpu.VMEM), pl.BlockSpec(memory_space=pl.ANY)
    dma = pltpu.SemaphoreType.DMA
    return pl.pallas_call(
        functools.partial(front_kernel, n_dev, n_group),
        out_shape=[
            jax.ShapeDtypeStruct((seq, width), BF16),
            jax.ShapeDtypeStruct((seq, width), BF16),
            jax.ShapeDtypeStruct((seq, head_dim), F32),
            jax.ShapeDtypeStruct((seq, head_dim), F32),
            jax.ShapeDtypeStruct((seq, head_dim), BF16),
            jax.ShapeDtypeStruct((seq, head_dim), BF16),
            jax.ShapeDtypeStruct((head_dim // 4, seq), F32),
            jax.ShapeDtypeStruct((head_dim // 4, seq), F32),
            jax.ShapeDtypeStruct((tokens, width), F32),
            jax.ShapeDtypeStruct((tokens, 1), F32),
        ],
        in_specs=[whole] * 6 + [anywhere] * 4,
        out_specs=[anywhere] * 2 + [whole] * 8,
        scratch_shapes=[
            pltpu.VMEM((tokens, width), BF16),
            pltpu.VMEM((width, 3 * head_dim), BF16),
            pltpu.VMEM((head_dim, width), BF16),
            pltpu.VMEM((heads_tile, d_block, head_dim), BF16),
            pltpu.VMEM((2, d_block, heads_tile, head_dim), BF16),
            pltpu.VMEM((2, 2 * tokens, width), BF16),
            pltpu.VMEM((2, 2 * tokens, width), BF16),
            pltpu.VMEM((n_dev,) + positions.shape, jnp.int32),
            dma((4, pieces)), dma((4, pieces)), dma((4, pieces)), dma((4, pieces)),
            dma((4, pieces)), dma((4, pieces)), dma((4, pieces)), dma((4, pieces)),
            dma((2,)), dma((2,)), dma((2,)), dma((n_dev,)), dma((n_dev,)), dma((3,)),
        ],
        compiler_params=pltpu.CompilerParams(collective_id=3, has_side_effects=True, vmem_limit_bytes=VMEM_LIMIT),
        cost_estimate=pl.CostEstimate(flops=8 * seq * width * head_dim, bytes_accessed=8 * seq * width, transcendentals=0),
        name="front",
    )(x_own, dy_own, positions, freq, gain, bias, w_out, w_query, w_key, w_value)


def causal(block):
    key = lax.broadcasted_iota(jnp.int32, (block, block), 0)
    query = lax.broadcasted_iota(jnp.int32, (block, block), 1)
    return key <= query


def part_sum(values):
    return jnp.sum(values.reshape(values.shape[0] // 8, 8, values.shape[1]), axis=0)


def attention_kernel(
    n_dev, n_group, q_heads, kv_heads, scale,
    q_raw, k_raw, v_ref, da_ref, cos_ref, sin_ref,
    at_ref, dqt_ref, a_ref, dq_ref, dkvt_ref, a_out, grad_out,
    q_ref, k_ref, qt_ref, kt_ref, vt_ref, dkv_ref, e_ref, dp_ref, peak_ref, dat_ref, mix_ref, acc_ref, land_one, land_two, kv_ref, kvt_ref,
    a_send, a_recv, q_send, q_recv, one_send, one_recv, two_send, two_recv, kv_send, kv_recv, near_send, near_recv, far_send, far_recv, fwd_send, fwd_recv, local,
):
    me = lax.axis_index(AXIS)
    seq, head_dim = v_ref.shape
    block = e_ref.shape[1]
    n_block = seq // block
    tokens = seq // n_dev
    half = block // 2
    fold = scale * math.log2(math.e)
    core, side = lax.rem(me, 2), lax.rem(me // 2, 2)
    group = me // n_group
    partner, across = me + 1 - 2 * core, me + 2 - 4 * side
    place, place_across = core * 2 + side, core * 2 + 1 - side
    place_partner, place_last = (1 - core) * 2 + side, (1 - core) * 2 + 1 - side

    def piece(index):
        return rows_of(index, tokens)

    def column(head):
        return rows_of(head, head_dim)

    a_copy = Exchange(lambda peer: a_ref.at[piece(peer)], lambda head: a_out.at[:, column(head)], lambda peer: a_send.at[peer], lambda head: a_recv.at[head])
    q_copy = Exchange(lambda peer: dq_ref.at[piece(peer)], lambda head: grad_out.at[:, column(head)], lambda peer: q_send.at[peer], lambda head: q_recv.at[head])
    kv_copy = [
        Exchange(
            lambda i, w=w: kv_ref.at[i, w],
            lambda head, w=w: grad_out.at[:, column(q_heads + w * kv_heads + head)],
            lambda i, w=w: kv_send.at[w, i],
            lambda head, w=w: kv_recv.at[w, head],
        )
        for w in range(2)
    ]

    def one_copy(i):
        return remote(dkv_ref.at[rows_of(i * 2 + 1 - core, half)], land_one.at[i], one_send.at[i], one_recv.at[i], partner)

    def two_copy(i):
        return remote(dkv_ref.at[piece(i * n_group + core * 2 + 1 - side)], land_two.at[i], two_send.at[i], two_recv.at[i], across)

    def near_copy(i, where):
        return remote(kvt_ref.at[i], dkvt_ref.at[:, piece(i * n_group + where)], near_send.at[i], near_recv.at[i], partner)

    def far_copy(i, where):
        return remote(kvt_ref.at[i], dkvt_ref.at[:, piece(i * n_group + where)], far_send.at[i], far_recv.at[i], across)

    def fwd_copy(i, where):
        view = dkvt_ref.at[:, piece(i * n_group + where)]
        return remote(view, view, fwd_send.at[i], fwd_recv.at[i], partner)

    def own_copy(i):
        return pltpu.make_async_copy(kvt_ref.at[i], dkvt_ref.at[:, piece(i * n_group + place)], local.at[i])

    def first(i):
        def send(u):
            peer = i * n_group + lax.rem(u + me, n_group)
            a_copy.start(peer, me, peer)
            q_copy.start(peer, me, peer)

        one_copy(i).start()

        @pl.when(i >= n_block // 2)
        def _():
            each(0, n_group, send)

    def second(i):
        one_copy(i).wait_recv()
        for part in (1 - side, side):
            rows = piece(i * n_group + core * 2 + part)
            dkv_ref[rows, :] += land_one[i, pl.ds(pl.multiple_of(part * tokens, tokens), tokens), :]
        two_copy(i).start()

    def close(i):
        two_copy(i).wait_recv()
        rows = piece(i * n_group + place)
        total = dkv_ref[rows, :] + land_two[i]
        dkt = rotate(total[:, :head_dim].T, cos_ref[:, rows], -sin_ref[:, rows]).astype(BF16)
        dv = total[:, head_dim:].astype(BF16)
        kvt_ref[i, :head_dim, :], kvt_ref[i, head_dim:, :] = dkt, dv.T
        kv_ref[i, 0], kv_ref[i, 1] = dkt.T, dv

    def spread(i):
        near_copy(i, place).start()
        far_copy(i, place).start()
        own_copy(i).start()
        for copy in kv_copy:
            copy.start(i, group, i * n_group + place)

    def forward(i):
        far_copy(i, place_across).wait_recv()
        fwd_copy(i, place_across).start()

    def stages(t):
        for late, stage in ((5, forward), (4, spread), (3, close), (2, second), (1, first)):
            @pl.when((t >= late) & (t < n_block + late))
            def _():
                stage(n_block - 1 - (t - late))

    full_barrier(n_dev)

    def prepare(i):
        rows = rows_of(i, block)
        for raw, turned, plain in ((q_raw, qt_ref, q_ref), (k_raw, kt_ref, k_ref)):
            t = rotate(raw[rows, :].T, cos_ref[:, rows], sin_ref[:, rows]).astype(BF16)
            turned[:, rows] = t
            plain[rows, :] = t.T
        vt_ref[:, rows] = v_ref[rows, :].T
        dkv_ref[rows, :] = jnp.zeros((block, 2 * head_dim), F32)

    each(0, n_block, prepare)

    def compute(i):
        own = rows_of(i, block)
        dat_ref[...] = da_ref[own, :].T
        mix_ref[...] = jnp.zeros_like(mix_ref)
        acc_ref[...] = jnp.zeros_like(acc_ref)

        def scores(j, carry, diagonal):
            peak, total, mixed = carry
            rows = rows_of(j, block)
            s = dot(k_ref[rows, :], qt_ref[:, own])
            if diagonal:
                s = jnp.where(causal(block), s, -1e30)
            top = jnp.maximum(peak, jnp.max(s, axis=0, keepdims=True))
            e = jnp.exp2((s - top) * fold)
            dp = dot(v_ref[rows, :], dat_ref[...])
            fade = jnp.exp2((peak - top) * fold)
            e_ref[rows, :] = e
            dp_ref[rows, :] = dp
            peak_ref[j] = top
            return top, total * fade + part_sum(e), mixed * fade + part_sum(e * dp)

        start = (jnp.full((1, block), -jnp.inf, F32), jnp.zeros((8, block), F32), jnp.zeros((8, block), F32))
        carry = lax.fori_loop(0, i, functools.partial(scores, diagonal=False), start)
        peak, total, mixed = scores(i, carry, True)
        inv = 1.0 / jnp.sum(total, axis=0, keepdims=True)
        row_dot = jnp.sum(mixed, axis=0, keepdims=True) * inv
        q_own, da_own = q_ref[own, :], da_ref[own, :]

        def grads(j):
            rows = rows_of(j, block)
            p = e_ref[rows, :] * (jnp.exp2((peak_ref[j] - peak) * fold) * inv)
            pb = p.astype(BF16)
            ds = ((dp_ref[rows, :] - row_dot) * (p * scale)).astype(BF16)
            dkv_ref[rows, :head_dim] += dot(ds, q_own)
            dkv_ref[rows, head_dim:] += dot(pb, da_own)
            mix_ref[...] += dot(vt_ref[:, rows], pb)
            acc_ref[...] += dot(kt_ref[:, rows], ds)

        each(0, i + 1, grads)
        at = mix_ref[...].astype(BF16)
        at_ref[:, own] = at
        a_ref[own, :] = at.T
        dqt = rotate(acc_ref[...], cos_ref[:, own], -sin_ref[:, own]).astype(BF16)
        dqt_ref[:, own] = dqt
        dq_ref[own, :] = dqt.T

    def iteration(t):
        stages(t)

        @pl.when(t < n_block)
        def _():
            compute(n_block - 1 - t)

    each(0, n_block + 5, iteration)

    def drain(i):
        one_copy(i).wait_send()
        two_copy(i).wait_send()
        near_copy(i, place).wait_send()
        near_copy(i, place_partner).wait_recv()
        far_copy(i, place).wait_send()
        fwd_copy(i, place_across).wait_send()
        fwd_copy(i, place_last).wait_recv()
        own_copy(i).wait()
        for copy in kv_copy:
            copy.sent(i, i * n_group + place)

    each(0, n_block, drain)

    def drain_sent(peer):
        for copy in (a_copy, q_copy):
            copy.sent(peer, peer)

    def drain_got(head):
        for copy in (a_copy, q_copy):
            copy.got(head)

    low = n_block // 2 * n_group
    each(low, n_dev, drain_sent)

    @pl.when(me >= low)
    def _():
        each(0, n_dev, drain_got)

    def drain_kv(head):
        for copy in kv_copy:
            copy.got(head)

    each(0, kv_heads, drain_kv)


def attention(n_dev, kv_heads, q, k, v, da, cos_tab, sin_tab):
    seq, head_dim = q.shape
    q_heads = n_dev
    n_group = q_heads // kv_heads
    tokens = seq // n_dev
    block = tokens * n_group
    n_block = seq // block
    whole, anywhere = pl.BlockSpec(memory_space=pltpu.VMEM), pl.BlockSpec(memory_space=pl.ANY)
    dma = pltpu.SemaphoreType.DMA
    return pl.pallas_call(
        functools.partial(attention_kernel, n_dev, n_group, q_heads, kv_heads, head_dim**-0.5),
        out_shape=[
            jax.ShapeDtypeStruct((head_dim, seq), BF16),
            jax.ShapeDtypeStruct((head_dim, seq), BF16),
            jax.ShapeDtypeStruct((seq, head_dim), BF16),
            jax.ShapeDtypeStruct((seq, head_dim), BF16),
            jax.ShapeDtypeStruct((2 * head_dim, seq), BF16),
            jax.ShapeDtypeStruct((tokens, q_heads * head_dim), BF16),
            jax.ShapeDtypeStruct((tokens, (q_heads + 2 * kv_heads) * head_dim), BF16),
        ],
        in_specs=[whole] * 6,
        out_specs=[whole] * 4 + [anywhere] * 3,
        scratch_shapes=[
            pltpu.VMEM((seq, head_dim), BF16),
            pltpu.VMEM((seq, head_dim), BF16),
            pltpu.VMEM((head_dim, seq), BF16),
            pltpu.VMEM((head_dim, seq), BF16),
            pltpu.VMEM((head_dim, seq), BF16),
            pltpu.VMEM((seq, 2 * head_dim), F32),
            pltpu.VMEM((seq, block), F32),
            pltpu.VMEM((seq, block), F32),
            pltpu.VMEM((n_block, 1, block), F32),
            pltpu.VMEM((head_dim, block), BF16),
            pltpu.VMEM((head_dim, block), F32),
            pltpu.VMEM((head_dim, block), F32),
            pltpu.VMEM((n_block, block // 2, 2 * head_dim), F32),
            pltpu.VMEM((n_block, tokens, 2 * head_dim), F32),
            pltpu.VMEM((n_block, 2, tokens, head_dim), BF16),
            pltpu.VMEM((n_block, 2 * head_dim, tokens), BF16),
            dma((n_dev,)), dma((n_dev,)), dma((n_dev,)), dma((n_dev,)),
            dma((n_block,)), dma((n_block,)), dma((n_block,)), dma((n_block,)), dma((2, n_block)), dma((2, kv_heads)),
            dma((n_block,)), dma((n_block,)), dma((n_block,)), dma((n_block,)), dma((n_block,)), dma((n_block,)), dma((n_block,)),
        ],
        compiler_params=pltpu.CompilerParams(collective_id=1, has_side_effects=True, vmem_limit_bytes=VMEM_LIMIT),
        cost_estimate=pl.CostEstimate(flops=6 * seq * seq * head_dim, bytes_accessed=18 * seq * head_dim, transcendentals=seq * seq // 2),
        name="attention",
    )(q, k, v, da, cos_tab, sin_tab)


def finish_kernel(
    n_dev, n_group, n_buf,
    h_ref, dy_ref, wq_ref, wk_ref, wv_ref, wo_ref, a_in, g_in, a_head, dq_head, dqt_ref, dkvt_ref, at_ref, x_ref, dy_own_ref, x_hat_ref, inv_ref, gain_ref,
    out_ref, gx_ref, gwo_ref, q_rows, kv_rows, sum_ref,
    a_ref, g_ref, buf, wq_buf, wk_buf, wv_buf, wq_out, wkv_out, dh_ref, part_ref, own_sum, sum_in, sum_mine,
    load_sem, q_send, q_recv, kv_send, kv_recv, s_send, s_recv, t_send, t_recv, a_send, a_recv, dq_send, dq_recv, local,
):
    me = lax.axis_index(AXIS)
    seq, width = h_ref.shape
    span = buf.shape[2]
    head_dim = dqt_ref.shape[0]
    depth = width // n_dev
    n_col = width // span
    per_col = span // depth
    member, group = lax.rem(me, n_group), me // n_group
    col_member = n_col // n_group
    per_member = n_dev // n_group
    n_sum = sum_mine.shape[0]
    q_rows_n = a_ref.shape[1]
    kv_rows_n = (g_ref.shape[1] - q_rows_n) // 2

    tokens = x_ref.shape[0]
    low = n_dev // n_group // 2 * n_group

    def cols(j):
        return rows_of(j, span)

    def turn(phase, j):
        return lax.rem(j + me // per_col, n_col) if phase == 0 else j

    def loads(phase, j, slot):
        if phase == 2:
            pairs = ((wq_ref, wq_buf), (wk_ref, wk_buf), (wv_ref, wv_buf))
            return [pltpu.make_async_copy(ref.at[cols(j)], to.at[slot], load_sem.at[slot, n]) for n, (ref, to) in enumerate(pairs)]
        ref = (h_ref, dy_ref, None, wo_ref)[phase]
        return [pltpu.make_async_copy(ref.at[:, cols(turn(phase, j))], buf.at[slot], load_sem.at[slot, 0])]

    def load(step):
        slot = lax.rem(step, n_buf)
        for phase in range(4):
            @pl.when((step >= phase * n_col) & (step < (phase + 1) * n_col))
            def _():
                for copy in loads(phase, step - phase * n_col, slot):
                    copy.start()

    q_copy = Exchange(lambda peer: wq_out.at[rows_of(peer, depth)], lambda head: q_rows.at[head], lambda peer: q_send.at[peer], lambda head: q_recv.at[head])
    kv_copy = Exchange(lambda i: wkv_out.at[rows_of(i, depth)], lambda head: kv_rows.at[head], lambda i: kv_send.at[i], lambda head: kv_recv.at[head])
    s_copy = Exchange(lambda peer: own_sum.at[pl.ds(peer * n_sum, n_sum)], lambda origin: sum_in.at[origin], lambda peer: s_send.at[peer], lambda origin: s_recv.at[origin])
    t_copy = Exchange(lambda peer: sum_mine, lambda origin: sum_ref.at[pl.ds(origin * n_sum, n_sum)], lambda peer: t_send.at[peer], lambda origin: t_recv.at[origin])

    def column(head):
        return rows_of(head, head_dim)

    a_copy = Exchange(lambda peer: a_head.at[rows_of(peer, tokens)], lambda head: a_ref.at[:, column(head)], lambda peer: a_send.at[peer], lambda head: a_recv.at[head])
    dq_copy = Exchange(lambda peer: dq_head.at[rows_of(peer, tokens)], lambda head: g_ref.at[:, column(head)], lambda peer: dq_send.at[peer], lambda head: dq_recv.at[head])

    def send_heads(step):
        peer = lax.rem(me + step, low)
        a_copy.start(peer, me, peer)
        dq_copy.start(peer, me, peer)

    own_kv = pltpu.make_async_copy(g_in.at[:, pl.ds(q_rows_n, 2 * kv_rows_n)], g_ref.at[:, pl.ds(q_rows_n, 2 * kv_rows_n)], local.at[0])
    own_a = pltpu.make_async_copy(a_in, a_ref, local.at[1])
    own_dq = pltpu.make_async_copy(g_in.at[:, pl.ds(0, q_rows_n)], g_ref.at[:, pl.ds(0, q_rows_n)], local.at[2])

    def send_q(j):
        def send(u):
            peer = turn(0, j) * per_col + lax.rem(u + me, per_col)
            q_copy.start(peer, me, peer)

        each(0, per_col, send)

    def run(phase, body):
        def step(j):
            number = phase * n_col + j
            slot = lax.rem(number, n_buf)
            for copy in loads(phase, j, slot):
                copy.wait()
            body(j, slot)
            load(number + n_buf)

        each(0, n_col, step)

    each(0, n_buf, load)
    own_kv.start()

    @pl.when(me >= low)
    def _():
        own_a.start()
        own_dq.start()

    full_barrier(n_dev)
    each(0, low, send_heads)

    def weight_columns(j, slot):
        @pl.when(j > 0)
        def _():
            send_q(j - 1)

        col = turn(0, j)
        wq_out[cols(col), :] = dot(dqt_ref[...], buf[slot]).T

        @pl.when(col // col_member == member)
        def _():
            wkv_out[cols(col - member * col_member), :] = dot(dkvt_ref[...], buf[slot]).T

    run(0, weight_columns)

    def send_kv(step):
        index = lax.rem(step + group, per_member)
        kv_copy.start(index, group, member * per_member + index)

    def weight_out(j, slot):
        gwo_ref[:, cols(j)] = dot(at_ref[...], buf[slot])

        @pl.when(j == 0)
        def _():
            send_q(n_col - 1)
            each(0, per_member, send_kv)

    run(1, weight_out)
    own_kv.wait()

    @pl.when(me >= low)
    def _():
        own_a.wait()
        own_dq.wait()

    def got_heads(head):
        a_copy.got(head)
        dq_copy.got(head)

    @pl.when(me < low)
    def _():
        each(0, n_dev, got_heads)

    def back(j, slot):
        def flat(ref):
            block = ref[slot]
            return block.reshape(block.shape[0], block.shape[1] * block.shape[2])

        grad_h = dot_t(g_ref[:, :q_rows_n], flat(wq_buf))
        grad_h += dot_t(g_ref[:, q_rows_n : q_rows_n + kv_rows_n], flat(wk_buf))
        dh_ref[:, cols(j)] = grad_h + dot_t(g_ref[:, q_rows_n + kv_rows_n :], flat(wv_buf))

    run(2, back)

    part_ref[...] = jnp.zeros_like(part_ref)
    gain = 1.0 + gain_ref[...]

    def norm(t):
        rows = rows_of(t, 16)
        grad_h, x_hat = dh_ref[rows, :], x_hat_ref[rows, :]
        grad_hat = grad_h * gain
        one = jnp.sum(grad_hat, axis=1, keepdims=True) * (1.0 / width)
        two = jnp.sum(grad_hat * x_hat, axis=1, keepdims=True) * (1.0 / width)
        back = inv_ref[rows, :] * (grad_hat - one - x_hat * two)
        gx_ref[rows, :] = (dy_own_ref[rows, :].astype(F32) + back).astype(BF16)
        part_ref[0] += part_sum(grad_h * x_hat)
        part_ref[1] += part_sum(grad_h)

    each(0, dh_ref.shape[0] // 16, norm)
    own_sum[...] = jnp.zeros_like(own_sum)
    for which in range(2):
        total = jnp.sum(part_ref[which], axis=0, keepdims=True)
        for c in range(width // 128):
            own_sum[c, pl.ds(which, 1), :] = total[:, c * 128 : (c + 1) * 128]

    def to_all(copy):
        def send(step):
            peer = lax.rem(me + step, n_dev)
            copy.start(peer, me, peer)

        each(0, n_dev, send)

    def add(origin):
        sum_mine[...] += sum_in[origin]

    def output(j, slot):
        @pl.when(j == 0)
        def _():
            to_all(s_copy)

        @pl.when(j == n_col // 2)
        def _():
            each(0, n_dev, s_copy.got)
            sum_mine[...] = jnp.zeros_like(sum_mine)
            each(0, n_dev, add)

        out_ref[:, cols(j)] = (x_ref[:, cols(j)].astype(F32) + dot(a_ref[...], buf[slot])).astype(BF16)

        @pl.when(j == n_col // 2)
        def _():
            to_all(t_copy)

    run(3, output)

    def drain(index):
        s_copy.sent(index, index)
        t_copy.sent(index, index)
        t_copy.got(index)
        q_copy.sent(index, index)
        q_copy.got(index)

    def drain_kv(index):
        kv_copy.sent(index, member * per_member + index)

    def drain_heads(peer):
        a_copy.sent(peer, peer)
        dq_copy.sent(peer, peer)

    each(0, n_dev, drain)
    each(0, low, drain_heads)
    each(0, per_member, drain_kv)
    each(0, kv_rows.shape[0], kv_copy.got)


def finish(n_dev, kv_heads, h_all, dy_all, wq, wk, wv, wo, a_in, g_in, a_head, dq_head, dqt, dkvt, at, x_own, dy_own, x_hat, inv_std, gain):
    seq, width = h_all.shape
    tokens = seq // n_dev
    head_dim = dqt.shape[0]
    q_heads = n_dev
    n_group = q_heads // kv_heads
    depth = width // n_dev
    span = math.lcm(depth, 128)
    n_buf = 3
    n_sum = -(-width // (128 * n_dev))
    sums = (n_sum * n_dev, 8, 128)
    whole, anywhere = pl.BlockSpec(memory_space=pltpu.VMEM), pl.BlockSpec(memory_space=pl.ANY)
    dma = pltpu.SemaphoreType.DMA
    return pl.pallas_call(
        functools.partial(finish_kernel, n_dev, n_group, n_buf),
        out_shape=[
            jax.ShapeDtypeStruct((tokens, width), BF16),
            jax.ShapeDtypeStruct((tokens, width), BF16),
            jax.ShapeDtypeStruct((head_dim, width), F32),
            jax.ShapeDtypeStruct((q_heads, depth, head_dim), F32),
            jax.ShapeDtypeStruct((kv_heads, depth, 2 * head_dim), F32),
            jax.ShapeDtypeStruct(sums, F32),
        ],
        in_specs=[anywhere] * 10 + [whole] * 8,
        out_specs=[whole] * 3 + [anywhere] * 2 + [whole],
        scratch_shapes=[
            pltpu.VMEM(a_in.shape, BF16),
            pltpu.VMEM(g_in.shape, BF16),
            pltpu.VMEM((n_buf, seq, span), BF16),
            pltpu.VMEM((n_buf, span) + wq.shape[1:], BF16),
            pltpu.VMEM((n_buf, span) + wk.shape[1:], BF16),
            pltpu.VMEM((n_buf, span) + wv.shape[1:], BF16),
            pltpu.VMEM((width, head_dim), F32),
            pltpu.VMEM((width // n_group, 2 * head_dim), F32),
            pltpu.VMEM((tokens, width), F32),
            pltpu.VMEM((2, 8, width), F32),
            pltpu.VMEM(sums, F32),
            pltpu.VMEM((n_dev, n_sum, 8, 128), F32),
            pltpu.VMEM((n_sum, 8, 128), F32),
            dma((n_buf, 3)), dma((n_dev,)), dma((n_dev,)), dma((n_dev // n_group,)), dma((kv_heads,)), dma((n_dev,)), dma((n_dev,)), dma((n_dev,)), dma((n_dev,)),
            dma((n_dev,)), dma((n_dev,)), dma((n_dev,)), dma((n_dev,)), dma((3,)),
        ],
        compiler_params=pltpu.CompilerParams(collective_id=2, has_side_effects=True, vmem_limit_bytes=VMEM_LIMIT),
        cost_estimate=pl.CostEstimate(flops=8 * seq * width * head_dim, bytes_accessed=8 * seq * width, transcendentals=0),
        name="finish",
    )(h_all, dy_all, wq, wk, wv, wo, a_in, g_in, a_head, dq_head, dqt, dkvt, at, x_own, dy_own, x_hat, inv_std, gain)


def solution(mesh):
    n_dev = mesh.shape[AXIS]

    def device_step(x_act, d_out, positions, ln_gain, ln_bias, w_query, w_key, w_value, w_out):
        n_batch, piece, width = x_act.shape
        q_heads, head_dim = w_query.shape[1:]
        kv_heads = w_key.shape[1]
        n_group = q_heads // kv_heads
        tokens = n_batch * piece

        x_own, dy_own = x_act.reshape(tokens, width), d_out.reshape(tokens, width)
        gain, bias = ln_gain.reshape(1, width), ln_bias.reshape(1, width)
        pos_tile = jnp.broadcast_to(positions.reshape(1, tokens), (8, tokens))
        freq = jnp.broadcast_to(frequencies(head_dim)[:, None], (head_dim // 4, tokens))
        h_all, dy_all, q, k, v, da, cos_tab, sin_tab, x_hat, inv_std = front(n_dev, n_group, x_own, dy_own, pos_tile, freq, gain, bias, w_out, w_query, w_key, w_value)
        at, dqt, a_head, dq_head, dkvt, a_own, g_own = attention(n_dev, kv_heads, q, k, v, da, cos_tab, sin_tab)
        block_out, grad_x, grad_wo, rows_wq, rows_wkv, sums = finish(
            n_dev, kv_heads, h_all, dy_all, w_query, w_key, w_value, w_out, a_own, g_own, a_head, dq_head, dqt, dkvt, at, x_own, dy_own, x_hat, inv_std, gain
        )
        grad_wq = jnp.swapaxes(rows_wq, 0, 1)
        grad_wk = jnp.swapaxes(rows_wkv[:, :, :head_dim], 0, 1)
        grad_wv = jnp.swapaxes(rows_wkv[:, :, head_dim:], 0, 1)
        n_lane = width // 128
        grad_gain, grad_bias = sums[:n_lane, 0].reshape(width), sums[:n_lane, 1].reshape(width)
        return (block_out.reshape(x_act.shape), grad_x.reshape(x_act.shape), grad_wq, grad_wk, grad_wv, grad_wo, grad_gain, grad_bias)

    return jax.shard_map(device_step, mesh=mesh, in_specs=(P("dp", AXIS, None), P("dp", AXIS, None), P("dp", AXIS), P(None), P(None), P(None, None, None), P(None, None, None), P(None, None, None), P(None, None)), out_specs=(P("dp", AXIS, None), P("dp", AXIS, None), P(("dp", AXIS), None, None), P(("dp", AXIS), None, None), P(("dp", AXIS), None, None), P(("dp", AXIS), None), P("dp"), P("dp")), check_vma=False)
```

```python
import functools
import math

import jax
import jax.numpy as jnp
from jax import lax
from jax.experimental import pallas as pl
from jax.experimental.pallas import tpu as pltpu
from jax.sharding import PartitionSpec as P

EPS = 1e-5
ROPE_BASE = 10000.0
BLOCK = 512
AXIS = "cp"
BF16, F32 = jnp.bfloat16, jnp.float32
VMEM_LIMIT = 63 * 1024 * 1024


def frequencies(head_dim):
    quarter = head_dim // 4
    return jnp.exp(jnp.arange(quarter, dtype=F32) * (-2.0 * math.log(ROPE_BASE) / (head_dim // 2)))


def rotate(values, cos, sin):
    quarter = cos.shape[0]
    first, second = values[:quarter], values[quarter : 2 * quarter]
    return jnp.concatenate([first * cos - second * sin, second * cos + first * sin, values[2 * quarter :]], axis=0)


def rows_of(index, size):
    return pl.ds(pl.multiple_of(index * size, size), size)


def dot(lhs, rhs):
    return jnp.dot(lhs, rhs, preferred_element_type=F32)


def dot_t(lhs, rhs):
    return lax.dot_general(lhs, rhs, (((1,), (1,)), ((), ())), preferred_element_type=F32)


def full_barrier(n_dev):
    me = lax.axis_index(AXIS)
    barrier = pltpu.get_barrier_semaphore()

    def tell(step):
        pl.semaphore_signal(barrier, inc=1, device_id={AXIS: lax.rem(me + step, n_dev)}, device_id_type=pl.DeviceIdType.MESH)

    each(1, n_dev, tell)
    pl.semaphore_wait(barrier, n_dev - 1)


def remote(src, dst, send_sem, recv_sem, peer):
    return pltpu.make_async_remote_copy(src_ref=src, dst_ref=dst, send_sem=send_sem, recv_sem=recv_sem, device_id={AXIS: peer}, device_id_type=pl.DeviceIdType.MESH)


def each(lower, upper, body):
    def step(index, carry):
        body(index)
        return carry

    lax.fori_loop(lower, upper, step, 0)


class Exchange:
    def __init__(self, src, dst, send, recv):
        self.src, self.dst, self.send, self.recv = src, dst, send, recv

    def start(self, index, slot, peer):
        me = lax.axis_index(AXIS)
        src, dst, recv = self.src(index), self.dst(slot), self.recv(slot)

        @pl.when(peer != me)
        def _():
            remote(src, dst, self.send(index), recv, peer).start()

        @pl.when(peer == me)
        def _():
            pltpu.make_async_copy(src, dst, recv).start()

    def sent(self, index, peer):
        me = lax.axis_index(AXIS)

        @pl.when(peer != me)
        def _():
            remote(self.src(index), self.src(index), self.send(index), self.send(index), me).wait_send()

    def got(self, slot):
        dst = self.dst(slot)
        remote(dst, dst, self.recv(slot), self.recv(slot), lax.axis_index(AXIS)).wait_recv()


def ring_order(side):
    queue, free, order = [(0.0, True, 0, 0), (0.0, False, 0, 0)], 0.0, []
    waiting = []
    while queue or waiting:
        if queue and (not waiting or free <= waiting[0][0]):
            at, along, s, h = queue.pop(0)
            free = max(free, at) + 1.0
            waiting.append((free + 0.5, (s + along, h + 1 - along)))
        else:
            at, (s, h) = waiting.pop(0)
            order.append((s, h))
            if h == 0 and s < side - 1:
                queue.append((at, True, s, h))
            if h < side - 1:
                queue.append((at, False, s, h))
    return order


def lookup(table, index):
    out = jnp.int32(table[0])
    for key, value in enumerate(table[1:], 1):
        out = jnp.where(index == key, jnp.int32(value), out)
    return out


class Ring:
    def __init__(self, n_dev, own, everything, ring_send, ring_recv, core_send, core_recv):
        self.own, self.all = own, everything
        self.ring_send, self.ring_recv, self.core_send, self.core_recv = ring_send, ring_recv, core_send, core_recv
        self.side = math.isqrt(n_dev // 2)
        self.tokens = own.shape[0]
        self.rows = self.tokens // 4
        self.me = lax.axis_index(AXIS)
        self.core = lax.rem(self.me, 2)
        self.x, self.y = lax.rem(self.me // 2, self.side), self.me // (2 * self.side)

    def device(self, colour, along, across, core):
        side = self.side
        x_first = 1 - colour // 2
        sign = 1 - 2 * lax.rem(colour, 2)
        dx = x_first * along + (1 - x_first) * across
        dy = x_first * across + (1 - x_first) * along
        x = lax.rem(self.x - sign * dx + 2 * side, side)
        y = lax.rem(self.y - sign * dy + 2 * side, side)
        return (y * side + x) * 2 + core

    def place(self, colour, s, h, core):
        return pl.ds(pl.multiple_of(self.device(colour, s, h, core) * self.tokens + colour * self.rows, self.rows), self.rows)

    def piece(self, colour, s, h):
        return self.all.at[self.place(colour, s, h, self.core)]

    def number(self, s, h):
        return s * self.side + h

    def ring_copy(self, colour, s, h, along, src=None):
        number = self.number(s + along, h + 1 - along)
        dst = self.piece(colour, s, h)
        peer = self.device(colour, -along, along - 1, self.core)
        return remote(dst if src is None else src, dst, self.ring_send.at[colour, number], self.ring_recv.at[colour, number], peer)

    def core_copy(self, colour, s, h, src=None):
        number = self.number(s, h)
        dst = self.piece(colour, s, h)
        return remote(dst if src is None else src, dst, self.core_send.at[colour, number], self.core_recv.at[colour, number], self.me + 1 - 2 * self.core)

    def arrival(self, colour, s, h):
        number = self.number(s, h)
        dst = self.piece(colour, s, h)
        return remote(dst, dst, self.ring_send.at[colour, number], self.ring_recv.at[colour, number], self.me)

    def core_arrival(self, colour, s, h):
        number = self.number(s, h)
        dst = self.all.at[self.place(colour, s, h, 1 - self.core)]
        return remote(dst, dst, self.core_send.at[colour, number], self.core_recv.at[colour, number], self.me)

    def begin(self):
        def one(colour):
            src = self.own.at[rows_of(colour, self.rows)]
            self.ring_copy(colour, 0, 0, 1, src).start()
            self.ring_copy(colour, 0, 0, 0, src).start()

        def other(colour):
            self.core_copy(colour, 0, 0, self.own.at[rows_of(colour, self.rows)]).start()

        each(0, 4, one)
        each(0, 4, other)

    def pass_on(self, s, h):
        def one(colour):
            self.arrival(colour, s, h).wait_recv()

            @pl.when((h == 0) & (s < self.side - 1))
            def _():
                self.ring_copy(colour, s, h, 1).start()

            @pl.when(h < self.side - 1)
            def _():
                self.ring_copy(colour, s, h, 0).start()

            self.core_copy(colour, s, h).start()

        each(0, 4, one)

    def got_core(self, s, h):
        each(0, 4, lambda colour: self.core_arrival(colour, s, h).wait_recv())

    def end(self):
        def sent(number):
            s, h = number // self.side, lax.rem(number, self.side)

            def one(colour):
                @pl.when((s > 0) | (h > 0))
                def _():
                    self.arrival(colour, s, h).wait_send()

                self.core_copy(colour, s, h).wait_send()

            each(0, 4, one)

        each(0, self.side * self.side, sent)


def front_kernel(
    n_dev, n_group, x_ref, dy_ref, pos_ref, freq_ref, gain_ref, bias_ref, wo_ref, wq_ref, wk_ref, wv_ref,
    h_all, dy_all, q_ref, k_ref, v_ref, da_ref, cos_ref, sin_ref, x_hat_ref, inv_ref,
    h_own, w_ref, wo_own, pick_ref, w_buf, h_buf, dy_buf, pos_in,
    h_send, h_recv, h_core_send, h_core_recv, dy_send, dy_recv, dy_core_send, dy_core_recv, w_sem, h_sem, dy_sem, pos_send, pos_recv, local,
):
    me = lax.axis_index(AXIS)
    tokens, width = x_ref.shape
    head_dim = v_ref.shape[1]
    heads_tile = w_buf.shape[2]
    d_block = w_buf.shape[1]
    h_ring = Ring(n_dev, h_own, h_all, h_send, h_recv, h_core_send, h_core_recv)
    dy_ring = Ring(n_dev, dy_ref, dy_all, dy_send, dy_recv, dy_core_send, dy_core_recv)
    rows_n = h_ring.rows
    order = [(0, 0)] + ring_order(h_ring.side)
    n_event = len(order)
    where = Exchange(lambda peer: pos_ref, lambda origin: pos_in.at[origin], lambda peer: pos_send.at[peer], lambda origin: pos_recv.at[origin])

    n_d = width // d_block
    kv_head = me // n_group

    def w_load(t, which):
        ref, head = ((wq_ref, me), (wk_ref, kv_head), (wv_ref, kv_head))[which]
        slot = lax.rem(t, 2)
        return pltpu.make_async_copy(ref.at[rows_of(t, d_block), rows_of(head // heads_tile, heads_tile)], w_buf.at[slot], w_sem.at[slot])

    own_dy = pltpu.make_async_copy(dy_ref, dy_all.at[rows_of(me, tokens)], local.at[0])
    own_h = pltpu.make_async_copy(h_own, h_all.at[rows_of(me, tokens)], local.at[1])
    own_wo = pltpu.make_async_copy(wo_ref.at[rows_of(me, head_dim)], wo_own, local.at[2])
    own_dy.start()
    own_wo.start()
    w_load(0, 0).start()
    full_barrier(n_dev)
    dy_ring.begin()

    gain, bias = 1.0 + gain_ref[...], bias_ref[...]

    def norm(t):
        rows = rows_of(t, 16)
        x = x_ref[rows, :].astype(F32)
        centered = x - jnp.sum(x, axis=1, keepdims=True) * (1.0 / width)
        inv = lax.rsqrt(jnp.sum(centered * centered, axis=1, keepdims=True) * (1.0 / width) + EPS)
        x_hat = centered * inv
        x_hat_ref[rows, :] = x_hat
        inv_ref[rows, :] = inv
        h_own[rows, :] = (x_hat * gain + bias).astype(BF16)

    each(0, tokens // 16, norm)

    def send_pos(step):
        peer = lax.rem(me + step, n_dev)
        where.start(peer, me, peer)

    each(0, n_dev, send_pos)
    h_ring.begin()
    own_h.start()

    for which in range(3):
        head = me if which == 0 else kv_head

        def pick(t):
            @pl.when(t + 1 < n_d)
            def _():
                w_load(t + 1, which).start()

            w_load(t, which).wait()
            pick_ref[...] = jnp.swapaxes(w_buf[lax.rem(t, 2)], 0, 1)
            w_ref[rows_of(t, d_block), which * head_dim : (which + 1) * head_dim] = pick_ref[lax.rem(head, heads_tile)]

        each(0, n_d, pick)
        if which < 2:
            w_load(0, which + 1).start()
        if which == 0:
            dy_ring.pass_on(*(jnp.int32(v) for v in order[1]))
        if which == 1:
            h_ring.pass_on(*(jnp.int32(v) for v in order[1]))
    own_wo.wait()
    own_dy.wait()
    own_h.wait()

    def tables(origin):
        where.got(origin)
        angles = freq_ref[...] * pos_in[origin, 0:1, :].astype(F32)
        cos_ref[:, rows_of(origin, tokens)] = jnp.cos(angles)
        sin_ref[:, rows_of(origin, tokens)] = jnp.sin(angles)

    def event(e):
        return lookup([p[0] for p in order], e), lookup([p[1] for p in order], e)

    def places_of(ring, s, h):
        return [ring.place(jnp.int32(colour), s, h, core) for colour in range(4) for core in range(2)]

    def fetch(ring, buf, sem, e):
        slot = lax.rem(e, 2)
        s, h = event(e)
        ring.got_core(s, h)
        for n, place in enumerate(places_of(ring, s, h)):
            pltpu.make_async_copy(ring.all.at[place], buf.at[slot, pl.ds(n * rows_n, rows_n)], sem.at[slot]).start()

    def fetched(ring, buf, sem, e):
        slot = lax.rem(e, 2)
        pltpu.make_async_copy(ring.all.at[pl.ds(0, 8 * rows_n)], buf.at[slot], sem.at[slot]).wait()
        return buf[slot]

    def gradient_rows(e):
        s, h = event(e)
        da = dot_t(fetched(dy_ring, dy_buf, dy_sem, e), wo_own[...]).astype(BF16)
        for n, place in enumerate(places_of(dy_ring, s, h)):
            da_ref[place, :] = da[n * rows_n : (n + 1) * rows_n]

    def project_rows(e):
        s, h = event(e)
        out = dot(fetched(h_ring, h_buf, h_sem, e), w_ref[...])
        for n, place in enumerate(places_of(h_ring, s, h)):
            part = out[n * rows_n : (n + 1) * rows_n]
            q_ref[place, :] = part[:, :head_dim]
            k_ref[place, :] = part[:, head_dim : 2 * head_dim]
            v_ref[place, :] = part[:, 2 * head_dim :].astype(BF16)

    def step(e):
        for ring, buf, sem, rows in ((dy_ring, dy_buf, dy_sem, gradient_rows), (h_ring, h_buf, h_sem, project_rows)):
            @pl.when((e > 1) & (e < n_event))
            def _():
                ring.pass_on(*event(e))

            @pl.when((e > 0) & (e <= n_event))
            def _():
                fetch(ring, buf, sem, e - 1)

            @pl.when(e > 1)
            def _():
                rows(e - 2)

        @pl.when(e == 3)
        def _():
            each(0, n_dev, tables)

    each(1, n_event + 2, step)
    h_ring.end()
    dy_ring.end()
    each(0, n_dev, lambda index: where.sent(index, index))


def front(n_dev, n_group, x_own, dy_own, positions, freq, gain, bias, w_out, w_query, w_key, w_value):
    tokens, width = x_own.shape
    head_dim = w_query.shape[2]
    seq = tokens * n_dev
    heads_tile = min(8, w_key.shape[1])
    d_block = 384
    pieces = math.isqrt(n_dev // 2) ** 2
    whole, anywhere = pl.BlockSpec(memory_space=pltpu.VMEM), pl.BlockSpec(memory_space=pl.ANY)
    dma = pltpu.SemaphoreType.DMA
    return pl.pallas_call(
        functools.partial(front_kernel, n_dev, n_group),
        out_shape=[
            jax.ShapeDtypeStruct((seq, width), BF16),
            jax.ShapeDtypeStruct((seq, width), BF16),
            jax.ShapeDtypeStruct((seq, head_dim), F32),
            jax.ShapeDtypeStruct((seq, head_dim), F32),
            jax.ShapeDtypeStruct((seq, head_dim), BF16),
            jax.ShapeDtypeStruct((seq, head_dim), BF16),
            jax.ShapeDtypeStruct((head_dim // 4, seq), F32),
            jax.ShapeDtypeStruct((head_dim // 4, seq), F32),
            jax.ShapeDtypeStruct((tokens, width), F32),
            jax.ShapeDtypeStruct((tokens, 1), F32),
        ],
        in_specs=[whole] * 6 + [anywhere] * 4,
        out_specs=[anywhere] * 2 + [whole] * 8,
        scratch_shapes=[
            pltpu.VMEM((tokens, width), BF16),
            pltpu.VMEM((width, 3 * head_dim), BF16),
            pltpu.VMEM((head_dim, width), BF16),
            pltpu.VMEM((heads_tile, d_block, head_dim), BF16),
            pltpu.VMEM((2, d_block, heads_tile, head_dim), BF16),
            pltpu.VMEM((2, 2 * tokens, width), BF16),
            pltpu.VMEM((2, 2 * tokens, width), BF16),
            pltpu.VMEM((n_dev,) + positions.shape, jnp.int32),
            dma((4, pieces)), dma((4, pieces)), dma((4, pieces)), dma((4, pieces)),
            dma((4, pieces)), dma((4, pieces)), dma((4, pieces)), dma((4, pieces)),
            dma((2,)), dma((2,)), dma((2,)), dma((n_dev,)), dma((n_dev,)), dma((3,)),
        ],
        compiler_params=pltpu.CompilerParams(collective_id=3, has_side_effects=True, vmem_limit_bytes=VMEM_LIMIT),
        cost_estimate=pl.CostEstimate(flops=8 * seq * width * head_dim, bytes_accessed=8 * seq * width, transcendentals=0),
        name="front",
    )(x_own, dy_own, positions, freq, gain, bias, w_out, w_query, w_key, w_value)


def causal(block):
    key = lax.broadcasted_iota(jnp.int32, (block, block), 0)
    query = lax.broadcasted_iota(jnp.int32, (block, block), 1)
    return key <= query


def part_sum(values):
    return jnp.sum(values.reshape(values.shape[0] // 8, 8, values.shape[1]), axis=0)


def main_kernel(
    n_dev, n_group, q_heads, kv_heads, n_buf, scale,
    q_raw, k_raw, v_ref, da_ref, cos_ref, sin_ref, x_ref, dy_own_ref, x_hat_ref, inv_ref, gain_ref, h_ref, dy_ref, wq_ref, wk_ref, wv_ref, wo_ref,
    out_ref, gx_ref, gwo_ref, q_rows, kv_rows, sum_ref,
    at_ref, dqt_ref, a_head, dq_head, dkvt_ref, a_ref, g_ref, dkv_ref, land_one, land_two, kv_ref, kvt_ref, wq_out, wkv_out, dh_ref, part_ref, own_sum, sum_in, sum_mine,
    a_send, a_recv, dq_send, dq_recv, one_send, one_recv, two_send, two_recv, kv_send, kv_recv, near_send, near_recv, far_send, far_recv, fwd_send, fwd_recv, local,
    load_sem, q_send, q_recv, wkv_send, wkv_recv, s_send, s_recv, t_send, t_recv,
):
    me = lax.axis_index(AXIS)
    seq, head_dim = v_ref.shape
    tokens, width = x_ref.shape
    block = tokens * n_group
    n_block = seq // block
    half = block // 2
    fold = scale * math.log2(math.e)
    core, side = lax.rem(me, 2), lax.rem(me // 2, 2)
    member, group = lax.rem(me, n_group), me // n_group
    partner, across = me + 1 - 2 * core, me + 2 - 4 * side
    place, place_across = core * 2 + side, core * 2 + 1 - side
    place_partner, place_last = (1 - core) * 2 + side, (1 - core) * 2 + 1 - side
    upper = n_block - n_block // 2
    low = (n_block - upper) * n_group
    depth = width // n_dev
    span = math.lcm(depth, 128)
    n_col = width // span
    per_col = span // depth
    col_member = n_col // n_group
    per_member = n_dev // n_group
    n_sum = sum_mine.shape[0]
    q_cols, kv_cols = q_heads * head_dim, kv_heads * head_dim

    def piece(index):
        return rows_of(index, tokens)

    def column(head):
        return rows_of(head, head_dim)

    def cols(j):
        return rows_of(j, span)

    a_copy = Exchange(lambda peer: a_head.at[piece(peer)], lambda head: a_ref.at[:, column(head)], lambda peer: a_send.at[peer], lambda head: a_recv.at[head])
    dq_copy = Exchange(lambda peer: dq_head.at[piece(peer)], lambda head: g_ref.at[:, column(head)], lambda peer: dq_send.at[peer], lambda head: dq_recv.at[head])
    kv_copy = [
        Exchange(
            lambda i, w=w: kv_ref.at[i, w],
            lambda head, w=w: g_ref.at[:, column(q_heads + w * kv_heads + head)],
            lambda i, w=w: kv_send.at[w, i],
            lambda head, w=w: kv_recv.at[w, head],
        )
        for w in range(2)
    ]
    q_copy = Exchange(lambda peer: wq_out.at[rows_of(peer, depth)], lambda head: q_rows.at[head], lambda peer: q_send.at[peer], lambda head: q_recv.at[head])
    wkv_copy = Exchange(lambda i: wkv_out.at[rows_of(i, depth)], lambda head: kv_rows.at[head], lambda i: wkv_send.at[i], lambda head: wkv_recv.at[head])
    s_copy = Exchange(lambda peer: own_sum.at[pl.ds(peer * n_sum, n_sum)], lambda origin: sum_in.at[origin], lambda peer: s_send.at[peer], lambda origin: s_recv.at[origin])
    t_copy = Exchange(lambda peer: sum_mine, lambda origin: sum_ref.at[pl.ds(origin * n_sum, n_sum)], lambda peer: t_send.at[peer], lambda origin: t_recv.at[origin])


    def one_copy(i):
        return remote(dkv_ref.at[rows_of(i * 2 + 1 - core, half)], land_one.at[i], one_send.at[i], one_recv.at[i], partner)

    def two_copy(i):
        return remote(dkv_ref.at[piece(i * n_group + core * 2 + 1 - side)], land_two.at[i], two_send.at[i], two_recv.at[i], across)

    def near_copy(i, where):
        return remote(kvt_ref.at[i], dkvt_ref.at[:, piece(i * n_group + where)], near_send.at[i], near_recv.at[i], partner)

    def far_copy(i, where):
        return remote(kvt_ref.at[i], dkvt_ref.at[:, piece(i * n_group + where)], far_send.at[i], far_recv.at[i], across)

    def fwd_copy(i, where):
        view = dkvt_ref.at[:, piece(i * n_group + where)]
        return remote(view, view, fwd_send.at[i], fwd_recv.at[i], partner)

    def first(i):
        one_copy(i).start()

    def second(i):
        one_copy(i).wait_recv()
        for part in (1 - side, side):
            rows = piece(i * n_group + core * 2 + part)
            dkv_ref[rows, :] += land_one[i, pl.ds(pl.multiple_of(part * tokens, tokens), tokens), :]
        two_copy(i).start()

    def close(i):
        two_copy(i).wait_recv()
        rows = piece(i * n_group + place)
        total = dkv_ref[rows, :] + land_two[i]
        dkt = rotate(total[:, :head_dim].T, cos_ref[:, rows], -sin_ref[:, rows]).astype(BF16)
        dv = total[:, head_dim:].astype(BF16)
        dvt = dv.T
        kvt_ref[i, :head_dim, :], kvt_ref[i, head_dim:, :] = dkt, dvt
        dkvt_ref[:head_dim, rows], dkvt_ref[head_dim:, rows] = dkt, dvt
        kv_ref[i, 0], kv_ref[i, 1] = dkt.T, dv

    def spread(i):
        far_copy(i, place).start()
        near_copy(i, place).start()
        for copy in kv_copy:
            copy.start(i, group, i * n_group + place)

    def forward(i):
        far_copy(i, place_across).wait_recv()
        fwd_copy(i, place_across).start()

    def stages(t):
        for late, stage in ((5, forward), (4, spread), (3, close), (2, second), (1, first)):
            @pl.when((t >= late) & (t < n_block + late))
            def _():
                stage(n_block - 1 - (t - late))

    def upper_pieces(t):
        @pl.when((t >= upper) & (t < n_block))
        def _():
            to = n_block - upper + lax.rem(group + t, upper)

            def send(u):
                peer = to * n_group + lax.rem(u + me, n_group)
                a_copy.start(peer, me, peer)
                dq_copy.start(peer, me, peer)

            each(0, n_group, send)

    def lower_piece(step):
        peer = lax.rem(me + step, low)
        a_copy.start(peer, me, peer)
        dq_copy.start(peer, me, peer)

    full_barrier(n_dev)

    def attention(q_ref, k_ref, qt_ref, kt_ref, vt_ref, e_ref, dp_ref, peak_ref, dat_ref, mix_ref, acc_ref):
        def prepare(i):
            rows = rows_of(i, block)
            for raw, turned, plain in ((q_raw, qt_ref, q_ref), (k_raw, kt_ref, k_ref)):
                t = rotate(raw[rows, :].T, cos_ref[:, rows], sin_ref[:, rows]).astype(BF16)
                turned[:, rows] = t
                plain[rows, :] = t.T
            vt_ref[:, rows] = v_ref[rows, :].T
            dkv_ref[rows, :] = jnp.zeros((block, 2 * head_dim), F32)

        each(0, n_block, prepare)

        def compute(i):
            own = rows_of(i, block)
            dat_ref[...] = da_ref[own, :].T
            mix_ref[...] = jnp.zeros_like(mix_ref)
            acc_ref[...] = jnp.zeros_like(acc_ref)

            def scores(j, carry, diagonal):
                peak, total, mixed = carry
                rows = rows_of(j, block)
                s = dot(k_ref[rows, :], qt_ref[:, own])
                if diagonal:
                    s = jnp.where(causal(block), s, -1e30)
                top = jnp.maximum(peak, jnp.max(s, axis=0, keepdims=True))
                e = jnp.exp2((s - top) * fold)
                dp = dot(v_ref[rows, :], dat_ref[...])
                fade = jnp.exp2((peak - top) * fold)
                e_ref[rows, :] = e
                dp_ref[rows, :] = dp
                peak_ref[j] = top
                return top, total * fade + part_sum(e), mixed * fade + part_sum(e * dp)

            start = (jnp.full((1, block), -jnp.inf, F32), jnp.zeros((8, block), F32), jnp.zeros((8, block), F32))
            carry = lax.fori_loop(0, i, functools.partial(scores, diagonal=False), start)
            peak, total, mixed = scores(i, carry, True)
            inv = 1.0 / jnp.sum(total, axis=0, keepdims=True)
            row_dot = jnp.sum(mixed, axis=0, keepdims=True) * inv
            q_own, da_own = q_ref[own, :], da_ref[own, :]

            def grads(j):
                rows = rows_of(j, block)
                p = e_ref[rows, :] * (jnp.exp2((peak_ref[j] - peak) * fold) * inv)
                pb = p.astype(BF16)
                ds = ((dp_ref[rows, :] - row_dot) * (p * scale)).astype(BF16)
                dkv_ref[rows, :head_dim] += dot(ds, q_own)
                dkv_ref[rows, head_dim:] += dot(pb, da_own)
                mix_ref[...] += dot(vt_ref[:, rows], pb)
                acc_ref[...] += dot(kt_ref[:, rows], ds)

            each(0, i + 1, grads)
            at = mix_ref[...].astype(BF16)
            at_ref[:, own] = at
            a_head[own, :] = at.T
            dqt = rotate(acc_ref[...], cos_ref[:, own], -sin_ref[:, own]).astype(BF16)
            dqt_ref[:, own] = dqt
            dq_head[own, :] = dqt.T

        def iteration(t):
            stages(t)
            upper_pieces(t)
            compute(n_block - 1 - t)

        each(0, n_block, iteration)

    pl.run_scoped(
        attention,
        pltpu.VMEM((seq, head_dim), BF16), pltpu.VMEM((seq, head_dim), BF16),
        pltpu.VMEM((head_dim, seq), BF16), pltpu.VMEM((head_dim, seq), BF16), pltpu.VMEM((head_dim, seq), BF16),
        pltpu.VMEM((seq, block), F32), pltpu.VMEM((seq, block), F32), pltpu.VMEM((n_block, 1, block), F32),
        pltpu.VMEM((head_dim, block), BF16), pltpu.VMEM((head_dim, block), F32), pltpu.VMEM((head_dim, block), F32),
    )

    def drain_sums():
        def one(i):
            one_copy(i).wait_send()
            two_copy(i).wait_send()
            near_copy(i, place).wait_send()
            near_copy(i, place_partner).wait_recv()
            far_copy(i, place).wait_send()
            fwd_copy(i, place_across).wait_send()
            fwd_copy(i, place_last).wait_recv()
            for copy in kv_copy:
                copy.sent(i, i * n_group + place)

        def head(index):
            for copy in kv_copy:
                copy.got(index)

        each(0, n_block, one)
        each(0, kv_heads, head)

    def products(buf, wq_buf, wk_buf, wv_buf):
        counts = (n_col, n_col, col_member, n_col, n_col)
        starts = [sum(counts[:n]) for n in range(len(counts))]

        def loads(phase, j, slot):
            if phase == 3:
                pairs = ((wq_ref, wq_buf), (wk_ref, wk_buf), (wv_ref, wv_buf))
                return [pltpu.make_async_copy(ref.at[cols(j)], to.at[slot], load_sem.at[slot, n]) for n, (ref, to) in enumerate(pairs)]
            ref = (h_ref, dy_ref, h_ref, None, wo_ref)[phase]
            col = member * col_member + j if phase == 2 else j
            return [pltpu.make_async_copy(ref.at[:, cols(col)], buf.at[slot], load_sem.at[slot, 0])]

        def load(step):
            slot = lax.rem(step, n_buf)
            for phase, (begin, count) in enumerate(zip(starts, counts)):
                @pl.when((step >= begin) & (step < begin + count))
                def _():
                    for copy in loads(phase, step - begin, slot):
                        copy.start()

        def run(phase, body):
            def step(j):
                number = starts[phase] + j
                slot = lax.rem(number, n_buf)
                for copy in loads(phase, j, slot):
                    copy.wait()
                body(j, slot)
                load(number + n_buf)

            each(0, counts[phase], step)

        def sums(number):
            for late, at in enumerate((0, n_col // 4, n_col * 5 // 8, n_col - 1, 2 * n_col - 1)):
                @pl.when(number == at)
                def _():
                    stages(n_block + late)
                    if late == 1:
                        each(0, low, lower_piece)

        each(0, n_buf, load)

        def weight_columns(j, slot):
            sums(j)
            wq_out[cols(j), :] = dot(dqt_ref[...], buf[slot]).T

        run(0, weight_columns)

        def send_rows(j):
            col = lax.rem(j + me // per_col, n_col)

            def send(u):
                peer = col * per_col + lax.rem(u + me, per_col)
                q_copy.start(peer, me, peer)

            each(0, per_col, send)

        def weight_out(j, slot):
            sums(n_col + j)
            gwo_ref[:, cols(j)] = dot(at_ref[...], buf[slot])
            send_rows(j)

        run(1, weight_out)
        drain_sums()

        def weight_kv(j, slot):
            wkv_out[cols(j), :] = dot(dkvt_ref[...], buf[slot]).T

        run(2, weight_kv)

        def got_heads(head):
            a_copy.got(head)
            dq_copy.got(head)

        each(0, n_dev, got_heads)

        def send_kv(step):
            index = lax.rem(step + group, per_member)
            wkv_copy.start(index, group, member * per_member + index)

        def back(j, slot):
            @pl.when(j == 0)
            def _():
                each(0, per_member, send_kv)

            def flat(ref):
                rows = ref[slot]
                return rows.reshape(rows.shape[0], rows.shape[1] * rows.shape[2])

            grad_h = dot_t(g_ref[:, :q_cols], flat(wq_buf))
            grad_h += dot_t(g_ref[:, q_cols : q_cols + kv_cols], flat(wk_buf))
            dh_ref[:, cols(j)] = grad_h + dot_t(g_ref[:, q_cols + kv_cols :], flat(wv_buf))

        run(3, back)

        part_ref[...] = jnp.zeros_like(part_ref)
        gain = 1.0 + gain_ref[...]

        def norm(t):
            rows = rows_of(t, 16)
            grad_h, x_hat = dh_ref[rows, :], x_hat_ref[rows, :]
            grad_hat = grad_h * gain
            one = jnp.sum(grad_hat, axis=1, keepdims=True) * (1.0 / width)
            two = jnp.sum(grad_hat * x_hat, axis=1, keepdims=True) * (1.0 / width)
            back = inv_ref[rows, :] * (grad_hat - one - x_hat * two)
            gx_ref[rows, :] = (dy_own_ref[rows, :].astype(F32) + back).astype(BF16)
            part_ref[0] += part_sum(grad_h * x_hat)
            part_ref[1] += part_sum(grad_h)

        each(0, tokens // 16, norm)
        own_sum[...] = jnp.zeros_like(own_sum)
        for which in range(2):
            total = jnp.sum(part_ref[which], axis=0, keepdims=True)
            for c in range(width // 128):
                own_sum[c, pl.ds(which, 1), :] = total[:, c * 128 : (c + 1) * 128]

        def to_all(copy):
            def send(step):
                peer = lax.rem(me + step, n_dev)
                copy.start(peer, me, peer)

            each(0, n_dev, send)

        def add(origin):
            sum_mine[...] += sum_in[origin]

        def output(j, slot):
            @pl.when(j == 0)
            def _():
                to_all(s_copy)

            @pl.when(j == n_col // 2)
            def _():
                each(0, n_dev, s_copy.got)
                sum_mine[...] = jnp.zeros_like(sum_mine)
                each(0, n_dev, add)

            out_ref[:, cols(j)] = (x_ref[:, cols(j)].astype(F32) + dot(a_ref[...], buf[slot])).astype(BF16)

            @pl.when(j == n_col // 2)
            def _():
                to_all(t_copy)

        run(4, output)

    pl.run_scoped(
        products,
        pltpu.VMEM((n_buf, seq, span), BF16),
        pltpu.VMEM((n_buf, span) + wq_ref.shape[1:], BF16),
        pltpu.VMEM((n_buf, span) + wk_ref.shape[1:], BF16),
        pltpu.VMEM((n_buf, span) + wv_ref.shape[1:], BF16),
    )

    def drain(index):
        for copy in (a_copy, dq_copy, s_copy, t_copy, q_copy):
            copy.sent(index, index)
        t_copy.got(index)
        q_copy.got(index)

    def drain_kv(index):
        wkv_copy.sent(index, member * per_member + index)

    each(0, n_dev, drain)
    each(0, per_member, drain_kv)
    each(0, kv_heads, wkv_copy.got)


def main(n_dev, q, k, v, da, cos_tab, sin_tab, x_own, dy_own, x_hat, inv_std, gain, h_all, dy_all, wq, wk, wv, wo):
    seq, head_dim = q.shape
    tokens, width = x_own.shape
    q_heads, kv_heads = wq.shape[1], wk.shape[1]
    n_group = q_heads // kv_heads
    n_block = n_dev // n_group
    depth = width // n_dev
    n_buf = 3
    n_sum = -(-width // (128 * n_dev))
    sums = (n_sum * n_dev, 8, 128)
    whole, anywhere = pl.BlockSpec(memory_space=pltpu.VMEM), pl.BlockSpec(memory_space=pl.ANY)
    dma = pltpu.SemaphoreType.DMA
    return pl.pallas_call(
        functools.partial(main_kernel, n_dev, n_group, q_heads, kv_heads, n_buf, head_dim**-0.5),
        out_shape=[
            jax.ShapeDtypeStruct((tokens, width), BF16),
            jax.ShapeDtypeStruct((tokens, width), BF16),
            jax.ShapeDtypeStruct((head_dim, width), F32),
            jax.ShapeDtypeStruct((q_heads, depth, head_dim), F32),
            jax.ShapeDtypeStruct((kv_heads, depth, 2 * head_dim), F32),
            jax.ShapeDtypeStruct(sums, F32),
        ],
        in_specs=[whole] * 11 + [anywhere] * 6,
        out_specs=[whole] * 3 + [anywhere] * 2 + [whole],
        scratch_shapes=[
            pltpu.VMEM((head_dim, seq), BF16),
            pltpu.VMEM((head_dim, seq), BF16),
            pltpu.VMEM((seq, head_dim), BF16),
            pltpu.VMEM((seq, head_dim), BF16),
            pltpu.VMEM((2 * head_dim, seq), BF16),
            pltpu.VMEM((tokens, q_heads * head_dim), BF16),
            pltpu.VMEM((tokens, (q_heads + 2 * kv_heads) * head_dim), BF16),
            pltpu.VMEM((seq, 2 * head_dim), F32),
            pltpu.VMEM((n_block, tokens * n_group // 2, 2 * head_dim), F32),
            pltpu.VMEM((n_block, tokens, 2 * head_dim), F32),
            pltpu.VMEM((n_block, 2, tokens, head_dim), BF16),
            pltpu.VMEM((n_block, 2 * head_dim, tokens), BF16),
            pltpu.VMEM((width, head_dim), F32),
            pltpu.VMEM((width // n_group, 2 * head_dim), F32),
            pltpu.VMEM((tokens, width), F32),
            pltpu.VMEM((2, 8, width), F32),
            pltpu.VMEM(sums, F32),
            pltpu.VMEM((n_dev, n_sum, 8, 128), F32),
            pltpu.VMEM((n_sum, 8, 128), F32),
            dma((n_dev,)), dma((n_dev,)), dma((n_dev,)), dma((n_dev,)),
            dma((n_block,)), dma((n_block,)), dma((n_block,)), dma((n_block,)), dma((2, n_block)), dma((2, kv_heads)),
            dma((n_block,)), dma((n_block,)), dma((n_block,)), dma((n_block,)), dma((n_block,)), dma((n_block,)), dma((1,)),
            dma((n_buf, 3)), dma((n_dev,)), dma((n_dev,)), dma((n_dev // n_group,)), dma((kv_heads,)), dma((n_dev,)), dma((n_dev,)), dma((n_dev,)), dma((n_dev,)),
        ],
        compiler_params=pltpu.CompilerParams(collective_id=1, has_side_effects=True, vmem_limit_bytes=VMEM_LIMIT),
        cost_estimate=pl.CostEstimate(flops=6 * seq * seq * head_dim + 8 * seq * width * head_dim, bytes_accessed=8 * seq * width, transcendentals=seq * seq // 2),
        name="main",
    )(q, k, v, da, cos_tab, sin_tab, x_own, dy_own, x_hat, inv_std, gain, h_all, dy_all, wq, wk, wv, wo)


def solution(mesh):
    n_dev = mesh.shape[AXIS]

    def device_step(x_act, d_out, positions, ln_gain, ln_bias, w_query, w_key, w_value, w_out):
        n_batch, piece, width = x_act.shape
        q_heads, head_dim = w_query.shape[1:]
        kv_heads = w_key.shape[1]
        n_group = q_heads // kv_heads
        tokens = n_batch * piece

        x_own, dy_own = x_act.reshape(tokens, width), d_out.reshape(tokens, width)
        gain, bias = ln_gain.reshape(1, width), ln_bias.reshape(1, width)
        pos_tile = jnp.broadcast_to(positions.reshape(1, tokens), (8, tokens))
        freq = jnp.broadcast_to(frequencies(head_dim)[:, None], (head_dim // 4, tokens))
        h_all, dy_all, q, k, v, da, cos_tab, sin_tab, x_hat, inv_std = front(n_dev, n_group, x_own, dy_own, pos_tile, freq, gain, bias, w_out, w_query, w_key, w_value)
        block_out, grad_x, grad_wo, rows_wq, rows_wkv, sums = main(
            n_dev, q, k, v, da, cos_tab, sin_tab, x_own, dy_own, x_hat, inv_std, gain, h_all, dy_all, w_query, w_key, w_value, w_out
        )
        grad_wq = jnp.swapaxes(rows_wq, 0, 1)
        grad_wk = jnp.swapaxes(rows_wkv[:, :, :head_dim], 0, 1)
        grad_wv = jnp.swapaxes(rows_wkv[:, :, head_dim:], 0, 1)
        n_lane = width // 128
        grad_gain, grad_bias = sums[:n_lane, 0].reshape(width), sums[:n_lane, 1].reshape(width)
        return (block_out.reshape(x_act.shape), grad_x.reshape(x_act.shape), grad_wq, grad_wk, grad_wv, grad_wo, grad_gain, grad_bias)

    return jax.shard_map(device_step, mesh=mesh, in_specs=(P("dp", AXIS, None), P("dp", AXIS, None), P("dp", AXIS), P(None), P(None), P(None, None, None), P(None, None, None), P(None, None, None), P(None, None)), out_specs=(P("dp", AXIS, None), P("dp", AXIS, None), P(("dp", AXIS), None, None), P(("dp", AXIS), None, None), P(("dp", AXIS), None, None), P(("dp", AXIS), None), P("dp"), P("dp")), check_vma=False)
```

```python
import functools
import math

import jax
import jax.numpy as jnp
from jax import lax
from jax.experimental import pallas as pl
from jax.experimental.pallas import tpu as pltpu
from jax.sharding import PartitionSpec as P

EPS = 1e-5
ROPE_BASE = 10000.0
BLOCK = 512
AXIS = "cp"
BF16, F32 = jnp.bfloat16, jnp.float32
VMEM_LIMIT = 63 * 1024 * 1024


def frequencies(head_dim):
    quarter = head_dim // 4
    return jnp.exp(jnp.arange(quarter, dtype=F32) * (-2.0 * math.log(ROPE_BASE) / (head_dim // 2)))


def rotate(values, cos, sin):
    quarter = cos.shape[0]
    first, second = values[:quarter], values[quarter : 2 * quarter]
    return jnp.concatenate([first * cos - second * sin, second * cos + first * sin, values[2 * quarter :]], axis=0)


def rows_of(index, size):
    return pl.ds(pl.multiple_of(index * size, size), size)


def dot(lhs, rhs):
    return jnp.dot(lhs, rhs, preferred_element_type=F32)


def dot_t(lhs, rhs):
    return lax.dot_general(lhs, rhs, (((1,), (1,)), ((), ())), preferred_element_type=F32)


def full_barrier(n_dev):
    me = lax.axis_index(AXIS)
    barrier = pltpu.get_barrier_semaphore()

    def tell(step):
        pl.semaphore_signal(barrier, inc=1, device_id={AXIS: lax.rem(me + step, n_dev)}, device_id_type=pl.DeviceIdType.MESH)

    each(1, n_dev, tell)
    pl.semaphore_wait(barrier, n_dev - 1)


def remote(src, dst, send_sem, recv_sem, peer):
    return pltpu.make_async_remote_copy(src_ref=src, dst_ref=dst, send_sem=send_sem, recv_sem=recv_sem, device_id={AXIS: peer}, device_id_type=pl.DeviceIdType.MESH)


def each(lower, upper, body):
    def step(index, carry):
        body(index)
        return carry

    lax.fori_loop(lower, upper, step, 0)


class Exchange:
    def __init__(self, src, dst, send, recv):
        self.src, self.dst, self.send, self.recv = src, dst, send, recv

    def start(self, index, slot, peer):
        me = lax.axis_index(AXIS)
        src, dst, recv = self.src(index), self.dst(slot), self.recv(slot)

        @pl.when(peer != me)
        def _():
            remote(src, dst, self.send(index), recv, peer).start()

        @pl.when(peer == me)
        def _():
            pltpu.make_async_copy(src, dst, recv).start()

    def sent(self, index, peer):
        me = lax.axis_index(AXIS)

        @pl.when(peer != me)
        def _():
            remote(self.src(index), self.src(index), self.send(index), self.send(index), me).wait_send()

    def got(self, slot):
        dst = self.dst(slot)
        remote(dst, dst, self.recv(slot), self.recv(slot), lax.axis_index(AXIS)).wait_recv()


def ring_order(side):
    queue, free, order = [(0.0, True, 0, 0), (0.0, False, 0, 0)], 0.0, []
    waiting = []
    while queue or waiting:
        if queue and (not waiting or free <= waiting[0][0]):
            at, along, s, h = queue.pop(0)
            free = max(free, at) + 1.0
            waiting.append((free + 0.5, (s + along, h + 1 - along)))
        else:
            at, (s, h) = waiting.pop(0)
            order.append((s, h))
            if h == 0 and s < side - 1:
                queue.append((at, True, s, h))
            if h < side - 1:
                queue.append((at, False, s, h))
    return order


def lookup(table, index):
    out = jnp.int32(table[0])
    for key, value in enumerate(table[1:], 1):
        out = jnp.where(index == key, jnp.int32(value), out)
    return out


class Ring:
    def __init__(self, n_dev, own, everything, ring_send, ring_recv, core_send, core_recv):
        self.own, self.all = own, everything
        self.ring_send, self.ring_recv, self.core_send, self.core_recv = ring_send, ring_recv, core_send, core_recv
        self.side = math.isqrt(n_dev // 2)
        self.tokens = own.shape[0]
        self.rows = self.tokens // 4
        self.me = lax.axis_index(AXIS)
        self.core = lax.rem(self.me, 2)
        self.x, self.y = lax.rem(self.me // 2, self.side), self.me // (2 * self.side)

    def device(self, colour, along, across, core):
        side = self.side
        x_first = 1 - colour // 2
        sign = 1 - 2 * lax.rem(colour, 2)
        dx = x_first * along + (1 - x_first) * across
        dy = x_first * across + (1 - x_first) * along
        x = lax.rem(self.x - sign * dx + 2 * side, side)
        y = lax.rem(self.y - sign * dy + 2 * side, side)
        return (y * side + x) * 2 + core

    def place(self, colour, s, h, core):
        return pl.ds(pl.multiple_of(self.device(colour, s, h, core) * self.tokens + colour * self.rows, self.rows), self.rows)

    def piece(self, colour, s, h):
        return self.all.at[self.place(colour, s, h, self.core)]

    def number(self, s, h):
        return s * self.side + h

    def ring_copy(self, colour, s, h, along, src=None):
        number = self.number(s + along, h + 1 - along)
        dst = self.piece(colour, s, h)
        peer = self.device(colour, -along, along - 1, self.core)
        return remote(dst if src is None else src, dst, self.ring_send.at[colour, number], self.ring_recv.at[colour, number], peer)

    def core_copy(self, colour, s, h, src=None):
        number = self.number(s, h)
        dst = self.piece(colour, s, h)
        return remote(dst if src is None else src, dst, self.core_send.at[colour, number], self.core_recv.at[colour, number], self.me + 1 - 2 * self.core)

    def arrival(self, colour, s, h):
        number = self.number(s, h)
        dst = self.piece(colour, s, h)
        return remote(dst, dst, self.ring_send.at[colour, number], self.ring_recv.at[colour, number], self.me)

    def core_arrival(self, colour, s, h):
        number = self.number(s, h)
        dst = self.all.at[self.place(colour, s, h, 1 - self.core)]
        return remote(dst, dst, self.core_send.at[colour, number], self.core_recv.at[colour, number], self.me)

    def begin(self):
        def one(colour):
            src = self.own.at[rows_of(colour, self.rows)]
            self.ring_copy(colour, 0, 0, 1, src).start()
            self.ring_copy(colour, 0, 0, 0, src).start()

        def other(colour):
            self.core_copy(colour, 0, 0, self.own.at[rows_of(colour, self.rows)]).start()

        each(0, 4, one)
        each(0, 4, other)

    def pass_on(self, s, h):
        def one(colour):
            self.arrival(colour, s, h).wait_recv()

            @pl.when((h == 0) & (s < self.side - 1))
            def _():
                self.ring_copy(colour, s, h, 1).start()

            @pl.when(h < self.side - 1)
            def _():
                self.ring_copy(colour, s, h, 0).start()

            self.core_copy(colour, s, h).start()

        each(0, 4, one)

    def got_core(self, s, h):
        each(0, 4, lambda colour: self.core_arrival(colour, s, h).wait_recv())

    def end(self):
        def sent(number):
            s, h = number // self.side, lax.rem(number, self.side)

            def one(colour):
                @pl.when((s > 0) | (h > 0))
                def _():
                    self.arrival(colour, s, h).wait_send()

                self.core_copy(colour, s, h).wait_send()

            each(0, 4, one)

        each(0, self.side * self.side, sent)


def front_kernel(
    n_dev, n_group, x_ref, dy_ref, pos_ref, freq_ref, gain_ref, bias_ref, wo_ref, wq_ref, wk_ref, wv_ref,
    h_all, dy_all, q_ref, k_ref, v_ref, da_ref, cos_ref, sin_ref, x_hat_ref, inv_ref,
    h_own, w_ref, wo_own, pick_ref, w_buf, h_buf, dy_buf, pos_in,
    h_send, h_recv, h_core_send, h_core_recv, dy_send, dy_recv, dy_core_send, dy_core_recv, w_sem, h_sem, dy_sem, pos_send, pos_recv, local,
):
    me = lax.axis_index(AXIS)
    tokens, width = x_ref.shape
    head_dim = v_ref.shape[1]
    heads_tile = w_buf.shape[2]
    d_block = w_buf.shape[1]
    h_ring = Ring(n_dev, h_own, h_all, h_send, h_recv, h_core_send, h_core_recv)
    dy_ring = Ring(n_dev, dy_ref, dy_all, dy_send, dy_recv, dy_core_send, dy_core_recv)
    rows_n = h_ring.rows
    order = [(0, 0)] + ring_order(h_ring.side)
    n_event = len(order)
    where = Exchange(lambda peer: pos_ref, lambda origin: pos_in.at[origin], lambda peer: pos_send.at[peer], lambda origin: pos_recv.at[origin])

    n_d = width // d_block
    kv_head = me // n_group

    def w_load(t, which):
        ref, head = ((wq_ref, me), (wk_ref, kv_head), (wv_ref, kv_head))[which]
        slot = lax.rem(t, 2)
        return pltpu.make_async_copy(ref.at[rows_of(t, d_block), rows_of(head // heads_tile, heads_tile)], w_buf.at[slot], w_sem.at[slot])

    own_dy = pltpu.make_async_copy(dy_ref, dy_all.at[rows_of(me, tokens)], local.at[0])
    own_h = pltpu.make_async_copy(h_own, h_all.at[rows_of(me, tokens)], local.at[1])
    own_wo = pltpu.make_async_copy(wo_ref.at[rows_of(me, head_dim)], wo_own, local.at[2])
    own_dy.start()
    own_wo.start()
    w_load(0, 0).start()
    full_barrier(n_dev)
    dy_ring.begin()

    gain, bias = 1.0 + gain_ref[...], bias_ref[...]

    def norm(t):
        rows = rows_of(t, 16)
        x = x_ref[rows, :].astype(F32)
        centered = x - jnp.sum(x, axis=1, keepdims=True) * (1.0 / width)
        inv = lax.rsqrt(jnp.sum(centered * centered, axis=1, keepdims=True) * (1.0 / width) + EPS)
        x_hat = centered * inv
        x_hat_ref[rows, :] = x_hat
        inv_ref[rows, :] = inv
        h_own[rows, :] = (x_hat * gain + bias).astype(BF16)

    each(0, tokens // 16, norm)

    def send_pos(step):
        peer = lax.rem(me + step, n_dev)
        where.start(peer, me, peer)

    each(0, n_dev, send_pos)
    h_ring.begin()
    own_h.start()

    for which in range(3):
        head = me if which == 0 else kv_head

        def pick(t):
            @pl.when(t + 1 < n_d)
            def _():
                w_load(t + 1, which).start()

            w_load(t, which).wait()
            pick_ref[...] = jnp.swapaxes(w_buf[lax.rem(t, 2)], 0, 1)
            w_ref[rows_of(t, d_block), which * head_dim : (which + 1) * head_dim] = pick_ref[lax.rem(head, heads_tile)]

        each(0, n_d, pick)
        if which < 2:
            w_load(0, which + 1).start()
        if which == 0:
            dy_ring.pass_on(*(jnp.int32(v) for v in order[1]))
        if which == 1:
            h_ring.pass_on(*(jnp.int32(v) for v in order[1]))
    own_wo.wait()
    own_dy.wait()
    own_h.wait()

    def tables(origin):
        where.got(origin)
        angles = freq_ref[...] * pos_in[origin, 0:1, :].astype(F32)
        cos_ref[:, rows_of(origin, tokens)] = jnp.cos(angles)
        sin_ref[:, rows_of(origin, tokens)] = jnp.sin(angles)

    def event(e):
        return lookup([p[0] for p in order], e), lookup([p[1] for p in order], e)

    def places_of(ring, s, h):
        return [ring.place(jnp.int32(colour), s, h, core) for colour in range(4) for core in range(2)]

    def fetch(ring, buf, sem, e):
        slot = lax.rem(e, 2)
        s, h = event(e)
        ring.got_core(s, h)
        for n, place in enumerate(places_of(ring, s, h)):
            pltpu.make_async_copy(ring.all.at[place], buf.at[slot, pl.ds(n * rows_n, rows_n)], sem.at[slot]).start()

    def fetched(ring, buf, sem, e):
        slot = lax.rem(e, 2)
        pltpu.make_async_copy(ring.all.at[pl.ds(0, 8 * rows_n)], buf.at[slot], sem.at[slot]).wait()
        return buf[slot]

    def gradient_rows(e):
        s, h = event(e)
        da = dot_t(fetched(dy_ring, dy_buf, dy_sem, e), wo_own[...]).astype(BF16)
        for n, place in enumerate(places_of(dy_ring, s, h)):
            da_ref[place, :] = da[n * rows_n : (n + 1) * rows_n]

    def project_rows(e):
        s, h = event(e)
        out = dot(fetched(h_ring, h_buf, h_sem, e), w_ref[...])
        for n, place in enumerate(places_of(h_ring, s, h)):
            part = out[n * rows_n : (n + 1) * rows_n]
            q_ref[place, :] = part[:, :head_dim]
            k_ref[place, :] = part[:, head_dim : 2 * head_dim]
            v_ref[place, :] = part[:, 2 * head_dim :].astype(BF16)

    def step(e):
        for ring, buf, sem, rows in ((dy_ring, dy_buf, dy_sem, gradient_rows), (h_ring, h_buf, h_sem, project_rows)):
            @pl.when((e > 1) & (e < n_event))
            def _():
                ring.pass_on(*event(e))

            @pl.when((e > 0) & (e <= n_event))
            def _():
                fetch(ring, buf, sem, e - 1)

            @pl.when(e > 1)
            def _():
                rows(e - 2)

        @pl.when(e == 3)
        def _():
            each(0, n_dev, tables)

    each(1, n_event + 2, step)
    h_ring.end()
    dy_ring.end()
    each(0, n_dev, lambda index: where.sent(index, index))


def front(n_dev, n_group, x_own, dy_own, positions, freq, gain, bias, w_out, w_query, w_key, w_value):
    tokens, width = x_own.shape
    head_dim = w_query.shape[2]
    seq = tokens * n_dev
    heads_tile = min(8, w_key.shape[1])
    d_block = 384
    pieces = math.isqrt(n_dev // 2) ** 2
    whole, anywhere = pl.BlockSpec(memory_space=pltpu.VMEM), pl.BlockSpec(memory_space=pl.ANY)
    dma = pltpu.SemaphoreType.DMA
    return pl.pallas_call(
        functools.partial(front_kernel, n_dev, n_group),
        out_shape=[
            jax.ShapeDtypeStruct((seq, width), BF16),
            jax.ShapeDtypeStruct((seq, width), BF16),
            jax.ShapeDtypeStruct((seq, head_dim), F32),
            jax.ShapeDtypeStruct((seq, head_dim), F32),
            jax.ShapeDtypeStruct((seq, head_dim), BF16),
            jax.ShapeDtypeStruct((seq, head_dim), BF16),
            jax.ShapeDtypeStruct((head_dim // 4, seq), F32),
            jax.ShapeDtypeStruct((head_dim // 4, seq), F32),
            jax.ShapeDtypeStruct((tokens, width), F32),
            jax.ShapeDtypeStruct((tokens, 1), F32),
        ],
        in_specs=[whole] * 6 + [anywhere] * 4,
        out_specs=[anywhere] * 2 + [whole] * 8,
        scratch_shapes=[
            pltpu.VMEM((tokens, width), BF16),
            pltpu.VMEM((width, 3 * head_dim), BF16),
            pltpu.VMEM((head_dim, width), BF16),
            pltpu.VMEM((heads_tile, d_block, head_dim), BF16),
            pltpu.VMEM((2, d_block, heads_tile, head_dim), BF16),
            pltpu.VMEM((2, 2 * tokens, width), BF16),
            pltpu.VMEM((2, 2 * tokens, width), BF16),
            pltpu.VMEM((n_dev,) + positions.shape, jnp.int32),
            dma((4, pieces)), dma((4, pieces)), dma((4, pieces)), dma((4, pieces)),
            dma((4, pieces)), dma((4, pieces)), dma((4, pieces)), dma((4, pieces)),
            dma((2,)), dma((2,)), dma((2,)), dma((n_dev,)), dma((n_dev,)), dma((3,)),
        ],
        compiler_params=pltpu.CompilerParams(collective_id=3, has_side_effects=True, vmem_limit_bytes=VMEM_LIMIT),
        cost_estimate=pl.CostEstimate(flops=8 * seq * width * head_dim, bytes_accessed=8 * seq * width, transcendentals=0),
        name="front",
    )(x_own, dy_own, positions, freq, gain, bias, w_out, w_query, w_key, w_value)


def causal(block):
    key = lax.broadcasted_iota(jnp.int32, (block, block), 0)
    query = lax.broadcasted_iota(jnp.int32, (block, block), 1)
    return key <= query


def part_sum(values):
    return jnp.sum(values.reshape(values.shape[0] // 8, 8, values.shape[1]), axis=0)


def main_kernel(
    n_dev, n_group, q_heads, kv_heads, n_buf, scale,
    q_raw, k_raw, v_ref, da_ref, cos_ref, sin_ref, x_ref, dy_own_ref, x_hat_ref, inv_ref, gain_ref, h_ref, dy_ref, wq_ref, wk_ref, wv_ref, wo_ref,
    out_ref, gx_ref, gwo_ref, q_rows, kv_rows, sum_ref,
    at_ref, dqt_ref, a_head, dq_head, dkvt_ref, a_ref, g_ref, dkv_ref, land_one, land_two, kv_ref, kvt_ref, wq_out, wkv_out, dh_ref, part_ref, own_sum, sum_in, sum_mine,
    a_send, a_recv, dq_send, dq_recv, one_send, one_recv, two_send, two_recv, kv_send, kv_recv, near_send, near_recv, far_send, far_recv, fwd_send, fwd_recv, local,
    load_sem, q_send, q_recv, wkv_send, wkv_recv, s_send, s_recv, t_send, t_recv,
):
    me = lax.axis_index(AXIS)
    seq, head_dim = v_ref.shape
    tokens, width = x_ref.shape
    block = tokens * n_group
    n_block = seq // block
    half = block // 2
    fold = scale * math.log2(math.e)
    core, side = lax.rem(me, 2), lax.rem(me // 2, 2)
    member, group = lax.rem(me, n_group), me // n_group
    partner, across = me + 1 - 2 * core, me + 2 - 4 * side
    place, place_across = core * 2 + side, core * 2 + 1 - side
    place_partner, place_last = (1 - core) * 2 + side, (1 - core) * 2 + 1 - side
    shift = lax.rem(group, max(2, n_block * 3 // 4))
    depth = width // n_dev
    span = math.lcm(depth, 128)
    n_col = width // span
    per_col = span // depth
    col_member = n_col // n_group
    per_member = n_dev // n_group
    n_sum = sum_mine.shape[0]
    q_cols, kv_cols = q_heads * head_dim, kv_heads * head_dim

    def piece(index):
        return rows_of(index, tokens)

    def column(head):
        return rows_of(head, head_dim)

    def cols(j):
        return rows_of(j, span)

    a_copy = Exchange(lambda peer: a_head.at[piece(peer)], lambda head: a_ref.at[:, column(head)], lambda peer: a_send.at[peer], lambda head: a_recv.at[head])
    dq_copy = Exchange(lambda peer: dq_head.at[piece(peer)], lambda head: g_ref.at[:, column(head)], lambda peer: dq_send.at[peer], lambda head: dq_recv.at[head])
    kv_copy = [
        Exchange(
            lambda i, w=w: kv_ref.at[i, w],
            lambda head, w=w: g_ref.at[:, column(q_heads + w * kv_heads + head)],
            lambda i, w=w: kv_send.at[w, i],
            lambda head, w=w: kv_recv.at[w, head],
        )
        for w in range(2)
    ]
    q_copy = Exchange(lambda peer: wq_out.at[rows_of(peer, depth)], lambda head: q_rows.at[head], lambda peer: q_send.at[peer], lambda head: q_recv.at[head])
    wkv_copy = Exchange(lambda i: wkv_out.at[rows_of(i, depth)], lambda head: kv_rows.at[head], lambda i: wkv_send.at[i], lambda head: wkv_recv.at[head])
    s_copy = Exchange(lambda peer: own_sum.at[pl.ds(peer * n_sum, n_sum)], lambda origin: sum_in.at[origin], lambda peer: s_send.at[peer], lambda origin: s_recv.at[origin])
    t_copy = Exchange(lambda peer: sum_mine, lambda origin: sum_ref.at[pl.ds(origin * n_sum, n_sum)], lambda peer: t_send.at[peer], lambda origin: t_recv.at[origin])


    def one_copy(i):
        return remote(dkv_ref.at[rows_of(i * 2 + 1 - core, half)], land_one.at[i], one_send.at[i], one_recv.at[i], partner)

    def two_copy(i):
        return remote(dkv_ref.at[piece(i * n_group + core * 2 + 1 - side)], land_two.at[i], two_send.at[i], two_recv.at[i], across)

    def near_copy(i, where):
        return remote(kvt_ref.at[i], dkvt_ref.at[:, piece(i * n_group + where)], near_send.at[i], near_recv.at[i], partner)

    def far_copy(i, where):
        return remote(kvt_ref.at[i], dkvt_ref.at[:, piece(i * n_group + where)], far_send.at[i], far_recv.at[i], across)

    def fwd_copy(i, where):
        view = dkvt_ref.at[:, piece(i * n_group + where)]
        return remote(view, view, fwd_send.at[i], fwd_recv.at[i], partner)

    def first(i):
        one_copy(i).start()

    def second(i):
        one_copy(i).wait_recv()
        for part in (1 - side, side):
            rows = piece(i * n_group + core * 2 + part)
            dkv_ref[rows, :] += land_one[i, pl.ds(pl.multiple_of(part * tokens, tokens), tokens), :]
        two_copy(i).start()

    def close(i):
        two_copy(i).wait_recv()
        rows = piece(i * n_group + place)
        total = dkv_ref[rows, :] + land_two[i]
        dkt = rotate(total[:, :head_dim].T, cos_ref[:, rows], -sin_ref[:, rows]).astype(BF16)
        dv = total[:, head_dim:].astype(BF16)
        dvt = dv.T
        kvt_ref[i, :head_dim, :], kvt_ref[i, head_dim:, :] = dkt, dvt
        dkvt_ref[:head_dim, rows], dkvt_ref[head_dim:, rows] = dkt, dvt
        kv_ref[i, 0], kv_ref[i, 1] = dkt.T, dv

    def spread(i):
        far_copy(i, place).start()
        near_copy(i, place).start()
        for copy in kv_copy:
            copy.start(i, group, i * n_group + place)

    def forward(i):
        far_copy(i, place_across).wait_recv()
        fwd_copy(i, place_across).start()

    steps = (first, second, close, spread, forward)

    def block_at(t):
        return lax.rem(shift - 1 - t + 2 * n_block, n_block)

    def stages(t):
        for late in range(len(steps), 0, -1):
            n = t - late - shift

            @pl.when(n >= 0)
            def _():
                steps[late - 1](n_block - 1 - n)

    def stage_rest(late):
        each(jnp.maximum(n_block - late - shift, 0), n_block, lambda n: steps[late - 1](n_block - 1 - n))

    def send_pieces(i):
        def send(u):
            peer = i * n_group + lax.rem(u + me, n_group)
            a_copy.start(peer, me, peer)
            dq_copy.start(peer, me, peer)

        each(0, n_group, send)

    full_barrier(n_dev)

    def attention(q_ref, k_ref, qt_ref, kt_ref, vt_ref, e_ref, dp_ref, peak_ref, dat_ref, mix_ref, acc_ref):
        def prepare(i):
            rows = rows_of(i, block)
            for raw, turned, plain in ((q_raw, qt_ref, q_ref), (k_raw, kt_ref, k_ref)):
                t = rotate(raw[rows, :].T, cos_ref[:, rows], sin_ref[:, rows]).astype(BF16)
                turned[:, rows] = t
                plain[rows, :] = t.T
            vt_ref[:, rows] = v_ref[rows, :].T
            dkv_ref[rows, :] = jnp.zeros((block, 2 * head_dim), F32)

        each(0, n_block, prepare)

        def compute(i):
            own = rows_of(i, block)
            dat_ref[...] = da_ref[own, :].T
            mix_ref[...] = jnp.zeros_like(mix_ref)
            acc_ref[...] = jnp.zeros_like(acc_ref)

            def scores(j, carry, diagonal):
                peak, total, mixed = carry
                rows = rows_of(j, block)
                s = dot(k_ref[rows, :], qt_ref[:, own])
                if diagonal:
                    s = jnp.where(causal(block), s, -1e30)
                top = jnp.maximum(peak, jnp.max(s, axis=0, keepdims=True))
                e = jnp.exp2((s - top) * fold)
                dp = dot(v_ref[rows, :], dat_ref[...])
                fade = jnp.exp2((peak - top) * fold)
                e_ref[rows, :] = e
                dp_ref[rows, :] = dp
                peak_ref[j] = top
                return top, total * fade + part_sum(e), mixed * fade + part_sum(e * dp)

            start = (jnp.full((1, block), -jnp.inf, F32), jnp.zeros((8, block), F32), jnp.zeros((8, block), F32))
            carry = lax.fori_loop(0, i, functools.partial(scores, diagonal=False), start)
            peak, total, mixed = scores(i, carry, True)
            inv = 1.0 / jnp.sum(total, axis=0, keepdims=True)
            row_dot = jnp.sum(mixed, axis=0, keepdims=True) * inv
            q_own, da_own = q_ref[own, :], da_ref[own, :]

            def grads(j):
                rows = rows_of(j, block)
                p = e_ref[rows, :] * (jnp.exp2((peak_ref[j] - peak) * fold) * inv)
                pb = p.astype(BF16)
                ds = ((dp_ref[rows, :] - row_dot) * (p * scale)).astype(BF16)
                dkv_ref[rows, :head_dim] += dot(ds, q_own)
                dkv_ref[rows, head_dim:] += dot(pb, da_own)
                mix_ref[...] += dot(vt_ref[:, rows], pb)
                acc_ref[...] += dot(kt_ref[:, rows], ds)

            each(0, i + 1, grads)
            at = mix_ref[...].astype(BF16)
            at_ref[:, own] = at
            a_head[own, :] = at.T
            dqt = rotate(acc_ref[...], cos_ref[:, own], -sin_ref[:, own]).astype(BF16)
            dqt_ref[:, own] = dqt
            dq_head[own, :] = dqt.T

        def iteration(t):
            stages(t)

            @pl.when(t > 0)
            def _():
                send_pieces(block_at(t - 1))

            compute(block_at(t))

        each(0, n_block, iteration)

    pl.run_scoped(
        attention,
        pltpu.VMEM((seq, head_dim), BF16), pltpu.VMEM((seq, head_dim), BF16),
        pltpu.VMEM((head_dim, seq), BF16), pltpu.VMEM((head_dim, seq), BF16), pltpu.VMEM((head_dim, seq), BF16),
        pltpu.VMEM((seq, block), F32), pltpu.VMEM((seq, block), F32), pltpu.VMEM((n_block, 1, block), F32),
        pltpu.VMEM((head_dim, block), BF16), pltpu.VMEM((head_dim, block), F32), pltpu.VMEM((head_dim, block), F32),
    )

    def drain_sums():
        def one(i):
            one_copy(i).wait_send()
            two_copy(i).wait_send()
            near_copy(i, place).wait_send()
            near_copy(i, place_partner).wait_recv()
            far_copy(i, place).wait_send()
            fwd_copy(i, place_across).wait_send()
            fwd_copy(i, place_last).wait_recv()
            for copy in kv_copy:
                copy.sent(i, i * n_group + place)

        def head(index):
            for copy in kv_copy:
                copy.got(index)

        each(0, n_block, one)
        each(0, kv_heads, head)

    stage_rest(1)
    send_pieces(block_at(n_block - 1))

    def products(buf, wq_buf, wk_buf, wv_buf):
        counts = (n_col, n_col, n_col, col_member, n_col, n_col)
        starts = [sum(counts[:n]) for n in range(len(counts))]

        def loads(phase, j, slot):
            if phase == 2:
                return [pltpu.make_async_copy(wq_ref.at[cols(j)], wq_buf.at[slot], load_sem.at[slot, 0])]
            if phase == 4:
                pairs = ((wk_ref, wk_buf), (wv_ref, wv_buf))
                return [pltpu.make_async_copy(ref.at[cols(j)], to.at[slot], load_sem.at[slot, n]) for n, (ref, to) in enumerate(pairs)]
            ref = (h_ref, dy_ref, None, h_ref, None, wo_ref)[phase]
            col = member * col_member + j if phase == 3 else j
            return [pltpu.make_async_copy(ref.at[:, cols(col)], buf.at[slot], load_sem.at[slot, 0])]

        def load(step):
            slot = lax.rem(step, n_buf)
            for phase, (begin, count) in enumerate(zip(starts, counts)):
                @pl.when((step >= begin) & (step < begin + count))
                def _():
                    for copy in loads(phase, step - begin, slot):
                        copy.start()

        def run(phase, body):
            def step(j):
                number = starts[phase] + j
                slot = lax.rem(number, n_buf)
                for copy in loads(phase, j, slot):
                    copy.wait()
                body(j, slot)
                load(number + n_buf)

            each(0, counts[phase], step)

        each(0, n_buf, load)

        def weight_columns(j, slot):
            @pl.when(j == n_col // 4)
            def _():
                stage_rest(2)

            wq_out[cols(j), :] = dot(dqt_ref[...], buf[slot]).T

        run(0, weight_columns)

        def send_rows(j):
            col = lax.rem(j + me // per_col, n_col)

            def send(u):
                peer = col * per_col + lax.rem(u + me, per_col)
                q_copy.start(peer, me, peer)

            each(0, per_col, send)

        def weight_out(j, slot):
            @pl.when(j < n_col // 2)
            def _():
                send_rows(j)

            gwo_ref[:, cols(j)] = dot(at_ref[...], buf[slot])

        run(1, weight_out)

        def got_heads(head):
            a_copy.got(head)
            dq_copy.got(head)

        each(0, n_dev, got_heads)

        def flat(ref, slot):
            rows = ref[slot]
            return rows.reshape(rows.shape[0], rows.shape[1] * rows.shape[2])

        def back_query(j, slot):
            for late, at in ((3, n_col // 4), (4, n_col * 3 // 8), (5, n_col * 3 // 4)):
                @pl.when(j == at)
                def _():
                    stage_rest(late)

            @pl.when(j >= n_col // 2)
            def _():
                send_rows(j)

            dh_ref[:, cols(j)] = dot_t(g_ref[:, :q_cols], flat(wq_buf, slot))

        run(2, back_query)
        drain_sums()

        def weight_kv(j, slot):
            wkv_out[cols(j), :] = dot(dkvt_ref[...], buf[slot]).T

        run(3, weight_kv)

        def send_kv(step):
            index = lax.rem(step + group, per_member)
            wkv_copy.start(index, group, member * per_member + index)

        def back_kv(j, slot):
            @pl.when(j == 0)
            def _():
                each(0, per_member, send_kv)

            grad_h = dot_t(g_ref[:, q_cols : q_cols + kv_cols], flat(wk_buf, slot))
            dh_ref[:, cols(j)] += grad_h + dot_t(g_ref[:, q_cols + kv_cols :], flat(wv_buf, slot))

        run(4, back_kv)

        part_ref[...] = jnp.zeros_like(part_ref)
        gain = 1.0 + gain_ref[...]

        def norm(t):
            rows = rows_of(t, 16)
            grad_h, x_hat = dh_ref[rows, :], x_hat_ref[rows, :]
            grad_hat = grad_h * gain
            one = jnp.sum(grad_hat, axis=1, keepdims=True) * (1.0 / width)
            two = jnp.sum(grad_hat * x_hat, axis=1, keepdims=True) * (1.0 / width)
            back = inv_ref[rows, :] * (grad_hat - one - x_hat * two)
            gx_ref[rows, :] = (dy_own_ref[rows, :].astype(F32) + back).astype(BF16)
            part_ref[0] += part_sum(grad_h * x_hat)
            part_ref[1] += part_sum(grad_h)

        each(0, tokens // 16, norm)
        own_sum[...] = jnp.zeros_like(own_sum)
        for which in range(2):
            total = jnp.sum(part_ref[which], axis=0, keepdims=True)
            for c in range(width // 128):
                own_sum[c, pl.ds(which, 1), :] = total[:, c * 128 : (c + 1) * 128]

        def to_all(copy):
            def send(step):
                peer = lax.rem(me + step, n_dev)
                copy.start(peer, me, peer)

            each(0, n_dev, send)

        def add(origin):
            sum_mine[...] += sum_in[origin]

        def output(j, slot):
            @pl.when(j == 0)
            def _():
                to_all(s_copy)

            @pl.when(j == n_col // 2)
            def _():
                each(0, n_dev, s_copy.got)
                sum_mine[...] = jnp.zeros_like(sum_mine)
                each(0, n_dev, add)

            out_ref[:, cols(j)] = (x_ref[:, cols(j)].astype(F32) + dot(a_ref[...], buf[slot])).astype(BF16)

            @pl.when(j == n_col // 2)
            def _():
                to_all(t_copy)

        run(5, output)

    pl.run_scoped(
        products,
        pltpu.VMEM((n_buf, seq, span), BF16),
        pltpu.VMEM((n_buf, span) + wq_ref.shape[1:], BF16),
        pltpu.VMEM((n_buf, span) + wk_ref.shape[1:], BF16),
        pltpu.VMEM((n_buf, span) + wv_ref.shape[1:], BF16),
    )

    def drain(index):
        for copy in (a_copy, dq_copy, s_copy, t_copy, q_copy):
            copy.sent(index, index)
        t_copy.got(index)
        q_copy.got(index)

    def drain_kv(index):
        wkv_copy.sent(index, member * per_member + index)

    each(0, n_dev, drain)
    each(0, per_member, drain_kv)
    each(0, kv_heads, wkv_copy.got)


def main(n_dev, q, k, v, da, cos_tab, sin_tab, x_own, dy_own, x_hat, inv_std, gain, h_all, dy_all, wq, wk, wv, wo):
    seq, head_dim = q.shape
    tokens, width = x_own.shape
    q_heads, kv_heads = wq.shape[1], wk.shape[1]
    n_group = q_heads // kv_heads
    n_block = n_dev // n_group
    depth = width // n_dev
    n_buf = 3
    n_sum = -(-width // (128 * n_dev))
    sums = (n_sum * n_dev, 8, 128)
    whole, anywhere = pl.BlockSpec(memory_space=pltpu.VMEM), pl.BlockSpec(memory_space=pl.ANY)
    dma = pltpu.SemaphoreType.DMA
    return pl.pallas_call(
        functools.partial(main_kernel, n_dev, n_group, q_heads, kv_heads, n_buf, head_dim**-0.5),
        out_shape=[
            jax.ShapeDtypeStruct((tokens, width), BF16),
            jax.ShapeDtypeStruct((tokens, width), BF16),
            jax.ShapeDtypeStruct((head_dim, width), F32),
            jax.ShapeDtypeStruct((q_heads, depth, head_dim), F32),
            jax.ShapeDtypeStruct((kv_heads, depth, 2 * head_dim), F32),
            jax.ShapeDtypeStruct(sums, F32),
        ],
        in_specs=[whole] * 11 + [anywhere] * 6,
        out_specs=[whole] * 3 + [anywhere] * 2 + [whole],
        scratch_shapes=[
            pltpu.VMEM((head_dim, seq), BF16),
            pltpu.VMEM((head_dim, seq), BF16),
            pltpu.VMEM((seq, head_dim), BF16),
            pltpu.VMEM((seq, head_dim), BF16),
            pltpu.VMEM((2 * head_dim, seq), BF16),
            pltpu.VMEM((tokens, q_heads * head_dim), BF16),
            pltpu.VMEM((tokens, (q_heads + 2 * kv_heads) * head_dim), BF16),
            pltpu.VMEM((seq, 2 * head_dim), F32),
            pltpu.VMEM((n_block, tokens * n_group // 2, 2 * head_dim), F32),
            pltpu.VMEM((n_block, tokens, 2 * head_dim), F32),
            pltpu.VMEM((n_block, 2, tokens, head_dim), BF16),
            pltpu.VMEM((n_block, 2 * head_dim, tokens), BF16),
            pltpu.VMEM((width, head_dim), F32),
            pltpu.VMEM((width // n_group, 2 * head_dim), F32),
            pltpu.VMEM((tokens, width), F32),
            pltpu.VMEM((2, 8, width), F32),
            pltpu.VMEM(sums, F32),
            pltpu.VMEM((n_dev, n_sum, 8, 128), F32),
            pltpu.VMEM((n_sum, 8, 128), F32),
            dma((n_dev,)), dma((n_dev,)), dma((n_dev,)), dma((n_dev,)),
            dma((n_block,)), dma((n_block,)), dma((n_block,)), dma((n_block,)), dma((2, n_block)), dma((2, kv_heads)),
            dma((n_block,)), dma((n_block,)), dma((n_block,)), dma((n_block,)), dma((n_block,)), dma((n_block,)), dma((1,)),
            dma((n_buf, 3)), dma((n_dev,)), dma((n_dev,)), dma((n_dev // n_group,)), dma((kv_heads,)), dma((n_dev,)), dma((n_dev,)), dma((n_dev,)), dma((n_dev,)),
        ],
        compiler_params=pltpu.CompilerParams(collective_id=1, has_side_effects=True, vmem_limit_bytes=VMEM_LIMIT),
        cost_estimate=pl.CostEstimate(flops=6 * seq * seq * head_dim + 8 * seq * width * head_dim, bytes_accessed=8 * seq * width, transcendentals=seq * seq // 2),
        name="main",
    )(q, k, v, da, cos_tab, sin_tab, x_own, dy_own, x_hat, inv_std, gain, h_all, dy_all, wq, wk, wv, wo)


def solution(mesh):
    n_dev = mesh.shape[AXIS]

    def device_step(x_act, d_out, positions, ln_gain, ln_bias, w_query, w_key, w_value, w_out):
        n_batch, piece, width = x_act.shape
        q_heads, head_dim = w_query.shape[1:]
        kv_heads = w_key.shape[1]
        n_group = q_heads // kv_heads
        tokens = n_batch * piece

        x_own, dy_own = x_act.reshape(tokens, width), d_out.reshape(tokens, width)
        gain, bias = ln_gain.reshape(1, width), ln_bias.reshape(1, width)
        pos_tile = jnp.broadcast_to(positions.reshape(1, tokens), (8, tokens))
        freq = jnp.broadcast_to(frequencies(head_dim)[:, None], (head_dim // 4, tokens))
        h_all, dy_all, q, k, v, da, cos_tab, sin_tab, x_hat, inv_std = front(n_dev, n_group, x_own, dy_own, pos_tile, freq, gain, bias, w_out, w_query, w_key, w_value)
        block_out, grad_x, grad_wo, rows_wq, rows_wkv, sums = main(
            n_dev, q, k, v, da, cos_tab, sin_tab, x_own, dy_own, x_hat, inv_std, gain, h_all, dy_all, w_query, w_key, w_value, w_out
        )
        grad_wq = jnp.swapaxes(rows_wq, 0, 1)
        grad_wk = jnp.swapaxes(rows_wkv[:, :, :head_dim], 0, 1)
        grad_wv = jnp.swapaxes(rows_wkv[:, :, head_dim:], 0, 1)
        n_lane = width // 128
        grad_gain, grad_bias = sums[:n_lane, 0].reshape(width), sums[:n_lane, 1].reshape(width)
        return (block_out.reshape(x_act.shape), grad_x.reshape(x_act.shape), grad_wq, grad_wk, grad_wv, grad_wo, grad_gain, grad_bias)

    return jax.shard_map(device_step, mesh=mesh, in_specs=(P("dp", AXIS, None), P("dp", AXIS, None), P("dp", AXIS), P(None), P(None), P(None, None, None), P(None, None, None), P(None, None, None), P(None, None)), out_specs=(P("dp", AXIS, None), P("dp", AXIS, None), P(("dp", AXIS), None, None), P(("dp", AXIS), None, None), P(("dp", AXIS), None, None), P(("dp", AXIS), None), P("dp"), P("dp")), check_vma=False)
```

```python
import functools
import math

import jax
import jax.numpy as jnp
from jax import lax
from jax.experimental import pallas as pl
from jax.experimental.pallas import tpu as pltpu
from jax.sharding import PartitionSpec as P

EPS = 1e-5
ROPE_BASE = 10000.0
BLOCK = 512
AXIS = "cp"
BF16, F32 = jnp.bfloat16, jnp.float32
VMEM_LIMIT = 63 * 1024 * 1024
FLAGS = {}


def frequencies(head_dim):
    quarter = head_dim // 4
    return jnp.exp(jnp.arange(quarter, dtype=F32) * (-2.0 * math.log(ROPE_BASE) / (head_dim // 2)))


def rotate(values, cos, sin):
    quarter = cos.shape[0]
    first, second = values[:quarter], values[quarter : 2 * quarter]
    return jnp.concatenate([first * cos - second * sin, second * cos + first * sin, values[2 * quarter :]], axis=0)


def rows_of(index, size):
    return pl.ds(pl.multiple_of(index * size, size), size)


def dot(lhs, rhs):
    return jnp.dot(lhs, rhs, preferred_element_type=F32)


def dot_t(lhs, rhs):
    return lax.dot_general(lhs, rhs, (((1,), (1,)), ((), ())), preferred_element_type=F32)


def full_barrier(n_dev):
    me = lax.axis_index(AXIS)
    barrier = pltpu.get_barrier_semaphore()

    def tell(step):
        pl.semaphore_signal(barrier, inc=1, device_id={AXIS: lax.rem(me + step, n_dev)}, device_id_type=pl.DeviceIdType.MESH)

    each(1, n_dev, tell)
    pl.semaphore_wait(barrier, n_dev - 1)


def remote(src, dst, send_sem, recv_sem, peer):
    return pltpu.make_async_remote_copy(src_ref=src, dst_ref=dst, send_sem=send_sem, recv_sem=recv_sem, device_id={AXIS: peer}, device_id_type=pl.DeviceIdType.MESH)


def each(lower, upper, body):
    def step(index, carry):
        body(index)
        return carry

    lax.fori_loop(lower, upper, step, 0)


class Exchange:
    def __init__(self, src, dst, send, recv):
        self.src, self.dst, self.send, self.recv = src, dst, send, recv

    def start(self, index, slot, peer):
        me = lax.axis_index(AXIS)
        src, dst, recv = self.src(index), self.dst(slot), self.recv(slot)

        @pl.when(peer != me)
        def _():
            remote(src, dst, self.send(index), recv, peer).start()

        @pl.when(peer == me)
        def _():
            pltpu.make_async_copy(src, dst, recv).start()

    def sent(self, index, peer):
        me = lax.axis_index(AXIS)

        @pl.when(peer != me)
        def _():
            remote(self.src(index), self.src(index), self.send(index), self.send(index), me).wait_send()

    def got(self, slot):
        dst = self.dst(slot)
        remote(dst, dst, self.recv(slot), self.recv(slot), lax.axis_index(AXIS)).wait_recv()


def ring_order(side):
    queue, free, order = [(0.0, True, 0, 0), (0.0, False, 0, 0)], 0.0, []
    waiting = []
    while queue or waiting:
        if queue and (not waiting or free <= waiting[0][0]):
            at, along, s, h = queue.pop(0)
            free = max(free, at) + 1.0
            waiting.append((free + 0.5, (s + along, h + 1 - along)))
        else:
            at, (s, h) = waiting.pop(0)
            order.append((s, h))
            if h == 0 and s < side - 1:
                queue.append((at, True, s, h))
            if h < side - 1:
                queue.append((at, False, s, h))
    return order


def lookup(table, index):
    out = jnp.int32(table[0])
    for key, value in enumerate(table[1:], 1):
        out = jnp.where(index == key, jnp.int32(value), out)
    return out


class Ring:
    def __init__(self, n_dev, own, everything, ring_send, ring_recv, core_send, core_recv):
        self.own, self.all = own, everything
        self.ring_send, self.ring_recv, self.core_send, self.core_recv = ring_send, ring_recv, core_send, core_recv
        self.side = math.isqrt(n_dev // 2)
        self.tokens = own.shape[0]
        self.rows = self.tokens // 4
        self.me = lax.axis_index(AXIS)
        self.core = lax.rem(self.me, 2)
        self.x, self.y = lax.rem(self.me // 2, self.side), self.me // (2 * self.side)

    def device(self, colour, along, across, core):
        side = self.side
        x_first = 1 - colour // 2
        sign = 1 - 2 * lax.rem(colour, 2)
        dx = x_first * along + (1 - x_first) * across
        dy = x_first * across + (1 - x_first) * along
        x = lax.rem(self.x - sign * dx + 2 * side, side)
        y = lax.rem(self.y - sign * dy + 2 * side, side)
        return (y * side + x) * 2 + core

    def place(self, colour, s, h, core):
        return pl.ds(pl.multiple_of(self.device(colour, s, h, core) * self.tokens + colour * self.rows, self.rows), self.rows)

    def piece(self, colour, s, h):
        return self.all.at[self.place(colour, s, h, self.core)]

    def number(self, s, h):
        return s * self.side + h

    def ring_copy(self, colour, s, h, along, src=None):
        number = self.number(s + along, h + 1 - along)
        dst = self.piece(colour, s, h)
        peer = self.device(colour, -along, along - 1, self.core)
        return remote(dst if src is None else src, dst, self.ring_send.at[colour, number], self.ring_recv.at[colour, number], peer)

    def core_copy(self, colour, s, h, src=None):
        number = self.number(s, h)
        dst = self.piece(colour, s, h)
        return remote(dst if src is None else src, dst, self.core_send.at[colour, number], self.core_recv.at[colour, number], self.me + 1 - 2 * self.core)

    def arrival(self, colour, s, h):
        number = self.number(s, h)
        dst = self.piece(colour, s, h)
        return remote(dst, dst, self.ring_send.at[colour, number], self.ring_recv.at[colour, number], self.me)

    def core_arrival(self, colour, s, h):
        number = self.number(s, h)
        dst = self.all.at[self.place(colour, s, h, 1 - self.core)]
        return remote(dst, dst, self.core_send.at[colour, number], self.core_recv.at[colour, number], self.me)

    def begin(self):
        def one(colour):
            src = self.own.at[rows_of(colour, self.rows)]
            self.ring_copy(colour, 0, 0, 1, src).start()
            self.ring_copy(colour, 0, 0, 0, src).start()

        def other(colour):
            self.core_copy(colour, 0, 0, self.own.at[rows_of(colour, self.rows)]).start()

        each(0, 4, one)
        each(0, 4, other)

    def pass_on(self, s, h):
        def one(colour):
            self.arrival(colour, s, h).wait_recv()

            @pl.when((h == 0) & (s < self.side - 1))
            def _():
                self.ring_copy(colour, s, h, 1).start()

            @pl.when(h < self.side - 1)
            def _():
                self.ring_copy(colour, s, h, 0).start()

            self.core_copy(colour, s, h).start()

        each(0, 4, one)

    def got_core(self, s, h):
        each(0, 4, lambda colour: self.core_arrival(colour, s, h).wait_recv())

    def end(self):
        def sent(number):
            s, h = number // self.side, lax.rem(number, self.side)

            def one(colour):
                @pl.when((s > 0) | (h > 0))
                def _():
                    self.arrival(colour, s, h).wait_send()

                self.core_copy(colour, s, h).wait_send()

            each(0, 4, one)

        each(0, self.side * self.side, sent)


def front_part(
    n_dev, n_group, x_ref, dy_ref, pos_ref, freq_ref, gain_ref, bias_ref, wo_ref, wq_ref, wk_ref, wv_ref,
    h_all, dy_all, q_ref, k_ref, v_ref, da_ref, cos_ref, sin_ref, x_hat_ref, inv_ref, pos_in,
    h_send, h_recv, h_core_send, h_core_recv, dy_send, dy_recv, dy_core_send, dy_core_recv, w_sem, h_sem, dy_sem, pos_send, pos_recv, local,
    h_own, w_ref, wo_own, pick_ref, w_buf, h_buf, dy_buf,
):
    me = lax.axis_index(AXIS)
    tokens, width = x_ref.shape
    head_dim = v_ref.shape[1]
    heads_tile = w_buf.shape[2]
    d_block = w_buf.shape[1]
    h_ring = Ring(n_dev, h_own, h_all, h_send, h_recv, h_core_send, h_core_recv)
    dy_ring = Ring(n_dev, dy_ref, dy_all, dy_send, dy_recv, dy_core_send, dy_core_recv)
    rows_n = h_ring.rows
    order = [(0, 0)] + ring_order(h_ring.side)
    n_event = len(order)
    where = Exchange(lambda peer: pos_ref, lambda origin: pos_in.at[origin], lambda peer: pos_send.at[peer], lambda origin: pos_recv.at[origin])

    n_d = width // d_block
    kv_head = me // n_group

    def w_load(t, which):
        ref, head = ((wq_ref, me), (wk_ref, kv_head), (wv_ref, kv_head))[which]
        slot = lax.rem(t, 2)
        return pltpu.make_async_copy(ref.at[rows_of(t, d_block), rows_of(head // heads_tile, heads_tile)], w_buf.at[slot], w_sem.at[slot])

    own_dy = pltpu.make_async_copy(dy_ref, dy_all.at[rows_of(me, tokens)], local.at[0])
    own_h = pltpu.make_async_copy(h_own, h_all.at[rows_of(me, tokens)], local.at[1])
    own_wo = pltpu.make_async_copy(wo_ref.at[rows_of(me, head_dim)], wo_own, local.at[2])
    own_dy.start()
    own_wo.start()
    w_load(0, 0).start()
    full_barrier(n_dev)
    dy_ring.begin()

    gain, bias = 1.0 + gain_ref[...], bias_ref[...]

    def norm(t):
        rows = rows_of(t, 16)
        x = x_ref[rows, :].astype(F32)
        centered = x - jnp.sum(x, axis=1, keepdims=True) * (1.0 / width)
        inv = lax.rsqrt(jnp.sum(centered * centered, axis=1, keepdims=True) * (1.0 / width) + EPS)
        x_hat = centered * inv
        x_hat_ref[rows, :] = x_hat
        inv_ref[rows, :] = inv
        h_own[rows, :] = (x_hat * gain + bias).astype(BF16)

    each(0, tokens // 16, norm)

    def send_pos(step):
        peer = lax.rem(me + step, n_dev)
        where.start(peer, me, peer)

    each(0, n_dev, send_pos)
    h_ring.begin()
    own_h.start()

    for which in range(3):
        head = me if which == 0 else kv_head

        def pick(t):
            @pl.when(t + 1 < n_d)
            def _():
                w_load(t + 1, which).start()

            w_load(t, which).wait()
            pick_ref[...] = jnp.swapaxes(w_buf[lax.rem(t, 2)], 0, 1)
            w_ref[rows_of(t, d_block), which * head_dim : (which + 1) * head_dim] = pick_ref[lax.rem(head, heads_tile)]

        each(0, n_d, pick)
        if which < 2:
            w_load(0, which + 1).start()
        if which == 0:
            dy_ring.pass_on(*(jnp.int32(v) for v in order[1]))
        if which == 1:
            h_ring.pass_on(*(jnp.int32(v) for v in order[1]))
    own_wo.wait()
    own_dy.wait()
    own_h.wait()

    def tables(origin):
        where.got(origin)
        angles = freq_ref[...] * pos_in[origin, 0:1, :].astype(F32)
        cos_ref[:, rows_of(origin, tokens)] = jnp.cos(angles)
        sin_ref[:, rows_of(origin, tokens)] = jnp.sin(angles)

    def event(e):
        return lookup([p[0] for p in order], e), lookup([p[1] for p in order], e)

    def places_of(ring, s, h):
        return [ring.place(jnp.int32(colour), s, h, core) for colour in range(4) for core in range(2)]

    def fetch(ring, buf, sem, e):
        slot = lax.rem(e, 2)
        s, h = event(e)
        ring.got_core(s, h)
        for n, place in enumerate(places_of(ring, s, h)):
            pltpu.make_async_copy(ring.all.at[place], buf.at[slot, pl.ds(n * rows_n, rows_n)], sem.at[slot]).start()

    def fetched(ring, buf, sem, e):
        slot = lax.rem(e, 2)
        pltpu.make_async_copy(ring.all.at[pl.ds(0, 8 * rows_n)], buf.at[slot], sem.at[slot]).wait()
        return buf[slot]

    def gradient_rows(e):
        s, h = event(e)
        da = dot_t(fetched(dy_ring, dy_buf, dy_sem, e), wo_own[...]).astype(BF16)
        for n, place in enumerate(places_of(dy_ring, s, h)):
            da_ref[place, :] = da[n * rows_n : (n + 1) * rows_n]

    def project_rows(e):
        s, h = event(e)
        out = dot(fetched(h_ring, h_buf, h_sem, e), w_ref[...])
        for n, place in enumerate(places_of(h_ring, s, h)):
            part = out[n * rows_n : (n + 1) * rows_n]
            q_ref[place, :] = part[:, :head_dim]
            k_ref[place, :] = part[:, head_dim : 2 * head_dim]
            v_ref[place, :] = part[:, 2 * head_dim :].astype(BF16)

    def step(e):
        for ring, buf, sem, rows in ((dy_ring, dy_buf, dy_sem, gradient_rows), (h_ring, h_buf, h_sem, project_rows)):
            @pl.when((e > 1) & (e < n_event))
            def _():
                ring.pass_on(*event(e))

            @pl.when((e > 0) & (e <= n_event))
            def _():
                fetch(ring, buf, sem, e - 1)

            @pl.when(e > 1)
            def _():
                rows(e - 2)

        @pl.when(e == 3)
        def _():
            each(0, n_dev, tables)

    each(1, n_event + 2, step)
    h_ring.end()
    dy_ring.end()
    each(0, n_dev, lambda index: where.sent(index, index))


def causal(block):
    key = lax.broadcasted_iota(jnp.int32, (block, block), 0)
    query = lax.broadcasted_iota(jnp.int32, (block, block), 1)
    return key <= query


def part_sum(values):
    return jnp.sum(values.reshape(values.shape[0] // 8, 8, values.shape[1]), axis=0)


def main_part(
    n_dev, n_group, q_heads, kv_heads, n_buf, scale,
    q_raw, k_raw, v_ref, da_ref, cos_ref, sin_ref, x_ref, dy_own_ref, x_hat_ref, inv_ref, gain_ref, h_ref, dy_ref, wq_ref, wk_ref, wv_ref, wo_ref,
    out_ref, gx_ref, gwo_ref, q_rows, kv_rows, sum_ref,
    at_ref, dqt_ref, a_head, dq_head, dkvt_ref, a_ref, g_ref, dkv_ref, land_one, land_two, kv_ref, kvt_ref, wq_out, wkv_out, dh_ref, part_ref, own_sum, sum_in, sum_mine,
    a_send, a_recv, dq_send, dq_recv, one_send, one_recv, two_send, two_recv, kv_send, kv_recv, near_send, near_recv, far_send, far_recv, fwd_send, fwd_recv,
    load_sem, q_send, q_recv, wkv_send, wkv_recv, s_send, s_recv, t_send, t_recv,
):
    me = lax.axis_index(AXIS)
    seq, head_dim = v_ref.shape
    tokens, width = x_ref.shape
    block = tokens * n_group
    n_block = seq // block
    half = block // 2
    fold = scale * math.log2(math.e)
    core, side = lax.rem(me, 2), lax.rem(me // 2, 2)
    member, group = lax.rem(me, n_group), me // n_group
    partner, across = me + 1 - 2 * core, me + 2 - 4 * side
    place, place_across = core * 2 + side, core * 2 + 1 - side
    place_partner, place_last = (1 - core) * 2 + side, (1 - core) * 2 + 1 - side
    shift = lax.rem(group, max(2, n_block * 3 // 4))
    depth = width // n_dev
    span = math.lcm(depth, 128)
    n_col = width // span
    per_col = span // depth
    col_member = n_col // n_group
    per_member = n_dev // n_group
    n_sum = sum_mine.shape[0]
    q_cols, kv_cols = q_heads * head_dim, kv_heads * head_dim

    def piece(index):
        return rows_of(index, tokens)

    def column(head):
        return rows_of(head, head_dim)

    def cols(j):
        return rows_of(j, span)

    a_copy = Exchange(lambda peer: a_head.at[piece(peer)], lambda head: a_ref.at[:, column(head)], lambda peer: a_send.at[peer], lambda head: a_recv.at[head])
    dq_copy = Exchange(lambda peer: dq_head.at[piece(peer)], lambda head: g_ref.at[:, column(head)], lambda peer: dq_send.at[peer], lambda head: dq_recv.at[head])
    kv_copy = [
        Exchange(
            lambda i, w=w: kv_ref.at[i, w],
            lambda head, w=w: g_ref.at[:, column(q_heads + w * kv_heads + head)],
            lambda i, w=w: kv_send.at[w, i],
            lambda head, w=w: kv_recv.at[w, head],
        )
        for w in range(2)
    ]
    q_copy = Exchange(lambda peer: wq_out.at[rows_of(peer, depth)], lambda head: q_rows.at[head], lambda peer: q_send.at[peer], lambda head: q_recv.at[head])
    wkv_copy = Exchange(lambda i: wkv_out.at[rows_of(i, depth)], lambda head: kv_rows.at[head], lambda i: wkv_send.at[i], lambda head: wkv_recv.at[head])
    s_copy = Exchange(lambda peer: own_sum.at[pl.ds(peer * n_sum, n_sum)], lambda origin: sum_in.at[origin], lambda peer: s_send.at[peer], lambda origin: s_recv.at[origin])
    t_copy = Exchange(lambda peer: sum_mine, lambda origin: sum_ref.at[pl.ds(origin * n_sum, n_sum)], lambda peer: t_send.at[peer], lambda origin: t_recv.at[origin])


    def one_copy(i):
        return remote(dkv_ref.at[rows_of(i * 2 + 1 - core, half)], land_one.at[i], one_send.at[i], one_recv.at[i], partner)

    def two_copy(i):
        return remote(dkv_ref.at[piece(i * n_group + core * 2 + 1 - side)], land_two.at[i], two_send.at[i], two_recv.at[i], across)

    def near_copy(i, where):
        return remote(kvt_ref.at[i], dkvt_ref.at[:, piece(i * n_group + where)], near_send.at[i], near_recv.at[i], partner)

    def far_copy(i, where):
        return remote(kvt_ref.at[i], dkvt_ref.at[:, piece(i * n_group + where)], far_send.at[i], far_recv.at[i], across)

    def fwd_copy(i, where):
        view = dkvt_ref.at[:, piece(i * n_group + where)]
        return remote(view, view, fwd_send.at[i], fwd_recv.at[i], partner)

    def first(i):
        one_copy(i).start()

    def second(i):
        one_copy(i).wait_recv()
        for part in (1 - side, side):
            rows = piece(i * n_group + core * 2 + part)
            dkv_ref[rows, :] += land_one[i, pl.ds(pl.multiple_of(part * tokens, tokens), tokens), :]
        two_copy(i).start()

    def close(i):
        two_copy(i).wait_recv()
        rows = piece(i * n_group + place)
        total = dkv_ref[rows, :] + land_two[i]
        dkt = rotate(total[:, :head_dim].T, cos_ref[:, rows], -sin_ref[:, rows]).astype(BF16)
        dv = total[:, head_dim:].astype(BF16)
        dvt = dv.T
        kvt_ref[i, :head_dim, :], kvt_ref[i, head_dim:, :] = dkt, dvt
        dkvt_ref[:head_dim, rows], dkvt_ref[head_dim:, rows] = dkt, dvt
        kv_ref[i, 0], kv_ref[i, 1] = dkt.T, dv

    def spread(i):
        far_copy(i, place).start()
        near_copy(i, place).start()
        for copy in kv_copy:
            copy.start(i, group, i * n_group + place)

    def forward(i):
        far_copy(i, place_across).wait_recv()
        fwd_copy(i, place_across).start()

    steps = (first, second, close, spread, forward)

    def block_at(t):
        return lax.rem(shift - 1 - t + 2 * n_block, n_block)

    def stages(t):
        for late in range(len(steps), 0, -1):
            n = t - late - shift

            @pl.when(n >= 0)
            def _():
                steps[late - 1](n_block - 1 - n)

    def stage_rest(late):
        each(jnp.maximum(n_block - late - shift, 0), n_block, lambda n: steps[late - 1](n_block - 1 - n))

    def send_pieces(i):
        def send(u):
            peer = i * n_group + lax.rem(u + me, n_group)
            a_copy.start(peer, me, peer)
            dq_copy.start(peer, me, peer)

        each(0, n_group, send)

    def attention(q_ref, k_ref, qt_ref, kt_ref, vt_ref, e_ref, dp_ref, peak_ref, dat_ref, mix_ref, acc_ref):
        def prepare(i):
            rows = rows_of(i, block)
            for raw, turned, plain in ((q_raw, qt_ref, q_ref), (k_raw, kt_ref, k_ref)):
                t = rotate(raw[rows, :].T, cos_ref[:, rows], sin_ref[:, rows]).astype(BF16)
                turned[:, rows] = t
                plain[rows, :] = t.T
            vt_ref[:, rows] = v_ref[rows, :].T
            dkv_ref[rows, :] = jnp.zeros((block, 2 * head_dim), F32)

        each(0, n_block, prepare)

        def compute(i):
            own = rows_of(i, block)
            dat_ref[...] = da_ref[own, :].T
            mix_ref[...] = jnp.zeros_like(mix_ref)
            acc_ref[...] = jnp.zeros_like(acc_ref)

            def scores(j, carry, diagonal):
                peak, total, mixed = carry
                rows = rows_of(j, block)
                s = dot(k_ref[rows, :], qt_ref[:, own])
                if diagonal:
                    s = jnp.where(causal(block), s, -1e30)
                top = jnp.maximum(peak, jnp.max(s, axis=0, keepdims=True))
                e = jnp.exp2((s - top) * fold)
                dp = dot(v_ref[rows, :], dat_ref[...])
                fade = jnp.exp2((peak - top) * fold)
                e_ref[rows, :] = e
                dp_ref[rows, :] = dp
                peak_ref[j] = top
                return top, total * fade + part_sum(e), mixed * fade + part_sum(e * dp)

            start = (jnp.full((1, block), -jnp.inf, F32), jnp.zeros((8, block), F32), jnp.zeros((8, block), F32))
            carry = lax.fori_loop(0, i, functools.partial(scores, diagonal=False), start)
            peak, total, mixed = scores(i, carry, True)
            inv = 1.0 / jnp.sum(total, axis=0, keepdims=True)
            row_dot = jnp.sum(mixed, axis=0, keepdims=True) * inv
            q_own, da_own = q_ref[own, :], da_ref[own, :]

            def grads(j):
                rows = rows_of(j, block)
                p = e_ref[rows, :] * (jnp.exp2((peak_ref[j] - peak) * fold) * inv)
                pb = p.astype(BF16)
                ds = ((dp_ref[rows, :] - row_dot) * (p * scale)).astype(BF16)
                dkv_ref[rows, :head_dim] += dot(ds, q_own)
                dkv_ref[rows, head_dim:] += dot(pb, da_own)
                mix_ref[...] += dot(vt_ref[:, rows], pb)
                acc_ref[...] += dot(kt_ref[:, rows], ds)

            each(0, i + 1, grads)
            at = mix_ref[...].astype(BF16)
            at_ref[:, own] = at
            a_head[own, :] = at.T
            dqt = rotate(acc_ref[...], cos_ref[:, own], -sin_ref[:, own]).astype(BF16)
            dqt_ref[:, own] = dqt
            dq_head[own, :] = dqt.T

        def iteration(t):
            stages(t)

            @pl.when(t > 0)
            def _():
                send_pieces(block_at(t - 1))

            compute(block_at(t))

        each(0, n_block, iteration)

    pl.run_scoped(
        attention,
        pltpu.VMEM((seq, head_dim), BF16), pltpu.VMEM((seq, head_dim), BF16),
        pltpu.VMEM((head_dim, seq), BF16), pltpu.VMEM((head_dim, seq), BF16), pltpu.VMEM((head_dim, seq), BF16),
        pltpu.VMEM((seq, block), F32), pltpu.VMEM((seq, block), F32), pltpu.VMEM((n_block, 1, block), F32),
        pltpu.VMEM((head_dim, block), BF16), pltpu.VMEM((head_dim, block), F32), pltpu.VMEM((head_dim, block), F32),
    )

    def drain_sums():
        def one(i):
            one_copy(i).wait_send()
            two_copy(i).wait_send()
            near_copy(i, place).wait_send()
            near_copy(i, place_partner).wait_recv()
            far_copy(i, place).wait_send()
            fwd_copy(i, place_across).wait_send()
            fwd_copy(i, place_last).wait_recv()
            for copy in kv_copy:
                copy.sent(i, i * n_group + place)

        def head(index):
            for copy in kv_copy:
                copy.got(index)

        each(0, n_block, one)
        each(0, kv_heads, head)

    stage_rest(1)
    send_pieces(block_at(n_block - 1))

    def products(buf, wq_buf, wk_buf, wv_buf):
        counts = (n_col, n_col, n_col, col_member, n_col, n_col)
        starts = [sum(counts[:n]) for n in range(len(counts))]

        def loads(phase, j, slot):
            if phase == 2:
                return [pltpu.make_async_copy(wq_ref.at[cols(j)], wq_buf.at[slot], load_sem.at[slot, 0])]
            if phase == 4:
                pairs = ((wk_ref, wk_buf), (wv_ref, wv_buf))
                return [pltpu.make_async_copy(ref.at[cols(j)], to.at[slot], load_sem.at[slot, n]) for n, (ref, to) in enumerate(pairs)]
            ref = (h_ref, dy_ref, None, h_ref, None, wo_ref)[phase]
            col = member * col_member + j if phase == 3 else j
            return [pltpu.make_async_copy(ref.at[:, cols(col)], buf.at[slot], load_sem.at[slot, 0])]

        def load(step):
            slot = lax.rem(step, n_buf)
            for phase, (begin, count) in enumerate(zip(starts, counts)):
                @pl.when((step >= begin) & (step < begin + count))
                def _():
                    for copy in loads(phase, step - begin, slot):
                        copy.start()

        def run(phase, body):
            def step(j):
                number = starts[phase] + j
                slot = lax.rem(number, n_buf)
                for copy in loads(phase, j, slot):
                    copy.wait()
                body(j, slot)
                load(number + n_buf)

            each(0, counts[phase], step)

        each(0, n_buf, load)

        def weight_columns(j, slot):
            @pl.when(j == n_col // 4)
            def _():
                stage_rest(2)

            wq_out[cols(j), :] = dot(dqt_ref[...], buf[slot]).T

        run(0, weight_columns)

        def send_rows(j):
            col = lax.rem(j + me // per_col, n_col)

            def send(u):
                peer = col * per_col + lax.rem(u + me, per_col)
                q_copy.start(peer, me, peer)

            each(0, per_col, send)

        def weight_out(j, slot):
            @pl.when(j < n_col // 2)
            def _():
                send_rows(j)

            gwo_ref[:, cols(j)] = dot(at_ref[...], buf[slot])

        run(1, weight_out)

        def got_heads(head):
            a_copy.got(head)
            dq_copy.got(head)

        each(0, n_dev, got_heads)

        def flat(ref, slot):
            rows = ref[slot]
            return rows.reshape(rows.shape[0], rows.shape[1] * rows.shape[2])

        def back_query(j, slot):
            for late, at in ((3, n_col // 4), (4, n_col * 3 // 8), (5, n_col * 3 // 4)):
                @pl.when(j == at)
                def _():
                    stage_rest(late)

            @pl.when(j >= n_col // 2)
            def _():
                send_rows(j)

            dh_ref[:, cols(j)] = dot_t(g_ref[:, :q_cols], flat(wq_buf, slot))

        run(2, back_query)
        drain_sums()

        def weight_kv(j, slot):
            wkv_out[cols(j), :] = dot(dkvt_ref[...], buf[slot]).T

        run(3, weight_kv)

        def send_kv(step):
            index = lax.rem(step + group, per_member)
            wkv_copy.start(index, group, member * per_member + index)

        def back_kv(j, slot):
            @pl.when(j == 0)
            def _():
                each(0, per_member, send_kv)

            grad_h = dot_t(g_ref[:, q_cols : q_cols + kv_cols], flat(wk_buf, slot))
            dh_ref[:, cols(j)] += grad_h + dot_t(g_ref[:, q_cols + kv_cols :], flat(wv_buf, slot))

        run(4, back_kv)

        part_ref[...] = jnp.zeros_like(part_ref)
        gain = 1.0 + gain_ref[...]

        def norm(t):
            rows = rows_of(t, 16)
            grad_h, x_hat = dh_ref[rows, :], x_hat_ref[rows, :]
            grad_hat = grad_h * gain
            one = jnp.sum(grad_hat, axis=1, keepdims=True) * (1.0 / width)
            two = jnp.sum(grad_hat * x_hat, axis=1, keepdims=True) * (1.0 / width)
            back = inv_ref[rows, :] * (grad_hat - one - x_hat * two)
            gx_ref[rows, :] = (dy_own_ref[rows, :].astype(F32) + back).astype(BF16)
            part_ref[0] += part_sum(grad_h * x_hat)
            part_ref[1] += part_sum(grad_h)

        each(0, tokens // 16, norm)
        own_sum[...] = jnp.zeros_like(own_sum)
        for which in range(2):
            total = jnp.sum(part_ref[which], axis=0, keepdims=True)
            for c in range(width // 128):
                own_sum[c, pl.ds(which, 1), :] = total[:, c * 128 : (c + 1) * 128]

        def to_all(copy):
            def send(step):
                peer = lax.rem(me + step, n_dev)
                copy.start(peer, me, peer)

            each(0, n_dev, send)

        def add(origin):
            sum_mine[...] += sum_in[origin]

        def output(j, slot):
            @pl.when(j == 0)
            def _():
                to_all(s_copy)

            @pl.when(j == n_col // 2)
            def _():
                each(0, n_dev, s_copy.got)
                sum_mine[...] = jnp.zeros_like(sum_mine)
                each(0, n_dev, add)

            out_ref[:, cols(j)] = (x_ref[:, cols(j)].astype(F32) + dot(a_ref[...], buf[slot])).astype(BF16)

            @pl.when(j == n_col // 2)
            def _():
                to_all(t_copy)

        run(5, output)

    pl.run_scoped(
        products,
        pltpu.VMEM((n_buf, seq, span), BF16),
        pltpu.VMEM((n_buf, span) + wq_ref.shape[1:], BF16),
        pltpu.VMEM((n_buf, span) + wk_ref.shape[1:], BF16),
        pltpu.VMEM((n_buf, span) + wv_ref.shape[1:], BF16),
    )

    def drain(index):
        for copy in (a_copy, dq_copy, s_copy, t_copy, q_copy):
            copy.sent(index, index)
        t_copy.got(index)
        q_copy.got(index)

    def drain_kv(index):
        wkv_copy.sent(index, member * per_member + index)

    each(0, n_dev, drain)
    each(0, per_member, drain_kv)
    each(0, kv_heads, wkv_copy.got)


def block_kernel(n_dev, q_heads, kv_heads, n_buf, scale, *refs):
    x_ref, dy_ref, pos_ref, freq_ref, gain_ref, bias_ref, wo_ref, wq_ref, wk_ref, wv_ref = refs[:10]
    outs, (h_all, dy_all) = refs[10:16], refs[16:18]
    heads, pos_in, refs = refs[18:26], refs[26], refs[27:]
    front_sems, main_refs = refs[:14], refs[14:]
    tokens, width = x_ref.shape
    head_dim = wq_ref.shape[2]
    heads_tile = min(8, kv_heads)
    d_block = math.lcm(width // n_dev, 128)
    n_group = q_heads // kv_heads
    weights = (wo_ref, wq_ref, wk_ref, wv_ref)
    pl.run_scoped(
        functools.partial(front_part, n_dev, n_group, x_ref, dy_ref, pos_ref, freq_ref, gain_ref, bias_ref, *weights, h_all, dy_all, *heads, pos_in, *front_sems),
        pltpu.VMEM((tokens, width), BF16),
        pltpu.VMEM((width, 3 * head_dim), BF16),
        pltpu.VMEM((head_dim, width), BF16),
        pltpu.VMEM((heads_tile, d_block, head_dim), BF16),
        pltpu.VMEM((2, d_block, heads_tile, head_dim), BF16),
        pltpu.VMEM((2, 2 * tokens, width), BF16),
        pltpu.VMEM((2, 2 * tokens, width), BF16),
    )
    q, k, v, da, cos, sin, x_hat, inv = heads
    main_part(
        n_dev, n_group, q_heads, kv_heads, n_buf, scale,
        q, k, v, da, cos, sin, x_ref, dy_ref, x_hat, inv, gain_ref, h_all, dy_all, wq_ref, wk_ref, wv_ref, wo_ref, *outs, *main_refs,
    )


def whole_block(n_dev, x_own, dy_own, positions, freq, gain, bias, wo, wq, wk, wv):
    tokens, width = x_own.shape
    q_heads, head_dim = wq.shape[1:]
    kv_heads = wk.shape[1]
    seq = tokens * n_dev
    n_group = q_heads // kv_heads
    n_block = n_dev // n_group
    depth = width // n_dev
    n_buf = 3
    n_sum = -(-width // (128 * n_dev))
    sums = (n_sum * n_dev, 8, 128)
    pieces = math.isqrt(n_dev // 2) ** 2
    whole, anywhere = pl.BlockSpec(memory_space=pltpu.VMEM), pl.BlockSpec(memory_space=pl.ANY)
    dma = pltpu.SemaphoreType.DMA
    return pl.pallas_call(
        functools.partial(block_kernel, n_dev, q_heads, kv_heads, n_buf, head_dim**-0.5),
        out_shape=[
            jax.ShapeDtypeStruct((tokens, width), BF16),
            jax.ShapeDtypeStruct((tokens, width), BF16),
            jax.ShapeDtypeStruct((head_dim, width), F32),
            jax.ShapeDtypeStruct((q_heads, depth, head_dim), F32),
            jax.ShapeDtypeStruct((kv_heads, depth, 2 * head_dim), F32),
            jax.ShapeDtypeStruct(sums, F32),
            jax.ShapeDtypeStruct((seq, width), BF16),
            jax.ShapeDtypeStruct((seq, width), BF16),
        ],
        in_specs=[whole] * 6 + [anywhere] * 4,
        out_specs=[whole] * 3 + [anywhere] * 2 + [whole] + [anywhere] * 2,
        scratch_shapes=[
            pltpu.VMEM((seq, head_dim), F32),
            pltpu.VMEM((seq, head_dim), F32),
            pltpu.VMEM((seq, head_dim), BF16),
            pltpu.VMEM((seq, head_dim), BF16),
            pltpu.VMEM((head_dim // 4, seq), F32),
            pltpu.VMEM((head_dim // 4, seq), F32),
            pltpu.VMEM((tokens, width), F32),
            pltpu.VMEM((tokens, 1), F32),
            pltpu.VMEM((n_dev,) + positions.shape, jnp.int32),
            dma((4, pieces)), dma((4, pieces)), dma((4, pieces)), dma((4, pieces)),
            dma((4, pieces)), dma((4, pieces)), dma((4, pieces)), dma((4, pieces)),
            dma((2,)), dma((2,)), dma((2,)), dma((n_dev,)), dma((n_dev,)), dma((3,)),
            pltpu.VMEM((head_dim, seq), BF16),
            pltpu.VMEM((head_dim, seq), BF16),
            pltpu.VMEM((seq, head_dim), BF16),
            pltpu.VMEM((seq, head_dim), BF16),
            pltpu.VMEM((2 * head_dim, seq), BF16),
            pltpu.VMEM((tokens, q_heads * head_dim), BF16),
            pltpu.VMEM((tokens, (q_heads + 2 * kv_heads) * head_dim), BF16),
            pltpu.VMEM((seq, 2 * head_dim), F32),
            pltpu.VMEM((n_block, tokens * n_group // 2, 2 * head_dim), F32),
            pltpu.VMEM((n_block, tokens, 2 * head_dim), F32),
            pltpu.VMEM((n_block, 2, tokens, head_dim), BF16),
            pltpu.VMEM((n_block, 2 * head_dim, tokens), BF16),
            pltpu.VMEM((width, head_dim), F32),
            pltpu.VMEM((width // n_group, 2 * head_dim), F32),
            pltpu.VMEM((tokens, width), F32),
            pltpu.VMEM((2, 8, width), F32),
            pltpu.VMEM(sums, F32),
            pltpu.VMEM((n_dev, n_sum, 8, 128), F32),
            pltpu.VMEM((n_sum, 8, 128), F32),
            dma((n_dev,)), dma((n_dev,)), dma((n_dev,)), dma((n_dev,)),
            dma((n_block,)), dma((n_block,)), dma((n_block,)), dma((n_block,)), dma((2, n_block)), dma((2, kv_heads)),
            dma((n_block,)), dma((n_block,)), dma((n_block,)), dma((n_block,)), dma((n_block,)), dma((n_block,)),
            dma((n_buf, 3)), dma((n_dev,)), dma((n_dev,)), dma((n_dev // n_group,)), dma((kv_heads,)), dma((n_dev,)), dma((n_dev,)), dma((n_dev,)), dma((n_dev,)),
        ],
        compiler_params=pltpu.CompilerParams(collective_id=1, has_side_effects=True, vmem_limit_bytes=VMEM_LIMIT, flags=FLAGS),
        cost_estimate=pl.CostEstimate(flops=6 * seq * seq * head_dim + 16 * seq * width * head_dim, bytes_accessed=16 * seq * width, transcendentals=seq * seq // 2),
        name="block",
    )(x_own, dy_own, positions, freq, gain, bias, wo, wq, wk, wv)


def solution(mesh):
    n_dev = mesh.shape[AXIS]

    def device_step(x_act, d_out, positions, ln_gain, ln_bias, w_query, w_key, w_value, w_out):
        n_batch, piece, width = x_act.shape
        q_heads, head_dim = w_query.shape[1:]
        tokens = n_batch * piece

        x_own, dy_own = x_act.reshape(tokens, width), d_out.reshape(tokens, width)
        gain, bias = ln_gain.reshape(1, width), ln_bias.reshape(1, width)
        pos_tile = jnp.broadcast_to(positions.reshape(1, tokens), (8, tokens))
        freq = jnp.broadcast_to(frequencies(head_dim)[:, None], (head_dim // 4, tokens))
        block_out, grad_x, grad_wo, rows_wq, rows_wkv, sums, _, _ = whole_block(n_dev, x_own, dy_own, pos_tile, freq, gain, bias, w_out, w_query, w_key, w_value)
        grad_wq = jnp.swapaxes(rows_wq, 0, 1)
        grad_wk = jnp.swapaxes(rows_wkv[:, :, :head_dim], 0, 1)
        grad_wv = jnp.swapaxes(rows_wkv[:, :, head_dim:], 0, 1)
        n_lane = width // 128
        grad_gain, grad_bias = sums[:n_lane, 0].reshape(width), sums[:n_lane, 1].reshape(width)
        return (block_out.reshape(x_act.shape), grad_x.reshape(x_act.shape), grad_wq, grad_wk, grad_wv, grad_wo, grad_gain, grad_bias)

    return jax.shard_map(device_step, mesh=mesh, in_specs=(P("dp", AXIS, None), P("dp", AXIS, None), P("dp", AXIS), P(None), P(None), P(None, None, None), P(None, None, None), P(None, None, None), P(None, None)), out_specs=(P("dp", AXIS, None), P("dp", AXIS, None), P(("dp", AXIS), None, None), P(("dp", AXIS), None, None), P(("dp", AXIS), None, None), P(("dp", AXIS), None), P("dp"), P("dp")), check_vma=False)
```

```python
import functools
import math

import jax
import jax.numpy as jnp
import numpy as np
from jax import lax
from jax.experimental import pallas as pl
from jax.experimental.pallas import tpu as pltpu
from jax.sharding import PartitionSpec as P

EPS = 1e-5
ROPE_BASE = 10000.0
BLOCK = 512
AXIS = "cp"
BF16, F32 = jnp.bfloat16, jnp.float32
VMEM_LIMIT = 67043328
FLAGS = {}


def frequencies(head_dim, tokens):
    quarter = head_dim // 4
    freq = np.exp(np.arange(quarter, dtype=np.float32) * np.float32(-2.0 * math.log(ROPE_BASE) / (head_dim // 2)))
    return jnp.asarray(np.broadcast_to(freq[:, None], (quarter, tokens)))


def rotate(values, cos, sin):
    quarter = cos.shape[0]
    first, second = values[:quarter], values[quarter : 2 * quarter]
    return jnp.concatenate([first * cos - second * sin, second * cos + first * sin, values[2 * quarter :]], axis=0)


def rows_of(index, size):
    return pl.ds(pl.multiple_of(index * size, size), size)


def dot(lhs, rhs):
    return jnp.dot(lhs, rhs, preferred_element_type=F32)


def dot_t(lhs, rhs):
    return lax.dot_general(lhs, rhs, (((1,), (1,)), ((), ())), preferred_element_type=F32)


def full_barrier(n_dev):
    me = lax.axis_index(AXIS)
    barrier = pltpu.get_barrier_semaphore()

    def tell(step):
        pl.semaphore_signal(barrier, inc=1, device_id={AXIS: lax.rem(me + step, n_dev)}, device_id_type=pl.DeviceIdType.MESH)

    each(1, n_dev, tell)
    pl.semaphore_wait(barrier, n_dev - 1)


def remote(src, dst, send_sem, recv_sem, peer):
    return pltpu.make_async_remote_copy(src_ref=src, dst_ref=dst, send_sem=send_sem, recv_sem=recv_sem, device_id={AXIS: peer}, device_id_type=pl.DeviceIdType.MESH)


def each(lower, upper, body):
    def step(index, carry):
        body(index)
        return carry

    lax.fori_loop(lower, upper, step, 0)


def alternate(index, step, size):
    away = (step + 1) // 2
    return lax.rem(index + jnp.where(lax.rem(step, 2) == 1, away, size - away), size)


class Exchange:
    def __init__(self, src, dst, send, recv):
        self.src, self.dst, self.send, self.recv = src, dst, send, recv

    def start(self, index, slot, peer):
        me = lax.axis_index(AXIS)
        src, dst, recv = self.src(index), self.dst(slot), self.recv(slot)

        @pl.when(peer != me)
        def _():
            remote(src, dst, self.send(index), recv, peer).start()

        @pl.when(peer == me)
        def _():
            pltpu.make_async_copy(src, dst, recv).start()

    def sent(self, index, peer):
        me = lax.axis_index(AXIS)

        @pl.when(peer != me)
        def _():
            remote(self.src(index), self.src(index), self.send(index), self.send(index), me).wait_send()

    def got(self, slot):
        dst = self.dst(slot)
        remote(dst, dst, self.recv(slot), self.recv(slot), lax.axis_index(AXIS)).wait_recv()


def ring_order(side):
    queue, free, order = [(0.0, True, 0, 0), (0.0, False, 0, 0)], 0.0, []
    waiting = []
    while queue or waiting:
        if queue and (not waiting or free <= waiting[0][0]):
            at, along, s, h = queue.pop(0)
            free = max(free, at) + 1.0
            waiting.append((free + 0.5, (s + along, h + 1 - along)))
        else:
            at, (s, h) = waiting.pop(0)
            order.append((s, h))
            if h == 0 and s < side - 1:
                queue.append((at, True, s, h))
            if h < side - 1:
                queue.append((at, False, s, h))
    return order


def lookup(table, index):
    out = jnp.int32(table[0])
    for key, value in enumerate(table[1:], 1):
        out = jnp.where(index == key, jnp.int32(value), out)
    return out


class Ring:
    def __init__(self, n_dev, own, everything, ring_send, ring_recv, core_send, core_recv):
        self.own, self.all = own, everything
        self.ring_send, self.ring_recv, self.core_send, self.core_recv = ring_send, ring_recv, core_send, core_recv
        self.side = math.isqrt(n_dev // 2)
        self.tokens = own.shape[0]
        self.rows = self.tokens // 4
        self.me = lax.axis_index(AXIS)
        self.core = lax.rem(self.me, 2)
        self.x, self.y = lax.rem(self.me // 2, self.side), self.me // (2 * self.side)

    def device(self, colour, along, across, core):
        side = self.side
        x_first = 1 - colour // 2
        sign = 1 - 2 * lax.rem(colour, 2)
        dx = x_first * along + (1 - x_first) * across
        dy = x_first * across + (1 - x_first) * along
        x = lax.rem(self.x - sign * dx + 2 * side, side)
        y = lax.rem(self.y - sign * dy + 2 * side, side)
        return (y * side + x) * 2 + core

    def place(self, colour, s, h, core):
        return pl.ds(pl.multiple_of(self.device(colour, s, h, core) * self.tokens + colour * self.rows, self.rows), self.rows)

    def piece(self, colour, s, h):
        return self.all.at[self.place(colour, s, h, self.core)]

    def number(self, s, h):
        return s * self.side + h

    def ring_copy(self, colour, s, h, along, src=None):
        number = self.number(s + along, h + 1 - along)
        dst = self.piece(colour, s, h)
        peer = self.device(colour, -along, along - 1, self.core)
        return remote(dst if src is None else src, dst, self.ring_send.at[colour, number], self.ring_recv.at[colour, number], peer)

    def core_copy(self, colour, s, h, src=None):
        number = self.number(s, h)
        dst = self.piece(colour, s, h)
        return remote(dst if src is None else src, dst, self.core_send.at[colour, number], self.core_recv.at[colour, number], self.me + 1 - 2 * self.core)

    def arrival(self, colour, s, h):
        number = self.number(s, h)
        dst = self.piece(colour, s, h)
        return remote(dst, dst, self.ring_send.at[colour, number], self.ring_recv.at[colour, number], self.me)

    def core_arrival(self, colour, s, h):
        number = self.number(s, h)
        dst = self.all.at[self.place(colour, s, h, 1 - self.core)]
        return remote(dst, dst, self.core_send.at[colour, number], self.core_recv.at[colour, number], self.me)

    def begin(self):
        def one(colour):
            src = self.own.at[rows_of(colour, self.rows)]
            self.ring_copy(colour, 0, 0, 1, src).start()
            self.ring_copy(colour, 0, 0, 0, src).start()

        def other(colour):
            self.core_copy(colour, 0, 0, self.own.at[rows_of(colour, self.rows)]).start()

        each(0, 4, one)
        each(0, 4, other)

    def pass_on(self, s, h):
        def one(colour):
            self.arrival(colour, s, h).wait_recv()

            @pl.when((h == 0) & (s < self.side - 1))
            def _():
                self.ring_copy(colour, s, h, 1).start()

            @pl.when(h < self.side - 1)
            def _():
                self.ring_copy(colour, s, h, 0).start()

            self.core_copy(colour, s, h).start()

        each(0, 4, one)

    def got_core(self, s, h):
        each(0, 4, lambda colour: self.core_arrival(colour, s, h).wait_recv())

    def end(self):
        def sent(number):
            s, h = number // self.side, lax.rem(number, self.side)

            def one(colour):
                @pl.when((s > 0) | (h > 0))
                def _():
                    self.arrival(colour, s, h).wait_send()

                self.core_copy(colour, s, h).wait_send()

            each(0, 4, one)

        each(0, self.side * self.side, sent)


def front_part(
    n_dev, n_group, x_ref, dy_ref, pos_ref, freq_ref, gain_ref, bias_ref, wo_ref, wq_ref, wk_ref, wv_ref,
    h_all, dy_all, q_ref, k_ref, v_ref, da_ref, cos_ref, sin_ref, x_hat_ref, inv_ref, pos_in,
    h_send, h_recv, h_core_send, h_core_recv, dy_send, dy_recv, dy_core_send, dy_core_recv, w_sem, h_sem, dy_sem, pos_send, pos_recv, local,
    h_own, w_ref, wo_own, pick_ref, w_buf, h_buf, dy_buf, pos_own,
):
    me = lax.axis_index(AXIS)
    tokens, width = x_ref.shape
    head_dim = v_ref.shape[1]
    heads_tile = w_buf.shape[2]
    d_block = w_buf.shape[1]
    h_ring = Ring(n_dev, h_own, h_all, h_send, h_recv, h_core_send, h_core_recv)
    dy_ring = Ring(n_dev, dy_ref, dy_all, dy_send, dy_recv, dy_core_send, dy_core_recv)
    rows_n = h_ring.rows
    order = [(0, 0)] + ring_order(h_ring.side)
    n_event = len(order)
    where = Exchange(lambda peer: pos_own, lambda origin: pos_in.at[origin], lambda peer: pos_send.at[peer], lambda origin: pos_recv.at[origin])

    n_d = width // d_block
    kv_head = me // n_group

    def w_load(t, which):
        ref, head = ((wq_ref, me), (wk_ref, kv_head), (wv_ref, kv_head))[which]
        slot = lax.rem(t, 2)
        return pltpu.make_async_copy(ref.at[rows_of(t, d_block), rows_of(head // heads_tile, heads_tile)], w_buf.at[slot], w_sem.at[slot])

    own_dy = pltpu.make_async_copy(dy_ref, dy_all.at[rows_of(me, tokens)], local.at[0])
    own_h = pltpu.make_async_copy(h_own, h_all.at[rows_of(me, tokens)], local.at[1])
    own_wo = pltpu.make_async_copy(wo_ref.at[rows_of(me, head_dim)], wo_own, local.at[2])
    own_dy.start()
    own_wo.start()
    w_load(0, 0).start()
    pos_own[...] = jnp.broadcast_to(pos_ref[...], pos_own.shape)
    full_barrier(n_dev)
    dy_ring.begin()

    gain, bias = 1.0 + gain_ref[...], bias_ref[...]

    def norm(t):
        rows = rows_of(t, 16)
        x = x_ref[rows, :].astype(F32)
        centered = x - jnp.sum(x, axis=1, keepdims=True) * (1.0 / width)
        inv = lax.rsqrt(jnp.sum(centered * centered, axis=1, keepdims=True) * (1.0 / width) + EPS)
        x_hat = centered * inv
        x_hat_ref[rows, :] = x_hat
        inv_ref[rows, :] = inv
        h_own[rows, :] = (x_hat * gain + bias).astype(BF16)

    each(0, tokens // 16, norm)

    def send_pos(step):
        peer = alternate(me, step, n_dev)
        where.start(peer, me, peer)

    each(0, n_dev, send_pos)
    h_ring.begin()
    own_h.start()

    for which in range(3):
        head = me if which == 0 else kv_head

        def pick(t):
            @pl.when(t + 1 < n_d)
            def _():
                w_load(t + 1, which).start()

            w_load(t, which).wait()
            pick_ref[...] = jnp.swapaxes(w_buf[lax.rem(t, 2)], 0, 1)
            w_ref[rows_of(t, d_block), which * head_dim : (which + 1) * head_dim] = pick_ref[lax.rem(head, heads_tile)]

        each(0, n_d, pick)
        if which < 2:
            w_load(0, which + 1).start()
        if which == 0:
            dy_ring.pass_on(*(jnp.int32(v) for v in order[1]))
        if which == 1:
            h_ring.pass_on(*(jnp.int32(v) for v in order[1]))
    own_wo.wait()
    own_dy.wait()
    own_h.wait()

    def tables(origin):
        where.got(origin)
        angles = freq_ref[...] * pos_in[origin, 0:1, :].astype(F32)
        cos_ref[:, rows_of(origin, tokens)] = jnp.cos(angles)
        sin_ref[:, rows_of(origin, tokens)] = jnp.sin(angles)

    def event(e):
        return lookup([p[0] for p in order], e), lookup([p[1] for p in order], e)

    def places_of(ring, s, h):
        return [ring.place(jnp.int32(colour), s, h, core) for colour in range(4) for core in range(2)]

    def fetch(ring, buf, sem, e):
        slot = lax.rem(e, 2)
        s, h = event(e)
        ring.got_core(s, h)
        for n, place in enumerate(places_of(ring, s, h)):
            pltpu.make_async_copy(ring.all.at[place], buf.at[slot, pl.ds(n * rows_n, rows_n)], sem.at[slot]).start()

    def fetched(ring, buf, sem, e):
        slot = lax.rem(e, 2)
        pltpu.make_async_copy(ring.all.at[pl.ds(0, 8 * rows_n)], buf.at[slot], sem.at[slot]).wait()
        return buf[slot]

    def gradient_rows(e):
        s, h = event(e)
        da = dot_t(fetched(dy_ring, dy_buf, dy_sem, e), wo_own[...]).astype(BF16)
        for n, place in enumerate(places_of(dy_ring, s, h)):
            da_ref[place, :] = da[n * rows_n : (n + 1) * rows_n]

    def project_rows(e):
        s, h = event(e)
        out = dot(fetched(h_ring, h_buf, h_sem, e), w_ref[...])
        for n, place in enumerate(places_of(h_ring, s, h)):
            part = out[n * rows_n : (n + 1) * rows_n]
            q_ref[place, :] = part[:, :head_dim]
            k_ref[place, :] = part[:, head_dim : 2 * head_dim]
            v_ref[place, :] = part[:, 2 * head_dim :].astype(BF16)

    def step(e):
        for ring, buf, sem, rows in ((dy_ring, dy_buf, dy_sem, gradient_rows), (h_ring, h_buf, h_sem, project_rows)):
            @pl.when((e > 1) & (e < n_event))
            def _():
                ring.pass_on(*event(e))

            @pl.when((e > 0) & (e <= n_event))
            def _():
                fetch(ring, buf, sem, e - 1)

            @pl.when(e > 1)
            def _():
                rows(e - 2)

        @pl.when(e == 3)
        def _():
            each(0, n_dev, tables)

    each(1, n_event + 2, step)
    h_ring.end()
    dy_ring.end()
    each(0, n_dev, lambda index: where.sent(index, index))


def causal(block):
    key = lax.broadcasted_iota(jnp.int32, (block, block), 0)
    query = lax.broadcasted_iota(jnp.int32, (block, block), 1)
    return key <= query


def part_sum(values):
    return jnp.sum(values.reshape(values.shape[0] // 8, 8, values.shape[1]), axis=0)


def main_part(
    n_dev, n_group, q_heads, kv_heads, n_buf, scale,
    q_raw, k_raw, v_ref, da_ref, cos_ref, sin_ref, x_ref, dy_own_ref, x_hat_ref, inv_ref, gain_ref, h_ref, dy_ref, wq_ref, wk_ref, wv_ref, wo_ref,
    out_ref, gx_ref, gwo_ref, gwq_ref, gwk_ref, gwv_ref, gain_out, bias_out,
    q_rows, kv_rows, sum_ref, at_ref, dqt_ref, a_head, dq_head, dkvt_ref, a_ref, g_ref, dkv_ref, land_one, land_two, kv_ref, kvt_ref, wq_out, wkv_out, dh_ref, part_ref, own_sum, sum_in, sum_mine,
    a_send, a_recv, dq_send, dq_recv, one_send, one_recv, two_send, two_recv, kv_send, kv_recv, near_send, near_recv,
    load_sem, q_send, q_recv, wkv_send, wkv_recv, s_send, s_recv, t_send, t_recv,
):
    me = lax.axis_index(AXIS)
    seq, head_dim = v_ref.shape
    tokens, width = x_ref.shape
    block = tokens * n_group
    n_block = seq // block
    half = block // 2
    fold = scale * math.log2(math.e)
    core, side = lax.rem(me, 2), lax.rem(me // 2, 2)
    member, group = lax.rem(me, n_group), me // n_group
    partner, across = me + 1 - 2 * core, me + 2 - 4 * side
    shift = lax.rem(group, max(2, n_block * 3 // 4))
    depth = width // n_dev
    span = math.lcm(depth, 128)
    n_col = width // span
    per_col = span // depth
    per_core = n_dev // 2
    n_sum = sum_mine.shape[0]
    q_cols = q_heads * head_dim

    def piece(index):
        return rows_of(index, tokens)

    def column(head):
        return rows_of(head, head_dim)

    def cols(j):
        return rows_of(j, span)

    a_copy = Exchange(lambda peer: a_head.at[piece(peer)], lambda head: a_ref.at[:, column(head)], lambda peer: a_send.at[peer], lambda head: a_recv.at[head])
    dq_copy = Exchange(lambda peer: dq_head.at[piece(peer)], lambda head: g_ref.at[:, column(head)], lambda peer: dq_send.at[peer], lambda head: dq_recv.at[head])
    kv_copy = Exchange(lambda n: kv_ref.at[n // 2, piece(lax.rem(n, 2))], lambda slot: g_ref.at[:, column(q_heads + slot)], lambda n: kv_send.at[n], lambda slot: kv_recv.at[slot])
    q_copy = Exchange(lambda peer: wq_out.at[rows_of(peer, depth)], lambda head: q_rows.at[head], lambda peer: q_send.at[peer], lambda head: q_recv.at[head])
    wkv_copy = Exchange(lambda i: wkv_out.at[rows_of(i, depth)], lambda head: kv_rows.at[head], lambda i: wkv_send.at[i], lambda head: wkv_recv.at[head])
    s_copy = Exchange(lambda peer: own_sum.at[pl.ds(peer * n_sum, n_sum)], lambda origin: sum_in.at[origin], lambda peer: s_send.at[peer], lambda origin: s_recv.at[origin])
    t_copy = Exchange(lambda peer: sum_mine, lambda origin: sum_ref.at[pl.ds(origin * n_sum, n_sum)], lambda peer: t_send.at[peer], lambda origin: t_recv.at[origin])


    def one_copy(i):
        return remote(dkv_ref.at[rows_of(i * 2 + 1 - core, half)], land_one.at[i], one_send.at[i], one_recv.at[i], partner)

    kind = side * kv_heads + group

    def half_of(i, which):
        return rows_of(i * 2 + which, half)

    def two_copy(i):
        return remote(dkv_ref.at[half_of(i, core), column(1 - side)], land_two.at[i], two_send.at[i], two_recv.at[i], across)

    def near_copy(i, which):
        return remote(kvt_ref.at[i], dkvt_ref.at[:, half_of(i, which)], near_send.at[i], near_recv.at[i], partner)

    def first(i):
        one_copy(i).start()

    def second(i):
        one_copy(i).wait_recv()
        for which in (1 - side, side):
            dkv_ref[half_of(i, core), column(which)] += land_one[i, :, column(which)]
        two_copy(i).start()

    def close(i):
        two_copy(i).wait_recv()
        rows = half_of(i, core)
        total = (dkv_ref[rows, column(side)] + land_two[i]).T

        def keep(values):
            values = values.astype(BF16)
            kvt_ref[i] = values
            dkvt_ref[:, rows] = values
            kv_ref[i] = values.T

        @pl.when(side == 0)
        def _():
            keep(rotate(total, cos_ref[:, rows], -sin_ref[:, rows]))

        @pl.when(side == 1)
        def _():
            keep(total)

    def spread(i):
        near_copy(i, core).start()
        for u in range(2):
            kv_copy.start(i * 2 + u, kind, i * n_group + core * 2 + u)

    steps = (first, second, close, spread)

    def block_at(t):
        return lax.rem(shift - 1 - t + 2 * n_block, n_block)

    def stages(t):
        for late in range(len(steps), 0, -1):
            n = t - late - shift

            @pl.when(n >= 0)
            def _():
                steps[late - 1](n_block - 1 - n)

    def stage_rest(late):
        each(jnp.maximum(n_block - late - shift, 0), n_block, lambda n: steps[late - 1](n_block - 1 - n))

    def send_pieces(i):
        def send(u):
            peer = i * n_group + lax.rem(u + me, n_group)
            a_copy.start(peer, me, peer)
            dq_copy.start(peer, me, peer)

        each(0, n_group, send)

    def attention(q_ref, k_ref, qt_ref, kt_ref, vt_ref, e_ref, dp_ref, peak_ref, dat_ref, mix_ref, acc_ref):
        def prepare(i):
            rows = rows_of(i, block)
            for raw, turned, plain in ((q_raw, qt_ref, q_ref), (k_raw, kt_ref, k_ref)):
                t = rotate(raw[rows, :].T, cos_ref[:, rows], sin_ref[:, rows]).astype(BF16)
                turned[:, rows] = t
                plain[rows, :] = t.T
            vt_ref[:, rows] = v_ref[rows, :].T
            dkv_ref[rows, :] = jnp.zeros((block, 2 * head_dim), F32)

        each(0, n_block, prepare)

        def compute(i):
            own = rows_of(i, block)
            dat_ref[...] = da_ref[own, :].T
            mix_ref[...] = jnp.zeros_like(mix_ref)
            acc_ref[...] = jnp.zeros_like(acc_ref)

            def scores(j, carry, diagonal):
                peak, total, mixed = carry
                rows = rows_of(j, block)
                s = dot(k_ref[rows, :], qt_ref[:, own])
                if diagonal:
                    s = jnp.where(causal(block), s, -1e30)
                top = jnp.maximum(peak, jnp.max(s, axis=0, keepdims=True))
                e = jnp.exp2((s - top) * fold)
                dp = dot(v_ref[rows, :], dat_ref[...])
                fade = jnp.exp2((peak - top) * fold)
                e_ref[rows, :] = e
                dp_ref[rows, :] = dp
                peak_ref[j] = top
                return top, total * fade + part_sum(e), mixed * fade + part_sum(e * dp)

            start = (jnp.full((1, block), -jnp.inf, F32), jnp.zeros((8, block), F32), jnp.zeros((8, block), F32))
            carry = lax.fori_loop(0, i, functools.partial(scores, diagonal=False), start)
            peak, total, mixed = scores(i, carry, True)
            inv = 1.0 / jnp.sum(total, axis=0, keepdims=True)
            row_dot = jnp.sum(mixed, axis=0, keepdims=True) * inv
            q_own, da_own = q_ref[own, :], da_ref[own, :]

            def grads(j):
                rows = rows_of(j, block)
                p = e_ref[rows, :] * (jnp.exp2((peak_ref[j] - peak) * fold) * inv)
                pb = p.astype(BF16)
                ds = ((dp_ref[rows, :] - row_dot) * (p * scale)).astype(BF16)
                dkv_ref[rows, :head_dim] += dot(ds, q_own)
                dkv_ref[rows, head_dim:] += dot(pb, da_own)
                mix_ref[...] += dot(vt_ref[:, rows], pb)
                acc_ref[...] += dot(kt_ref[:, rows], ds)

            each(0, i + 1, grads)
            at = mix_ref[...].astype(BF16)
            at_ref[:, own] = at
            a_head[own, :] = at.T
            dqt = rotate(acc_ref[...], cos_ref[:, own], -sin_ref[:, own]).astype(BF16)
            dqt_ref[:, own] = dqt
            dq_head[own, :] = dqt.T

        def iteration(t):
            stages(t)

            @pl.when(t > 0)
            def _():
                send_pieces(block_at(t - 1))

            compute(block_at(t))

        each(0, n_block, iteration)

    pl.run_scoped(
        attention,
        pltpu.VMEM((seq, head_dim), BF16), pltpu.VMEM((seq, head_dim), BF16),
        pltpu.VMEM((head_dim, seq), BF16), pltpu.VMEM((head_dim, seq), BF16), pltpu.VMEM((head_dim, seq), BF16),
        pltpu.VMEM((seq, block), F32), pltpu.VMEM((seq, block), F32), pltpu.VMEM((n_block, 1, block), F32),
        pltpu.VMEM((head_dim, block), BF16), pltpu.VMEM((head_dim, block), F32), pltpu.VMEM((head_dim, block), F32),
    )

    def drain_sums():
        def one(i):
            one_copy(i).wait_send()
            two_copy(i).wait_send()
            near_copy(i, core).wait_send()
            near_copy(i, 1 - core).wait_recv()
            for u in range(2):
                kv_copy.sent(i * 2 + u, i * n_group + core * 2 + u)

        each(0, n_block, one)
        each(0, 2 * kv_heads, kv_copy.got)

    stage_rest(1)
    send_pieces(block_at(n_block - 1))

    def products(buf, w_buf):
        counts = (n_col, n_col, n_col, n_col // 2, n_col, n_col)
        starts = [sum(counts[:n]) for n in range(len(counts))]

        def loads(phase, j, slot):
            if phase == 2:
                return [pltpu.make_async_copy(wq_ref.at[cols(j)], w_buf.at[slot], load_sem.at[slot, 0])]
            if phase == 4:
                return [pltpu.make_async_copy(ref.at[cols(j)], w_buf.at[slot, :, pl.ds(n * kv_heads, kv_heads)], load_sem.at[slot, n]) for n, ref in enumerate((wk_ref, wv_ref))]
            ref = (h_ref, dy_ref, None, h_ref, None, wo_ref)[phase]
            col = core * (n_col // 2) + j if phase == 3 else j
            return [pltpu.make_async_copy(ref.at[:, cols(col)], buf.at[slot], load_sem.at[slot, 0])]

        def load(step):
            slot = lax.rem(step, n_buf)
            for phase, (begin, count) in enumerate(zip(starts, counts)):
                @pl.when((step >= begin) & (step < begin + count))
                def _():
                    for copy in loads(phase, step - begin, slot):
                        copy.start()

        def run(phase, body):
            def step(j):
                number = starts[phase] + j
                slot = lax.rem(number, n_buf)
                for copy in loads(phase, j, slot):
                    copy.wait()
                body(j, slot)
                load(number + n_buf)

            each(0, counts[phase], step)

        each(0, n_buf, load)

        def weight_columns(j, slot):
            @pl.when(j == n_col // 4)
            def _():
                stage_rest(2)

            wq_out[cols(j), :] = dot(dqt_ref[...], buf[slot]).T

        run(0, weight_columns)

        def send_rows(j):
            col = alternate(me // per_col, j, n_col)

            def send(u):
                peer = col * per_col + lax.rem(u + me, per_col)
                q_copy.start(peer, me, peer)

            each(0, per_col, send)

        def weight_out(j, slot):
            @pl.when(j < n_col // 2)
            def _():
                send_rows(j)

            gwo_ref[:, cols(j)] = dot(at_ref[...], buf[slot])

        run(1, weight_out)

        def got_heads(head):
            a_copy.got(head)
            dq_copy.got(head)

        each(0, n_dev, got_heads)

        def flat(slot, n_head):
            rows = w_buf[slot, :, :n_head, :]
            return rows.reshape(rows.shape[0], n_head * head_dim)

        def back_query(j, slot):
            for late, at in ((3, n_col // 4), (4, n_col * 3 // 8)):
                @pl.when(j == at)
                def _():
                    stage_rest(late)

            @pl.when(j >= n_col // 2)
            def _():
                send_rows(j)

            dh_ref[:, cols(j)] = dot_t(g_ref[:, :q_cols], flat(slot, q_heads))

        run(2, back_query)
        drain_sums()

        def weight_kv(j, slot):
            wkv_out[cols(j), :] = dot(dkvt_ref[...], buf[slot]).T

        run(3, weight_kv)

        def send_kv(step):
            index = alternate(lax.rem(me, per_core), step, per_core)
            wkv_copy.start(index, kind, core * per_core + index)

        def back_kv(j, slot):
            @pl.when(j == 0)
            def _():
                each(0, per_core, send_kv)

            dh_ref[:, cols(j)] += dot_t(g_ref[:, q_cols:], flat(slot, 2 * kv_heads))

        run(4, back_kv)

        part_ref[...] = jnp.zeros_like(part_ref)
        gain = 1.0 + gain_ref[...]

        def norm(t):
            rows = rows_of(t, 16)
            grad_h, x_hat = dh_ref[rows, :], x_hat_ref[rows, :]
            grad_hat = grad_h * gain
            one = jnp.sum(grad_hat, axis=1, keepdims=True) * (1.0 / width)
            two = jnp.sum(grad_hat * x_hat, axis=1, keepdims=True) * (1.0 / width)
            back = inv_ref[rows, :] * (grad_hat - one - x_hat * two)
            gx_ref[rows, :] = (dy_own_ref[rows, :].astype(F32) + back).astype(BF16)
            part_ref[0] += part_sum(grad_h * x_hat)
            part_ref[1] += part_sum(grad_h)

        each(0, tokens // 16, norm)
        own_sum[...] = jnp.zeros_like(own_sum)
        for which in range(2):
            total = jnp.sum(part_ref[which], axis=0, keepdims=True)
            for c in range(width // 128):
                own_sum[c, pl.ds(which, 1), :] = total[:, c * 128 : (c + 1) * 128]

        def to_all(copy):
            def send(step):
                peer = alternate(me, step, n_dev)
                copy.start(peer, me, peer)

            each(0, n_dev, send)

        def add(origin):
            sum_mine[...] += sum_in[origin]

        def output(j, slot):
            @pl.when(j == 0)
            def _():
                to_all(s_copy)

            @pl.when(j == n_col // 2)
            def _():
                each(0, n_dev, s_copy.got)
                sum_mine[...] = jnp.zeros_like(sum_mine)
                each(0, n_dev, add)

            out_ref[:, cols(j)] = (x_ref[:, cols(j)].astype(F32) + dot(a_ref[...], buf[slot])).astype(BF16)

            @pl.when(j == n_col // 2)
            def _():
                to_all(t_copy)

        run(5, output)

    pl.run_scoped(
        products,
        pltpu.VMEM((n_buf, seq, span), BF16),
        pltpu.VMEM((n_buf, span) + wq_ref.shape[1:], BF16),
    )

    def drain(index):
        for copy in (a_copy, dq_copy, s_copy, t_copy, q_copy):
            copy.sent(index, index)
        t_copy.got(index)
        q_copy.got(index)

    def drain_kv(index):
        wkv_copy.sent(index, core * per_core + index)

    each(0, n_dev, drain)
    each(0, per_core, drain_kv)
    each(0, 2 * kv_heads, wkv_copy.got)

    def settle(t):
        rows = rows_of(t, 8)
        gwq_ref[rows] = jnp.swapaxes(q_rows[:, rows, :], 0, 1)
        gwk_ref[rows] = jnp.swapaxes(kv_rows[:kv_heads, rows, :], 0, 1)
        gwv_ref[rows] = jnp.swapaxes(kv_rows[kv_heads:, rows, :], 0, 1)

    each(0, depth // 8, settle)
    for c in range(width // 128):
        gain_out[:, c * 128 : (c + 1) * 128] = sum_ref[c, 0:1, :]
        bias_out[:, c * 128 : (c + 1) * 128] = sum_ref[c, 1:2, :]


def block_kernel(n_dev, q_heads, kv_heads, n_buf, scale, *refs):
    x_ref, dy_ref, pos_ref, freq_ref, gain_ref, bias_ref, wo_ref, wq_ref, wk_ref, wv_ref = refs[:10]
    outs, (h_all, dy_all) = refs[10:18], refs[18:20]
    heads, pos_in, refs = refs[20:28], refs[28], refs[29:]
    front_sems, main_refs = refs[:14], refs[14:]
    tokens, width = x_ref.shape
    head_dim = wq_ref.shape[2]
    heads_tile = min(8, kv_heads)
    d_block = math.lcm(width // n_dev, 128)
    n_group = q_heads // kv_heads
    weights = (wo_ref, wq_ref, wk_ref, wv_ref)
    pl.run_scoped(
        functools.partial(front_part, n_dev, n_group, x_ref, dy_ref, pos_ref, freq_ref, gain_ref, bias_ref, *weights, h_all, dy_all, *heads, pos_in, *front_sems),
        pltpu.VMEM((tokens, width), BF16),
        pltpu.VMEM((width, 3 * head_dim), BF16),
        pltpu.VMEM((head_dim, width), BF16),
        pltpu.VMEM((heads_tile, d_block, head_dim), BF16),
        pltpu.VMEM((2, d_block, heads_tile, head_dim), BF16),
        pltpu.VMEM((2, 2 * tokens, width), BF16),
        pltpu.VMEM((2, 2 * tokens, width), BF16),
        pltpu.VMEM(pos_in.shape[1:], jnp.int32),
    )
    q, k, v, da, cos, sin, x_hat, inv = heads
    main_part(
        n_dev, n_group, q_heads, kv_heads, n_buf, scale,
        q, k, v, da, cos, sin, x_ref, dy_ref, x_hat, inv, gain_ref, h_all, dy_all, wq_ref, wk_ref, wv_ref, wo_ref, *outs, *main_refs,
    )


def whole_block(n_dev, x_own, dy_own, positions, freq, gain, bias, wo, wq, wk, wv):
    tokens, width = x_own.shape
    q_heads, head_dim = wq.shape[1:]
    kv_heads = wk.shape[1]
    seq = tokens * n_dev
    n_group = q_heads // kv_heads
    n_block = n_dev // n_group
    depth = width // n_dev
    n_buf = 3
    n_sum = -(-width // (128 * n_dev))
    sums = (n_sum * n_dev, 8, 128)
    pieces = math.isqrt(n_dev // 2) ** 2
    whole, anywhere = pl.BlockSpec(memory_space=pltpu.VMEM), pl.BlockSpec(memory_space=pl.ANY)
    dma = pltpu.SemaphoreType.DMA
    return pl.pallas_call(
        functools.partial(block_kernel, n_dev, q_heads, kv_heads, n_buf, head_dim**-0.5),
        out_shape=[
            jax.ShapeDtypeStruct((tokens, width), BF16),
            jax.ShapeDtypeStruct((tokens, width), BF16),
            jax.ShapeDtypeStruct((head_dim, width), F32),
            jax.ShapeDtypeStruct((depth, q_heads, head_dim), F32),
            jax.ShapeDtypeStruct((depth, kv_heads, head_dim), F32),
            jax.ShapeDtypeStruct((depth, kv_heads, head_dim), F32),
            jax.ShapeDtypeStruct((1, width), F32),
            jax.ShapeDtypeStruct((1, width), F32),
            jax.ShapeDtypeStruct((seq, width), BF16),
            jax.ShapeDtypeStruct((seq, width), BF16),
        ],
        in_specs=[whole] * 6 + [anywhere] * 4,
        out_specs=[whole] * 8 + [anywhere] * 2,
        scratch_shapes=[
            pltpu.VMEM((seq, head_dim), F32),
            pltpu.VMEM((seq, head_dim), F32),
            pltpu.VMEM((seq, head_dim), BF16),
            pltpu.VMEM((seq, head_dim), BF16),
            pltpu.VMEM((head_dim // 4, seq), F32),
            pltpu.VMEM((head_dim // 4, seq), F32),
            pltpu.VMEM((tokens, width), F32),
            pltpu.VMEM((tokens, 1), F32),
            pltpu.VMEM((n_dev, 8, tokens), jnp.int32),
            dma((4, pieces)), dma((4, pieces)), dma((4, pieces)), dma((4, pieces)),
            dma((4, pieces)), dma((4, pieces)), dma((4, pieces)), dma((4, pieces)),
            dma((2,)), dma((2,)), dma((2,)), dma((n_dev,)), dma((n_dev,)), dma((3,)),
            pltpu.VMEM((q_heads, depth, head_dim), F32),
            pltpu.VMEM((2 * kv_heads, depth, head_dim), F32),
            pltpu.VMEM(sums, F32),
            pltpu.VMEM((head_dim, seq), BF16),
            pltpu.VMEM((head_dim, seq), BF16),
            pltpu.VMEM((seq, head_dim), BF16),
            pltpu.VMEM((seq, head_dim), BF16),
            pltpu.VMEM((head_dim, seq), BF16),
            pltpu.VMEM((tokens, q_heads * head_dim), BF16),
            pltpu.VMEM((tokens, (q_heads + 2 * kv_heads) * head_dim), BF16),
            pltpu.VMEM((seq, 2 * head_dim), F32),
            pltpu.VMEM((n_block, tokens * n_group // 2, 2 * head_dim), F32),
            pltpu.VMEM((n_block, tokens * n_group // 2, head_dim), F32),
            pltpu.VMEM((n_block, tokens * n_group // 2, head_dim), BF16),
            pltpu.VMEM((n_block, head_dim, tokens * n_group // 2), BF16),
            pltpu.VMEM((width, head_dim), F32),
            pltpu.VMEM((width // 2, head_dim), F32),
            pltpu.VMEM((tokens, width), F32),
            pltpu.VMEM((2, 8, width), F32),
            pltpu.VMEM(sums, F32),
            pltpu.VMEM((n_dev, n_sum, 8, 128), F32),
            pltpu.VMEM((n_sum, 8, 128), F32),
            dma((n_dev,)), dma((n_dev,)), dma((n_dev,)), dma((n_dev,)),
            dma((n_block,)), dma((n_block,)), dma((n_block,)), dma((n_block,)), dma((2 * n_block,)), dma((2 * kv_heads,)), dma((n_block,)), dma((n_block,)),
            dma((n_buf, 3)), dma((n_dev,)), dma((n_dev,)), dma((n_dev // 2,)), dma((2 * kv_heads,)), dma((n_dev,)), dma((n_dev,)), dma((n_dev,)), dma((n_dev,)),
        ],
        compiler_params=pltpu.CompilerParams(collective_id=1, has_side_effects=True, vmem_limit_bytes=VMEM_LIMIT, flags=FLAGS),
        cost_estimate=pl.CostEstimate(flops=6 * seq * seq * head_dim + 16 * seq * width * head_dim, bytes_accessed=16 * seq * width, transcendentals=seq * seq // 2),
        name="block",
    )(x_own, dy_own, positions, freq, gain, bias, wo, wq, wk, wv)


def solution(mesh):
    n_dev = mesh.shape[AXIS]

    def device_step(x_act, d_out, positions, ln_gain, ln_bias, w_query, w_key, w_value, w_out):
        n_batch, piece, width = x_act.shape
        head_dim = w_query.shape[2]
        tokens = n_batch * piece

        x_own, dy_own = x_act.reshape(tokens, width), d_out.reshape(tokens, width)
        gain, bias = ln_gain.reshape(1, width), ln_bias.reshape(1, width)
        block_out, grad_x, grad_wo, grad_wq, grad_wk, grad_wv, grad_gain, grad_bias, _, _ = whole_block(
            n_dev, x_own, dy_own, positions.reshape(1, tokens), frequencies(head_dim, tokens), gain, bias, w_out, w_query, w_key, w_value
        )
        return (block_out.reshape(x_act.shape), grad_x.reshape(x_act.shape), grad_wq, grad_wk, grad_wv, grad_wo, grad_gain.reshape(width), grad_bias.reshape(width))

    return jax.shard_map(device_step, mesh=mesh, in_specs=(P("dp", AXIS, None), P("dp", AXIS, None), P("dp", AXIS), P(None), P(None), P(None, None, None), P(None, None, None), P(None, None, None), P(None, None)), out_specs=(P("dp", AXIS, None), P("dp", AXIS, None), P(("dp", AXIS), None, None), P(("dp", AXIS), None, None), P(("dp", AXIS), None, None), P(("dp", AXIS), None), P("dp"), P("dp")), check_vma=False)
```

```python
import functools
import math

import jax
import jax.numpy as jnp
import numpy as np
from jax import lax
from jax.experimental import pallas as pl
from jax.experimental.pallas import tpu as pltpu
from jax.sharding import PartitionSpec as P

EPS = 1e-5
ROPE_BASE = 10000.0
BLOCK = 512
AXIS = "cp"
BF16, F32 = jnp.bfloat16, jnp.float32
VMEM_LIMIT = 67043328
FLAGS = {}
SERVE = 7


def frequencies(head_dim, tokens):
    quarter = head_dim // 4
    freq = np.exp(np.arange(quarter, dtype=np.float32) * np.float32(-2.0 * math.log(ROPE_BASE) / (head_dim // 2)))
    return jnp.asarray(np.broadcast_to(freq[:, None], (quarter, tokens)))


def rotate(values, cos, sin):
    quarter = cos.shape[0]
    first, second = values[:quarter], values[quarter : 2 * quarter]
    return jnp.concatenate([first * cos - second * sin, second * cos + first * sin, values[2 * quarter :]], axis=0)


def rows_of(index, size):
    return pl.ds(pl.multiple_of(index * size, size), size)


def dot(lhs, rhs):
    return jnp.dot(lhs, rhs, preferred_element_type=F32)


def dot_t(lhs, rhs):
    return lax.dot_general(lhs, rhs, (((1,), (1,)), ((), ())), preferred_element_type=F32)


def full_barrier(n_dev):
    me = lax.axis_index(AXIS)
    barrier = pltpu.get_barrier_semaphore()

    def tell(step):
        pl.semaphore_signal(barrier, inc=1, device_id={AXIS: lax.rem(me + step, n_dev)}, device_id_type=pl.DeviceIdType.MESH)

    each(1, n_dev, tell)
    pl.semaphore_wait(barrier, n_dev - 1)


def remote(src, dst, send_sem, recv_sem, peer):
    return pltpu.make_async_remote_copy(src_ref=src, dst_ref=dst, send_sem=send_sem, recv_sem=recv_sem, device_id={AXIS: peer}, device_id_type=pl.DeviceIdType.MESH)


def each(lower, upper, body):
    def step(index, carry):
        body(index)
        return carry

    lax.fori_loop(lower, upper, step, 0)


def alternate(index, step, size):
    away = (step + 1) // 2
    return lax.rem(index + jnp.where(lax.rem(step, 2) == 1, away, size - away), size)


class Exchange:
    def __init__(self, src, dst, send, recv):
        self.src, self.dst, self.send, self.recv = src, dst, send, recv

    def start(self, index, slot, peer):
        me = lax.axis_index(AXIS)
        src, dst, recv = self.src(index), self.dst(slot), self.recv(slot)

        @pl.when(peer != me)
        def _():
            remote(src, dst, self.send(index), recv, peer).start()

        @pl.when(peer == me)
        def _():
            pltpu.make_async_copy(src, dst, recv).start()

    def sent(self, index, peer):
        me = lax.axis_index(AXIS)

        @pl.when(peer != me)
        def _():
            remote(self.src(index), self.src(index), self.send(index), self.send(index), me).wait_send()

    def got(self, slot):
        dst = self.dst(slot)
        remote(dst, dst, self.recv(slot), self.recv(slot), lax.axis_index(AXIS)).wait_recv()


def ring_order(side):
    queue, free, order = [(0.0, True, 0, 0), (0.0, False, 0, 0)], 0.0, []
    waiting = []
    while queue or waiting:
        if queue and (not waiting or free <= waiting[0][0]):
            at, along, s, h = queue.pop(0)
            free = max(free, at) + 1.0
            waiting.append((free + 0.5, (s + along, h + 1 - along)))
        else:
            at, (s, h) = waiting.pop(0)
            order.append((s, h))
            if h == 0 and s < side - 1:
                queue.append((at, True, s, h))
            if h < side - 1:
                queue.append((at, False, s, h))
    return order


def lookup(table, index):
    out = jnp.int32(table[0])
    for key, value in enumerate(table[1:], 1):
        out = jnp.where(index == key, jnp.int32(value), out)
    return out


class Ring:
    def __init__(self, n_dev, own, everything, ring_send, ring_recv, core_send, core_recv):
        self.own, self.all = own, everything
        self.ring_send, self.ring_recv, self.core_send, self.core_recv = ring_send, ring_recv, core_send, core_recv
        self.side = math.isqrt(n_dev // 2)
        self.tokens = own.shape[0]
        self.rows = self.tokens // 4
        self.me = lax.axis_index(AXIS)
        self.core = lax.rem(self.me, 2)
        self.x, self.y = lax.rem(self.me // 2, self.side), self.me // (2 * self.side)

    def device(self, colour, along, across, core):
        side = self.side
        x_first = 1 - colour // 2
        sign = 1 - 2 * lax.rem(colour, 2)
        dx = x_first * along + (1 - x_first) * across
        dy = x_first * across + (1 - x_first) * along
        x = lax.rem(self.x - sign * dx + 2 * side, side)
        y = lax.rem(self.y - sign * dy + 2 * side, side)
        return (y * side + x) * 2 + core

    def place(self, colour, s, h, core):
        return pl.ds(pl.multiple_of(self.device(colour, s, h, core) * self.tokens + colour * self.rows, self.rows), self.rows)

    def piece(self, colour, s, h):
        return self.all.at[self.place(colour, s, h, self.core)]

    def number(self, s, h):
        return s * self.side + h

    def ring_copy(self, colour, s, h, along, src=None):
        number = self.number(s + along, h + 1 - along)
        dst = self.piece(colour, s, h)
        peer = self.device(colour, -along, along - 1, self.core)
        return remote(dst if src is None else src, dst, self.ring_send.at[colour, number], self.ring_recv.at[colour, number], peer)

    def core_copy(self, colour, s, h, src=None):
        number = self.number(s, h)
        dst = self.piece(colour, s, h)
        return remote(dst if src is None else src, dst, self.core_send.at[colour, number], self.core_recv.at[colour, number], self.me + 1 - 2 * self.core)

    def arrival(self, colour, s, h):
        number = self.number(s, h)
        dst = self.piece(colour, s, h)
        return remote(dst, dst, self.ring_send.at[colour, number], self.ring_recv.at[colour, number], self.me)

    def core_arrival(self, colour, s, h):
        number = self.number(s, h)
        dst = self.all.at[self.place(colour, s, h, 1 - self.core)]
        return remote(dst, dst, self.core_send.at[colour, number], self.core_recv.at[colour, number], self.me)

    def begin(self):
        def one(colour):
            src = self.own.at[rows_of(colour, self.rows)]
            self.ring_copy(colour, 0, 0, 1, src).start()
            self.ring_copy(colour, 0, 0, 0, src).start()

        def other(colour):
            self.core_copy(colour, 0, 0, self.own.at[rows_of(colour, self.rows)]).start()

        each(0, 4, one)
        each(0, 4, other)

    def pass_on(self, s, h):
        def one(colour):
            self.arrival(colour, s, h).wait_recv()

            @pl.when((h == 0) & (s < self.side - 1))
            def _():
                self.ring_copy(colour, s, h, 1).start()

            @pl.when(h < self.side - 1)
            def _():
                self.ring_copy(colour, s, h, 0).start()

            self.core_copy(colour, s, h).start()

        each(0, 4, one)

    def got_core(self, s, h):
        each(0, 4, lambda colour: self.core_arrival(colour, s, h).wait_recv())

    def end(self):
        def sent(number):
            s, h = number // self.side, lax.rem(number, self.side)

            def one(colour):
                @pl.when((s > 0) | (h > 0))
                def _():
                    self.arrival(colour, s, h).wait_send()

                self.core_copy(colour, s, h).wait_send()

            each(0, 4, one)

        each(0, self.side * self.side, sent)


def front_part(
    n_dev, n_group, x_ref, dy_ref, pos_ref, freq_ref, gain_ref, bias_ref, wo_ref, wq_ref, wk_ref, wv_ref,
    h_all, dy_all, q_ref, k_ref, v_ref, da_ref, cos_ref, sin_ref, x_hat_ref, inv_ref, pos_in,
    h_send, h_recv, h_core_send, h_core_recv, dy_send, dy_recv, dy_core_send, dy_core_recv, w_sem, h_sem, wo_sem, pos_send, pos_recv, local, da_send, da_recv,
    h_own, w_ref, pick_ref, w_buf, h_buf, wo_buf, da_buf, pos_own,
):
    me = lax.axis_index(AXIS)
    tokens, width = x_ref.shape
    head_dim = v_ref.shape[1]
    heads_tile = w_buf.shape[2]
    d_block = w_buf.shape[1]
    span = wo_buf.shape[1]
    n_wo = wo_ref.shape[0] // span
    per_wo = span // head_dim
    h_ring = Ring(n_dev, h_own, h_all, h_send, h_recv, h_core_send, h_core_recv)
    dy_ring = Ring(n_dev, dy_ref, dy_all, dy_send, dy_recv, dy_core_send, dy_core_recv)
    rows_n = h_ring.rows
    order = [(0, 0)] + ring_order(h_ring.side)
    n_event = len(order)
    where = Exchange(lambda peer: pos_own, lambda origin: pos_in.at[origin], lambda peer: pos_send.at[peer], lambda origin: pos_recv.at[origin])

    da_copy = Exchange(lambda peer: da_buf.at[peer], lambda origin: da_ref.at[rows_of(origin, tokens)], lambda peer: da_send.at[peer], lambda origin: da_recv.at[origin])

    n_d = width // d_block
    kv_head = me // n_group

    def w_load(t, which):
        ref, head = ((wq_ref, me), (wk_ref, kv_head), (wv_ref, kv_head))[which]
        slot = lax.rem(t, 2)
        return pltpu.make_async_copy(ref.at[rows_of(t, d_block), rows_of(head // heads_tile, heads_tile)], w_buf.at[slot], w_sem.at[slot])

    own_dy = pltpu.make_async_copy(dy_ref, dy_all.at[rows_of(me, tokens)], local.at[0])
    own_h = pltpu.make_async_copy(h_own, h_all.at[rows_of(me, tokens)], local.at[1])
    own_dy.start()
    w_load(0, 0).start()

    def wo_turn(t):
        return alternate(me // per_wo, t, n_wo)

    def wo_load(t):
        slot = lax.rem(t, 2)
        return pltpu.make_async_copy(wo_ref.at[rows_of(wo_turn(t), span)], wo_buf.at[slot], wo_sem.at[slot])

    wo_load(jnp.int32(0)).start()
    wo_load(jnp.int32(1)).start()
    pos_own[...] = jnp.broadcast_to(pos_ref[...], pos_own.shape)
    gain, bias = 1.0 + gain_ref[...], bias_ref[...]

    def norm(t):
        rows = rows_of(t, 16)
        x = x_ref[rows, :].astype(F32)
        centered = x - jnp.sum(x, axis=1, keepdims=True) * (1.0 / width)
        inv = lax.rsqrt(jnp.sum(centered * centered, axis=1, keepdims=True) * (1.0 / width) + EPS)
        x_hat = centered * inv
        x_hat_ref[rows, :] = x_hat
        inv_ref[rows, :] = inv
        h_own[rows, :] = (x_hat * gain + bias).astype(BF16)

    each(0, tokens // 16, norm)
    full_barrier(n_dev)

    def send_pos(step):
        peer = alternate(me, step, n_dev)
        where.start(peer, me, peer)

    h_ring.begin()
    each(0, n_dev, send_pos)
    own_h.start()

    for which in range(3):
        head = me if which == 0 else kv_head

        def pick(t):
            @pl.when(t + 1 < n_d)
            def _():
                w_load(t + 1, which).start()

            w_load(t, which).wait()
            pick_ref[...] = jnp.swapaxes(w_buf[lax.rem(t, 2)], 0, 1)
            w_ref[rows_of(t, d_block), which * head_dim : (which + 1) * head_dim] = pick_ref[lax.rem(head, heads_tile)]

        each(0, n_d, pick)
        if which < 2:
            w_load(0, which + 1).start()
        if which == 1:
            h_ring.pass_on(*(jnp.int32(v) for v in order[1]))
    own_dy.wait()
    own_h.wait()

    def tables(origin):
        where.got(origin)
        angles = freq_ref[...] * pos_in[origin, 0:1, :].astype(F32)
        cos_ref[:, rows_of(origin, tokens)] = jnp.cos(angles)
        sin_ref[:, rows_of(origin, tokens)] = jnp.sin(angles)

    def event(e):
        return lookup([p[0] for p in order], e), lookup([p[1] for p in order], e)

    def places_of(ring, s, h):
        return [ring.place(jnp.int32(colour), s, h, core) for colour in range(4) for core in range(2)]

    def fetch(ring, buf, sem, e):
        slot = lax.rem(e, 2)
        s, h = event(e)
        ring.got_core(s, h)
        for n, place in enumerate(places_of(ring, s, h)):
            pltpu.make_async_copy(ring.all.at[place], buf.at[slot, pl.ds(n * rows_n, rows_n)], sem.at[slot]).start()

    def fetched(ring, buf, sem, e):
        slot = lax.rem(e, 2)
        pltpu.make_async_copy(ring.all.at[pl.ds(0, 8 * rows_n)], buf.at[slot], sem.at[slot]).wait()
        return buf[slot]

    def send_da(t):
        def one(u):
            peer = wo_turn(t) * per_wo + lax.rem(u + me, per_wo)
            da_copy.start(peer, me, peer)

        each(0, per_wo, one)

    def make_da(t):
        @pl.when((t > 0) & (t <= n_wo))
        def _():
            send_da(t - 1)

        @pl.when((t >= 0) & (t < n_wo))
        def _():
            wo_load(t).wait()
            da = dot_t(dy_ref[...], wo_buf[lax.rem(t, 2)]).astype(BF16)
            for u in range(per_wo):
                da_buf[wo_turn(t) * per_wo + u] = da[:, u * head_dim : (u + 1) * head_dim]

            @pl.when(t + 2 < n_wo)
            def _():
                wo_load(t + 2).start()

    def project_rows(e):
        s, h = event(e)
        out = dot(fetched(h_ring, h_buf, h_sem, e), w_ref[...])
        for n, place in enumerate(places_of(h_ring, s, h)):
            part = out[n * rows_n : (n + 1) * rows_n]
            q_ref[place, :] = part[:, :head_dim]
            k_ref[place, :] = part[:, head_dim : 2 * head_dim]
            v_ref[place, :] = part[:, 2 * head_dim :].astype(BF16)

    def step(e):
        @pl.when((e > 1) & (e < n_event))
        def _():
            h_ring.pass_on(*event(e))

        @pl.when(e == max(n_event - 3, 1))
        def _():
            dy_ring.begin()

        @pl.when(e <= n_event)
        def _():
            fetch(h_ring, h_buf, h_sem, e - 1)

        make_da(e - 1)

        @pl.when((e > 1) & (e < n_event + 2))
        def _():
            project_rows(e - 2)

        @pl.when(e == 3)
        def _():
            each(0, n_dev, tables)

    each(1, max(n_event, n_wo) + 2, step)
    h_ring.end()

    def drain(index):
        where.sent(index, index)
        da_copy.sent(index, index)
        da_copy.got(index)

    each(0, n_dev, drain)


def causal(block):
    key = lax.broadcasted_iota(jnp.int32, (block, block), 0)
    query = lax.broadcasted_iota(jnp.int32, (block, block), 1)
    return key <= query


def part_sum(values):
    return jnp.sum(values.reshape(values.shape[0] // 8, 8, values.shape[1]), axis=0)


def main_part(
    ring_sems, n_dev, n_group, q_heads, kv_heads, n_buf, scale,
    q_raw, k_raw, v_ref, da_ref, cos_ref, sin_ref, x_ref, dy_own_ref, x_hat_ref, inv_ref, gain_ref, h_ref, dy_ref, wq_ref, wk_ref, wv_ref, wo_ref,
    out_ref, gx_ref, gwo_ref, gwq_ref, gwk_ref, gwv_ref, gain_out, bias_out,
    q_rows, kv_rows, sum_ref, at_ref, dqt_ref, a_head, dq_head, dkvt_ref, a_ref, g_ref, dkv_ref, land_one, land_two, kv_ref, kvt_ref, wq_out, wkv_out, dh_ref, part_ref, own_sum, sum_in, sum_mine,
    a_send, a_recv, dq_send, dq_recv, one_send, one_recv, two_send, two_recv, kv_send, kv_recv, near_send, near_recv,
    load_sem, q_send, q_recv, wkv_send, wkv_recv, s_send, s_recv, t_send, t_recv,
):
    me = lax.axis_index(AXIS)
    seq, head_dim = v_ref.shape
    tokens, width = x_ref.shape
    block = tokens * n_group
    n_block = seq // block
    half = block // 2
    fold = scale * math.log2(math.e)
    core, side = lax.rem(me, 2), lax.rem(me // 2, 2)
    member, group = lax.rem(me, n_group), me // n_group
    partner, across = me + 1 - 2 * core, me + 2 - 4 * side
    shift = lax.rem(group, max(2, n_block * 3 // 4))
    depth = width // n_dev
    span = math.lcm(depth, 128)
    n_col = width // span
    per_col = span // depth
    per_core = n_dev // 2
    n_sum = sum_mine.shape[0]
    q_cols = q_heads * head_dim

    def piece(index):
        return rows_of(index, tokens)

    def column(head):
        return rows_of(head, head_dim)

    def cols(j):
        return rows_of(j, span)

    a_copy = Exchange(lambda peer: a_head.at[piece(peer)], lambda head: a_ref.at[:, column(head)], lambda peer: a_send.at[peer], lambda head: a_recv.at[head])
    dq_copy = Exchange(lambda peer: dq_head.at[piece(peer)], lambda head: g_ref.at[:, column(head)], lambda peer: dq_send.at[peer], lambda head: dq_recv.at[head])
    kv_copy = Exchange(lambda n: kv_ref.at[n // 2, piece(lax.rem(n, 2))], lambda slot: g_ref.at[:, column(q_heads + slot)], lambda n: kv_send.at[n], lambda slot: kv_recv.at[slot])
    q_copy = Exchange(lambda peer: wq_out.at[rows_of(peer, depth)], lambda head: q_rows.at[head], lambda peer: q_send.at[peer], lambda head: q_recv.at[head])
    wkv_copy = Exchange(lambda i: wkv_out.at[rows_of(i, depth)], lambda head: kv_rows.at[head], lambda i: wkv_send.at[i], lambda head: wkv_recv.at[head])
    s_copy = Exchange(lambda peer: own_sum.at[pl.ds(peer * n_sum, n_sum)], lambda origin: sum_in.at[origin], lambda peer: s_send.at[peer], lambda origin: s_recv.at[origin])
    t_copy = Exchange(lambda peer: sum_mine, lambda origin: sum_ref.at[pl.ds(origin * n_sum, n_sum)], lambda peer: t_send.at[peer], lambda origin: t_recv.at[origin])


    def one_copy(i):
        return remote(dkv_ref.at[rows_of(i * 2 + 1 - core, half)], land_one.at[i], one_send.at[i], one_recv.at[i], partner)

    kind = side * kv_heads + group

    def half_of(i, which):
        return rows_of(i * 2 + which, half)

    def two_copy(i):
        return remote(dkv_ref.at[half_of(i, core), column(1 - side)], land_two.at[i], two_send.at[i], two_recv.at[i], across)

    def near_copy(i, which):
        return remote(kvt_ref.at[i], dkvt_ref.at[:, half_of(i, which)], near_send.at[i], near_recv.at[i], partner)

    def first(i):
        one_copy(i).start()

    def second(i):
        one_copy(i).wait_recv()
        for which in (1 - side, side):
            dkv_ref[half_of(i, core), column(which)] += land_one[i, :, column(which)]
        two_copy(i).start()

    def close(i):
        two_copy(i).wait_recv()
        rows = half_of(i, core)
        total = (dkv_ref[rows, column(side)] + land_two[i]).T

        def keep(values):
            values = values.astype(BF16)
            kvt_ref[i] = values
            dkvt_ref[:, rows] = values
            kv_ref[i] = values.T

        @pl.when(side == 0)
        def _():
            keep(rotate(total, cos_ref[:, rows], -sin_ref[:, rows]))

        @pl.when(side == 1)
        def _():
            keep(total)

    def spread(i):
        near_copy(i, core).start()
        for u in range(2):
            kv_copy.start(i * 2 + u, kind, i * n_group + core * 2 + u)

    steps = (first, second, close, spread)

    def block_at(t):
        return lax.rem(shift - 1 - t + 2 * n_block, n_block)

    def stages(t):
        for late in range(len(steps), 0, -1):
            n = t - late - shift

            @pl.when(n >= 0)
            def _():
                steps[late - 1](n_block - 1 - n)

    def stage_rest(late):
        each(jnp.maximum(n_block - late - shift, 0), n_block, lambda n: steps[late - 1](n_block - 1 - n))

    def send_pieces(i):
        def send(u):
            peer = i * n_group + lax.rem(u + me, n_group)
            a_copy.start(peer, me, peer)
            dq_copy.start(peer, me, peer)

        each(0, n_group, send)

    dy_ring = Ring(n_dev, dy_own_ref, dy_ref, *ring_sems)
    order = [(0, 0)] + ring_order(dy_ring.side)
    n_served = min(len(order) - 1, (n_block * (n_block + 1) - 1) // SERVE + 1)

    def serve(number):
        @pl.when(number < len(order))
        def _():
            dy_ring.pass_on(lookup([p[0] for p in order], number), lookup([p[1] for p in order], number))

    def tick(count):
        @pl.when(lax.rem(count, SERVE) == 0)
        def _():
            serve(count // SERVE + 1)

    def attention(q_ref, k_ref, qt_ref, kt_ref, vt_ref, e_ref, dp_ref, peak_ref, dat_ref, mix_ref, acc_ref):
        def prepare(i):
            rows = rows_of(i, block)
            for raw, turned, plain in ((q_raw, qt_ref, q_ref), (k_raw, kt_ref, k_ref)):
                t = rotate(raw[rows, :].T, cos_ref[:, rows], sin_ref[:, rows]).astype(BF16)
                turned[:, rows] = t
                plain[rows, :] = t.T
            vt_ref[:, rows] = v_ref[rows, :].T
            dkv_ref[rows, :] = jnp.zeros((block, 2 * head_dim), F32)

        each(0, n_block, prepare)

        def compute(i, done):
            own = rows_of(i, block)
            dat_ref[...] = da_ref[own, :].T
            mix_ref[...] = jnp.zeros_like(mix_ref)
            acc_ref[...] = jnp.zeros_like(acc_ref)

            def scores(j, carry, diagonal):
                peak, total, mixed = carry
                tick(done + j)
                rows = rows_of(j, block)
                s = dot(k_ref[rows, :], qt_ref[:, own])
                if diagonal:
                    s = jnp.where(causal(block), s, -1e30)
                top = jnp.maximum(peak, jnp.max(s, axis=0, keepdims=True))
                e = jnp.exp2((s - top) * fold)
                dp = dot(v_ref[rows, :], dat_ref[...])
                fade = jnp.exp2((peak - top) * fold)
                e_ref[rows, :] = e
                dp_ref[rows, :] = dp
                peak_ref[j] = top
                return top, total * fade + part_sum(e), mixed * fade + part_sum(e * dp)

            start = (jnp.full((1, block), -jnp.inf, F32), jnp.zeros((8, block), F32), jnp.zeros((8, block), F32))
            carry = lax.fori_loop(0, i, functools.partial(scores, diagonal=False), start)
            peak, total, mixed = scores(i, carry, True)
            inv = 1.0 / jnp.sum(total, axis=0, keepdims=True)
            row_dot = jnp.sum(mixed, axis=0, keepdims=True) * inv
            q_own, da_own = q_ref[own, :], da_ref[own, :]

            def grads(j):
                tick(done + i + 1 + j)
                rows = rows_of(j, block)
                p = e_ref[rows, :] * (jnp.exp2((peak_ref[j] - peak) * fold) * inv)
                pb = p.astype(BF16)
                ds = ((dp_ref[rows, :] - row_dot) * (p * scale)).astype(BF16)
                dkv_ref[rows, :head_dim] += dot(ds, q_own)
                dkv_ref[rows, head_dim:] += dot(pb, da_own)
                mix_ref[...] += dot(vt_ref[:, rows], pb)
                acc_ref[...] += dot(kt_ref[:, rows], ds)

            each(0, i + 1, grads)
            at = mix_ref[...].astype(BF16)
            at_ref[:, own] = at
            a_head[own, :] = at.T
            dqt = rotate(acc_ref[...], cos_ref[:, own], -sin_ref[:, own]).astype(BF16)
            dqt_ref[:, own] = dqt
            dq_head[own, :] = dqt.T

        def iteration(t, done):
            stages(t)

            @pl.when(t > 0)
            def _():
                send_pieces(block_at(t - 1))

            i = block_at(t)
            compute(i, done)
            return done + 2 * (i + 1)

        lax.fori_loop(0, n_block, iteration, jnp.int32(0))

    pl.run_scoped(
        attention,
        pltpu.VMEM((seq, head_dim), BF16), pltpu.VMEM((seq, head_dim), BF16),
        pltpu.VMEM((head_dim, seq), BF16), pltpu.VMEM((head_dim, seq), BF16), pltpu.VMEM((head_dim, seq), BF16),
        pltpu.VMEM((seq, block), F32), pltpu.VMEM((seq, block), F32), pltpu.VMEM((n_block, 1, block), F32),
        pltpu.VMEM((head_dim, block), BF16), pltpu.VMEM((head_dim, block), F32), pltpu.VMEM((head_dim, block), F32),
    )

    def drain_sums():
        def one(i):
            one_copy(i).wait_send()
            two_copy(i).wait_send()
            near_copy(i, core).wait_send()
            near_copy(i, 1 - core).wait_recv()
            for u in range(2):
                kv_copy.sent(i * 2 + u, i * n_group + core * 2 + u)

        each(0, n_block, one)
        each(0, 2 * kv_heads, kv_copy.got)

    stage_rest(1)
    send_pieces(block_at(n_block - 1))

    def products(buf, w_buf):
        counts = (n_col, n_col, n_col, n_col // 2, n_col, n_col)
        starts = [sum(counts[:n]) for n in range(len(counts))]

        def loads(phase, j, slot):
            if phase == 1:
                return [pltpu.make_async_copy(wq_ref.at[cols(j)], w_buf.at[slot], load_sem.at[slot, 0])]
            if phase == 4:
                return [pltpu.make_async_copy(ref.at[cols(j)], w_buf.at[slot, :, pl.ds(n * kv_heads, kv_heads)], load_sem.at[slot, n]) for n, ref in enumerate((wk_ref, wv_ref))]
            ref = (h_ref, None, wo_ref, h_ref, None, dy_ref)[phase]
            col = core * (n_col // 2) + j if phase == 3 else j
            return [pltpu.make_async_copy(ref.at[:, cols(col)], buf.at[slot], load_sem.at[slot, 0])]

        def load(step):
            slot = lax.rem(step, n_buf)
            for phase, (begin, count) in enumerate(zip(starts, counts)):
                @pl.when((step >= begin) & (step < begin + count))
                def _():
                    for copy in loads(phase, step - begin, slot):
                        copy.start()

        def run(phase, body):
            def step(j):
                number = starts[phase] + j
                slot = lax.rem(number, n_buf)
                for copy in loads(phase, j, slot):
                    copy.wait()
                body(j, slot)
                load(number + n_buf)

            each(0, counts[phase], step)

        each(0, n_buf, load)

        def serve_late(number):
            for r in range(len(order) - 1 - n_served):
                @pl.when(number == 1 + 4 * r)
                def _():
                    serve(jnp.int32(n_served + 1 + r))

        def weight_columns(j, slot):
            serve_late(j)

            @pl.when(j == n_col // 4)
            def _():
                stage_rest(2)

            wq_out[cols(j), :] = dot(dqt_ref[...], buf[slot]).T

        run(0, weight_columns)

        def send_rows(j):
            col = alternate(me // per_col, j, n_col)

            def send(u):
                peer = col * per_col + lax.rem(u + me, per_col)
                q_copy.start(peer, me, peer)

            each(0, per_col, send)

        def got_heads(head):
            a_copy.got(head)
            dq_copy.got(head)

        each(0, n_dev, got_heads)

        def flat(slot, n_head):
            rows = w_buf[slot, :, :n_head, :]
            return rows.reshape(rows.shape[0], n_head * head_dim)

        def back_query(j, slot):
            serve_late(n_col + j)
            for late, at in ((3, n_col * 3 // 4), (4, n_col - 1)):
                @pl.when(j == at)
                def _():
                    stage_rest(late)

            @pl.when(j < n_col // 2)
            def _():
                send_rows(j)

            dh_ref[:, cols(j)] = dot_t(g_ref[:, :q_cols], flat(slot, q_heads))

        run(1, back_query)

        def output(j, slot):
            @pl.when(j < n_col // 2)
            def _():
                send_rows(n_col // 2 + j)

            out_ref[:, cols(j)] = (x_ref[:, cols(j)].astype(F32) + dot(a_ref[...], buf[slot])).astype(BF16)

        run(2, output)
        drain_sums()

        def weight_kv(j, slot):
            wkv_out[cols(j), :] = dot(dkvt_ref[...], buf[slot]).T

        run(3, weight_kv)
        for s, h in order:
            dy_ring.got_core(jnp.int32(s), jnp.int32(h))

        def send_kv(step):
            index = alternate(lax.rem(me, per_core), step, per_core)
            wkv_copy.start(index, kind, core * per_core + index)

        def back_kv(j, slot):
            @pl.when(j == 0)
            def _():
                each(0, per_core, send_kv)

            dh_ref[:, cols(j)] += dot_t(g_ref[:, q_cols:], flat(slot, 2 * kv_heads))

        run(4, back_kv)

        part_ref[...] = jnp.zeros_like(part_ref)
        gain = 1.0 + gain_ref[...]

        def norm(t):
            rows = rows_of(t, 16)
            grad_h, x_hat = dh_ref[rows, :], x_hat_ref[rows, :]
            grad_hat = grad_h * gain
            one = jnp.sum(grad_hat, axis=1, keepdims=True) * (1.0 / width)
            two = jnp.sum(grad_hat * x_hat, axis=1, keepdims=True) * (1.0 / width)
            back = inv_ref[rows, :] * (grad_hat - one - x_hat * two)
            gx_ref[rows, :] = (dy_own_ref[rows, :].astype(F32) + back).astype(BF16)
            part_ref[0] += part_sum(grad_h * x_hat)
            part_ref[1] += part_sum(grad_h)

        each(0, tokens // 16, norm)
        own_sum[...] = jnp.zeros_like(own_sum)
        for which in range(2):
            total = jnp.sum(part_ref[which], axis=0, keepdims=True)
            for c in range(width // 128):
                own_sum[c, pl.ds(which, 1), :] = total[:, c * 128 : (c + 1) * 128]

        def to_all(copy):
            def send(step):
                peer = alternate(me, step, n_dev)
                copy.start(peer, me, peer)

            each(0, n_dev, send)

        def add(origin):
            sum_mine[...] += sum_in[origin]

        def weight_out(j, slot):
            @pl.when(j == 0)
            def _():
                to_all(s_copy)

            @pl.when(j == n_col // 2)
            def _():
                each(0, n_dev, s_copy.got)
                sum_mine[...] = jnp.zeros_like(sum_mine)
                each(0, n_dev, add)

            gwo_ref[:, cols(j)] = dot(at_ref[...], buf[slot])

            @pl.when(j == n_col // 2)
            def _():
                to_all(t_copy)

        run(5, weight_out)

    pl.run_scoped(
        products,
        pltpu.VMEM((n_buf, seq, span), BF16),
        pltpu.VMEM((n_buf, span) + wq_ref.shape[1:], BF16),
    )

    dy_ring.end()

    def drain(index):
        for copy in (a_copy, dq_copy, s_copy, t_copy, q_copy):
            copy.sent(index, index)
        t_copy.got(index)
        q_copy.got(index)

    def drain_kv(index):
        wkv_copy.sent(index, core * per_core + index)

    each(0, n_dev, drain)
    each(0, per_core, drain_kv)
    each(0, 2 * kv_heads, wkv_copy.got)

    def settle(t):
        rows = rows_of(t, 8)
        gwq_ref[rows] = jnp.swapaxes(q_rows[:, rows, :], 0, 1)
        gwk_ref[rows] = jnp.swapaxes(kv_rows[:kv_heads, rows, :], 0, 1)
        gwv_ref[rows] = jnp.swapaxes(kv_rows[kv_heads:, rows, :], 0, 1)

    each(0, depth // 8, settle)
    for c in range(width // 128):
        gain_out[:, c * 128 : (c + 1) * 128] = sum_ref[c, 0:1, :]
        bias_out[:, c * 128 : (c + 1) * 128] = sum_ref[c, 1:2, :]


def block_kernel(n_dev, q_heads, kv_heads, n_buf, scale, *refs):
    x_ref, dy_ref, pos_ref, freq_ref, gain_ref, bias_ref, wo_ref, wq_ref, wk_ref, wv_ref = refs[:10]
    outs, (h_all, dy_all) = refs[10:18], refs[18:20]
    heads, pos_in, refs = refs[20:28], refs[28], refs[29:]
    front_sems, main_refs = refs[:16], refs[16:]
    tokens, width = x_ref.shape
    head_dim = wq_ref.shape[2]
    heads_tile = min(8, kv_heads)
    d_block = math.lcm(width // n_dev, 128)
    n_group = q_heads // kv_heads
    weights = (wo_ref, wq_ref, wk_ref, wv_ref)
    pl.run_scoped(
        functools.partial(front_part, n_dev, n_group, x_ref, dy_ref, pos_ref, freq_ref, gain_ref, bias_ref, *weights, h_all, dy_all, *heads, pos_in, *front_sems),
        pltpu.VMEM((tokens, width), BF16),
        pltpu.VMEM((width, 3 * head_dim), BF16),
        pltpu.VMEM((heads_tile, d_block, head_dim), BF16),
        pltpu.VMEM((2, d_block, heads_tile, head_dim), BF16),
        pltpu.VMEM((2, 2 * tokens, width), BF16),
        pltpu.VMEM((2, min(BLOCK, q_heads * head_dim // 2), width), BF16),
        pltpu.VMEM((n_dev, tokens, head_dim), BF16),
        pltpu.VMEM(pos_in.shape[1:], jnp.int32),
    )
    q, k, v, da, cos, sin, x_hat, inv = heads
    main_part(
        front_sems[4:8], n_dev, n_group, q_heads, kv_heads, n_buf, scale,
        q, k, v, da, cos, sin, x_ref, dy_ref, x_hat, inv, gain_ref, h_all, dy_all, wq_ref, wk_ref, wv_ref, wo_ref, *outs, *main_refs,
    )


def whole_block(n_dev, x_own, dy_own, positions, freq, gain, bias, wo, wq, wk, wv):
    tokens, width = x_own.shape
    q_heads, head_dim = wq.shape[1:]
    kv_heads = wk.shape[1]
    seq = tokens * n_dev
    n_group = q_heads // kv_heads
    n_block = n_dev // n_group
    depth = width // n_dev
    n_buf = 3
    n_sum = -(-width // (128 * n_dev))
    sums = (n_sum * n_dev, 8, 128)
    pieces = math.isqrt(n_dev // 2) ** 2
    whole, anywhere = pl.BlockSpec(memory_space=pltpu.VMEM), pl.BlockSpec(memory_space=pl.ANY)
    dma = pltpu.SemaphoreType.DMA
    return pl.pallas_call(
        functools.partial(block_kernel, n_dev, q_heads, kv_heads, n_buf, head_dim**-0.5),
        out_shape=[
            jax.ShapeDtypeStruct((tokens, width), BF16),
            jax.ShapeDtypeStruct((tokens, width), BF16),
            jax.ShapeDtypeStruct((head_dim, width), F32),
            jax.ShapeDtypeStruct((depth, q_heads, head_dim), F32),
            jax.ShapeDtypeStruct((depth, kv_heads, head_dim), F32),
            jax.ShapeDtypeStruct((depth, kv_heads, head_dim), F32),
            jax.ShapeDtypeStruct((1, width), F32),
            jax.ShapeDtypeStruct((1, width), F32),
            jax.ShapeDtypeStruct((seq, width), BF16),
            jax.ShapeDtypeStruct((seq, width), BF16),
        ],
        in_specs=[whole] * 6 + [anywhere] * 4,
        out_specs=[whole] * 8 + [anywhere] * 2,
        scratch_shapes=[
            pltpu.VMEM((seq, head_dim), F32),
            pltpu.VMEM((seq, head_dim), F32),
            pltpu.VMEM((seq, head_dim), BF16),
            pltpu.VMEM((seq, head_dim), BF16),
            pltpu.VMEM((head_dim // 4, seq), F32),
            pltpu.VMEM((head_dim // 4, seq), F32),
            pltpu.VMEM((tokens, width), F32),
            pltpu.VMEM((tokens, 1), F32),
            pltpu.VMEM((n_dev, 8, tokens), jnp.int32),
            dma((4, pieces)), dma((4, pieces)), dma((4, pieces)), dma((4, pieces)),
            dma((4, pieces)), dma((4, pieces)), dma((4, pieces)), dma((4, pieces)),
            dma((2,)), dma((2,)), dma((2,)), dma((n_dev,)), dma((n_dev,)), dma((3,)), dma((n_dev,)), dma((n_dev,)),
            pltpu.VMEM((q_heads, depth, head_dim), F32),
            pltpu.VMEM((2 * kv_heads, depth, head_dim), F32),
            pltpu.VMEM(sums, F32),
            pltpu.VMEM((head_dim, seq), BF16),
            pltpu.VMEM((head_dim, seq), BF16),
            pltpu.VMEM((seq, head_dim), BF16),
            pltpu.VMEM((seq, head_dim), BF16),
            pltpu.VMEM((head_dim, seq), BF16),
            pltpu.VMEM((tokens, q_heads * head_dim), BF16),
            pltpu.VMEM((tokens, (q_heads + 2 * kv_heads) * head_dim), BF16),
            pltpu.VMEM((seq, 2 * head_dim), F32),
            pltpu.VMEM((n_block, tokens * n_group // 2, 2 * head_dim), F32),
            pltpu.VMEM((n_block, tokens * n_group // 2, head_dim), F32),
            pltpu.VMEM((n_block, tokens * n_group // 2, head_dim), BF16),
            pltpu.VMEM((n_block, head_dim, tokens * n_group // 2), BF16),
            pltpu.VMEM((width, head_dim), F32),
            pltpu.VMEM((width // 2, head_dim), F32),
            pltpu.VMEM((tokens, width), F32),
            pltpu.VMEM((2, 8, width), F32),
            pltpu.VMEM(sums, F32),
            pltpu.VMEM((n_dev, n_sum, 8, 128), F32),
            pltpu.VMEM((n_sum, 8, 128), F32),
            dma((n_dev,)), dma((n_dev,)), dma((n_dev,)), dma((n_dev,)),
            dma((n_block,)), dma((n_block,)), dma((n_block,)), dma((n_block,)), dma((2 * n_block,)), dma((2 * kv_heads,)), dma((n_block,)), dma((n_block,)),
            dma((n_buf, 3)), dma((n_dev,)), dma((n_dev,)), dma((n_dev // 2,)), dma((2 * kv_heads,)), dma((n_dev,)), dma((n_dev,)), dma((n_dev,)), dma((n_dev,)),
        ],
        compiler_params=pltpu.CompilerParams(collective_id=1, has_side_effects=True, vmem_limit_bytes=VMEM_LIMIT, flags=FLAGS),
        cost_estimate=pl.CostEstimate(flops=6 * seq * seq * head_dim + 16 * seq * width * head_dim, bytes_accessed=16 * seq * width, transcendentals=seq * seq // 2),
        name="block",
    )(x_own, dy_own, positions, freq, gain, bias, wo, wq, wk, wv)


def solution(mesh):
    n_dev = mesh.shape[AXIS]

    def device_step(x_act, d_out, positions, ln_gain, ln_bias, w_query, w_key, w_value, w_out):
        n_batch, piece, width = x_act.shape
        head_dim = w_query.shape[2]
        tokens = n_batch * piece

        x_own, dy_own = x_act.reshape(tokens, width), d_out.reshape(tokens, width)
        gain, bias = ln_gain.reshape(1, width), ln_bias.reshape(1, width)
        block_out, grad_x, grad_wo, grad_wq, grad_wk, grad_wv, grad_gain, grad_bias, _, _ = whole_block(
            n_dev, x_own, dy_own, positions.reshape(1, tokens), frequencies(head_dim, tokens), gain, bias, w_out, w_query, w_key, w_value
        )
        return (block_out.reshape(x_act.shape), grad_x.reshape(x_act.shape), grad_wq, grad_wk, grad_wv, grad_wo, grad_gain.reshape(width), grad_bias.reshape(width))

    return jax.shard_map(device_step, mesh=mesh, in_specs=(P("dp", AXIS, None), P("dp", AXIS, None), P("dp", AXIS), P(None), P(None), P(None, None, None), P(None, None, None), P(None, None, None), P(None, None)), out_specs=(P("dp", AXIS, None), P("dp", AXIS, None), P(("dp", AXIS), None, None), P(("dp", AXIS), None, None), P(("dp", AXIS), None, None), P(("dp", AXIS), None), P("dp"), P("dp")), check_vma=False)
```

```python
import functools
import math

import jax
import jax.numpy as jnp
import numpy as np
from jax import lax
from jax.experimental import pallas as pl
from jax.experimental.pallas import tpu as pltpu
from jax.sharding import PartitionSpec as P

EPS = 1e-5
ROPE_BASE = 10000.0
BLOCK = 512
AXIS = "cp"
BF16, F32 = jnp.bfloat16, jnp.float32
VMEM_LIMIT = 67043328
FLAGS = {}
SERVE = 7


def frequencies(head_dim, tokens):
    quarter = head_dim // 4
    freq = np.exp(np.arange(quarter, dtype=np.float32) * np.float32(-2.0 * math.log(ROPE_BASE) / (head_dim // 2)))
    return jnp.asarray(np.broadcast_to(freq[:, None], (quarter, tokens)))


def rotate(values, cos, sin):
    quarter = cos.shape[0]
    first, second = values[:quarter], values[quarter : 2 * quarter]
    return jnp.concatenate([first * cos - second * sin, second * cos + first * sin, values[2 * quarter :]], axis=0)


def rows_of(index, size):
    return pl.ds(pl.multiple_of(index * size, size), size)


def dot(lhs, rhs):
    return jnp.dot(lhs, rhs, preferred_element_type=F32)


def dot_t(lhs, rhs):
    return lax.dot_general(lhs, rhs, (((1,), (1,)), ((), ())), preferred_element_type=F32)


def full_barrier(n_dev):
    me = lax.axis_index(AXIS)
    barrier = pltpu.get_barrier_semaphore()

    def tell(step):
        pl.semaphore_signal(barrier, inc=1, device_id={AXIS: lax.rem(me + step, n_dev)}, device_id_type=pl.DeviceIdType.MESH)

    each(1, n_dev, tell)
    pl.semaphore_wait(barrier, n_dev - 1)


def remote(src, dst, send_sem, recv_sem, peer):
    return pltpu.make_async_remote_copy(src_ref=src, dst_ref=dst, send_sem=send_sem, recv_sem=recv_sem, device_id={AXIS: peer}, device_id_type=pl.DeviceIdType.MESH)


def each(lower, upper, body):
    def step(index, carry):
        body(index)
        return carry

    lax.fori_loop(lower, upper, step, 0)


def alternate(index, step, size):
    away = (step + 1) // 2
    return lax.rem(index + jnp.where(lax.rem(step, 2) == 1, away, size - away), size)


class Exchange:
    def __init__(self, src, dst, send, recv):
        self.src, self.dst, self.send, self.recv = src, dst, send, recv

    def start(self, index, slot, peer):
        me = lax.axis_index(AXIS)
        src, dst, recv = self.src(index), self.dst(slot), self.recv(slot)

        @pl.when(peer != me)
        def _():
            remote(src, dst, self.send(index), recv, peer).start()

        @pl.when(peer == me)
        def _():
            pltpu.make_async_copy(src, dst, recv).start()

    def sent(self, index, peer):
        me = lax.axis_index(AXIS)

        @pl.when(peer != me)
        def _():
            remote(self.src(index), self.src(index), self.send(index), self.send(index), me).wait_send()

    def got(self, slot):
        dst = self.dst(slot)
        remote(dst, dst, self.recv(slot), self.recv(slot), lax.axis_index(AXIS)).wait_recv()


def early_events(n_event):
    return 2 if n_event > 4 else 0


def ring_order(side):
    queue, free, order = [(0.0, True, 0, 0), (0.0, False, 0, 0)], 0.0, []
    waiting = []
    while queue or waiting:
        if queue and (not waiting or free <= waiting[0][0]):
            at, along, s, h = queue.pop(0)
            free = max(free, at) + 1.0
            waiting.append((free + 0.5, (s + along, h + 1 - along)))
        else:
            at, (s, h) = waiting.pop(0)
            order.append((s, h))
            if h == 0 and s < side - 1:
                queue.append((at, True, s, h))
            if h < side - 1:
                queue.append((at, False, s, h))
    return order


def lookup(table, index):
    out = jnp.int32(table[0])
    for key, value in enumerate(table[1:], 1):
        out = jnp.where(index == key, jnp.int32(value), out)
    return out


def even_rows(tokens):
    return tokens // 4, tokens // 4


def lean_rows(tokens):
    return tokens * 5 // 16, tokens * 3 // 16


class Ring:
    def __init__(self, n_dev, own, everything, rows, ring_send, ring_recv, core_send, core_recv):
        self.own, self.all, self.rows = own, everything, rows
        self.ring_send, self.ring_recv, self.core_send, self.core_recv = ring_send, ring_recv, core_send, core_recv
        self.side = math.isqrt(n_dev // 2)
        self.tokens = own.shape[0]
        self.me = lax.axis_index(AXIS)
        self.core = lax.rem(self.me, 2)
        self.x, self.y = lax.rem(self.me // 2, self.side), self.me // (2 * self.side)

    def each_colour(self, body):
        for kind in range(2):
            each(0, 2, lambda way: body((kind, way)))

    def device(self, colour, along, across, core):
        side = self.side
        kind, way = colour
        sign = 1 - 2 * way
        dx, dy = (along, across) if kind == 0 else (across, along)
        x = lax.rem(self.x - sign * dx + 2 * side, side)
        y = lax.rem(self.y - sign * dy + 2 * side, side)
        return (y * side + x) * 2 + core

    def within(self, colour):
        kind, way = colour
        return kind * 2 * self.rows[0] + way * self.rows[kind]

    def place(self, colour, s, h, core):
        return pl.ds(pl.multiple_of(self.device(colour, s, h, core) * self.tokens + self.within(colour), 8), self.rows[colour[0]])

    def piece(self, colour, s, h):
        return self.all.at[self.place(colour, s, h, self.core)]

    def own_piece(self, colour):
        return self.own.at[pl.ds(pl.multiple_of(self.within(colour), 8), self.rows[colour[0]])]

    def sem(self, sems, colour, s, h):
        return sems.at[colour[0] * 2 + colour[1], s * self.side + h]

    def ring_copy(self, colour, s, h, along, src=None):
        to = (s + along, h + 1 - along)
        dst = self.piece(colour, s, h)
        peer = self.device(colour, -along, along - 1, self.core)
        return remote(dst if src is None else src, dst, self.sem(self.ring_send, colour, *to), self.sem(self.ring_recv, colour, *to), peer)

    def core_copy(self, colour, s, h, src=None):
        dst = self.piece(colour, s, h)
        return remote(dst if src is None else src, dst, self.sem(self.core_send, colour, s, h), self.sem(self.core_recv, colour, s, h), self.me + 1 - 2 * self.core)

    def arrival(self, colour, s, h):
        dst = self.piece(colour, s, h)
        return remote(dst, dst, self.sem(self.ring_send, colour, s, h), self.sem(self.ring_recv, colour, s, h), self.me)

    def core_arrival(self, colour, s, h):
        dst = self.all.at[self.place(colour, s, h, 1 - self.core)]
        return remote(dst, dst, self.sem(self.core_send, colour, s, h), self.sem(self.core_recv, colour, s, h), self.me)

    def begin(self):
        def one(colour):
            self.ring_copy(colour, 0, 0, 1, self.own_piece(colour)).start()
            self.ring_copy(colour, 0, 0, 0, self.own_piece(colour)).start()

        self.each_colour(one)
        self.each_colour(lambda colour: self.core_copy(colour, 0, 0, self.own_piece(colour)).start())

    def pass_on(self, s, h):
        def one(colour):
            self.arrival(colour, s, h).wait_recv()

            @pl.when((h == 0) & (s < self.side - 1))
            def _():
                self.ring_copy(colour, s, h, 1).start()

            @pl.when(h < self.side - 1)
            def _():
                self.ring_copy(colour, s, h, 0).start()

            self.core_copy(colour, s, h).start()

        self.each_colour(one)

    def got_core(self, s, h):
        self.each_colour(lambda colour: self.core_arrival(colour, s, h).wait_recv())

    def end(self):
        def sent(number):
            s, h = number // self.side, lax.rem(number, self.side)

            def one(colour):
                @pl.when((s > 0) | (h > 0))
                def _():
                    self.arrival(colour, s, h).wait_send()

                self.core_copy(colour, s, h).wait_send()

            self.each_colour(one)

        each(0, self.side * self.side, sent)


def front_part(
    n_dev, n_group, x_ref, dy_ref, pos_ref, freq_ref, gain_ref, bias_ref, wo_ref, wq_ref, wk_ref, wv_ref,
    h_all, dy_all, q_ref, k_ref, v_ref, da_ref, cos_ref, sin_ref, x_hat_ref, inv_ref, pos_in,
    h_send, h_recv, h_core_send, h_core_recv, dy_send, dy_recv, dy_core_send, dy_core_recv, w_sem, h_sem, wo_sem, pos_send, pos_recv, local, da_send, da_recv,
    h_own, w_ref, pick_ref, w_buf, h_buf, wo_buf, da_buf, pos_own,
):
    me = lax.axis_index(AXIS)
    tokens, width = x_ref.shape
    head_dim = v_ref.shape[1]
    heads_tile = w_buf.shape[2]
    d_block = w_buf.shape[1]
    span = wo_buf.shape[1]
    n_wo = wo_ref.shape[0] // span
    per_wo = span // head_dim
    h_ring = Ring(n_dev, h_own, h_all, even_rows(tokens), h_send, h_recv, h_core_send, h_core_recv)
    dy_ring = Ring(n_dev, dy_ref, dy_all, lean_rows(tokens), dy_send, dy_recv, dy_core_send, dy_core_recv)
    rows_n = h_ring.rows[0]
    order = [(0, 0)] + ring_order(h_ring.side)
    n_event = len(order)
    where = Exchange(lambda peer: pos_own, lambda origin: pos_in.at[origin], lambda peer: pos_send.at[peer], lambda origin: pos_recv.at[origin])

    da_copy = Exchange(lambda peer: da_buf.at[peer], lambda origin: da_ref.at[rows_of(origin, tokens)], lambda peer: da_send.at[peer], lambda origin: da_recv.at[origin])

    n_d = width // d_block
    kv_head = me // n_group

    def w_load(t, which):
        ref, head = ((wq_ref, me), (wk_ref, kv_head), (wv_ref, kv_head))[which]
        slot = lax.rem(t, 2)
        return pltpu.make_async_copy(ref.at[rows_of(t, d_block), rows_of(head // heads_tile, heads_tile)], w_buf.at[slot], w_sem.at[slot])

    own_dy = pltpu.make_async_copy(dy_ref, dy_all.at[rows_of(me, tokens)], local.at[0])
    own_h = pltpu.make_async_copy(h_own, h_all.at[rows_of(me, tokens)], local.at[1])
    own_dy.start()
    w_load(0, 0).start()

    def wo_turn(t):
        return alternate(me // per_wo, t, n_wo)

    def wo_load(t):
        slot = lax.rem(t, 2)
        return pltpu.make_async_copy(wo_ref.at[rows_of(wo_turn(t), span)], wo_buf.at[slot], wo_sem.at[slot])

    wo_load(jnp.int32(0)).start()
    wo_load(jnp.int32(1)).start()
    pos_own[...] = jnp.broadcast_to(pos_ref[...], pos_own.shape)
    gain, bias = 1.0 + gain_ref[...], bias_ref[...]

    def norm(t):
        rows = rows_of(t, 16)
        x = x_ref[rows, :].astype(F32)
        centered = x - jnp.sum(x, axis=1, keepdims=True) * (1.0 / width)
        inv = lax.rsqrt(jnp.sum(centered * centered, axis=1, keepdims=True) * (1.0 / width) + EPS)
        x_hat = centered * inv
        x_hat_ref[rows, :] = x_hat
        inv_ref[rows, :] = inv
        h_own[rows, :] = (x_hat * gain + bias).astype(BF16)

    each(0, tokens // 16, norm)
    full_barrier(n_dev)

    def send_pos(step):
        peer = alternate(me, step, n_dev)
        where.start(peer, me, peer)

    h_ring.begin()
    each(0, n_dev, send_pos)
    own_h.start()

    for which in range(3):
        head = me if which == 0 else kv_head

        def pick(t):
            @pl.when(t + 1 < n_d)
            def _():
                w_load(t + 1, which).start()

            w_load(t, which).wait()
            pick_ref[...] = jnp.swapaxes(w_buf[lax.rem(t, 2)], 0, 1)
            w_ref[rows_of(t, d_block), which * head_dim : (which + 1) * head_dim] = pick_ref[lax.rem(head, heads_tile)]

        each(0, n_d, pick)
        if which < 2:
            w_load(0, which + 1).start()
        if which == 1:
            h_ring.pass_on(*(jnp.int32(v) for v in order[1]))
    own_dy.wait()
    own_h.wait()

    def tables(origin):
        where.got(origin)
        angles = freq_ref[...] * pos_in[origin, 0:1, :].astype(F32)
        cos_ref[:, rows_of(origin, tokens)] = jnp.cos(angles)
        sin_ref[:, rows_of(origin, tokens)] = jnp.sin(angles)

    def event(e):
        return lookup([p[0] for p in order], e), lookup([p[1] for p in order], e)

    def places_of(ring, s, h):
        return [ring.place((kind, way), s, h, core) for kind in range(2) for way in range(2) for core in range(2)]

    def fetch(ring, buf, sem, e):
        slot = lax.rem(e, 2)
        s, h = event(e)
        ring.got_core(s, h)
        for n, place in enumerate(places_of(ring, s, h)):
            pltpu.make_async_copy(ring.all.at[place], buf.at[slot, pl.ds(n * rows_n, rows_n)], sem.at[slot]).start()

    def fetched(ring, buf, sem, e):
        slot = lax.rem(e, 2)
        pltpu.make_async_copy(ring.all.at[pl.ds(0, 8 * rows_n)], buf.at[slot], sem.at[slot]).wait()
        return buf[slot]

    def send_da(t):
        def one(u):
            peer = wo_turn(t) * per_wo + lax.rem(u + me, per_wo)
            da_copy.start(peer, me, peer)

        each(0, per_wo, one)

    def make_da(t):
        @pl.when((t > 0) & (t <= n_wo))
        def _():
            send_da(t - 1)

        @pl.when((t >= 0) & (t < n_wo))
        def _():
            wo_load(t).wait()
            da = dot_t(dy_ref[...], wo_buf[lax.rem(t, 2)]).astype(BF16)
            for u in range(per_wo):
                da_buf[wo_turn(t) * per_wo + u] = da[:, u * head_dim : (u + 1) * head_dim]

            @pl.when(t + 2 < n_wo)
            def _():
                wo_load(t + 2).start()

    def project_rows(e):
        s, h = event(e)
        out = dot(fetched(h_ring, h_buf, h_sem, e), w_ref[...])
        for n, place in enumerate(places_of(h_ring, s, h)):
            part = out[n * rows_n : (n + 1) * rows_n]
            q_ref[place, :] = part[:, :head_dim]
            k_ref[place, :] = part[:, head_dim : 2 * head_dim]
            v_ref[place, :] = part[:, 2 * head_dim :].astype(BF16)

    def step(e):
        @pl.when((e > 1) & (e < n_event))
        def _():
            h_ring.pass_on(*event(e))

        @pl.when(e == max(n_event - 5, 1))
        def _():
            dy_ring.begin()

        for number in range(1, early_events(n_event) + 1):
            @pl.when(e == n_event - 3 + 2 * number)
            def _():
                dy_ring.pass_on(*(jnp.int32(v) for v in order[number]))

        @pl.when(e <= n_event)
        def _():
            fetch(h_ring, h_buf, h_sem, e - 1)

        make_da(e - 1)

        @pl.when((e > 1) & (e < n_event + 2))
        def _():
            project_rows(e - 2)

        @pl.when(e == 3)
        def _():
            each(0, n_dev, tables)

    each(1, max(n_event, n_wo) + 2, step)
    h_ring.end()

    def drain(index):
        where.sent(index, index)
        da_copy.sent(index, index)
        da_copy.got(index)

    each(0, n_dev, drain)


def causal(block):
    key = lax.broadcasted_iota(jnp.int32, (block, block), 0)
    query = lax.broadcasted_iota(jnp.int32, (block, block), 1)
    return key <= query


def part_sum(values):
    return jnp.sum(values.reshape(values.shape[0] // 8, 8, values.shape[1]), axis=0)


def main_part(
    ring_sems, n_dev, n_group, q_heads, kv_heads, n_buf, scale,
    q_raw, k_raw, v_ref, da_ref, cos_ref, sin_ref, x_ref, dy_own_ref, x_hat_ref, inv_ref, gain_ref, h_ref, dy_ref, wq_ref, wk_ref, wv_ref, wo_ref,
    out_ref, gx_ref, gwo_ref, gwq_ref, gwk_ref, gwv_ref, gain_out, bias_out,
    q_rows, kv_rows, sum_ref, at_ref, dqt_ref, a_head, dq_head, dkvt_ref, a_ref, g_ref, dkv_ref, land_one, land_two, kv_ref, kvt_ref, wq_out, wkv_out, dh_ref, part_ref, own_sum, sum_in, sum_mine,
    a_send, a_recv, dq_send, dq_recv, one_send, one_recv, two_send, two_recv, kv_send, kv_recv, near_send, near_recv,
    load_sem, q_send, q_recv, wkv_send, wkv_recv, s_send, s_recv, t_send, t_recv,
):
    me = lax.axis_index(AXIS)
    seq, head_dim = v_ref.shape
    tokens, width = x_ref.shape
    block = tokens * n_group
    n_block = seq // block
    half = block // 2
    fold = scale * math.log2(math.e)
    core, side = lax.rem(me, 2), lax.rem(me // 2, 2)
    member, group = lax.rem(me, n_group), me // n_group
    partner, across = me + 1 - 2 * core, me + 2 - 4 * side
    shift = lax.rem(group, max(2, n_block * 3 // 4))
    depth = width // n_dev
    span = math.lcm(depth, 128)
    n_col = width // span
    per_col = span // depth
    per_core = n_dev // 2
    n_sum = sum_mine.shape[0]
    q_cols = q_heads * head_dim

    def piece(index):
        return rows_of(index, tokens)

    def column(head):
        return rows_of(head, head_dim)

    def cols(j):
        return rows_of(j, span)

    a_copy = Exchange(lambda peer: a_head.at[piece(peer)], lambda head: a_ref.at[:, column(head)], lambda peer: a_send.at[peer], lambda head: a_recv.at[head])
    dq_copy = Exchange(lambda peer: dq_head.at[piece(peer)], lambda head: g_ref.at[:, column(head)], lambda peer: dq_send.at[peer], lambda head: dq_recv.at[head])
    kv_copy = Exchange(lambda n: kv_ref.at[n // 2, piece(lax.rem(n, 2))], lambda slot: g_ref.at[:, column(q_heads + slot)], lambda n: kv_send.at[n], lambda slot: kv_recv.at[slot])
    q_copy = Exchange(lambda peer: wq_out.at[rows_of(peer, depth)], lambda head: q_rows.at[head], lambda peer: q_send.at[peer], lambda head: q_recv.at[head])
    wkv_copy = Exchange(lambda i: wkv_out.at[rows_of(i, depth)], lambda head: kv_rows.at[head], lambda i: wkv_send.at[i], lambda head: wkv_recv.at[head])
    s_copy = Exchange(lambda peer: own_sum.at[pl.ds(peer * n_sum, n_sum)], lambda origin: sum_in.at[origin], lambda peer: s_send.at[peer], lambda origin: s_recv.at[origin])
    t_copy = Exchange(lambda peer: sum_mine, lambda origin: sum_ref.at[pl.ds(origin * n_sum, n_sum)], lambda peer: t_send.at[peer], lambda origin: t_recv.at[origin])


    def one_copy(i):
        return remote(dkv_ref.at[rows_of(i * 2 + 1 - core, half)], land_one.at[i], one_send.at[i], one_recv.at[i], partner)

    kind = side * kv_heads + group

    def half_of(i, which):
        return rows_of(i * 2 + which, half)

    def two_copy(i):
        return remote(dkv_ref.at[half_of(i, core), column(1 - side)], land_two.at[i], two_send.at[i], two_recv.at[i], across)

    def near_copy(i, which):
        return remote(kvt_ref.at[i], dkvt_ref.at[:, half_of(i, which)], near_send.at[i], near_recv.at[i], partner)

    def first(i):
        one_copy(i).start()

    def second(i):
        one_copy(i).wait_recv()
        for which in (1 - side, side):
            dkv_ref[half_of(i, core), column(which)] += land_one[i, :, column(which)]
        two_copy(i).start()

    def close(i):
        two_copy(i).wait_recv()
        rows = half_of(i, core)
        total = (dkv_ref[rows, column(side)] + land_two[i]).T

        def keep(values):
            values = values.astype(BF16)
            kvt_ref[i] = values
            dkvt_ref[:, rows] = values
            kv_ref[i] = values.T

        @pl.when(side == 0)
        def _():
            keep(rotate(total, cos_ref[:, rows], -sin_ref[:, rows]))

        @pl.when(side == 1)
        def _():
            keep(total)

    def spread(i):
        near_copy(i, core).start()
        for u in range(2):
            kv_copy.start(i * 2 + u, kind, i * n_group + core * 2 + u)

    steps = (first, second, close, spread)

    def block_at(t):
        return lax.rem(shift - 1 - t + 2 * n_block, n_block)

    def stages(t):
        for late in range(len(steps), 0, -1):
            n = t - late - shift

            @pl.when(n >= 0)
            def _():
                steps[late - 1](n_block - 1 - n)

    def stage_rest(late):
        each(jnp.maximum(n_block - late - shift, 0), n_block, lambda n: steps[late - 1](n_block - 1 - n))

    def send_pieces(i):
        def send(u):
            peer = i * n_group + lax.rem(u + me, n_group)
            a_copy.start(peer, me, peer)
            dq_copy.start(peer, me, peer)

        each(0, n_group, send)

    dy_ring = Ring(n_dev, dy_own_ref, dy_ref, lean_rows(tokens), *ring_sems)
    order = [(0, 0)] + ring_order(dy_ring.side)
    n_early = early_events(len(order))
    n_served = min(len(order) - 1, n_early + (n_block * (n_block + 1) - 1) // SERVE + 1)

    def serve(number):
        @pl.when(number < len(order))
        def _():
            dy_ring.pass_on(lookup([p[0] for p in order], number), lookup([p[1] for p in order], number))

    def tick(count):
        @pl.when(lax.rem(count, SERVE) == 0)
        def _():
            serve(count // SERVE + 1 + n_early)

    def attention(q_ref, k_ref, qt_ref, kt_ref, vt_ref, e_ref, dp_ref, peak_ref, dat_ref, mix_ref, acc_ref):
        def prepare(i):
            rows = rows_of(i, block)
            for raw, turned, plain in ((q_raw, qt_ref, q_ref), (k_raw, kt_ref, k_ref)):
                t = rotate(raw[rows, :].T, cos_ref[:, rows], sin_ref[:, rows]).astype(BF16)
                turned[:, rows] = t
                plain[rows, :] = t.T
            vt_ref[:, rows] = v_ref[rows, :].T
            dkv_ref[rows, :] = jnp.zeros((block, 2 * head_dim), F32)

        each(0, n_block, prepare)

        def compute(i, done):
            own = rows_of(i, block)
            dat_ref[...] = da_ref[own, :].T
            mix_ref[...] = jnp.zeros_like(mix_ref)
            acc_ref[...] = jnp.zeros_like(acc_ref)

            def scores(j, carry, diagonal):
                peak, total, mixed = carry
                tick(done + j)
                rows = rows_of(j, block)
                s = dot(k_ref[rows, :], qt_ref[:, own])
                if diagonal:
                    s = jnp.where(causal(block), s, -1e30)
                top = jnp.maximum(peak, jnp.max(s, axis=0, keepdims=True))
                e = jnp.exp2((s - top) * fold)
                dp = dot(v_ref[rows, :], dat_ref[...])
                fade = jnp.exp2((peak - top) * fold)
                e_ref[rows, :] = e
                dp_ref[rows, :] = dp
                peak_ref[j] = top
                return top, total * fade + part_sum(e), mixed * fade + part_sum(e * dp)

            start = (jnp.full((1, block), -jnp.inf, F32), jnp.zeros((8, block), F32), jnp.zeros((8, block), F32))
            carry = lax.fori_loop(0, i, functools.partial(scores, diagonal=False), start)
            peak, total, mixed = scores(i, carry, True)
            inv = 1.0 / jnp.sum(total, axis=0, keepdims=True)
            row_dot = jnp.sum(mixed, axis=0, keepdims=True) * inv
            q_own, da_own = q_ref[own, :], da_ref[own, :]

            def grads(j):
                tick(done + i + 1 + j)
                rows = rows_of(j, block)
                p = e_ref[rows, :] * (jnp.exp2((peak_ref[j] - peak) * fold) * inv)
                pb = p.astype(BF16)
                ds = ((dp_ref[rows, :] - row_dot) * (p * scale)).astype(BF16)
                dkv_ref[rows, :head_dim] += dot(ds, q_own)
                dkv_ref[rows, head_dim:] += dot(pb, da_own)
                mix_ref[...] += dot(vt_ref[:, rows], pb)
                acc_ref[...] += dot(kt_ref[:, rows], ds)

            each(0, i + 1, grads)
            at = mix_ref[...].astype(BF16)
            at_ref[:, own] = at
            a_head[own, :] = at.T
            dqt = rotate(acc_ref[...], cos_ref[:, own], -sin_ref[:, own]).astype(BF16)
            dqt_ref[:, own] = dqt
            dq_head[own, :] = dqt.T

        def iteration(t, done):
            stages(t)

            @pl.when(t > 0)
            def _():
                send_pieces(block_at(t - 1))

            i = block_at(t)
            compute(i, done)
            return done + 2 * (i + 1)

        lax.fori_loop(0, n_block, iteration, jnp.int32(0))

    pl.run_scoped(
        attention,
        pltpu.VMEM((seq, head_dim), BF16), pltpu.VMEM((seq, head_dim), BF16),
        pltpu.VMEM((head_dim, seq), BF16), pltpu.VMEM((head_dim, seq), BF16), pltpu.VMEM((head_dim, seq), BF16),
        pltpu.VMEM((seq, block), F32), pltpu.VMEM((seq, block), F32), pltpu.VMEM((n_block, 1, block), F32),
        pltpu.VMEM((head_dim, block), BF16), pltpu.VMEM((head_dim, block), F32), pltpu.VMEM((head_dim, block), F32),
    )

    def drain_sums():
        def one(i):
            one_copy(i).wait_send()
            two_copy(i).wait_send()
            near_copy(i, core).wait_send()
            near_copy(i, 1 - core).wait_recv()
            for u in range(2):
                kv_copy.sent(i * 2 + u, i * n_group + core * 2 + u)

        each(0, n_block, one)
        each(0, 2 * kv_heads, kv_copy.got)

    stage_rest(1)
    send_pieces(block_at(n_block - 1))

    def products(buf, w_buf):
        counts = (n_col, n_col, n_col, n_col // 2, n_col, n_col)
        starts = [sum(counts[:n]) for n in range(len(counts))]

        def loads(phase, j, slot):
            if phase == 1:
                return [pltpu.make_async_copy(wq_ref.at[cols(j)], w_buf.at[slot], load_sem.at[slot, 0])]
            if phase == 4:
                return [pltpu.make_async_copy(ref.at[cols(j)], w_buf.at[slot, :, pl.ds(n * kv_heads, kv_heads)], load_sem.at[slot, n]) for n, ref in enumerate((wk_ref, wv_ref))]
            ref = (h_ref, None, wo_ref, h_ref, None, dy_ref)[phase]
            col = core * (n_col // 2) + j if phase == 3 else j
            return [pltpu.make_async_copy(ref.at[:, cols(col)], buf.at[slot], load_sem.at[slot, 0])]

        def load(step):
            slot = lax.rem(step, n_buf)
            for phase, (begin, count) in enumerate(zip(starts, counts)):
                @pl.when((step >= begin) & (step < begin + count))
                def _():
                    for copy in loads(phase, step - begin, slot):
                        copy.start()

        def run(phase, body):
            def step(j):
                number = starts[phase] + j
                slot = lax.rem(number, n_buf)
                for copy in loads(phase, j, slot):
                    copy.wait()
                body(j, slot)
                load(number + n_buf)

            each(0, counts[phase], step)

        each(0, n_buf, load)

        def serve_late(number):
            for r in range(len(order) - 1 - n_served):
                @pl.when(number == 1 + 4 * r)
                def _():
                    serve(jnp.int32(n_served + 1 + r))

        def weight_columns(j, slot):
            serve_late(j)

            @pl.when(j == n_col // 4)
            def _():
                stage_rest(2)

            wq_out[cols(j), :] = dot(dqt_ref[...], buf[slot]).T

        run(0, weight_columns)

        def send_rows(j):
            col = alternate(me // per_col, j, n_col)

            def send(u):
                peer = col * per_col + lax.rem(u + me, per_col)
                q_copy.start(peer, me, peer)

            each(0, per_col, send)

        def got_heads(head):
            a_copy.got(head)
            dq_copy.got(head)

        each(0, n_dev, got_heads)

        def flat(slot, n_head):
            rows = w_buf[slot, :, :n_head, :]
            return rows.reshape(rows.shape[0], n_head * head_dim)

        def back_query(j, slot):
            serve_late(n_col + j)
            for late, at in ((3, n_col * 3 // 4), (4, n_col - 1)):
                @pl.when(j == at)
                def _():
                    stage_rest(late)

            @pl.when(j < n_col // 2)
            def _():
                send_rows(j)

            dh_ref[:, cols(j)] = dot_t(g_ref[:, :q_cols], flat(slot, q_heads))

        run(1, back_query)

        def output(j, slot):
            @pl.when(j < n_col // 2)
            def _():
                send_rows(n_col // 2 + j)

            out_ref[:, cols(j)] = (x_ref[:, cols(j)].astype(F32) + dot(a_ref[...], buf[slot])).astype(BF16)

        run(2, output)
        drain_sums()

        def weight_kv(j, slot):
            wkv_out[cols(j), :] = dot(dkvt_ref[...], buf[slot]).T

        run(3, weight_kv)
        for s, h in order:
            dy_ring.got_core(jnp.int32(s), jnp.int32(h))

        def send_kv(step):
            index = alternate(lax.rem(me, per_core), step, per_core)
            wkv_copy.start(index, kind, core * per_core + index)

        def back_kv(j, slot):
            @pl.when(j == 0)
            def _():
                each(0, per_core, send_kv)

            dh_ref[:, cols(j)] += dot_t(g_ref[:, q_cols:], flat(slot, 2 * kv_heads))

        run(4, back_kv)

        part_ref[...] = jnp.zeros_like(part_ref)
        gain = 1.0 + gain_ref[...]

        def norm(t):
            rows = rows_of(t, 16)
            grad_h, x_hat = dh_ref[rows, :], x_hat_ref[rows, :]
            grad_hat = grad_h * gain
            one = jnp.sum(grad_hat, axis=1, keepdims=True) * (1.0 / width)
            two = jnp.sum(grad_hat * x_hat, axis=1, keepdims=True) * (1.0 / width)
            back = inv_ref[rows, :] * (grad_hat - one - x_hat * two)
            gx_ref[rows, :] = (dy_own_ref[rows, :].astype(F32) + back).astype(BF16)
            part_ref[0] += part_sum(grad_h * x_hat)
            part_ref[1] += part_sum(grad_h)

        each(0, tokens // 16, norm)
        own_sum[...] = jnp.zeros_like(own_sum)
        for which in range(2):
            total = jnp.sum(part_ref[which], axis=0, keepdims=True)
            for c in range(width // 128):
                own_sum[c, pl.ds(which, 1), :] = total[:, c * 128 : (c + 1) * 128]

        def to_all(copy):
            def send(step):
                peer = alternate(me, step, n_dev)
                copy.start(peer, me, peer)

            each(0, n_dev, send)

        def add(origin):
            sum_mine[...] += sum_in[origin]

        def weight_out(j, slot):
            @pl.when(j == 0)
            def _():
                to_all(s_copy)

            @pl.when(j == n_col // 2)
            def _():
                each(0, n_dev, s_copy.got)
                sum_mine[...] = jnp.zeros_like(sum_mine)
                each(0, n_dev, add)

            gwo_ref[:, cols(j)] = dot(at_ref[...], buf[slot])

            @pl.when(j == n_col // 2)
            def _():
                to_all(t_copy)

        run(5, weight_out)

    pl.run_scoped(
        products,
        pltpu.VMEM((n_buf, seq, span), BF16),
        pltpu.VMEM((n_buf, span) + wq_ref.shape[1:], BF16),
    )

    dy_ring.end()

    def drain(index):
        for copy in (a_copy, dq_copy, s_copy, t_copy, q_copy):
            copy.sent(index, index)
        t_copy.got(index)
        q_copy.got(index)

    def drain_kv(index):
        wkv_copy.sent(index, core * per_core + index)

    each(0, n_dev, drain)
    each(0, per_core, drain_kv)
    each(0, 2 * kv_heads, wkv_copy.got)

    def settle(t):
        rows = rows_of(t, 8)
        gwq_ref[rows] = jnp.swapaxes(q_rows[:, rows, :], 0, 1)
        gwk_ref[rows] = jnp.swapaxes(kv_rows[:kv_heads, rows, :], 0, 1)
        gwv_ref[rows] = jnp.swapaxes(kv_rows[kv_heads:, rows, :], 0, 1)

    each(0, depth // 8, settle)
    for c in range(width // 128):
        gain_out[:, c * 128 : (c + 1) * 128] = sum_ref[c, 0:1, :]
        bias_out[:, c * 128 : (c + 1) * 128] = sum_ref[c, 1:2, :]


def block_kernel(n_dev, q_heads, kv_heads, n_buf, scale, *refs):
    x_ref, dy_ref, pos_ref, freq_ref, gain_ref, bias_ref, wo_ref, wq_ref, wk_ref, wv_ref = refs[:10]
    outs, (h_all, dy_all) = refs[10:18], refs[18:20]
    heads, pos_in, refs = refs[20:28], refs[28], refs[29:]
    front_sems, main_refs = refs[:16], refs[16:]
    tokens, width = x_ref.shape
    head_dim = wq_ref.shape[2]
    heads_tile = min(8, kv_heads)
    d_block = math.lcm(width // n_dev, 128)
    n_group = q_heads // kv_heads
    weights = (wo_ref, wq_ref, wk_ref, wv_ref)
    pl.run_scoped(
        functools.partial(front_part, n_dev, n_group, x_ref, dy_ref, pos_ref, freq_ref, gain_ref, bias_ref, *weights, h_all, dy_all, *heads, pos_in, *front_sems),
        pltpu.VMEM((tokens, width), BF16),
        pltpu.VMEM((width, 3 * head_dim), BF16),
        pltpu.VMEM((heads_tile, d_block, head_dim), BF16),
        pltpu.VMEM((2, d_block, heads_tile, head_dim), BF16),
        pltpu.VMEM((2, 2 * tokens, width), BF16),
        pltpu.VMEM((2, min(BLOCK, q_heads * head_dim // 2), width), BF16),
        pltpu.VMEM((n_dev, tokens, head_dim), BF16),
        pltpu.VMEM(pos_in.shape[1:], jnp.int32),
    )
    q, k, v, da, cos, sin, x_hat, inv = heads
    main_part(
        front_sems[4:8], n_dev, n_group, q_heads, kv_heads, n_buf, scale,
        q, k, v, da, cos, sin, x_ref, dy_ref, x_hat, inv, gain_ref, h_all, dy_all, wq_ref, wk_ref, wv_ref, wo_ref, *outs, *main_refs,
    )


def whole_block(n_dev, x_own, dy_own, positions, freq, gain, bias, wo, wq, wk, wv):
    tokens, width = x_own.shape
    q_heads, head_dim = wq.shape[1:]
    kv_heads = wk.shape[1]
    seq = tokens * n_dev
    n_group = q_heads // kv_heads
    n_block = n_dev // n_group
    depth = width // n_dev
    n_buf = 3
    n_sum = -(-width // (128 * n_dev))
    sums = (n_sum * n_dev, 8, 128)
    pieces = math.isqrt(n_dev // 2) ** 2
    whole, anywhere = pl.BlockSpec(memory_space=pltpu.VMEM), pl.BlockSpec(memory_space=pl.ANY)
    dma = pltpu.SemaphoreType.DMA
    return pl.pallas_call(
        functools.partial(block_kernel, n_dev, q_heads, kv_heads, n_buf, head_dim**-0.5),
        out_shape=[
            jax.ShapeDtypeStruct((tokens, width), BF16),
            jax.ShapeDtypeStruct((tokens, width), BF16),
            jax.ShapeDtypeStruct((head_dim, width), F32),
            jax.ShapeDtypeStruct((depth, q_heads, head_dim), F32),
            jax.ShapeDtypeStruct((depth, kv_heads, head_dim), F32),
            jax.ShapeDtypeStruct((depth, kv_heads, head_dim), F32),
            jax.ShapeDtypeStruct((1, width), F32),
            jax.ShapeDtypeStruct((1, width), F32),
            jax.ShapeDtypeStruct((seq, width), BF16),
            jax.ShapeDtypeStruct((seq, width), BF16),
        ],
        in_specs=[whole] * 6 + [anywhere] * 4,
        out_specs=[whole] * 8 + [anywhere] * 2,
        scratch_shapes=[
            pltpu.VMEM((seq, head_dim), F32),
            pltpu.VMEM((seq, head_dim), F32),
            pltpu.VMEM((seq, head_dim), BF16),
            pltpu.VMEM((seq, head_dim), BF16),
            pltpu.VMEM((head_dim // 4, seq), F32),
            pltpu.VMEM((head_dim // 4, seq), F32),
            pltpu.VMEM((tokens, width), F32),
            pltpu.VMEM((tokens, 1), F32),
            pltpu.VMEM((n_dev, 8, tokens), jnp.int32),
            dma((4, pieces)), dma((4, pieces)), dma((4, pieces)), dma((4, pieces)),
            dma((4, pieces)), dma((4, pieces)), dma((4, pieces)), dma((4, pieces)),
            dma((2,)), dma((2,)), dma((2,)), dma((n_dev,)), dma((n_dev,)), dma((3,)), dma((n_dev,)), dma((n_dev,)),
            pltpu.VMEM((q_heads, depth, head_dim), F32),
            pltpu.VMEM((2 * kv_heads, depth, head_dim), F32),
            pltpu.VMEM(sums, F32),
            pltpu.VMEM((head_dim, seq), BF16),
            pltpu.VMEM((head_dim, seq), BF16),
            pltpu.VMEM((seq, head_dim), BF16),
            pltpu.VMEM((seq, head_dim), BF16),
            pltpu.VMEM((head_dim, seq), BF16),
            pltpu.VMEM((tokens, q_heads * head_dim), BF16),
            pltpu.VMEM((tokens, (q_heads + 2 * kv_heads) * head_dim), BF16),
            pltpu.VMEM((seq, 2 * head_dim), F32),
            pltpu.VMEM((n_block, tokens * n_group // 2, 2 * head_dim), F32),
            pltpu.VMEM((n_block, tokens * n_group // 2, head_dim), F32),
            pltpu.VMEM((n_block, tokens * n_group // 2, head_dim), BF16),
            pltpu.VMEM((n_block, head_dim, tokens * n_group // 2), BF16),
            pltpu.VMEM((width, head_dim), F32),
            pltpu.VMEM((width // 2, head_dim), F32),
            pltpu.VMEM((tokens, width), F32),
            pltpu.VMEM((2, 8, width), F32),
            pltpu.VMEM(sums, F32),
            pltpu.VMEM((n_dev, n_sum, 8, 128), F32),
            pltpu.VMEM((n_sum, 8, 128), F32),
            dma((n_dev,)), dma((n_dev,)), dma((n_dev,)), dma((n_dev,)),
            dma((n_block,)), dma((n_block,)), dma((n_block,)), dma((n_block,)), dma((2 * n_block,)), dma((2 * kv_heads,)), dma((n_block,)), dma((n_block,)),
            dma((n_buf, 3)), dma((n_dev,)), dma((n_dev,)), dma((n_dev // 2,)), dma((2 * kv_heads,)), dma((n_dev,)), dma((n_dev,)), dma((n_dev,)), dma((n_dev,)),
        ],
        compiler_params=pltpu.CompilerParams(collective_id=1, has_side_effects=True, vmem_limit_bytes=VMEM_LIMIT, flags=FLAGS),
        cost_estimate=pl.CostEstimate(flops=6 * seq * seq * head_dim + 16 * seq * width * head_dim, bytes_accessed=16 * seq * width, transcendentals=seq * seq // 2),
        name="block",
    )(x_own, dy_own, positions, freq, gain, bias, wo, wq, wk, wv)


def solution(mesh):
    n_dev = mesh.shape[AXIS]

    def device_step(x_act, d_out, positions, ln_gain, ln_bias, w_query, w_key, w_value, w_out):
        n_batch, piece, width = x_act.shape
        head_dim = w_query.shape[2]
        tokens = n_batch * piece

        x_own, dy_own = x_act.reshape(tokens, width), d_out.reshape(tokens, width)
        gain, bias = ln_gain.reshape(1, width), ln_bias.reshape(1, width)
        block_out, grad_x, grad_wo, grad_wq, grad_wk, grad_wv, grad_gain, grad_bias, _, _ = whole_block(
            n_dev, x_own, dy_own, positions.reshape(1, tokens), frequencies(head_dim, tokens), gain, bias, w_out, w_query, w_key, w_value
        )
        return (block_out.reshape(x_act.shape), grad_x.reshape(x_act.shape), grad_wq, grad_wk, grad_wv, grad_wo, grad_gain.reshape(width), grad_bias.reshape(width))

    return jax.shard_map(device_step, mesh=mesh, in_specs=(P("dp", AXIS, None), P("dp", AXIS, None), P("dp", AXIS), P(None), P(None), P(None, None, None), P(None, None, None), P(None, None, None), P(None, None)), out_specs=(P("dp", AXIS, None), P("dp", AXIS, None), P(("dp", AXIS), None, None), P(("dp", AXIS), None, None), P(("dp", AXIS), None, None), P(("dp", AXIS), None), P("dp"), P("dp")), check_vma=False)
```

```python
import functools
import math

import jax
import jax.numpy as jnp
import numpy as np
from jax import lax
from jax.experimental import pallas as pl
from jax.experimental.pallas import tpu as pltpu
from jax.sharding import PartitionSpec as P

EPS = 1e-5
ROPE_BASE = 10000.0
BLOCK = 512
AXIS = "cp"
BF16, F32 = jnp.bfloat16, jnp.float32
VMEM_LIMIT = 67043328
FLAGS = {}
SERVE = 11


def frequencies(head_dim, tokens):
    quarter = head_dim // 4
    freq = np.exp(np.arange(quarter, dtype=np.float32) * np.float32(-2.0 * math.log(ROPE_BASE) / (head_dim // 2)))
    return jnp.asarray(np.broadcast_to(freq[:, None], (quarter, tokens)))


def rotate(values, cos, sin):
    quarter = cos.shape[0]
    first, second = values[:quarter], values[quarter : 2 * quarter]
    return jnp.concatenate([first * cos - second * sin, second * cos + first * sin, values[2 * quarter :]], axis=0)


def rows_of(index, size):
    return pl.ds(pl.multiple_of(index * size, size), size)


def dot(lhs, rhs):
    return jnp.dot(lhs, rhs, preferred_element_type=F32)


def dot_t(lhs, rhs):
    return lax.dot_general(lhs, rhs, (((1,), (1,)), ((), ())), preferred_element_type=F32)


def full_barrier(n_dev):
    me = lax.axis_index(AXIS)
    barrier = pltpu.get_barrier_semaphore()

    def tell(step):
        pl.semaphore_signal(barrier, inc=1, device_id={AXIS: lax.rem(me + step, n_dev)}, device_id_type=pl.DeviceIdType.MESH)

    each(1, n_dev, tell)
    pl.semaphore_wait(barrier, n_dev - 1)


def remote(src, dst, send_sem, recv_sem, peer):
    return pltpu.make_async_remote_copy(src_ref=src, dst_ref=dst, send_sem=send_sem, recv_sem=recv_sem, device_id={AXIS: peer}, device_id_type=pl.DeviceIdType.MESH)


def each(lower, upper, body):
    def step(index, carry):
        body(index)
        return carry

    lax.fori_loop(lower, upper, step, 0)


def alternate(index, step, size):
    away = (step + 1) // 2
    return lax.rem(index + jnp.where(lax.rem(step, 2) == 1, away, size - away), size)


class Exchange:
    def __init__(self, src, dst, send, recv):
        self.src, self.dst, self.send, self.recv = src, dst, send, recv

    def start(self, index, slot, peer):
        me = lax.axis_index(AXIS)
        src, dst, recv = self.src(index), self.dst(slot), self.recv(slot)

        @pl.when(peer != me)
        def _():
            remote(src, dst, self.send(index), recv, peer).start()

        @pl.when(peer == me)
        def _():
            pltpu.make_async_copy(src, dst, recv).start()

    def sent(self, index, peer):
        me = lax.axis_index(AXIS)

        @pl.when(peer != me)
        def _():
            remote(self.src(index), self.src(index), self.send(index), self.send(index), me).wait_send()

    def got(self, slot):
        dst = self.dst(slot)
        remote(dst, dst, self.recv(slot), self.recv(slot), lax.axis_index(AXIS)).wait_recv()


def early_events(n_event):
    return 2 if n_event > 4 else 0


def ring_order(side):
    queue, free, order = [(0.0, True, 0, 0), (0.0, False, 0, 0)], 0.0, []
    waiting = []
    while queue or waiting:
        if queue and (not waiting or free <= waiting[0][0]):
            at, along, s, h = queue.pop(0)
            free = max(free, at) + 1.0
            waiting.append((free + 0.5, (s + along, h + 1 - along)))
        else:
            at, (s, h) = waiting.pop(0)
            order.append((s, h))
            if h == 0 and s < side - 1:
                queue.append((at, True, s, h))
            if h < side - 1:
                queue.append((at, False, s, h))
    return order


def lookup(table, index):
    out = jnp.int32(table[0])
    for key, value in enumerate(table[1:], 1):
        out = jnp.where(index == key, jnp.int32(value), out)
    return out


def even_rows(tokens):
    return tokens // 4, tokens // 4


def lean_rows(tokens):
    return tokens * 5 // 16, tokens * 3 // 16


class Ring:
    def __init__(self, n_dev, own, everything, rows, ring_send, ring_recv, core_send, core_recv):
        self.own, self.all, self.rows = own, everything, rows
        self.ring_send, self.ring_recv, self.core_send, self.core_recv = ring_send, ring_recv, core_send, core_recv
        self.side = math.isqrt(n_dev // 2)
        self.tokens = own.shape[0]
        self.me = lax.axis_index(AXIS)
        self.core = lax.rem(self.me, 2)
        self.x, self.y = lax.rem(self.me // 2, self.side), self.me // (2 * self.side)

    def each_colour(self, body):
        for kind in range(2):
            each(0, 2, lambda way: body((kind, way)))

    def device(self, colour, along, across, core):
        side = self.side
        kind, way = colour
        sign = 1 - 2 * way
        dx, dy = (along, across) if kind == 0 else (across, along)
        x = lax.rem(self.x - sign * dx + 2 * side, side)
        y = lax.rem(self.y - sign * dy + 2 * side, side)
        return (y * side + x) * 2 + core

    def within(self, colour):
        kind, way = colour
        return kind * 2 * self.rows[0] + way * self.rows[kind]

    def place(self, colour, s, h, core):
        return pl.ds(pl.multiple_of(self.device(colour, s, h, core) * self.tokens + self.within(colour), 8), self.rows[colour[0]])

    def piece(self, colour, s, h):
        return self.all.at[self.place(colour, s, h, self.core)]

    def own_piece(self, colour):
        return self.own.at[pl.ds(pl.multiple_of(self.within(colour), 8), self.rows[colour[0]])]

    def sem(self, sems, colour, s, h):
        return sems.at[colour[0] * 2 + colour[1], s * self.side + h]

    def ring_copy(self, colour, s, h, along, src=None):
        to = (s + along, h + 1 - along)
        dst = self.piece(colour, s, h)
        peer = self.device(colour, -along, along - 1, self.core)
        return remote(dst if src is None else src, dst, self.sem(self.ring_send, colour, *to), self.sem(self.ring_recv, colour, *to), peer)

    def core_copy(self, colour, s, h, src=None):
        dst = self.piece(colour, s, h)
        return remote(dst if src is None else src, dst, self.sem(self.core_send, colour, s, h), self.sem(self.core_recv, colour, s, h), self.me + 1 - 2 * self.core)

    def arrival(self, colour, s, h):
        dst = self.piece(colour, s, h)
        return remote(dst, dst, self.sem(self.ring_send, colour, s, h), self.sem(self.ring_recv, colour, s, h), self.me)

    def core_arrival(self, colour, s, h):
        dst = self.all.at[self.place(colour, s, h, 1 - self.core)]
        return remote(dst, dst, self.sem(self.core_send, colour, s, h), self.sem(self.core_recv, colour, s, h), self.me)

    def begin(self):
        def one(colour):
            self.ring_copy(colour, 0, 0, 1, self.own_piece(colour)).start()
            self.ring_copy(colour, 0, 0, 0, self.own_piece(colour)).start()

        self.each_colour(one)
        self.each_colour(lambda colour: self.core_copy(colour, 0, 0, self.own_piece(colour)).start())

    def pass_on(self, s, h):
        def one(colour):
            self.arrival(colour, s, h).wait_recv()

            @pl.when((h == 0) & (s < self.side - 1))
            def _():
                self.ring_copy(colour, s, h, 1).start()

            @pl.when(h < self.side - 1)
            def _():
                self.ring_copy(colour, s, h, 0).start()

            self.core_copy(colour, s, h).start()

        self.each_colour(one)

    def got_core(self, s, h):
        self.each_colour(lambda colour: self.core_arrival(colour, s, h).wait_recv())

    def end(self):
        def sent(number):
            s, h = number // self.side, lax.rem(number, self.side)

            def one(colour):
                @pl.when((s > 0) | (h > 0))
                def _():
                    self.arrival(colour, s, h).wait_send()

                self.core_copy(colour, s, h).wait_send()

            self.each_colour(one)

        each(0, self.side * self.side, sent)


def front_part(
    n_dev, n_group, x_ref, dy_ref, pos_ref, freq_ref, gain_ref, bias_ref, wo_ref, wq_ref, wk_ref, wv_ref,
    h_all, dy_all, q_ref, k_ref, v_ref, da_ref, cos_ref, sin_ref, x_hat_ref, inv_ref, pos_in,
    h_send, h_recv, h_core_send, h_core_recv, dy_send, dy_recv, dy_core_send, dy_core_recv, w_sem, h_sem, wo_sem, pos_send, pos_recv, local, da_send, da_recv,
    h_own, w_ref, pick_ref, w_buf, h_buf, wo_buf, da_buf, pos_own,
):
    me = lax.axis_index(AXIS)
    tokens, width = x_ref.shape
    head_dim = v_ref.shape[1]
    heads_tile = w_buf.shape[2]
    d_block = w_buf.shape[1]
    span = wo_buf.shape[1]
    n_wo = wo_ref.shape[0] // span
    per_wo = span // head_dim
    h_ring = Ring(n_dev, h_own, h_all, even_rows(tokens), h_send, h_recv, h_core_send, h_core_recv)
    dy_ring = Ring(n_dev, dy_ref, dy_all, lean_rows(tokens), dy_send, dy_recv, dy_core_send, dy_core_recv)
    rows_n = h_ring.rows[0]
    order = [(0, 0)] + ring_order(h_ring.side)
    n_event = len(order)
    where = Exchange(lambda peer: pos_own, lambda origin: pos_in.at[origin], lambda peer: pos_send.at[peer], lambda origin: pos_recv.at[origin])

    da_copy = Exchange(lambda peer: da_buf.at[peer], lambda origin: da_ref.at[rows_of(origin, tokens)], lambda peer: da_send.at[peer], lambda origin: da_recv.at[origin])

    n_d = width // d_block
    kv_head = me // n_group

    def w_load(t, which):
        ref, head = ((wq_ref, me), (wk_ref, kv_head), (wv_ref, kv_head))[which]
        slot = lax.rem(t, 2)
        return pltpu.make_async_copy(ref.at[rows_of(t, d_block), rows_of(head // heads_tile, heads_tile)], w_buf.at[slot], w_sem.at[slot])

    own_dy = pltpu.make_async_copy(dy_ref, dy_all.at[rows_of(me, tokens)], local.at[0])
    own_h = pltpu.make_async_copy(h_own, h_all.at[rows_of(me, tokens)], local.at[1])
    own_dy.start()
    w_load(0, 0).start()

    def wo_turn(t):
        return alternate(me // per_wo, t, n_wo)

    def wo_load(t):
        slot = lax.rem(t, 2)
        return pltpu.make_async_copy(wo_ref.at[rows_of(wo_turn(t), span)], wo_buf.at[slot], wo_sem.at[slot])

    wo_load(jnp.int32(0)).start()
    wo_load(jnp.int32(1)).start()
    pos_own[...] = jnp.broadcast_to(pos_ref[...], pos_own.shape)
    gain, bias = 1.0 + gain_ref[...], bias_ref[...]

    def norm(t):
        rows = rows_of(t, 16)
        x = x_ref[rows, :].astype(F32)
        centered = x - jnp.sum(x, axis=1, keepdims=True) * (1.0 / width)
        inv = lax.rsqrt(jnp.sum(centered * centered, axis=1, keepdims=True) * (1.0 / width) + EPS)
        x_hat = centered * inv
        x_hat_ref[rows, :] = x_hat
        inv_ref[rows, :] = inv
        h_own[rows, :] = (x_hat * gain + bias).astype(BF16)

    each(0, tokens // 16, norm)
    full_barrier(n_dev)

    def send_pos(step):
        peer = alternate(me, step, n_dev)
        where.start(peer, me, peer)

    h_ring.begin()
    each(0, n_dev, send_pos)
    own_h.start()

    for which in range(3):
        head = me if which == 0 else kv_head

        def pick(t):
            @pl.when(t + 1 < n_d)
            def _():
                w_load(t + 1, which).start()

            w_load(t, which).wait()
            pick_ref[...] = jnp.swapaxes(w_buf[lax.rem(t, 2)], 0, 1)
            w_ref[rows_of(t, d_block), which * head_dim : (which + 1) * head_dim] = pick_ref[lax.rem(head, heads_tile)]

        each(0, n_d, pick)
        if which < 2:
            w_load(0, which + 1).start()
        if which == 1:
            h_ring.pass_on(*(jnp.int32(v) for v in order[1]))
    own_dy.wait()
    own_h.wait()

    def tables(origin):
        where.got(origin)
        angles = freq_ref[...] * pos_in[origin, 0:1, :].astype(F32)
        cos_ref[:, rows_of(origin, tokens)] = jnp.cos(angles)
        sin_ref[:, rows_of(origin, tokens)] = jnp.sin(angles)

    def event(e):
        return lookup([p[0] for p in order], e), lookup([p[1] for p in order], e)

    def places_of(ring, s, h):
        return [ring.place((kind, way), s, h, core) for kind in range(2) for way in range(2) for core in range(2)]

    def fetch(ring, buf, sem, e):
        slot = lax.rem(e, 2)
        s, h = event(e)
        ring.got_core(s, h)
        for n, place in enumerate(places_of(ring, s, h)):
            pltpu.make_async_copy(ring.all.at[place], buf.at[slot, pl.ds(n * rows_n, rows_n)], sem.at[slot]).start()

    def fetched(ring, buf, sem, e):
        slot = lax.rem(e, 2)
        pltpu.make_async_copy(ring.all.at[pl.ds(0, 8 * rows_n)], buf.at[slot], sem.at[slot]).wait()
        return buf[slot]

    def send_da(t):
        def one(u):
            peer = wo_turn(t) * per_wo + lax.rem(u + me, per_wo)
            da_copy.start(peer, me, peer)

        each(0, per_wo, one)

    def make_da(t):
        @pl.when((t > 0) & (t <= n_wo))
        def _():
            send_da(t - 1)

        @pl.when((t >= 0) & (t < n_wo))
        def _():
            wo_load(t).wait()
            da = dot_t(dy_ref[...], wo_buf[lax.rem(t, 2)]).astype(BF16)
            for u in range(per_wo):
                da_buf[wo_turn(t) * per_wo + u] = da[:, u * head_dim : (u + 1) * head_dim]

            @pl.when(t + 2 < n_wo)
            def _():
                wo_load(t + 2).start()

    def project_rows(e):
        s, h = event(e)
        out = dot(fetched(h_ring, h_buf, h_sem, e), w_ref[...])
        for n, place in enumerate(places_of(h_ring, s, h)):
            part = out[n * rows_n : (n + 1) * rows_n]
            q_ref[place, :] = part[:, :head_dim]
            k_ref[place, :] = part[:, head_dim : 2 * head_dim]
            v_ref[place, :] = part[:, 2 * head_dim :].astype(BF16)

    def step(e):
        @pl.when((e > 1) & (e < n_event))
        def _():
            h_ring.pass_on(*event(e))

        @pl.when(e == max(n_event - 5, 1))
        def _():
            dy_ring.begin()

        for number in range(1, early_events(n_event) + 1):
            @pl.when(e == n_event - 3 + 2 * number)
            def _():
                dy_ring.pass_on(*(jnp.int32(v) for v in order[number]))

        @pl.when(e <= n_event)
        def _():
            fetch(h_ring, h_buf, h_sem, e - 1)

        make_da(e - 1)

        @pl.when((e > 1) & (e < n_event + 2))
        def _():
            project_rows(e - 2)

        @pl.when(e == 3)
        def _():
            each(0, n_dev, tables)

    each(1, max(n_event, n_wo) + 2, step)
    h_ring.end()

    def drain(index):
        where.sent(index, index)
        da_copy.sent(index, index)
        da_copy.got(index)

    each(0, n_dev, drain)


def causal(block):
    key = lax.broadcasted_iota(jnp.int32, (block, block), 0)
    query = lax.broadcasted_iota(jnp.int32, (block, block), 1)
    return key <= query


def part_sum(values):
    return jnp.sum(values.reshape(values.shape[0] // 8, 8, values.shape[1]), axis=0)


def main_part(
    ring_sems, n_dev, n_group, q_heads, kv_heads, n_buf, scale,
    q_raw, k_raw, v_ref, da_ref, cos_ref, sin_ref, x_ref, dy_own_ref, x_hat_ref, inv_ref, gain_ref, h_ref, dy_ref, wq_ref, wk_ref, wv_ref, wo_ref,
    out_ref, gx_ref, gwo_ref, gwq_ref, gwk_ref, gwv_ref, gain_out, bias_out,
    q_rows, kv_rows, sum_ref, at_ref, dqt_ref, a_head, dq_head, dkvt_ref, a_ref, g_ref, dkv_ref, land_one, land_two, kv_ref, kvt_ref, wq_out, wkv_out, dh_ref, part_ref, own_sum, sum_in, sum_mine,
    a_send, a_recv, dq_send, dq_recv, one_send, one_recv, two_send, two_recv, kv_send, kv_recv, near_send, near_recv,
    load_sem, q_send, q_recv, wkv_send, wkv_recv, s_send, s_recv, t_send, t_recv,
):
    me = lax.axis_index(AXIS)
    seq, head_dim = v_ref.shape
    tokens, width = x_ref.shape
    block = tokens * n_group
    n_block = seq // block
    half = block // 2
    fold = scale * math.log2(math.e)
    core, side = lax.rem(me, 2), lax.rem(me // 2, 2)
    member, group = lax.rem(me, n_group), me // n_group
    partner, across = me + 1 - 2 * core, me + 2 - 4 * side
    shift = lax.rem(group, max(2, n_block * 3 // 4))
    depth = width // n_dev
    span = math.lcm(depth, 128)
    n_col = width // span
    per_col = span // depth
    per_core = n_dev // 2
    n_sum = sum_mine.shape[0]
    q_cols = q_heads * head_dim

    def piece(index):
        return rows_of(index, tokens)

    def column(head):
        return rows_of(head, head_dim)

    def cols(j):
        return rows_of(j, span)

    a_copy = Exchange(lambda peer: a_head.at[piece(peer)], lambda head: a_ref.at[:, column(head)], lambda peer: a_send.at[peer], lambda head: a_recv.at[head])
    dq_copy = Exchange(lambda peer: dq_head.at[piece(peer)], lambda head: g_ref.at[:, column(head)], lambda peer: dq_send.at[peer], lambda head: dq_recv.at[head])
    kv_copy = Exchange(lambda n: kv_ref.at[n // 2, piece(lax.rem(n, 2))], lambda slot: g_ref.at[:, column(q_heads + slot)], lambda n: kv_send.at[n], lambda slot: kv_recv.at[slot])
    q_copy = Exchange(lambda peer: wq_out.at[rows_of(peer, depth)], lambda head: q_rows.at[head], lambda peer: q_send.at[peer], lambda head: q_recv.at[head])
    wkv_copy = Exchange(lambda i: wkv_out.at[rows_of(i, depth)], lambda head: kv_rows.at[head], lambda i: wkv_send.at[i], lambda head: wkv_recv.at[head])
    s_copy = Exchange(lambda peer: own_sum.at[pl.ds(peer * n_sum, n_sum)], lambda origin: sum_in.at[origin], lambda peer: s_send.at[peer], lambda origin: s_recv.at[origin])
    t_copy = Exchange(lambda peer: sum_mine, lambda origin: sum_ref.at[pl.ds(origin * n_sum, n_sum)], lambda peer: t_send.at[peer], lambda origin: t_recv.at[origin])


    def one_copy(i):
        return remote(dkv_ref.at[rows_of(i * 2 + 1 - core, half)], land_one.at[i], one_send.at[i], one_recv.at[i], partner)

    kind = side * kv_heads + group

    def half_of(i, which):
        return rows_of(i * 2 + which, half)

    def two_copy(i):
        return remote(dkv_ref.at[half_of(i, core), column(1 - side)], land_two.at[i], two_send.at[i], two_recv.at[i], across)

    def near_copy(i, which):
        return remote(kvt_ref.at[i], dkvt_ref.at[:, half_of(i, which)], near_send.at[i], near_recv.at[i], partner)

    def first(i):
        one_copy(i).start()

    def second(i):
        one_copy(i).wait_recv()
        for which in (1 - side, side):
            dkv_ref[half_of(i, core), column(which)] += land_one[i, :, column(which)]
        two_copy(i).start()

    def close(i):
        two_copy(i).wait_recv()
        rows = half_of(i, core)
        total = (dkv_ref[rows, column(side)] + land_two[i]).T

        def keep(values):
            values = values.astype(BF16)
            kvt_ref[i] = values
            dkvt_ref[:, rows] = values
            kv_ref[i] = values.T

        @pl.when(side == 0)
        def _():
            keep(rotate(total, cos_ref[:, rows], -sin_ref[:, rows]))

        @pl.when(side == 1)
        def _():
            keep(total)

    def spread(i):
        near_copy(i, core).start()
        for u in range(2):
            kv_copy.start(i * 2 + u, kind, i * n_group + core * 2 + u)

    steps = (first, second, close, spread)

    def block_at(t):
        return lax.rem(shift - 1 - t + 2 * n_block, n_block)

    def stages(t):
        for late in range(len(steps), 0, -1):
            n = t - late - shift

            @pl.when(n >= 0)
            def _():
                steps[late - 1](n_block - 1 - n)

    def stage_rest(late):
        each(jnp.maximum(n_block - late - shift, 0), n_block, lambda n: steps[late - 1](n_block - 1 - n))

    def send_pieces(i):
        def send(u):
            peer = i * n_group + lax.rem(u + me, n_group)
            a_copy.start(peer, me, peer)
            dq_copy.start(peer, me, peer)

        each(0, n_group, send)

    dy_ring = Ring(n_dev, dy_own_ref, dy_ref, lean_rows(tokens), *ring_sems)
    order = [(0, 0)] + ring_order(dy_ring.side)
    n_early = early_events(len(order))
    n_served = min(len(order) - 1, n_early + (n_block * (n_block + 1) - 1) // SERVE + 1)

    def serve(number):
        @pl.when(number < len(order))
        def _():
            dy_ring.pass_on(lookup([p[0] for p in order], number), lookup([p[1] for p in order], number))

    def tick(count):
        @pl.when(lax.rem(count, SERVE) == 0)
        def _():
            serve(count // SERVE + 1 + n_early)

    def attention(q_ref, k_ref, qt_ref, kt_ref, vt_ref, e_ref, dp_ref, peak_ref, dat_ref, mix_ref, acc_ref):
        def prepare(i):
            rows = rows_of(i, block)
            for raw, turned, plain in ((q_raw, qt_ref, q_ref), (k_raw, kt_ref, k_ref)):
                t = rotate(raw[rows, :].T, cos_ref[:, rows], sin_ref[:, rows]).astype(BF16)
                turned[:, rows] = t
                plain[rows, :] = t.T
            vt_ref[:, rows] = v_ref[rows, :].T
            dkv_ref[rows, :] = jnp.zeros((block, 2 * head_dim), F32)

        each(0, n_block, prepare)

        def compute(i, done):
            own = rows_of(i, block)
            dat_ref[...] = da_ref[own, :].T
            mix_ref[...] = jnp.zeros_like(mix_ref)
            acc_ref[...] = jnp.zeros_like(acc_ref)

            def scores(j, carry, diagonal):
                peak, total, mixed = carry
                tick(done + j)
                rows = rows_of(j, block)
                s = dot(k_ref[rows, :], qt_ref[:, own])
                if diagonal:
                    s = jnp.where(causal(block), s, -1e30)
                top = jnp.maximum(peak, jnp.max(s, axis=0, keepdims=True))
                e = jnp.exp2((s - top) * fold)
                dp = dot(v_ref[rows, :], dat_ref[...])
                fade = jnp.exp2((peak - top) * fold)
                e_ref[rows, :] = e
                dp_ref[rows, :] = dp
                peak_ref[j] = top
                return top, total * fade + part_sum(e), mixed * fade + part_sum(e * dp)

            start = (jnp.full((1, block), -jnp.inf, F32), jnp.zeros((8, block), F32), jnp.zeros((8, block), F32))
            carry = lax.fori_loop(0, i, functools.partial(scores, diagonal=False), start)
            peak, total, mixed = scores(i, carry, True)
            inv = 1.0 / jnp.sum(total, axis=0, keepdims=True)
            row_dot = jnp.sum(mixed, axis=0, keepdims=True) * inv
            q_own, da_own = q_ref[own, :], da_ref[own, :]

            def grads(j):
                tick(done + i + 1 + j)
                rows = rows_of(j, block)
                p = e_ref[rows, :] * (jnp.exp2((peak_ref[j] - peak) * fold) * inv)
                pb = p.astype(BF16)
                ds = ((dp_ref[rows, :] - row_dot) * (p * scale)).astype(BF16)
                dkv_ref[rows, :head_dim] += dot(ds, q_own)
                dkv_ref[rows, head_dim:] += dot(pb, da_own)
                mix_ref[...] += dot(vt_ref[:, rows], pb)
                acc_ref[...] += dot(kt_ref[:, rows], ds)

            each(0, i + 1, grads)
            at = mix_ref[...].astype(BF16)
            at_ref[:, own] = at
            a_head[own, :] = at.T
            dqt = rotate(acc_ref[...], cos_ref[:, own], -sin_ref[:, own]).astype(BF16)
            dqt_ref[:, own] = dqt
            dq_head[own, :] = dqt.T

        def iteration(t, done):
            stages(t)

            @pl.when(t > 0)
            def _():
                send_pieces(block_at(t - 1))

            i = block_at(t)
            compute(i, done)
            return done + 2 * (i + 1)

        lax.fori_loop(0, n_block, iteration, jnp.int32(0))

    pl.run_scoped(
        attention,
        pltpu.VMEM((seq, head_dim), BF16), pltpu.VMEM((seq, head_dim), BF16),
        pltpu.VMEM((head_dim, seq), BF16), pltpu.VMEM((head_dim, seq), BF16), pltpu.VMEM((head_dim, seq), BF16),
        pltpu.VMEM((seq, block), F32), pltpu.VMEM((seq, block), F32), pltpu.VMEM((n_block, 1, block), F32),
        pltpu.VMEM((head_dim, block), BF16), pltpu.VMEM((head_dim, block), F32), pltpu.VMEM((head_dim, block), F32),
    )

    def drain_sums():
        def one(i):
            one_copy(i).wait_send()
            two_copy(i).wait_send()
            near_copy(i, core).wait_send()
            near_copy(i, 1 - core).wait_recv()
            for u in range(2):
                kv_copy.sent(i * 2 + u, i * n_group + core * 2 + u)

        each(0, n_block, one)
        each(0, 2 * kv_heads, kv_copy.got)

    stage_rest(1)
    send_pieces(block_at(n_block - 1))

    def products(buf, w_buf):
        counts = (n_col, n_col, n_col, n_col // 2, n_col, n_col)
        starts = [sum(counts[:n]) for n in range(len(counts))]

        def loads(phase, j, slot):
            if phase == 1:
                return [pltpu.make_async_copy(wq_ref.at[cols(j)], w_buf.at[slot], load_sem.at[slot, 0])]
            if phase == 4:
                return [pltpu.make_async_copy(ref.at[cols(j)], w_buf.at[slot, :, pl.ds(n * kv_heads, kv_heads)], load_sem.at[slot, n]) for n, ref in enumerate((wk_ref, wv_ref))]
            ref = (h_ref, None, wo_ref, h_ref, None, dy_ref)[phase]
            col = core * (n_col // 2) + j if phase == 3 else j
            return [pltpu.make_async_copy(ref.at[:, cols(col)], buf.at[slot], load_sem.at[slot, 0])]

        def load(step):
            slot = lax.rem(step, n_buf)
            for phase, (begin, count) in enumerate(zip(starts, counts)):
                @pl.when((step >= begin) & (step < begin + count))
                def _():
                    for copy in loads(phase, step - begin, slot):
                        copy.start()

        def serve_late(number):
            for r in range(len(order) - 1 - n_served):
                @pl.when(number == 3 + 6 * r)
                def _():
                    serve(jnp.int32(n_served + 1 + r))

        last = len(counts) - 1

        def run(phase, body):
            def step(j):
                number = starts[phase] + j
                slot = lax.rem(number, n_buf)
                for copy in loads(phase, j, slot):
                    copy.wait()
                if phase < last:
                    serve_late(number)
                body(j, slot)

                @pl.when((number + n_buf < starts[last]) | (phase == last))
                def _():
                    load(number + n_buf)

            each(0, counts[phase], step)

        each(0, n_buf, load)

        def weight_columns(j, slot):
            @pl.when(j == n_col // 4)
            def _():
                stage_rest(2)

            wq_out[cols(j), :] = dot(dqt_ref[...], buf[slot]).T

        run(0, weight_columns)

        def send_rows(j):
            col = alternate(me // per_col, j, n_col)

            def send(u):
                peer = col * per_col + lax.rem(u + me, per_col)
                q_copy.start(peer, me, peer)

            each(0, per_col, send)

        def got_heads(head):
            a_copy.got(head)
            dq_copy.got(head)

        each(0, n_dev, got_heads)

        def flat(slot, n_head):
            rows = w_buf[slot, :, :n_head, :]
            return rows.reshape(rows.shape[0], n_head * head_dim)

        def back_query(j, slot):
            for late, at in ((3, n_col * 3 // 4), (4, n_col - 1)):
                @pl.when(j == at)
                def _():
                    stage_rest(late)

            @pl.when(j < n_col // 2)
            def _():
                send_rows(j)

            dh_ref[:, cols(j)] = dot_t(g_ref[:, :q_cols], flat(slot, q_heads))

        run(1, back_query)

        def output(j, slot):
            @pl.when(j < n_col // 2)
            def _():
                send_rows(n_col // 2 + j)

            out_ref[:, cols(j)] = (x_ref[:, cols(j)].astype(F32) + dot(a_ref[...], buf[slot])).astype(BF16)

        run(2, output)
        drain_sums()

        def weight_kv(j, slot):
            wkv_out[cols(j), :] = dot(dkvt_ref[...], buf[slot]).T

        run(3, weight_kv)

        def send_kv(step):
            index = alternate(lax.rem(me, per_core), step, per_core)
            wkv_copy.start(index, kind, core * per_core + index)

        def back_kv(j, slot):
            @pl.when(j == 0)
            def _():
                each(0, per_core, send_kv)

            dh_ref[:, cols(j)] += dot_t(g_ref[:, q_cols:], flat(slot, 2 * kv_heads))

        run(4, back_kv)

        part_ref[...] = jnp.zeros_like(part_ref)
        gain = 1.0 + gain_ref[...]

        def norm(t):
            rows = rows_of(t, 16)
            grad_h, x_hat = dh_ref[rows, :], x_hat_ref[rows, :]
            grad_hat = grad_h * gain
            one = jnp.sum(grad_hat, axis=1, keepdims=True) * (1.0 / width)
            two = jnp.sum(grad_hat * x_hat, axis=1, keepdims=True) * (1.0 / width)
            back = inv_ref[rows, :] * (grad_hat - one - x_hat * two)
            gx_ref[rows, :] = (dy_own_ref[rows, :].astype(F32) + back).astype(BF16)
            part_ref[0] += part_sum(grad_h * x_hat)
            part_ref[1] += part_sum(grad_h)

        each(0, tokens // 16, norm)
        own_sum[...] = jnp.zeros_like(own_sum)
        for which in range(2):
            total = jnp.sum(part_ref[which], axis=0, keepdims=True)
            for c in range(width // 128):
                own_sum[c, pl.ds(which, 1), :] = total[:, c * 128 : (c + 1) * 128]

        def to_all(copy):
            def send(step):
                peer = alternate(me, step, n_dev)
                copy.start(peer, me, peer)

            each(0, n_dev, send)

        def add(origin):
            sum_mine[...] += sum_in[origin]

        def weight_out(j, slot):
            @pl.when(j == 0)
            def _():
                to_all(s_copy)

            @pl.when(j == n_col // 2)
            def _():
                each(0, n_dev, s_copy.got)
                sum_mine[...] = jnp.zeros_like(sum_mine)
                each(0, n_dev, add)

            gwo_ref[:, cols(j)] = dot(at_ref[...], buf[slot])

            @pl.when(j == n_col // 2)
            def _():
                to_all(t_copy)

        for s, h in order:
            dy_ring.got_core(jnp.int32(s), jnp.int32(h))
        each(starts[last], starts[last] + n_buf, load)
        run(last, weight_out)

    pl.run_scoped(
        products,
        pltpu.VMEM((n_buf, seq, span), BF16),
        pltpu.VMEM((n_buf, span) + wq_ref.shape[1:], BF16),
    )

    dy_ring.end()

    def drain(index):
        for copy in (a_copy, dq_copy, s_copy, t_copy, q_copy):
            copy.sent(index, index)
        t_copy.got(index)
        q_copy.got(index)

    def drain_kv(index):
        wkv_copy.sent(index, core * per_core + index)

    each(0, n_dev, drain)
    each(0, per_core, drain_kv)
    each(0, 2 * kv_heads, wkv_copy.got)

    def settle(t):
        rows = rows_of(t, 8)
        gwq_ref[rows] = jnp.swapaxes(q_rows[:, rows, :], 0, 1)
        gwk_ref[rows] = jnp.swapaxes(kv_rows[:kv_heads, rows, :], 0, 1)
        gwv_ref[rows] = jnp.swapaxes(kv_rows[kv_heads:, rows, :], 0, 1)

    each(0, depth // 8, settle)
    for c in range(width // 128):
        gain_out[:, c * 128 : (c + 1) * 128] = sum_ref[c, 0:1, :]
        bias_out[:, c * 128 : (c + 1) * 128] = sum_ref[c, 1:2, :]


def block_kernel(n_dev, q_heads, kv_heads, n_buf, scale, *refs):
    x_ref, dy_ref, pos_ref, freq_ref, gain_ref, bias_ref, wo_ref, wq_ref, wk_ref, wv_ref = refs[:10]
    outs, (h_all, dy_all) = refs[10:18], refs[18:20]
    heads, pos_in, refs = refs[20:28], refs[28], refs[29:]
    front_sems, main_refs = refs[:16], refs[16:]
    tokens, width = x_ref.shape
    head_dim = wq_ref.shape[2]
    heads_tile = min(8, kv_heads)
    d_block = math.lcm(width // n_dev, 128)
    n_group = q_heads // kv_heads
    weights = (wo_ref, wq_ref, wk_ref, wv_ref)
    pl.run_scoped(
        functools.partial(front_part, n_dev, n_group, x_ref, dy_ref, pos_ref, freq_ref, gain_ref, bias_ref, *weights, h_all, dy_all, *heads, pos_in, *front_sems),
        pltpu.VMEM((tokens, width), BF16),
        pltpu.VMEM((width, 3 * head_dim), BF16),
        pltpu.VMEM((heads_tile, d_block, head_dim), BF16),
        pltpu.VMEM((2, d_block, heads_tile, head_dim), BF16),
        pltpu.VMEM((2, 2 * tokens, width), BF16),
        pltpu.VMEM((2, min(BLOCK, q_heads * head_dim // 2), width), BF16),
        pltpu.VMEM((n_dev, tokens, head_dim), BF16),
        pltpu.VMEM(pos_in.shape[1:], jnp.int32),
    )
    q, k, v, da, cos, sin, x_hat, inv = heads
    main_part(
        front_sems[4:8], n_dev, n_group, q_heads, kv_heads, n_buf, scale,
        q, k, v, da, cos, sin, x_ref, dy_ref, x_hat, inv, gain_ref, h_all, dy_all, wq_ref, wk_ref, wv_ref, wo_ref, *outs, *main_refs,
    )


def whole_block(n_dev, x_own, dy_own, positions, freq, gain, bias, wo, wq, wk, wv):
    tokens, width = x_own.shape
    q_heads, head_dim = wq.shape[1:]
    kv_heads = wk.shape[1]
    seq = tokens * n_dev
    n_group = q_heads // kv_heads
    n_block = n_dev // n_group
    depth = width // n_dev
    n_buf = 3
    n_sum = -(-width // (128 * n_dev))
    sums = (n_sum * n_dev, 8, 128)
    pieces = math.isqrt(n_dev // 2) ** 2
    whole, anywhere = pl.BlockSpec(memory_space=pltpu.VMEM), pl.BlockSpec(memory_space=pl.ANY)
    dma = pltpu.SemaphoreType.DMA
    return pl.pallas_call(
        functools.partial(block_kernel, n_dev, q_heads, kv_heads, n_buf, head_dim**-0.5),
        out_shape=[
            jax.ShapeDtypeStruct((tokens, width), BF16),
            jax.ShapeDtypeStruct((tokens, width), BF16),
            jax.ShapeDtypeStruct((head_dim, width), F32),
            jax.ShapeDtypeStruct((depth, q_heads, head_dim), F32),
            jax.ShapeDtypeStruct((depth, kv_heads, head_dim), F32),
            jax.ShapeDtypeStruct((depth, kv_heads, head_dim), F32),
            jax.ShapeDtypeStruct((1, width), F32),
            jax.ShapeDtypeStruct((1, width), F32),
            jax.ShapeDtypeStruct((seq, width), BF16),
            jax.ShapeDtypeStruct((seq, width), BF16),
        ],
        in_specs=[whole] * 6 + [anywhere] * 4,
        out_specs=[whole] * 8 + [anywhere] * 2,
        scratch_shapes=[
            pltpu.VMEM((seq, head_dim), F32),
            pltpu.VMEM((seq, head_dim), F32),
            pltpu.VMEM((seq, head_dim), BF16),
            pltpu.VMEM((seq, head_dim), BF16),
            pltpu.VMEM((head_dim // 4, seq), F32),
            pltpu.VMEM((head_dim // 4, seq), F32),
            pltpu.VMEM((tokens, width), F32),
            pltpu.VMEM((tokens, 1), F32),
            pltpu.VMEM((n_dev, 8, tokens), jnp.int32),
            dma((4, pieces)), dma((4, pieces)), dma((4, pieces)), dma((4, pieces)),
            dma((4, pieces)), dma((4, pieces)), dma((4, pieces)), dma((4, pieces)),
            dma((2,)), dma((2,)), dma((2,)), dma((n_dev,)), dma((n_dev,)), dma((3,)), dma((n_dev,)), dma((n_dev,)),
            pltpu.VMEM((q_heads, depth, head_dim), F32),
            pltpu.VMEM((2 * kv_heads, depth, head_dim), F32),
            pltpu.VMEM(sums, F32),
            pltpu.VMEM((head_dim, seq), BF16),
            pltpu.VMEM((head_dim, seq), BF16),
            pltpu.VMEM((seq, head_dim), BF16),
            pltpu.VMEM((seq, head_dim), BF16),
            pltpu.VMEM((head_dim, seq), BF16),
            pltpu.VMEM((tokens, q_heads * head_dim), BF16),
            pltpu.VMEM((tokens, (q_heads + 2 * kv_heads) * head_dim), BF16),
            pltpu.VMEM((seq, 2 * head_dim), F32),
            pltpu.VMEM((n_block, tokens * n_group // 2, 2 * head_dim), F32),
            pltpu.VMEM((n_block, tokens * n_group // 2, head_dim), F32),
            pltpu.VMEM((n_block, tokens * n_group // 2, head_dim), BF16),
            pltpu.VMEM((n_block, head_dim, tokens * n_group // 2), BF16),
            pltpu.VMEM((width, head_dim), F32),
            pltpu.VMEM((width // 2, head_dim), F32),
            pltpu.VMEM((tokens, width), F32),
            pltpu.VMEM((2, 8, width), F32),
            pltpu.VMEM(sums, F32),
            pltpu.VMEM((n_dev, n_sum, 8, 128), F32),
            pltpu.VMEM((n_sum, 8, 128), F32),
            dma((n_dev,)), dma((n_dev,)), dma((n_dev,)), dma((n_dev,)),
            dma((n_block,)), dma((n_block,)), dma((n_block,)), dma((n_block,)), dma((2 * n_block,)), dma((2 * kv_heads,)), dma((n_block,)), dma((n_block,)),
            dma((n_buf, 3)), dma((n_dev,)), dma((n_dev,)), dma((n_dev // 2,)), dma((2 * kv_heads,)), dma((n_dev,)), dma((n_dev,)), dma((n_dev,)), dma((n_dev,)),
        ],
        compiler_params=pltpu.CompilerParams(collective_id=1, has_side_effects=True, vmem_limit_bytes=VMEM_LIMIT, flags=FLAGS),
        cost_estimate=pl.CostEstimate(flops=6 * seq * seq * head_dim + 16 * seq * width * head_dim, bytes_accessed=16 * seq * width, transcendentals=seq * seq // 2),
        name="block",
    )(x_own, dy_own, positions, freq, gain, bias, wo, wq, wk, wv)


def solution(mesh):
    n_dev = mesh.shape[AXIS]

    def device_step(x_act, d_out, positions, ln_gain, ln_bias, w_query, w_key, w_value, w_out):
        n_batch, piece, width = x_act.shape
        head_dim = w_query.shape[2]
        tokens = n_batch * piece

        x_own, dy_own = x_act.reshape(tokens, width), d_out.reshape(tokens, width)
        gain, bias = ln_gain.reshape(1, width), ln_bias.reshape(1, width)
        block_out, grad_x, grad_wo, grad_wq, grad_wk, grad_wv, grad_gain, grad_bias, _, _ = whole_block(
            n_dev, x_own, dy_own, positions.reshape(1, tokens), frequencies(head_dim, tokens), gain, bias, w_out, w_query, w_key, w_value
        )
        return (block_out.reshape(x_act.shape), grad_x.reshape(x_act.shape), grad_wq, grad_wk, grad_wv, grad_wo, grad_gain.reshape(width), grad_bias.reshape(width))

    return jax.shard_map(device_step, mesh=mesh, in_specs=(P("dp", AXIS, None), P("dp", AXIS, None), P("dp", AXIS), P(None), P(None), P(None, None, None), P(None, None, None), P(None, None, None), P(None, None)), out_specs=(P("dp", AXIS, None), P("dp", AXIS, None), P(("dp", AXIS), None, None), P(("dp", AXIS), None, None), P(("dp", AXIS), None, None), P(("dp", AXIS), None), P("dp"), P("dp")), check_vma=False)
```

```python
import functools
import math

import jax
import jax.numpy as jnp
import numpy as np
from jax import lax
from jax.experimental import pallas as pl
from jax.experimental.pallas import tpu as pltpu
from jax.sharding import PartitionSpec as P

EPS = 1e-5
ROPE_BASE = 10000.0
BLOCK = 512
AXIS = "cp"
BF16, F32 = jnp.bfloat16, jnp.float32
VMEM_LIMIT = 67043328
FLAGS = {}
SERVE = 11


def frequencies(head_dim, tokens):
    quarter = head_dim // 4
    freq = np.exp(np.arange(quarter, dtype=np.float32) * np.float32(-2.0 * math.log(ROPE_BASE) / (head_dim // 2)))
    return jnp.asarray(np.broadcast_to(freq[:, None], (quarter, tokens)))


def rotate(values, cos, sin):
    quarter = cos.shape[0]
    first, second = values[:quarter], values[quarter : 2 * quarter]
    return jnp.concatenate([first * cos - second * sin, second * cos + first * sin, values[2 * quarter :]], axis=0)


def rows_of(index, size):
    return pl.ds(pl.multiple_of(index * size, size), size)


def dot(lhs, rhs):
    return jnp.dot(lhs, rhs, preferred_element_type=F32)


def dot_t(lhs, rhs):
    return lax.dot_general(lhs, rhs, (((1,), (1,)), ((), ())), preferred_element_type=F32)


def full_barrier(n_dev):
    me = lax.axis_index(AXIS)
    barrier = pltpu.get_barrier_semaphore()

    def tell(step):
        pl.semaphore_signal(barrier, inc=1, device_id={AXIS: lax.rem(me + step, n_dev)}, device_id_type=pl.DeviceIdType.MESH)

    each(1, n_dev, tell)
    pl.semaphore_wait(barrier, n_dev - 1)


def remote(src, dst, send_sem, recv_sem, peer):
    return pltpu.make_async_remote_copy(src_ref=src, dst_ref=dst, send_sem=send_sem, recv_sem=recv_sem, device_id={AXIS: peer}, device_id_type=pl.DeviceIdType.MESH)


def each(lower, upper, body):
    def step(index, carry):
        body(index)
        return carry

    lax.fori_loop(lower, upper, step, 0)


def alternate(index, step, size):
    away = (step + 1) // 2
    return lax.rem(index + jnp.where(lax.rem(step, 2) == 1, away, size - away), size)


class Exchange:
    def __init__(self, src, dst, send, recv):
        self.src, self.dst, self.send, self.recv = src, dst, send, recv

    def start(self, index, slot, peer):
        me = lax.axis_index(AXIS)
        src, dst, recv = self.src(index), self.dst(slot), self.recv(slot)

        @pl.when(peer != me)
        def _():
            remote(src, dst, self.send(index), recv, peer).start()

        @pl.when(peer == me)
        def _():
            pltpu.make_async_copy(src, dst, recv).start()

    def sent(self, index, peer):
        me = lax.axis_index(AXIS)

        @pl.when(peer != me)
        def _():
            remote(self.src(index), self.src(index), self.send(index), self.send(index), me).wait_send()

    def got(self, slot):
        dst = self.dst(slot)
        remote(dst, dst, self.recv(slot), self.recv(slot), lax.axis_index(AXIS)).wait_recv()


def early_events(n_event):
    return 5 if n_event > 4 else 0


def ring_order(side):
    queue, free, order = [(0.0, True, 0, 0), (0.0, False, 0, 0)], 0.0, []
    waiting = []
    while queue or waiting:
        if queue and (not waiting or free <= waiting[0][0]):
            at, along, s, h = queue.pop(0)
            free = max(free, at) + 1.0
            waiting.append((free + 0.5, (s + along, h + 1 - along)))
        else:
            at, (s, h) = waiting.pop(0)
            order.append((s, h))
            if h == 0 and s < side - 1:
                queue.append((at, True, s, h))
            if h < side - 1:
                queue.append((at, False, s, h))
    return order


def lookup(table, index):
    out = jnp.int32(table[0])
    for key, value in enumerate(table[1:], 1):
        out = jnp.where(index == key, jnp.int32(value), out)
    return out


def even_rows(tokens):
    return tokens // 4, tokens // 4


def lean_rows(tokens):
    return tokens * 5 // 16, tokens * 3 // 16


class Ring:
    def __init__(self, n_dev, own, everything, rows, ring_send, ring_recv, core_send, core_recv):
        self.own, self.all, self.rows = own, everything, rows
        self.ring_send, self.ring_recv, self.core_send, self.core_recv = ring_send, ring_recv, core_send, core_recv
        self.side = math.isqrt(n_dev // 2)
        self.tokens = own.shape[0]
        self.me = lax.axis_index(AXIS)
        self.core = lax.rem(self.me, 2)
        self.x, self.y = lax.rem(self.me // 2, self.side), self.me // (2 * self.side)

    def each_colour(self, body):
        for kind in range(2):
            each(0, 2, lambda way: body((kind, way)))

    def device(self, colour, along, across, core):
        side = self.side
        kind, way = colour
        sign = 1 - 2 * way
        dx, dy = (along, across) if kind == 0 else (across, along)
        x = lax.rem(self.x - sign * dx + 2 * side, side)
        y = lax.rem(self.y - sign * dy + 2 * side, side)
        return (y * side + x) * 2 + core

    def within(self, colour):
        kind, way = colour
        return kind * 2 * self.rows[0] + way * self.rows[kind]

    def place(self, colour, s, h, core):
        return pl.ds(pl.multiple_of(self.device(colour, s, h, core) * self.tokens + self.within(colour), 8), self.rows[colour[0]])

    def piece(self, colour, s, h):
        return self.all.at[self.place(colour, s, h, self.core)]

    def own_piece(self, colour):
        return self.own.at[pl.ds(pl.multiple_of(self.within(colour), 8), self.rows[colour[0]])]

    def sem(self, sems, colour, s, h):
        return sems.at[colour[0] * 2 + colour[1], s * self.side + h]

    def ring_copy(self, colour, s, h, along, src=None):
        to = (s + along, h + 1 - along)
        dst = self.piece(colour, s, h)
        peer = self.device(colour, -along, along - 1, self.core)
        return remote(dst if src is None else src, dst, self.sem(self.ring_send, colour, *to), self.sem(self.ring_recv, colour, *to), peer)

    def core_copy(self, colour, s, h, src=None):
        dst = self.piece(colour, s, h)
        return remote(dst if src is None else src, dst, self.sem(self.core_send, colour, s, h), self.sem(self.core_recv, colour, s, h), self.me + 1 - 2 * self.core)

    def arrival(self, colour, s, h):
        dst = self.piece(colour, s, h)
        return remote(dst, dst, self.sem(self.ring_send, colour, s, h), self.sem(self.ring_recv, colour, s, h), self.me)

    def core_arrival(self, colour, s, h):
        dst = self.all.at[self.place(colour, s, h, 1 - self.core)]
        return remote(dst, dst, self.sem(self.core_send, colour, s, h), self.sem(self.core_recv, colour, s, h), self.me)

    def begin(self):
        def one(colour):
            self.ring_copy(colour, 0, 0, 1, self.own_piece(colour)).start()
            self.ring_copy(colour, 0, 0, 0, self.own_piece(colour)).start()

        self.each_colour(one)
        self.each_colour(lambda colour: self.core_copy(colour, 0, 0, self.own_piece(colour)).start())

    def pass_on(self, s, h):
        def one(colour):
            self.arrival(colour, s, h).wait_recv()

            @pl.when((h == 0) & (s < self.side - 1))
            def _():
                self.ring_copy(colour, s, h, 1).start()

            @pl.when(h < self.side - 1)
            def _():
                self.ring_copy(colour, s, h, 0).start()

            self.core_copy(colour, s, h).start()

        self.each_colour(one)

    def got_core(self, s, h):
        self.each_colour(lambda colour: self.core_arrival(colour, s, h).wait_recv())

    def end(self):
        def sent(number):
            s, h = number // self.side, lax.rem(number, self.side)

            def one(colour):
                @pl.when((s > 0) | (h > 0))
                def _():
                    self.arrival(colour, s, h).wait_send()

                self.core_copy(colour, s, h).wait_send()

            self.each_colour(one)

        each(0, self.side * self.side, sent)


def front_part(
    n_dev, n_group, x_ref, dy_ref, pos_ref, freq_ref, gain_ref, bias_ref, wo_ref, wq_ref, wk_ref, wv_ref,
    h_all, dy_all, q_ref, k_ref, v_ref, da_ref, cos_ref, sin_ref, x_hat_ref, inv_ref, pos_in,
    h_send, h_recv, h_core_send, h_core_recv, dy_send, dy_recv, dy_core_send, dy_core_recv, w_sem, h_sem, wo_sem, pos_send, pos_recv, local, da_send, da_recv,
    h_own, w_ref, pick_ref, w_buf, h_buf, wo_buf, da_buf, pos_own,
):
    me = lax.axis_index(AXIS)
    tokens, width = x_ref.shape
    head_dim = v_ref.shape[1]
    heads_tile = w_buf.shape[2]
    d_block = w_buf.shape[1]
    span = wo_buf.shape[1]
    n_wo = wo_ref.shape[0] // span
    per_wo = span // head_dim
    h_ring = Ring(n_dev, h_own, h_all, even_rows(tokens), h_send, h_recv, h_core_send, h_core_recv)
    dy_ring = Ring(n_dev, dy_ref, dy_all, lean_rows(tokens), dy_send, dy_recv, dy_core_send, dy_core_recv)
    rows_n = h_ring.rows[0]
    order = [(0, 0)] + ring_order(h_ring.side)
    n_event = len(order)
    where = Exchange(lambda peer: pos_own, lambda origin: pos_in.at[origin], lambda peer: pos_send.at[peer], lambda origin: pos_recv.at[origin])

    da_copy = Exchange(lambda peer: da_buf.at[peer], lambda origin: da_ref.at[rows_of(origin, tokens)], lambda peer: da_send.at[peer], lambda origin: da_recv.at[origin])

    n_d = width // d_block
    kv_head = me // n_group

    def w_load(t, which):
        ref, head = ((wq_ref, me), (wk_ref, kv_head), (wv_ref, kv_head))[which]
        slot = lax.rem(t, 2)
        return pltpu.make_async_copy(ref.at[rows_of(t, d_block), rows_of(head // heads_tile, heads_tile)], w_buf.at[slot], w_sem.at[slot])

    own_dy = pltpu.make_async_copy(dy_ref, dy_all.at[rows_of(me, tokens)], local.at[0])
    own_h = pltpu.make_async_copy(h_own, h_all.at[rows_of(me, tokens)], local.at[1])
    own_dy.start()
    w_load(0, 0).start()

    def wo_turn(t):
        return alternate(me // per_wo, t, n_wo)

    def wo_load(t):
        slot = lax.rem(t, 2)
        return pltpu.make_async_copy(wo_ref.at[rows_of(wo_turn(t), span)], wo_buf.at[slot], wo_sem.at[slot])

    wo_load(jnp.int32(0)).start()
    wo_load(jnp.int32(1)).start()
    pos_own[...] = jnp.broadcast_to(pos_ref[...], pos_own.shape)
    gain, bias = 1.0 + gain_ref[...], bias_ref[...]

    def norm(t):
        rows = rows_of(t, 16)
        x = x_ref[rows, :].astype(F32)
        centered = x - jnp.sum(x, axis=1, keepdims=True) * (1.0 / width)
        inv = lax.rsqrt(jnp.sum(centered * centered, axis=1, keepdims=True) * (1.0 / width) + EPS)
        x_hat = centered * inv
        x_hat_ref[rows, :] = x_hat
        inv_ref[rows, :] = inv
        h_own[rows, :] = (x_hat * gain + bias).astype(BF16)

    each(0, tokens // 16, norm)
    full_barrier(n_dev)

    def send_pos(step):
        peer = alternate(me, step, n_dev)
        where.start(peer, me, peer)

    h_ring.begin()
    each(0, n_dev, send_pos)
    own_h.start()

    for which in range(3):
        head = me if which == 0 else kv_head

        def pick(t):
            @pl.when(t + 1 < n_d)
            def _():
                w_load(t + 1, which).start()

            w_load(t, which).wait()
            pick_ref[...] = jnp.swapaxes(w_buf[lax.rem(t, 2)], 0, 1)
            w_ref[rows_of(t, d_block), which * head_dim : (which + 1) * head_dim] = pick_ref[lax.rem(head, heads_tile)]

        each(0, n_d, pick)
        if which < 2:
            w_load(0, which + 1).start()
        if which == 1:
            h_ring.pass_on(*(jnp.int32(v) for v in order[1]))
    own_dy.wait()
    own_h.wait()

    def tables(origin):
        where.got(origin)
        angles = freq_ref[...] * pos_in[origin, 0:1, :].astype(F32)
        cos_ref[:, rows_of(origin, tokens)] = jnp.cos(angles)
        sin_ref[:, rows_of(origin, tokens)] = jnp.sin(angles)

    def event(e):
        return lookup([p[0] for p in order], e), lookup([p[1] for p in order], e)

    def places_of(ring, s, h):
        return [ring.place((kind, way), s, h, core) for kind in range(2) for way in range(2) for core in range(2)]

    def fetch(ring, buf, sem, e):
        slot = lax.rem(e, 2)
        s, h = event(e)
        ring.got_core(s, h)
        for n, place in enumerate(places_of(ring, s, h)):
            pltpu.make_async_copy(ring.all.at[place], buf.at[slot, pl.ds(n * rows_n, rows_n)], sem.at[slot]).start()

    def fetched(ring, buf, sem, e):
        slot = lax.rem(e, 2)
        pltpu.make_async_copy(ring.all.at[pl.ds(0, 8 * rows_n)], buf.at[slot], sem.at[slot]).wait()
        return buf[slot]

    def send_da(t):
        def one(u):
            peer = wo_turn(t) * per_wo + lax.rem(u + me, per_wo)
            da_copy.start(peer, me, peer)

        each(0, per_wo, one)

    def make_da(t):
        @pl.when((t > 0) & (t <= n_wo))
        def _():
            send_da(t - 1)

        @pl.when((t >= 0) & (t < n_wo))
        def _():
            wo_load(t).wait()
            da = dot_t(dy_ref[...], wo_buf[lax.rem(t, 2)]).astype(BF16)
            for u in range(per_wo):
                da_buf[wo_turn(t) * per_wo + u] = da[:, u * head_dim : (u + 1) * head_dim]

            @pl.when(t + 2 < n_wo)
            def _():
                wo_load(t + 2).start()

    def project_rows(e):
        s, h = event(e)
        out = dot(fetched(h_ring, h_buf, h_sem, e), w_ref[...])
        for n, place in enumerate(places_of(h_ring, s, h)):
            part = out[n * rows_n : (n + 1) * rows_n]
            q_ref[place, :] = part[:, :head_dim]
            k_ref[place, :] = part[:, head_dim : 2 * head_dim]
            v_ref[place, :] = part[:, 2 * head_dim :].astype(BF16)

    def step(e):
        @pl.when((e > 1) & (e < n_event))
        def _():
            h_ring.pass_on(*event(e))

        @pl.when(e == max(n_event - 11, 1))
        def _():
            dy_ring.begin()

        for number in range(1, early_events(n_event) + 1):
            @pl.when(e == n_event - 10 + 2 * number)
            def _():
                dy_ring.pass_on(*(jnp.int32(v) for v in order[number]))

        @pl.when(e <= n_event)
        def _():
            fetch(h_ring, h_buf, h_sem, e - 1)

        make_da(e - 1)

        @pl.when((e > 1) & (e < n_event + 2))
        def _():
            project_rows(e - 2)

        @pl.when(e == 3)
        def _():
            each(0, n_dev, tables)

    each(1, max(n_event, n_wo) + 2, step)
    h_ring.end()

    def drain(index):
        where.sent(index, index)
        da_copy.sent(index, index)
        da_copy.got(index)

    each(0, n_dev, drain)


def causal(block):
    key = lax.broadcasted_iota(jnp.int32, (block, block), 0)
    query = lax.broadcasted_iota(jnp.int32, (block, block), 1)
    return key <= query


def part_sum(values):
    return jnp.sum(values.reshape(values.shape[0] // 8, 8, values.shape[1]), axis=0)


def main_part(
    ring_sems, n_dev, n_group, q_heads, kv_heads, n_buf, scale,
    q_raw, k_raw, v_ref, da_ref, cos_ref, sin_ref, x_ref, dy_own_ref, x_hat_ref, inv_ref, gain_ref, h_ref, dy_ref, wq_ref, wk_ref, wv_ref, wo_ref,
    out_ref, gx_ref, gwo_ref, gwq_ref, gwk_ref, gwv_ref, gain_out, bias_out,
    q_rows, kv_rows, sum_ref, at_ref, dqt_ref, a_head, dq_head, dkvt_ref, a_ref, g_ref, dkv_ref, land_one, land_two, kv_ref, kvt_ref, wq_out, wkv_out, dh_ref, part_ref, own_sum, sum_in, sum_mine,
    a_send, a_recv, dq_send, dq_recv, one_send, one_recv, two_send, two_recv, kv_send, kv_recv, near_send, near_recv,
    load_sem, q_send, q_recv, wkv_send, wkv_recv, s_send, s_recv, t_send, t_recv,
):
    me = lax.axis_index(AXIS)
    seq, head_dim = v_ref.shape
    tokens, width = x_ref.shape
    block = tokens * n_group
    n_block = seq // block
    half = block // 2
    fold = scale * math.log2(math.e)
    core, side = lax.rem(me, 2), lax.rem(me // 2, 2)
    member, group = lax.rem(me, n_group), me // n_group
    partner, across = me + 1 - 2 * core, me + 2 - 4 * side
    shift = lax.rem(group, max(2, n_block * 3 // 4))
    depth = width // n_dev
    span = math.lcm(depth, 128)
    n_col = width // span
    per_col = span // depth
    per_core = n_dev // 2
    n_sum = sum_mine.shape[0]
    q_cols = q_heads * head_dim

    def piece(index):
        return rows_of(index, tokens)

    def column(head):
        return rows_of(head, head_dim)

    def cols(j):
        return rows_of(j, span)

    a_copy = Exchange(lambda peer: a_head.at[piece(peer)], lambda head: a_ref.at[:, column(head)], lambda peer: a_send.at[peer], lambda head: a_recv.at[head])
    dq_copy = Exchange(lambda peer: dq_head.at[piece(peer)], lambda head: g_ref.at[:, column(head)], lambda peer: dq_send.at[peer], lambda head: dq_recv.at[head])
    kv_copy = Exchange(lambda n: kv_ref.at[n // 2, piece(lax.rem(n, 2))], lambda slot: g_ref.at[:, column(q_heads + slot)], lambda n: kv_send.at[n], lambda slot: kv_recv.at[slot])
    q_copy = Exchange(lambda peer: wq_out.at[rows_of(peer, depth)], lambda head: q_rows.at[head], lambda peer: q_send.at[peer], lambda head: q_recv.at[head])
    wkv_copy = Exchange(lambda i: wkv_out.at[rows_of(i, depth)], lambda head: kv_rows.at[head], lambda i: wkv_send.at[i], lambda head: wkv_recv.at[head])
    s_copy = Exchange(lambda peer: own_sum.at[pl.ds(peer * n_sum, n_sum)], lambda origin: sum_in.at[origin], lambda peer: s_send.at[peer], lambda origin: s_recv.at[origin])
    t_copy = Exchange(lambda peer: sum_mine, lambda origin: sum_ref.at[pl.ds(origin * n_sum, n_sum)], lambda peer: t_send.at[peer], lambda origin: t_recv.at[origin])


    def one_copy(i):
        return remote(dkv_ref.at[rows_of(i * 2 + 1 - core, half)], land_one.at[i], one_send.at[i], one_recv.at[i], partner)

    kind = side * kv_heads + group

    def half_of(i, which):
        return rows_of(i * 2 + which, half)

    def two_copy(i):
        return remote(dkv_ref.at[half_of(i, core), column(1 - side)], land_two.at[i], two_send.at[i], two_recv.at[i], across)

    def near_copy(i, which):
        return remote(kvt_ref.at[i], dkvt_ref.at[:, half_of(i, which)], near_send.at[i], near_recv.at[i], partner)

    def first(i):
        one_copy(i).start()

    def second(i):
        one_copy(i).wait_recv()
        for which in (1 - side, side):
            dkv_ref[half_of(i, core), column(which)] += land_one[i, :, column(which)]
        two_copy(i).start()

    def close(i):
        two_copy(i).wait_recv()
        rows = half_of(i, core)
        total = (dkv_ref[rows, column(side)] + land_two[i]).T

        def keep(values):
            values = values.astype(BF16)
            kvt_ref[i] = values
            dkvt_ref[:, rows] = values
            kv_ref[i] = values.T

        @pl.when(side == 0)
        def _():
            keep(rotate(total, cos_ref[:, rows], -sin_ref[:, rows]))

        @pl.when(side == 1)
        def _():
            keep(total)

    def spread(i):
        near_copy(i, core).start()
        for u in range(2):
            kv_copy.start(i * 2 + u, kind, i * n_group + core * 2 + u)

    steps = (first, second, close, spread)

    def block_at(t):
        return lax.rem(shift - 1 - t + 2 * n_block, n_block)

    def stages(t):
        for late in range(len(steps), 0, -1):
            n = t - late - shift

            @pl.when(n >= 0)
            def _():
                steps[late - 1](n_block - 1 - n)

    def stage_rest(late):
        each(jnp.maximum(n_block - late - shift, 0), n_block, lambda n: steps[late - 1](n_block - 1 - n))

    def send_pieces(i):
        def send(u):
            peer = i * n_group + lax.rem(u + me, n_group)
            a_copy.start(peer, me, peer)
            dq_copy.start(peer, me, peer)

        each(0, n_group, send)

    dy_ring = Ring(n_dev, dy_own_ref, dy_ref, lean_rows(tokens), *ring_sems)
    order = [(0, 0)] + ring_order(dy_ring.side)
    n_early = early_events(len(order))
    n_served = min(len(order) - 1, n_early + (n_block * (n_block + 1) - 1) // SERVE + 1)

    def serve(number):
        @pl.when(number < len(order))
        def _():
            dy_ring.pass_on(lookup([p[0] for p in order], number), lookup([p[1] for p in order], number))

    def tick(count):
        @pl.when(lax.rem(count, SERVE) == 0)
        def _():
            serve(count // SERVE + 1 + n_early)

    def attention(q_ref, k_ref, qt_ref, kt_ref, vt_ref, e_ref, dp_ref, peak_ref, dat_ref, mix_ref, acc_ref):
        def prepare(i):
            rows = rows_of(i, block)
            for raw, turned, plain in ((q_raw, qt_ref, q_ref), (k_raw, kt_ref, k_ref)):
                t = rotate(raw[rows, :].T, cos_ref[:, rows], sin_ref[:, rows]).astype(BF16)
                turned[:, rows] = t
                plain[rows, :] = t.T
            vt_ref[:, rows] = v_ref[rows, :].T
            dkv_ref[rows, :] = jnp.zeros((block, 2 * head_dim), F32)

        each(0, n_block, prepare)

        def compute(i, done):
            own = rows_of(i, block)
            dat_ref[...] = da_ref[own, :].T
            mix_ref[...] = jnp.zeros_like(mix_ref)
            acc_ref[...] = jnp.zeros_like(acc_ref)

            def scores(j, carry, diagonal):
                peak, total, mixed = carry
                tick(done + j)
                rows = rows_of(j, block)
                s = dot(k_ref[rows, :], qt_ref[:, own])
                if diagonal:
                    s = jnp.where(causal(block), s, -1e30)
                top = jnp.maximum(peak, jnp.max(s, axis=0, keepdims=True))
                e = jnp.exp2((s - top) * fold)
                dp = dot(v_ref[rows, :], dat_ref[...])
                fade = jnp.exp2((peak - top) * fold)
                e_ref[rows, :] = e
                dp_ref[rows, :] = dp
                peak_ref[j] = top
                return top, total * fade + part_sum(e), mixed * fade + part_sum(e * dp)

            start = (jnp.full((1, block), -jnp.inf, F32), jnp.zeros((8, block), F32), jnp.zeros((8, block), F32))
            carry = lax.fori_loop(0, i, functools.partial(scores, diagonal=False), start)
            peak, total, mixed = scores(i, carry, True)
            inv = 1.0 / jnp.sum(total, axis=0, keepdims=True)
            row_dot = jnp.sum(mixed, axis=0, keepdims=True) * inv
            q_own, da_own = q_ref[own, :], da_ref[own, :]

            def grads(j):
                tick(done + i + 1 + j)
                rows = rows_of(j, block)
                p = e_ref[rows, :] * (jnp.exp2((peak_ref[j] - peak) * fold) * inv)
                pb = p.astype(BF16)
                ds = ((dp_ref[rows, :] - row_dot) * (p * scale)).astype(BF16)
                dkv_ref[rows, :head_dim] += dot(ds, q_own)
                dkv_ref[rows, head_dim:] += dot(pb, da_own)
                mix_ref[...] += dot(vt_ref[:, rows], pb)
                acc_ref[...] += dot(kt_ref[:, rows], ds)

            each(0, i + 1, grads)
            at = mix_ref[...].astype(BF16)
            at_ref[:, own] = at
            a_head[own, :] = at.T
            dqt = rotate(acc_ref[...], cos_ref[:, own], -sin_ref[:, own]).astype(BF16)
            dqt_ref[:, own] = dqt
            dq_head[own, :] = dqt.T

        def iteration(t, done):
            stages(t)

            @pl.when(t > 0)
            def _():
                send_pieces(block_at(t - 1))

            i = block_at(t)
            compute(i, done)
            return done + 2 * (i + 1)

        lax.fori_loop(0, n_block, iteration, jnp.int32(0))

    pl.run_scoped(
        attention,
        pltpu.VMEM((seq, head_dim), BF16), pltpu.VMEM((seq, head_dim), BF16),
        pltpu.VMEM((head_dim, seq), BF16), pltpu.VMEM((head_dim, seq), BF16), pltpu.VMEM((head_dim, seq), BF16),
        pltpu.VMEM((seq, block), F32), pltpu.VMEM((seq, block), F32), pltpu.VMEM((n_block, 1, block), F32),
        pltpu.VMEM((head_dim, block), BF16), pltpu.VMEM((head_dim, block), F32), pltpu.VMEM((head_dim, block), F32),
    )

    def drain_sums():
        def one(i):
            one_copy(i).wait_send()
            two_copy(i).wait_send()
            near_copy(i, core).wait_send()
            near_copy(i, 1 - core).wait_recv()
            for u in range(2):
                kv_copy.sent(i * 2 + u, i * n_group + core * 2 + u)

        each(0, n_block, one)
        each(0, 2 * kv_heads, kv_copy.got)

    stage_rest(1)
    send_pieces(block_at(n_block - 1))

    def products(buf, w_buf):
        counts = (n_col, n_col, n_col, n_col // 2, n_col, n_col)
        starts = [sum(counts[:n]) for n in range(len(counts))]

        def loads(phase, j, slot):
            if phase == 1:
                return [pltpu.make_async_copy(wq_ref.at[cols(j)], w_buf.at[slot], load_sem.at[slot, 0])]
            if phase == 4:
                return [pltpu.make_async_copy(ref.at[cols(j)], w_buf.at[slot, :, pl.ds(n * kv_heads, kv_heads)], load_sem.at[slot, n]) for n, ref in enumerate((wk_ref, wv_ref))]
            ref = (h_ref, None, wo_ref, h_ref, None, dy_ref)[phase]
            col = core * (n_col // 2) + j if phase == 3 else j
            return [pltpu.make_async_copy(ref.at[:, cols(col)], buf.at[slot], load_sem.at[slot, 0])]

        def load(step):
            slot = lax.rem(step, n_buf)
            for phase, (begin, count) in enumerate(zip(starts, counts)):
                @pl.when((step >= begin) & (step < begin + count))
                def _():
                    for copy in loads(phase, step - begin, slot):
                        copy.start()

        def serve_late(number):
            for r in range(len(order) - 1 - n_served):
                @pl.when(number == 3 + 6 * r)
                def _():
                    serve(jnp.int32(n_served + 1 + r))

        last = len(counts) - 1

        def run(phase, body):
            def step(j):
                number = starts[phase] + j
                slot = lax.rem(number, n_buf)
                for copy in loads(phase, j, slot):
                    copy.wait()
                if phase < last:
                    serve_late(number)
                body(j, slot)

                @pl.when((number + n_buf < starts[last]) | (phase == last))
                def _():
                    load(number + n_buf)

            each(0, counts[phase], step)

        each(0, n_buf, load)

        def weight_columns(j, slot):
            @pl.when(j == n_col // 4)
            def _():
                stage_rest(2)

            wq_out[cols(j), :] = dot(dqt_ref[...], buf[slot]).T

        run(0, weight_columns)

        def send_rows(j):
            col = alternate(me // per_col, j, n_col)

            def send(u):
                peer = col * per_col + lax.rem(u + me, per_col)
                q_copy.start(peer, me, peer)

            each(0, per_col, send)

        def got_heads(head):
            a_copy.got(head)
            dq_copy.got(head)

        each(0, n_dev, got_heads)

        def flat(slot, n_head):
            rows = w_buf[slot, :, :n_head, :]
            return rows.reshape(rows.shape[0], n_head * head_dim)

        def back_query(j, slot):
            for late, at in ((3, n_col * 3 // 4), (4, n_col - 1)):
                @pl.when(j == at)
                def _():
                    stage_rest(late)

            @pl.when(j < n_col // 2)
            def _():
                send_rows(j)

            dh_ref[:, cols(j)] = dot_t(g_ref[:, :q_cols], flat(slot, q_heads))

        run(1, back_query)

        def output(j, slot):
            @pl.when(j < n_col // 2)
            def _():
                send_rows(n_col // 2 + j)

            out_ref[:, cols(j)] = (x_ref[:, cols(j)].astype(F32) + dot(a_ref[...], buf[slot])).astype(BF16)

        run(2, output)
        drain_sums()

        def weight_kv(j, slot):
            wkv_out[cols(j), :] = dot(dkvt_ref[...], buf[slot]).T

        run(3, weight_kv)

        def send_kv(step):
            index = alternate(lax.rem(me, per_core), step, per_core)
            wkv_copy.start(index, kind, core * per_core + index)

        def back_kv(j, slot):
            @pl.when(j == 0)
            def _():
                each(0, per_core, send_kv)

            dh_ref[:, cols(j)] += dot_t(g_ref[:, q_cols:], flat(slot, 2 * kv_heads))

        run(4, back_kv)

        part_ref[...] = jnp.zeros_like(part_ref)
        gain = 1.0 + gain_ref[...]

        def norm(t):
            rows = rows_of(t, 16)
            grad_h, x_hat = dh_ref[rows, :], x_hat_ref[rows, :]
            grad_hat = grad_h * gain
            one = jnp.sum(grad_hat, axis=1, keepdims=True) * (1.0 / width)
            two = jnp.sum(grad_hat * x_hat, axis=1, keepdims=True) * (1.0 / width)
            back = inv_ref[rows, :] * (grad_hat - one - x_hat * two)
            gx_ref[rows, :] = (dy_own_ref[rows, :].astype(F32) + back).astype(BF16)
            part_ref[0] += part_sum(grad_h * x_hat)
            part_ref[1] += part_sum(grad_h)

        each(0, tokens // 16, norm)
        own_sum[...] = jnp.zeros_like(own_sum)
        for which in range(2):
            total = jnp.sum(part_ref[which], axis=0, keepdims=True)
            for c in range(width // 128):
                own_sum[c, pl.ds(which, 1), :] = total[:, c * 128 : (c + 1) * 128]

        def to_all(copy):
            def send(step):
                peer = alternate(me, step, n_dev)
                copy.start(peer, me, peer)

            each(0, n_dev, send)

        def add(origin):
            sum_mine[...] += sum_in[origin]

        def weight_out(j, slot):
            @pl.when(j == 0)
            def _():
                to_all(s_copy)

            @pl.when(j == n_col // 2)
            def _():
                each(0, n_dev, s_copy.got)
                sum_mine[...] = jnp.zeros_like(sum_mine)
                each(0, n_dev, add)

            gwo_ref[:, cols(j)] = dot(at_ref[...], buf[slot])

            @pl.when(j == n_col // 2)
            def _():
                to_all(t_copy)

        for s, h in order:
            dy_ring.got_core(jnp.int32(s), jnp.int32(h))
        each(starts[last], starts[last] + n_buf, load)
        run(last, weight_out)

    pl.run_scoped(
        products,
        pltpu.VMEM((n_buf, seq, span), BF16),
        pltpu.VMEM((n_buf, span) + wq_ref.shape[1:], BF16),
    )

    dy_ring.end()

    def drain(index):
        for copy in (a_copy, dq_copy, s_copy, t_copy, q_copy):
            copy.sent(index, index)
        t_copy.got(index)
        q_copy.got(index)

    def drain_kv(index):
        wkv_copy.sent(index, core * per_core + index)

    each(0, n_dev, drain)
    each(0, per_core, drain_kv)
    each(0, 2 * kv_heads, wkv_copy.got)

    def settle(t):
        rows = rows_of(t, 8)
        gwq_ref[rows] = jnp.swapaxes(q_rows[:, rows, :], 0, 1)
        gwk_ref[rows] = jnp.swapaxes(kv_rows[:kv_heads, rows, :], 0, 1)
        gwv_ref[rows] = jnp.swapaxes(kv_rows[kv_heads:, rows, :], 0, 1)

    each(0, depth // 8, settle)
    for c in range(width // 128):
        gain_out[:, c * 128 : (c + 1) * 128] = sum_ref[c, 0:1, :]
        bias_out[:, c * 128 : (c + 1) * 128] = sum_ref[c, 1:2, :]


def block_kernel(n_dev, q_heads, kv_heads, n_buf, scale, *refs):
    x_ref, dy_ref, pos_ref, freq_ref, gain_ref, bias_ref, wo_ref, wq_ref, wk_ref, wv_ref = refs[:10]
    outs, (h_all, dy_all) = refs[10:18], refs[18:20]
    heads, pos_in, refs = refs[20:28], refs[28], refs[29:]
    front_sems, main_refs = refs[:16], refs[16:]
    tokens, width = x_ref.shape
    head_dim = wq_ref.shape[2]
    heads_tile = min(8, kv_heads)
    d_block = math.lcm(width // n_dev, 128)
    n_group = q_heads // kv_heads
    weights = (wo_ref, wq_ref, wk_ref, wv_ref)
    pl.run_scoped(
        functools.partial(front_part, n_dev, n_group, x_ref, dy_ref, pos_ref, freq_ref, gain_ref, bias_ref, *weights, h_all, dy_all, *heads, pos_in, *front_sems),
        pltpu.VMEM((tokens, width), BF16),
        pltpu.VMEM((width, 3 * head_dim), BF16),
        pltpu.VMEM((heads_tile, d_block, head_dim), BF16),
        pltpu.VMEM((2, d_block, heads_tile, head_dim), BF16),
        pltpu.VMEM((2, 2 * tokens, width), BF16),
        pltpu.VMEM((2, min(BLOCK, q_heads * head_dim // 2), width), BF16),
        pltpu.VMEM((n_dev, tokens, head_dim), BF16),
        pltpu.VMEM(pos_in.shape[1:], jnp.int32),
    )
    q, k, v, da, cos, sin, x_hat, inv = heads
    main_part(
        front_sems[4:8], n_dev, n_group, q_heads, kv_heads, n_buf, scale,
        q, k, v, da, cos, sin, x_ref, dy_ref, x_hat, inv, gain_ref, h_all, dy_all, wq_ref, wk_ref, wv_ref, wo_ref, *outs, *main_refs,
    )


def whole_block(n_dev, x_own, dy_own, positions, freq, gain, bias, wo, wq, wk, wv):
    tokens, width = x_own.shape
    q_heads, head_dim = wq.shape[1:]
    kv_heads = wk.shape[1]
    seq = tokens * n_dev
    n_group = q_heads // kv_heads
    n_block = n_dev // n_group
    depth = width // n_dev
    n_buf = 3
    n_sum = -(-width // (128 * n_dev))
    sums = (n_sum * n_dev, 8, 128)
    pieces = math.isqrt(n_dev // 2) ** 2
    whole, anywhere = pl.BlockSpec(memory_space=pltpu.VMEM), pl.BlockSpec(memory_space=pl.ANY)
    dma = pltpu.SemaphoreType.DMA
    return pl.pallas_call(
        functools.partial(block_kernel, n_dev, q_heads, kv_heads, n_buf, head_dim**-0.5),
        out_shape=[
            jax.ShapeDtypeStruct((tokens, width), BF16),
            jax.ShapeDtypeStruct((tokens, width), BF16),
            jax.ShapeDtypeStruct((head_dim, width), F32),
            jax.ShapeDtypeStruct((depth, q_heads, head_dim), F32),
            jax.ShapeDtypeStruct((depth, kv_heads, head_dim), F32),
            jax.ShapeDtypeStruct((depth, kv_heads, head_dim), F32),
            jax.ShapeDtypeStruct((1, width), F32),
            jax.ShapeDtypeStruct((1, width), F32),
            jax.ShapeDtypeStruct((seq, width), BF16),
            jax.ShapeDtypeStruct((seq, width), BF16),
        ],
        in_specs=[whole] * 6 + [anywhere] * 4,
        out_specs=[whole] * 8 + [anywhere] * 2,
        scratch_shapes=[
            pltpu.VMEM((seq, head_dim), F32),
            pltpu.VMEM((seq, head_dim), F32),
            pltpu.VMEM((seq, head_dim), BF16),
            pltpu.VMEM((seq, head_dim), BF16),
            pltpu.VMEM((head_dim // 4, seq), F32),
            pltpu.VMEM((head_dim // 4, seq), F32),
            pltpu.VMEM((tokens, width), F32),
            pltpu.VMEM((tokens, 1), F32),
            pltpu.VMEM((n_dev, 8, tokens), jnp.int32),
            dma((4, pieces)), dma((4, pieces)), dma((4, pieces)), dma((4, pieces)),
            dma((4, pieces)), dma((4, pieces)), dma((4, pieces)), dma((4, pieces)),
            dma((2,)), dma((2,)), dma((2,)), dma((n_dev,)), dma((n_dev,)), dma((3,)), dma((n_dev,)), dma((n_dev,)),
            pltpu.VMEM((q_heads, depth, head_dim), F32),
            pltpu.VMEM((2 * kv_heads, depth, head_dim), F32),
            pltpu.VMEM(sums, F32),
            pltpu.VMEM((head_dim, seq), BF16),
            pltpu.VMEM((head_dim, seq), BF16),
            pltpu.VMEM((seq, head_dim), BF16),
            pltpu.VMEM((seq, head_dim), BF16),
            pltpu.VMEM((head_dim, seq), BF16),
            pltpu.VMEM((tokens, q_heads * head_dim), BF16),
            pltpu.VMEM((tokens, (q_heads + 2 * kv_heads) * head_dim), BF16),
            pltpu.VMEM((seq, 2 * head_dim), F32),
            pltpu.VMEM((n_block, tokens * n_group // 2, 2 * head_dim), F32),
            pltpu.VMEM((n_block, tokens * n_group // 2, head_dim), F32),
            pltpu.VMEM((n_block, tokens * n_group // 2, head_dim), BF16),
            pltpu.VMEM((n_block, head_dim, tokens * n_group // 2), BF16),
            pltpu.VMEM((width, head_dim), F32),
            pltpu.VMEM((width // 2, head_dim), F32),
            pltpu.VMEM((tokens, width), F32),
            pltpu.VMEM((2, 8, width), F32),
            pltpu.VMEM(sums, F32),
            pltpu.VMEM((n_dev, n_sum, 8, 128), F32),
            pltpu.VMEM((n_sum, 8, 128), F32),
            dma((n_dev,)), dma((n_dev,)), dma((n_dev,)), dma((n_dev,)),
            dma((n_block,)), dma((n_block,)), dma((n_block,)), dma((n_block,)), dma((2 * n_block,)), dma((2 * kv_heads,)), dma((n_block,)), dma((n_block,)),
            dma((n_buf, 3)), dma((n_dev,)), dma((n_dev,)), dma((n_dev // 2,)), dma((2 * kv_heads,)), dma((n_dev,)), dma((n_dev,)), dma((n_dev,)), dma((n_dev,)),
        ],
        compiler_params=pltpu.CompilerParams(collective_id=1, has_side_effects=True, vmem_limit_bytes=VMEM_LIMIT, flags=FLAGS),
        cost_estimate=pl.CostEstimate(flops=6 * seq * seq * head_dim + 16 * seq * width * head_dim, bytes_accessed=16 * seq * width, transcendentals=seq * seq // 2),
        name="block",
    )(x_own, dy_own, positions, freq, gain, bias, wo, wq, wk, wv)


def solution(mesh):
    n_dev = mesh.shape[AXIS]

    def device_step(x_act, d_out, positions, ln_gain, ln_bias, w_query, w_key, w_value, w_out):
        n_batch, piece, width = x_act.shape
        head_dim = w_query.shape[2]
        tokens = n_batch * piece

        x_own, dy_own = x_act.reshape(tokens, width), d_out.reshape(tokens, width)
        gain, bias = ln_gain.reshape(1, width), ln_bias.reshape(1, width)
        block_out, grad_x, grad_wo, grad_wq, grad_wk, grad_wv, grad_gain, grad_bias, _, _ = whole_block(
            n_dev, x_own, dy_own, positions.reshape(1, tokens), frequencies(head_dim, tokens), gain, bias, w_out, w_query, w_key, w_value
        )
        return (block_out.reshape(x_act.shape), grad_x.reshape(x_act.shape), grad_wq, grad_wk, grad_wv, grad_wo, grad_gain.reshape(width), grad_bias.reshape(width))

    return jax.shard_map(device_step, mesh=mesh, in_specs=(P("dp", AXIS, None), P("dp", AXIS, None), P("dp", AXIS), P(None), P(None), P(None, None, None), P(None, None, None), P(None, None, None), P(None, None)), out_specs=(P("dp", AXIS, None), P("dp", AXIS, None), P(("dp", AXIS), None, None), P(("dp", AXIS), None, None), P(("dp", AXIS), None, None), P(("dp", AXIS), None), P("dp"), P("dp")), check_vma=False)
```

```python
import functools
import math

import jax
import jax.numpy as jnp
import numpy as np
from jax import lax
from jax.experimental import pallas as pl
from jax.experimental.pallas import tpu as pltpu
from jax.sharding import PartitionSpec as P

EPS = 1e-5
ROPE_BASE = 10000.0
BLOCK = 512
AXIS = "cp"
BF16, F32 = jnp.bfloat16, jnp.float32
VMEM_LIMIT = 67043328
FLAGS = {}
SERVE = 9


def frequencies(head_dim, tokens):
    quarter = head_dim // 4
    freq = np.exp(np.arange(quarter, dtype=np.float32) * np.float32(-2.0 * math.log(ROPE_BASE) / (head_dim // 2)))
    return jnp.asarray(np.broadcast_to(freq[:, None], (quarter, tokens)))


def rotate(values, cos, sin):
    quarter = cos.shape[0]
    first, second = values[:quarter], values[quarter : 2 * quarter]
    return jnp.concatenate([first * cos - second * sin, second * cos + first * sin, values[2 * quarter :]], axis=0)


def rows_of(index, size):
    return pl.ds(pl.multiple_of(index * size, size), size)


def dot(lhs, rhs):
    return jnp.dot(lhs, rhs, preferred_element_type=F32)


def dot_t(lhs, rhs):
    return lax.dot_general(lhs, rhs, (((1,), (1,)), ((), ())), preferred_element_type=F32)


def full_barrier(n_dev):
    me = lax.axis_index(AXIS)
    barrier = pltpu.get_barrier_semaphore()

    def tell(step):
        pl.semaphore_signal(barrier, inc=1, device_id={AXIS: lax.rem(me + step, n_dev)}, device_id_type=pl.DeviceIdType.MESH)

    each(1, n_dev, tell)
    pl.semaphore_wait(barrier, n_dev - 1)


def remote(src, dst, send_sem, recv_sem, peer):
    return pltpu.make_async_remote_copy(src_ref=src, dst_ref=dst, send_sem=send_sem, recv_sem=recv_sem, device_id={AXIS: peer}, device_id_type=pl.DeviceIdType.MESH)


def each(lower, upper, body):
    def step(index, carry):
        body(index)
        return carry

    lax.fori_loop(lower, upper, step, 0)


def alternate(index, step, size):
    away = (step + 1) // 2
    return lax.rem(index + jnp.where(lax.rem(step, 2) == 1, away, size - away), size)


class Exchange:
    def __init__(self, src, dst, send, recv):
        self.src, self.dst, self.send, self.recv = src, dst, send, recv

    def start(self, index, slot, peer):
        me = lax.axis_index(AXIS)
        src, dst, recv = self.src(index), self.dst(slot), self.recv(slot)

        @pl.when(peer != me)
        def _():
            remote(src, dst, self.send(index), recv, peer).start()

        @pl.when(peer == me)
        def _():
            pltpu.make_async_copy(src, dst, recv).start()

    def sent(self, index, peer):
        me = lax.axis_index(AXIS)

        @pl.when(peer != me)
        def _():
            remote(self.src(index), self.src(index), self.send(index), self.send(index), me).wait_send()

    def got(self, slot):
        dst = self.dst(slot)
        remote(dst, dst, self.recv(slot), self.recv(slot), lax.axis_index(AXIS)).wait_recv()


def ring_order(side):
    queue, free, order = [(0.0, True, 0, 0), (0.0, False, 0, 0)], 0.0, []
    waiting = []
    while queue or waiting:
        if queue and (not waiting or free <= waiting[0][0]):
            at, along, s, h = queue.pop(0)
            free = max(free, at) + 1.0
            waiting.append((free + 0.5, (s + along, h + 1 - along)))
        else:
            at, (s, h) = waiting.pop(0)
            order.append((s, h))
            if h == 0 and s < side - 1:
                queue.append((at, True, s, h))
            if h < side - 1:
                queue.append((at, False, s, h))
    return order


def lookup(table, index):
    out = jnp.int32(table[0])
    for key, value in enumerate(table[1:], 1):
        out = jnp.where(index == key, jnp.int32(value), out)
    return out


def even_rows(tokens):
    return tokens // 4, tokens // 4


def lean_rows(tokens):
    return tokens * 5 // 16, tokens * 3 // 16


class Ring:
    def __init__(self, n_dev, own, everything, rows, ring_send, ring_recv, core_send, core_recv):
        self.own, self.all, self.rows = own, everything, rows
        self.ring_send, self.ring_recv, self.core_send, self.core_recv = ring_send, ring_recv, core_send, core_recv
        self.side = math.isqrt(n_dev // 2)
        self.tokens = own.shape[0]
        self.me = lax.axis_index(AXIS)
        self.core = lax.rem(self.me, 2)
        self.x, self.y = lax.rem(self.me // 2, self.side), self.me // (2 * self.side)

    def each_colour(self, body):
        for kind in range(2):
            each(0, 2, lambda way: body((kind, way)))

    def device(self, colour, along, across, core):
        side = self.side
        kind, way = colour
        sign = 1 - 2 * way
        dx, dy = (along, across) if kind == 0 else (across, along)
        x = lax.rem(self.x - sign * dx + 2 * side, side)
        y = lax.rem(self.y - sign * dy + 2 * side, side)
        return (y * side + x) * 2 + core

    def within(self, colour):
        kind, way = colour
        return kind * 2 * self.rows[0] + way * self.rows[kind]

    def place(self, colour, s, h, core):
        return pl.ds(pl.multiple_of(self.device(colour, s, h, core) * self.tokens + self.within(colour), 8), self.rows[colour[0]])

    def piece(self, colour, s, h):
        return self.all.at[self.place(colour, s, h, self.core)]

    def own_piece(self, colour):
        return self.own.at[pl.ds(pl.multiple_of(self.within(colour), 8), self.rows[colour[0]])]

    def sem(self, sems, colour, s, h):
        return sems.at[colour[0] * 2 + colour[1], s * self.side + h]

    def ring_copy(self, colour, s, h, along, src=None):
        to = (s + along, h + 1 - along)
        dst = self.piece(colour, s, h)
        peer = self.device(colour, -along, along - 1, self.core)
        return remote(dst if src is None else src, dst, self.sem(self.ring_send, colour, *to), self.sem(self.ring_recv, colour, *to), peer)

    def core_copy(self, colour, s, h, src=None):
        dst = self.piece(colour, s, h)
        return remote(dst if src is None else src, dst, self.sem(self.core_send, colour, s, h), self.sem(self.core_recv, colour, s, h), self.me + 1 - 2 * self.core)

    def arrival(self, colour, s, h):
        dst = self.piece(colour, s, h)
        return remote(dst, dst, self.sem(self.ring_send, colour, s, h), self.sem(self.ring_recv, colour, s, h), self.me)

    def core_arrival(self, colour, s, h):
        dst = self.all.at[self.place(colour, s, h, 1 - self.core)]
        return remote(dst, dst, self.sem(self.core_send, colour, s, h), self.sem(self.core_recv, colour, s, h), self.me)

    def begin(self):
        def one(colour):
            self.ring_copy(colour, 0, 0, 1, self.own_piece(colour)).start()
            self.ring_copy(colour, 0, 0, 0, self.own_piece(colour)).start()

        self.each_colour(one)
        self.each_colour(lambda colour: self.core_copy(colour, 0, 0, self.own_piece(colour)).start())

    def pass_on(self, s, h):
        def one(colour):
            self.arrival(colour, s, h).wait_recv()

            @pl.when((h == 0) & (s < self.side - 1))
            def _():
                self.ring_copy(colour, s, h, 1).start()

            @pl.when(h < self.side - 1)
            def _():
                self.ring_copy(colour, s, h, 0).start()

            self.core_copy(colour, s, h).start()

        self.each_colour(one)

    def got_core(self, s, h):
        self.each_colour(lambda colour: self.core_arrival(colour, s, h).wait_recv())

    def end(self):
        def sent(number):
            s, h = number // self.side, lax.rem(number, self.side)

            def one(colour):
                @pl.when((s > 0) | (h > 0))
                def _():
                    self.arrival(colour, s, h).wait_send()

                self.core_copy(colour, s, h).wait_send()

            self.each_colour(one)

        each(0, self.side * self.side, sent)


def front_part(
    n_dev, n_group, x_ref, dy_ref, pos_ref, freq_ref, gain_ref, bias_ref, wo_ref, wq_ref, wk_ref, wv_ref,
    h_all, dy_all, q_ref, k_ref, v_ref, da_ref, cos_ref, sin_ref, x_hat_ref, inv_ref, pos_in,
    h_send, h_recv, h_core_send, h_core_recv, dy_send, dy_recv, dy_core_send, dy_core_recv, w_sem, h_sem, wo_sem, pos_send, pos_recv, local, da_send, da_recv,
    h_own, w_ref, pick_ref, w_buf, h_buf, wo_buf, da_buf, pos_own,
):
    me = lax.axis_index(AXIS)
    tokens, width = x_ref.shape
    head_dim = v_ref.shape[1]
    heads_tile = w_buf.shape[2]
    d_block = w_buf.shape[1]
    span = wo_buf.shape[1]
    n_wo = wo_ref.shape[0] // span
    per_wo = span // head_dim
    h_ring = Ring(n_dev, h_own, h_all, even_rows(tokens), h_send, h_recv, h_core_send, h_core_recv)
    dy_ring = Ring(n_dev, dy_ref, dy_all, lean_rows(tokens), dy_send, dy_recv, dy_core_send, dy_core_recv)
    rows_n = h_ring.rows[0]
    order = [(0, 0)] + ring_order(h_ring.side)
    n_event = len(order)
    where = Exchange(lambda peer: pos_own, lambda origin: pos_in.at[origin], lambda peer: pos_send.at[peer], lambda origin: pos_recv.at[origin])

    da_copy = Exchange(lambda peer: da_buf.at[peer], lambda origin: da_ref.at[rows_of(origin, tokens)], lambda peer: da_send.at[peer], lambda origin: da_recv.at[origin])

    n_d = width // d_block
    kv_head = me // n_group

    def w_load(t, which):
        ref, head = ((wq_ref, me), (wk_ref, kv_head), (wv_ref, kv_head))[which]
        slot = lax.rem(t, 2)
        return pltpu.make_async_copy(ref.at[rows_of(t, d_block), rows_of(head // heads_tile, heads_tile)], w_buf.at[slot], w_sem.at[slot])

    own_dy = pltpu.make_async_copy(dy_ref, dy_all.at[rows_of(me, tokens)], local.at[0])
    own_h = pltpu.make_async_copy(h_own, h_all.at[rows_of(me, tokens)], local.at[1])
    own_dy.start()
    w_load(0, 0).start()

    def wo_turn(t):
        return alternate(me // per_wo, t, n_wo)

    def wo_load(t):
        slot = lax.rem(t, 2)
        return pltpu.make_async_copy(wo_ref.at[rows_of(wo_turn(t), span)], wo_buf.at[slot], wo_sem.at[slot])

    wo_load(jnp.int32(0)).start()
    wo_load(jnp.int32(1)).start()
    pos_own[...] = jnp.broadcast_to(pos_ref[...], pos_own.shape)
    gain, bias = 1.0 + gain_ref[...], bias_ref[...]

    def norm(t):
        rows = rows_of(t, 16)
        x = x_ref[rows, :].astype(F32)
        centered = x - jnp.sum(x, axis=1, keepdims=True) * (1.0 / width)
        inv = lax.rsqrt(jnp.sum(centered * centered, axis=1, keepdims=True) * (1.0 / width) + EPS)
        x_hat = centered * inv
        x_hat_ref[rows, :] = x_hat
        inv_ref[rows, :] = inv
        h_own[rows, :] = (x_hat * gain + bias).astype(BF16)

    each(0, tokens // 16, norm)
    full_barrier(n_dev)

    def send_pos(step):
        peer = alternate(me, step, n_dev)
        where.start(peer, me, peer)

    h_ring.begin()
    each(0, n_dev, send_pos)
    own_h.start()

    for which in range(3):
        head = me if which == 0 else kv_head

        def pick(t):
            @pl.when(t + 1 < n_d)
            def _():
                w_load(t + 1, which).start()

            w_load(t, which).wait()
            pick_ref[...] = jnp.swapaxes(w_buf[lax.rem(t, 2)], 0, 1)
            w_ref[rows_of(t, d_block), which * head_dim : (which + 1) * head_dim] = pick_ref[lax.rem(head, heads_tile)]

        each(0, n_d, pick)
        if which < 2:
            w_load(0, which + 1).start()
        if which == 1:
            h_ring.pass_on(*(jnp.int32(v) for v in order[1]))
    own_dy.wait()
    own_h.wait()

    def tables(origin):
        where.got(origin)
        angles = freq_ref[...] * pos_in[origin, 0:1, :].astype(F32)
        cos_ref[:, rows_of(origin, tokens)] = jnp.cos(angles)
        sin_ref[:, rows_of(origin, tokens)] = jnp.sin(angles)

    def event(e):
        return lookup([p[0] for p in order], e), lookup([p[1] for p in order], e)

    def places_of(ring, s, h):
        return [ring.place((kind, way), s, h, core) for kind in range(2) for way in range(2) for core in range(2)]

    def fetch(ring, buf, sem, e):
        slot = lax.rem(e, 2)
        s, h = event(e)
        ring.got_core(s, h)
        for n, place in enumerate(places_of(ring, s, h)):
            pltpu.make_async_copy(ring.all.at[place], buf.at[slot, pl.ds(n * rows_n, rows_n)], sem.at[slot]).start()

    def fetched(ring, buf, sem, e):
        slot = lax.rem(e, 2)
        pltpu.make_async_copy(ring.all.at[pl.ds(0, 8 * rows_n)], buf.at[slot], sem.at[slot]).wait()
        return buf[slot]

    def send_da(t):
        def one(u):
            peer = wo_turn(t) * per_wo + lax.rem(u + me, per_wo)
            da_copy.start(peer, me, peer)

        each(0, per_wo, one)

    def make_da(t):
        @pl.when((t > 0) & (t <= n_wo))
        def _():
            send_da(t - 1)

        @pl.when((t >= 0) & (t < n_wo))
        def _():
            wo_load(t).wait()
            da = dot_t(dy_ref[...], wo_buf[lax.rem(t, 2)]).astype(BF16)
            for u in range(per_wo):
                da_buf[wo_turn(t) * per_wo + u] = da[:, u * head_dim : (u + 1) * head_dim]

            @pl.when(t + 2 < n_wo)
            def _():
                wo_load(t + 2).start()

    def project_rows(e):
        s, h = event(e)
        out = dot(fetched(h_ring, h_buf, h_sem, e), w_ref[...])
        for n, place in enumerate(places_of(h_ring, s, h)):
            part = out[n * rows_n : (n + 1) * rows_n]
            q_ref[place, :] = part[:, :head_dim]
            k_ref[place, :] = part[:, head_dim : 2 * head_dim]
            v_ref[place, :] = part[:, 2 * head_dim :].astype(BF16)

    def step(e):
        @pl.when((e > 1) & (e < n_event))
        def _():
            h_ring.pass_on(*event(e))

        @pl.when(e == n_event - 1)
        def _():
            dy_ring.begin()

        @pl.when(e <= n_event)
        def _():
            fetch(h_ring, h_buf, h_sem, e - 1)

        make_da(e - 1)

        @pl.when((e > 1) & (e < n_event + 2))
        def _():
            project_rows(e - 2)

        @pl.when(e == 3)
        def _():
            each(0, n_dev, tables)

    each(1, max(n_event, n_wo) + 2, step)
    h_ring.end()

    def drain(index):
        where.sent(index, index)
        da_copy.sent(index, index)
        da_copy.got(index)

    each(0, n_dev, drain)


def causal(block):
    key = lax.broadcasted_iota(jnp.int32, (block, block), 0)
    query = lax.broadcasted_iota(jnp.int32, (block, block), 1)
    return key <= query


def part_sum(values):
    return jnp.sum(values.reshape(values.shape[0] // 8, 8, values.shape[1]), axis=0)


def main_part(
    ring_sems, n_dev, n_group, q_heads, kv_heads, n_buf, scale,
    q_raw, k_raw, v_ref, da_ref, cos_ref, sin_ref, x_ref, dy_own_ref, x_hat_ref, inv_ref, gain_ref, h_ref, dy_ref, wq_ref, wk_ref, wv_ref, wo_ref,
    out_ref, gx_ref, gwo_ref, gwq_ref, gwk_ref, gwv_ref, gain_out, bias_out,
    q_rows, kv_rows, sum_ref, at_ref, dqt_ref, a_head, dq_head, dkvt_ref, a_ref, g_ref, dkv_ref, land_one, land_two, kv_ref, kvt_ref, wq_out, wkv_out, dh_ref, part_ref, own_sum, sum_in, sum_mine,
    a_send, a_recv, dq_send, dq_recv, one_send, one_recv, two_send, two_recv, kv_send, kv_recv, near_send, near_recv,
    load_sem, q_send, q_recv, wkv_send, wkv_recv, s_send, s_recv, t_send, t_recv,
):
    me = lax.axis_index(AXIS)
    seq, head_dim = v_ref.shape
    tokens, width = x_ref.shape
    block = tokens * n_group
    n_block = seq // block
    half = block // 2
    fold = scale * math.log2(math.e)
    core, side = lax.rem(me, 2), lax.rem(me // 2, 2)
    member, group = lax.rem(me, n_group), me // n_group
    partner, across = me + 1 - 2 * core, me + 2 - 4 * side
    shift = lax.rem(group, max(2, n_block * 3 // 4))
    depth = width // n_dev
    span = math.lcm(depth, 128)
    n_col = width // span
    per_col = span // depth
    per_core = n_dev // 2
    n_sum = sum_mine.shape[0]
    q_cols = q_heads * head_dim

    def piece(index):
        return rows_of(index, tokens)

    def column(head):
        return rows_of(head, head_dim)

    def cols(j):
        return rows_of(j, span)

    a_copy = Exchange(lambda peer: a_head.at[piece(peer)], lambda head: a_ref.at[:, column(head)], lambda peer: a_send.at[peer], lambda head: a_recv.at[head])
    dq_copy = Exchange(lambda peer: dq_head.at[piece(peer)], lambda head: g_ref.at[:, column(head)], lambda peer: dq_send.at[peer], lambda head: dq_recv.at[head])
    kv_copy = Exchange(lambda n: kv_ref.at[n // 2, piece(lax.rem(n, 2))], lambda slot: g_ref.at[:, column(q_heads + slot)], lambda n: kv_send.at[n], lambda slot: kv_recv.at[slot])
    q_copy = Exchange(lambda peer: wq_out.at[rows_of(peer, depth)], lambda head: q_rows.at[head], lambda peer: q_send.at[peer], lambda head: q_recv.at[head])
    wkv_copy = Exchange(lambda i: wkv_out.at[rows_of(i, depth)], lambda head: kv_rows.at[head], lambda i: wkv_send.at[i], lambda head: wkv_recv.at[head])
    s_copy = Exchange(lambda peer: own_sum.at[pl.ds(peer * n_sum, n_sum)], lambda origin: sum_in.at[origin], lambda peer: s_send.at[peer], lambda origin: s_recv.at[origin])
    t_copy = Exchange(lambda peer: sum_mine, lambda origin: sum_ref.at[pl.ds(origin * n_sum, n_sum)], lambda peer: t_send.at[peer], lambda origin: t_recv.at[origin])


    def one_copy(i):
        return remote(dkv_ref.at[rows_of(i * 2 + 1 - core, half)], land_one.at[i], one_send.at[i], one_recv.at[i], partner)

    kind = side * kv_heads + group

    def half_of(i, which):
        return rows_of(i * 2 + which, half)

    def two_copy(i):
        return remote(dkv_ref.at[half_of(i, core), column(1 - side)], land_two.at[i], two_send.at[i], two_recv.at[i], across)

    def near_copy(i, which):
        return remote(kvt_ref.at[i], dkvt_ref.at[:, half_of(i, which)], near_send.at[i], near_recv.at[i], partner)

    def first(i):
        one_copy(i).start()

    def second(i):
        one_copy(i).wait_recv()
        for which in (1 - side, side):
            dkv_ref[half_of(i, core), column(which)] += land_one[i, :, column(which)]
        two_copy(i).start()

    def close(i):
        two_copy(i).wait_recv()
        rows = half_of(i, core)
        total = (dkv_ref[rows, column(side)] + land_two[i]).T

        def keep(values):
            values = values.astype(BF16)
            kvt_ref[i] = values
            dkvt_ref[:, rows] = values
            kv_ref[i] = values.T

        @pl.when(side == 0)
        def _():
            keep(rotate(total, cos_ref[:, rows], -sin_ref[:, rows]))

        @pl.when(side == 1)
        def _():
            keep(total)

    def spread(i):
        near_copy(i, core).start()
        for u in range(2):
            kv_copy.start(i * 2 + u, kind, i * n_group + core * 2 + u)

    steps = (first, second, close, spread)

    def block_at(t):
        return lax.rem(shift - 1 - t + 2 * n_block, n_block)

    def stages(t):
        for late in range(len(steps), 0, -1):
            n = t - late - shift

            @pl.when(n >= 0)
            def _():
                steps[late - 1](n_block - 1 - n)

    def stage_rest(late):
        each(jnp.maximum(n_block - late - shift, 0), n_block, lambda n: steps[late - 1](n_block - 1 - n))

    def send_pieces(i):
        def send(u):
            peer = i * n_group + lax.rem(u + me, n_group)
            a_copy.start(peer, me, peer)
            dq_copy.start(peer, me, peer)

        each(0, n_group, send)

    dy_ring = Ring(n_dev, dy_own_ref, dy_ref, lean_rows(tokens), *ring_sems)
    order = [(0, 0)] + ring_order(dy_ring.side)
    n_served = min(len(order) - 1, n_block * (n_block + 1) // SERVE)

    def serve(number):
        @pl.when(number < len(order))
        def _():
            dy_ring.pass_on(lookup([p[0] for p in order], number), lookup([p[1] for p in order], number))

    def tick(count):
        @pl.when(lax.rem(count, SERVE) == SERVE - 1)
        def _():
            serve(count // SERVE + 1)

    def attention(q_ref, k_ref, qt_ref, kt_ref, vt_ref, e_ref, dp_ref, peak_ref, dat_ref, mix_ref, acc_ref):
        def prepare(i):
            rows = rows_of(i, block)
            for raw, turned, plain in ((q_raw, qt_ref, q_ref), (k_raw, kt_ref, k_ref)):
                t = rotate(raw[rows, :].T, cos_ref[:, rows], sin_ref[:, rows]).astype(BF16)
                turned[:, rows] = t
                plain[rows, :] = t.T
            vt_ref[:, rows] = v_ref[rows, :].T
            dkv_ref[rows, :] = jnp.zeros((block, 2 * head_dim), F32)

        each(0, n_block, prepare)

        def compute(i, done):
            own = rows_of(i, block)
            dat_ref[...] = da_ref[own, :].T
            mix_ref[...] = jnp.zeros_like(mix_ref)
            acc_ref[...] = jnp.zeros_like(acc_ref)

            def scores(j, carry, diagonal):
                peak, total, mixed = carry
                tick(done + j)
                rows = rows_of(j, block)
                s = dot(k_ref[rows, :], qt_ref[:, own])
                if diagonal:
                    s = jnp.where(causal(block), s, -1e30)
                top = jnp.maximum(peak, jnp.max(s, axis=0, keepdims=True))
                e = jnp.exp2((s - top) * fold)
                dp = dot(v_ref[rows, :], dat_ref[...])
                fade = jnp.exp2((peak - top) * fold)
                e_ref[rows, :] = e
                dp_ref[rows, :] = dp
                peak_ref[j] = top
                return top, total * fade + part_sum(e), mixed * fade + part_sum(e * dp)

            start = (jnp.full((1, block), -jnp.inf, F32), jnp.zeros((8, block), F32), jnp.zeros((8, block), F32))
            carry = lax.fori_loop(0, i, functools.partial(scores, diagonal=False), start)
            peak, total, mixed = scores(i, carry, True)
            inv = 1.0 / jnp.sum(total, axis=0, keepdims=True)
            row_dot = jnp.sum(mixed, axis=0, keepdims=True) * inv
            q_own, da_own = q_ref[own, :], da_ref[own, :]

            def grads(j):
                tick(done + i + 1 + j)
                rows = rows_of(j, block)
                p = e_ref[rows, :] * (jnp.exp2((peak_ref[j] - peak) * fold) * inv)
                pb = p.astype(BF16)
                ds = ((dp_ref[rows, :] - row_dot) * (p * scale)).astype(BF16)
                dkv_ref[rows, :head_dim] += dot(ds, q_own)
                dkv_ref[rows, head_dim:] += dot(pb, da_own)
                mix_ref[...] += dot(vt_ref[:, rows], pb)
                acc_ref[...] += dot(kt_ref[:, rows], ds)

            each(0, i + 1, grads)
            at = mix_ref[...].astype(BF16)
            at_ref[:, own] = at
            a_head[own, :] = at.T
            dqt = rotate(acc_ref[...], cos_ref[:, own], -sin_ref[:, own]).astype(BF16)
            dqt_ref[:, own] = dqt
            dq_head[own, :] = dqt.T

        def iteration(t, done):
            stages(t)

            @pl.when(t > 0)
            def _():
                send_pieces(block_at(t - 1))

            i = block_at(t)
            compute(i, done)
            return done + 2 * (i + 1)

        lax.fori_loop(0, n_block, iteration, jnp.int32(0))

    pl.run_scoped(
        attention,
        pltpu.VMEM((seq, head_dim), BF16), pltpu.VMEM((seq, head_dim), BF16),
        pltpu.VMEM((head_dim, seq), BF16), pltpu.VMEM((head_dim, seq), BF16), pltpu.VMEM((head_dim, seq), BF16),
        pltpu.VMEM((seq, block), F32), pltpu.VMEM((seq, block), F32), pltpu.VMEM((n_block, 1, block), F32),
        pltpu.VMEM((head_dim, block), BF16), pltpu.VMEM((head_dim, block), F32), pltpu.VMEM((head_dim, block), F32),
    )

    def drain_sums():
        def one(i):
            one_copy(i).wait_send()
            two_copy(i).wait_send()
            near_copy(i, core).wait_send()
            near_copy(i, 1 - core).wait_recv()
            for u in range(2):
                kv_copy.sent(i * 2 + u, i * n_group + core * 2 + u)

        each(0, n_block, one)
        each(0, 2 * kv_heads, kv_copy.got)

    stage_rest(1)
    send_pieces(block_at(n_block - 1))

    def products(buf, w_buf):
        counts = (n_col, n_col, n_col, n_col // 2, n_col, n_col)
        starts = [sum(counts[:n]) for n in range(len(counts))]

        def loads(phase, j, slot):
            if phase == 1:
                return [pltpu.make_async_copy(wq_ref.at[cols(j)], w_buf.at[slot], load_sem.at[slot, 0])]
            if phase == 4:
                return [pltpu.make_async_copy(ref.at[cols(j)], w_buf.at[slot, :, pl.ds(n * kv_heads, kv_heads)], load_sem.at[slot, n]) for n, ref in enumerate((wk_ref, wv_ref))]
            ref = (h_ref, None, wo_ref, h_ref, None, dy_ref)[phase]
            col = core * (n_col // 2) + j if phase == 3 else j
            return [pltpu.make_async_copy(ref.at[:, cols(col)], buf.at[slot], load_sem.at[slot, 0])]

        def load(step):
            slot = lax.rem(step, n_buf)
            for phase, (begin, count) in enumerate(zip(starts, counts)):
                @pl.when((step >= begin) & (step < begin + count))
                def _():
                    for copy in loads(phase, step - begin, slot):
                        copy.start()

        def serve_late(number):
            for r in range(len(order) - 1 - n_served):
                @pl.when(number == 2 + 5 * r)
                def _():
                    serve(jnp.int32(n_served + 1 + r))

        last = len(counts) - 1

        def run(phase, body):
            def step(j):
                number = starts[phase] + j
                slot = lax.rem(number, n_buf)
                for copy in loads(phase, j, slot):
                    copy.wait()
                if phase < last:
                    serve_late(number)
                body(j, slot)

                @pl.when((number + n_buf < starts[last]) | (phase == last))
                def _():
                    load(number + n_buf)

            each(0, counts[phase], step)

        each(0, n_buf, load)

        def weight_columns(j, slot):
            @pl.when(j == n_col // 4)
            def _():
                stage_rest(2)

            wq_out[cols(j), :] = dot(dqt_ref[...], buf[slot]).T

        run(0, weight_columns)

        def send_rows(j):
            col = alternate(me // per_col, j, n_col)

            def send(u):
                peer = col * per_col + lax.rem(u + me, per_col)
                q_copy.start(peer, me, peer)

            each(0, per_col, send)

        def got_heads(head):
            a_copy.got(head)
            dq_copy.got(head)

        each(0, n_dev, got_heads)

        def flat(slot, n_head):
            rows = w_buf[slot, :, :n_head, :]
            return rows.reshape(rows.shape[0], n_head * head_dim)

        def back_query(j, slot):
            for late, at in ((3, n_col * 3 // 4), (4, n_col - 1)):
                @pl.when(j == at)
                def _():
                    stage_rest(late)

            @pl.when(j < n_col // 2)
            def _():
                send_rows(j)

            dh_ref[:, cols(j)] = dot_t(g_ref[:, :q_cols], flat(slot, q_heads))

        run(1, back_query)

        def output(j, slot):
            @pl.when(j < n_col // 2)
            def _():
                send_rows(n_col // 2 + j)

            out_ref[:, cols(j)] = (x_ref[:, cols(j)].astype(F32) + dot(a_ref[...], buf[slot])).astype(BF16)

        run(2, output)
        drain_sums()

        def weight_kv(j, slot):
            wkv_out[cols(j), :] = dot(dkvt_ref[...], buf[slot]).T

        run(3, weight_kv)

        def send_kv(step):
            index = alternate(lax.rem(me, per_core), step, per_core)
            wkv_copy.start(index, kind, core * per_core + index)

        def back_kv(j, slot):
            @pl.when(j == 0)
            def _():
                each(0, per_core, send_kv)

            dh_ref[:, cols(j)] += dot_t(g_ref[:, q_cols:], flat(slot, 2 * kv_heads))

        run(4, back_kv)

        part_ref[...] = jnp.zeros_like(part_ref)
        gain = 1.0 + gain_ref[...]

        def norm(t):
            rows = rows_of(t, 16)
            grad_h, x_hat = dh_ref[rows, :], x_hat_ref[rows, :]
            grad_hat = grad_h * gain
            one = jnp.sum(grad_hat, axis=1, keepdims=True) * (1.0 / width)
            two = jnp.sum(grad_hat * x_hat, axis=1, keepdims=True) * (1.0 / width)
            back = inv_ref[rows, :] * (grad_hat - one - x_hat * two)
            gx_ref[rows, :] = (dy_own_ref[rows, :].astype(F32) + back).astype(BF16)
            part_ref[0] += part_sum(grad_h * x_hat)
            part_ref[1] += part_sum(grad_h)

        each(0, tokens // 16, norm)
        own_sum[...] = jnp.zeros_like(own_sum)
        for which in range(2):
            total = jnp.sum(part_ref[which], axis=0, keepdims=True)
            for c in range(width // 128):
                own_sum[c, pl.ds(which, 1), :] = total[:, c * 128 : (c + 1) * 128]

        def to_all(copy):
            def send(step):
                peer = alternate(me, step, n_dev)
                copy.start(peer, me, peer)

            each(0, n_dev, send)

        def add(origin):
            sum_mine[...] += sum_in[origin]

        def weight_out(j, slot):
            @pl.when(j == 0)
            def _():
                to_all(s_copy)

            @pl.when(j == n_col // 2)
            def _():
                each(0, n_dev, s_copy.got)
                sum_mine[...] = jnp.zeros_like(sum_mine)
                each(0, n_dev, add)

            gwo_ref[:, cols(j)] = dot(at_ref[...], buf[slot])

            @pl.when(j == n_col // 2)
            def _():
                to_all(t_copy)

        for s, h in order:
            dy_ring.got_core(jnp.int32(s), jnp.int32(h))
        each(starts[last], starts[last] + n_buf, load)
        run(last, weight_out)

    pl.run_scoped(
        products,
        pltpu.VMEM((n_buf, seq, span), BF16),
        pltpu.VMEM((n_buf, span) + wq_ref.shape[1:], BF16),
    )

    dy_ring.end()

    def drain(index):
        for copy in (a_copy, dq_copy, s_copy, t_copy, q_copy):
            copy.sent(index, index)
        t_copy.got(index)
        q_copy.got(index)

    def drain_kv(index):
        wkv_copy.sent(index, core * per_core + index)

    each(0, n_dev, drain)
    each(0, per_core, drain_kv)
    each(0, 2 * kv_heads, wkv_copy.got)

    def settle(t):
        rows = rows_of(t, 8)
        gwq_ref[rows] = jnp.swapaxes(q_rows[:, rows, :], 0, 1)
        gwk_ref[rows] = jnp.swapaxes(kv_rows[:kv_heads, rows, :], 0, 1)
        gwv_ref[rows] = jnp.swapaxes(kv_rows[kv_heads:, rows, :], 0, 1)

    each(0, depth // 8, settle)
    for c in range(width // 128):
        gain_out[:, c * 128 : (c + 1) * 128] = sum_ref[c, 0:1, :]
        bias_out[:, c * 128 : (c + 1) * 128] = sum_ref[c, 1:2, :]


def block_kernel(n_dev, q_heads, kv_heads, n_buf, scale, *refs):
    x_ref, dy_ref, pos_ref, freq_ref, gain_ref, bias_ref, wo_ref, wq_ref, wk_ref, wv_ref = refs[:10]
    outs, (h_all, dy_all) = refs[10:18], refs[18:20]
    heads, pos_in, refs = refs[20:28], refs[28], refs[29:]
    front_sems, main_refs = refs[:16], refs[16:]
    tokens, width = x_ref.shape
    head_dim = wq_ref.shape[2]
    heads_tile = min(8, kv_heads)
    d_block = math.lcm(width // n_dev, 128)
    n_group = q_heads // kv_heads
    weights = (wo_ref, wq_ref, wk_ref, wv_ref)
    pl.run_scoped(
        functools.partial(front_part, n_dev, n_group, x_ref, dy_ref, pos_ref, freq_ref, gain_ref, bias_ref, *weights, h_all, dy_all, *heads, pos_in, *front_sems),
        pltpu.VMEM((tokens, width), BF16),
        pltpu.VMEM((width, 3 * head_dim), BF16),
        pltpu.VMEM((heads_tile, d_block, head_dim), BF16),
        pltpu.VMEM((2, d_block, heads_tile, head_dim), BF16),
        pltpu.VMEM((2, 2 * tokens, width), BF16),
        pltpu.VMEM((2, min(BLOCK, q_heads * head_dim // 2), width), BF16),
        pltpu.VMEM((n_dev, tokens, head_dim), BF16),
        pltpu.VMEM(pos_in.shape[1:], jnp.int32),
    )
    q, k, v, da, cos, sin, x_hat, inv = heads
    main_part(
        front_sems[4:8], n_dev, n_group, q_heads, kv_heads, n_buf, scale,
        q, k, v, da, cos, sin, x_ref, dy_ref, x_hat, inv, gain_ref, h_all, dy_all, wq_ref, wk_ref, wv_ref, wo_ref, *outs, *main_refs,
    )


def whole_block(n_dev, x_own, dy_own, positions, freq, gain, bias, wo, wq, wk, wv):
    tokens, width = x_own.shape
    q_heads, head_dim = wq.shape[1:]
    kv_heads = wk.shape[1]
    seq = tokens * n_dev
    n_group = q_heads // kv_heads
    n_block = n_dev // n_group
    depth = width // n_dev
    n_buf = 3
    n_sum = -(-width // (128 * n_dev))
    sums = (n_sum * n_dev, 8, 128)
    pieces = math.isqrt(n_dev // 2) ** 2
    whole, anywhere = pl.BlockSpec(memory_space=pltpu.VMEM), pl.BlockSpec(memory_space=pl.ANY)
    dma = pltpu.SemaphoreType.DMA
    return pl.pallas_call(
        functools.partial(block_kernel, n_dev, q_heads, kv_heads, n_buf, head_dim**-0.5),
        out_shape=[
            jax.ShapeDtypeStruct((tokens, width), BF16),
            jax.ShapeDtypeStruct((tokens, width), BF16),
            jax.ShapeDtypeStruct((head_dim, width), F32),
            jax.ShapeDtypeStruct((depth, q_heads, head_dim), F32),
            jax.ShapeDtypeStruct((depth, kv_heads, head_dim), F32),
            jax.ShapeDtypeStruct((depth, kv_heads, head_dim), F32),
            jax.ShapeDtypeStruct((1, width), F32),
            jax.ShapeDtypeStruct((1, width), F32),
            jax.ShapeDtypeStruct((seq, width), BF16),
            jax.ShapeDtypeStruct((seq, width), BF16),
        ],
        in_specs=[whole] * 6 + [anywhere] * 4,
        out_specs=[whole] * 8 + [anywhere] * 2,
        scratch_shapes=[
            pltpu.VMEM((seq, head_dim), F32),
            pltpu.VMEM((seq, head_dim), F32),
            pltpu.VMEM((seq, head_dim), BF16),
            pltpu.VMEM((seq, head_dim), BF16),
            pltpu.VMEM((head_dim // 4, seq), F32),
            pltpu.VMEM((head_dim // 4, seq), F32),
            pltpu.VMEM((tokens, width), F32),
            pltpu.VMEM((tokens, 1), F32),
            pltpu.VMEM((n_dev, 8, tokens), jnp.int32),
            dma((4, pieces)), dma((4, pieces)), dma((4, pieces)), dma((4, pieces)),
            dma((4, pieces)), dma((4, pieces)), dma((4, pieces)), dma((4, pieces)),
            dma((2,)), dma((2,)), dma((2,)), dma((n_dev,)), dma((n_dev,)), dma((3,)), dma((n_dev,)), dma((n_dev,)),
            pltpu.VMEM((q_heads, depth, head_dim), F32),
            pltpu.VMEM((2 * kv_heads, depth, head_dim), F32),
            pltpu.VMEM(sums, F32),
            pltpu.VMEM((head_dim, seq), BF16),
            pltpu.VMEM((head_dim, seq), BF16),
            pltpu.VMEM((seq, head_dim), BF16),
            pltpu.VMEM((seq, head_dim), BF16),
            pltpu.VMEM((head_dim, seq), BF16),
            pltpu.VMEM((tokens, q_heads * head_dim), BF16),
            pltpu.VMEM((tokens, (q_heads + 2 * kv_heads) * head_dim), BF16),
            pltpu.VMEM((seq, 2 * head_dim), F32),
            pltpu.VMEM((n_block, tokens * n_group // 2, 2 * head_dim), F32),
            pltpu.VMEM((n_block, tokens * n_group // 2, head_dim), F32),
            pltpu.VMEM((n_block, tokens * n_group // 2, head_dim), BF16),
            pltpu.VMEM((n_block, head_dim, tokens * n_group // 2), BF16),
            pltpu.VMEM((width, head_dim), F32),
            pltpu.VMEM((width // 2, head_dim), F32),
            pltpu.VMEM((tokens, width), F32),
            pltpu.VMEM((2, 8, width), F32),
            pltpu.VMEM(sums, F32),
            pltpu.VMEM((n_dev, n_sum, 8, 128), F32),
            pltpu.VMEM((n_sum, 8, 128), F32),
            dma((n_dev,)), dma((n_dev,)), dma((n_dev,)), dma((n_dev,)),
            dma((n_block,)), dma((n_block,)), dma((n_block,)), dma((n_block,)), dma((2 * n_block,)), dma((2 * kv_heads,)), dma((n_block,)), dma((n_block,)),
            dma((n_buf, 3)), dma((n_dev,)), dma((n_dev,)), dma((n_dev // 2,)), dma((2 * kv_heads,)), dma((n_dev,)), dma((n_dev,)), dma((n_dev,)), dma((n_dev,)),
        ],
        compiler_params=pltpu.CompilerParams(collective_id=1, has_side_effects=True, vmem_limit_bytes=VMEM_LIMIT, flags=FLAGS),
        cost_estimate=pl.CostEstimate(flops=6 * seq * seq * head_dim + 16 * seq * width * head_dim, bytes_accessed=16 * seq * width, transcendentals=seq * seq // 2),
        name="block",
    )(x_own, dy_own, positions, freq, gain, bias, wo, wq, wk, wv)


def solution(mesh):
    n_dev = mesh.shape[AXIS]

    def device_step(x_act, d_out, positions, ln_gain, ln_bias, w_query, w_key, w_value, w_out):
        n_batch, piece, width = x_act.shape
        head_dim = w_query.shape[2]
        tokens = n_batch * piece

        x_own, dy_own = x_act.reshape(tokens, width), d_out.reshape(tokens, width)
        gain, bias = ln_gain.reshape(1, width), ln_bias.reshape(1, width)
        block_out, grad_x, grad_wo, grad_wq, grad_wk, grad_wv, grad_gain, grad_bias, _, _ = whole_block(
            n_dev, x_own, dy_own, positions.reshape(1, tokens), frequencies(head_dim, tokens), gain, bias, w_out, w_query, w_key, w_value
        )
        return (block_out.reshape(x_act.shape), grad_x.reshape(x_act.shape), grad_wq, grad_wk, grad_wv, grad_wo, grad_gain.reshape(width), grad_bias.reshape(width))

    return jax.shard_map(device_step, mesh=mesh, in_specs=(P("dp", AXIS, None), P("dp", AXIS, None), P("dp", AXIS), P(None), P(None), P(None, None, None), P(None, None, None), P(None, None, None), P(None, None)), out_specs=(P("dp", AXIS, None), P("dp", AXIS, None), P(("dp", AXIS), None, None), P(("dp", AXIS), None, None), P(("dp", AXIS), None, None), P(("dp", AXIS), None), P("dp"), P("dp")), check_vma=False)
```

```python
import functools
import math

import jax
import jax.numpy as jnp
import numpy as np
from jax import lax
from jax.experimental import pallas as pl
from jax.experimental.pallas import tpu as pltpu
from jax.sharding import PartitionSpec as P

EPS = 1e-5
ROPE_BASE = 10000.0
BLOCK = 512
AXIS = "cp"
BF16, F32 = jnp.bfloat16, jnp.float32
VMEM_LIMIT = 67043328
FLAGS = {}
SERVE = 14


def frequencies(head_dim, tokens):
    quarter = head_dim // 4
    freq = np.exp(np.arange(quarter, dtype=np.float32) * np.float32(-2.0 * math.log(ROPE_BASE) / (head_dim // 2)))
    return jnp.asarray(np.broadcast_to(freq[:, None], (quarter, tokens)))


def rotate(values, cos, sin):
    quarter = cos.shape[0]
    first, second = values[:quarter], values[quarter : 2 * quarter]
    return jnp.concatenate([first * cos - second * sin, second * cos + first * sin, values[2 * quarter :]], axis=0)


def rows_of(index, size):
    return pl.ds(pl.multiple_of(index * size, size), size)


def dot(lhs, rhs):
    return jnp.dot(lhs, rhs, preferred_element_type=F32)


def dot_t(lhs, rhs):
    return lax.dot_general(lhs, rhs, (((1,), (1,)), ((), ())), preferred_element_type=F32)


def full_barrier(n_dev):
    me = lax.axis_index(AXIS)
    barrier = pltpu.get_barrier_semaphore()

    def tell(step):
        pl.semaphore_signal(barrier, inc=1, device_id={AXIS: lax.rem(me + step, n_dev)}, device_id_type=pl.DeviceIdType.MESH)

    each(1, n_dev, tell)
    pl.semaphore_wait(barrier, n_dev - 1)


def remote(src, dst, send_sem, recv_sem, peer):
    return pltpu.make_async_remote_copy(src_ref=src, dst_ref=dst, send_sem=send_sem, recv_sem=recv_sem, device_id={AXIS: peer}, device_id_type=pl.DeviceIdType.MESH)


def each(lower, upper, body):
    def step(index, carry):
        body(index)
        return carry

    lax.fori_loop(lower, upper, step, 0)


def alternate(index, step, size):
    away = (step + 1) // 2
    return lax.rem(index + jnp.where(lax.rem(step, 2) == 1, away, size - away), size)


class Exchange:
    def __init__(self, src, dst, send, recv):
        self.src, self.dst, self.send, self.recv = src, dst, send, recv

    def start(self, index, slot, peer):
        me = lax.axis_index(AXIS)
        src, dst, recv = self.src(index), self.dst(slot), self.recv(slot)

        @pl.when(peer != me)
        def _():
            remote(src, dst, self.send(index), recv, peer).start()

        @pl.when(peer == me)
        def _():
            pltpu.make_async_copy(src, dst, recv).start()

    def sent(self, index, peer):
        me = lax.axis_index(AXIS)

        @pl.when(peer != me)
        def _():
            remote(self.src(index), self.src(index), self.send(index), self.send(index), me).wait_send()

    def got(self, slot):
        dst = self.dst(slot)
        remote(dst, dst, self.recv(slot), self.recv(slot), lax.axis_index(AXIS)).wait_recv()


def early_events(n_event):
    return 2 if n_event > 4 else 0


def ring_order(side):
    queue, free, order = [(0.0, True, 0, 0), (0.0, False, 0, 0)], 0.0, []
    waiting = []
    while queue or waiting:
        if queue and (not waiting or free <= waiting[0][0]):
            at, along, s, h = queue.pop(0)
            free = max(free, at) + 1.0
            waiting.append((free + 0.5, (s + along, h + 1 - along)))
        else:
            at, (s, h) = waiting.pop(0)
            order.append((s, h))
            if h == 0 and s < side - 1:
                queue.append((at, True, s, h))
            if h < side - 1:
                queue.append((at, False, s, h))
    return order


def lookup(table, index):
    out = jnp.int32(table[0])
    for key, value in enumerate(table[1:], 1):
        out = jnp.where(index == key, jnp.int32(value), out)
    return out


def even_rows(tokens):
    return tokens // 4, tokens // 4


def lean_rows(tokens):
    return tokens * 5 // 16, tokens * 3 // 16


class Ring:
    def __init__(self, n_dev, own, everything, rows, ring_send, ring_recv, core_send, core_recv):
        self.own, self.all, self.rows = own, everything, rows
        self.ring_send, self.ring_recv, self.core_send, self.core_recv = ring_send, ring_recv, core_send, core_recv
        self.side = math.isqrt(n_dev // 2)
        self.tokens = own.shape[0]
        self.me = lax.axis_index(AXIS)
        self.core = lax.rem(self.me, 2)
        self.x, self.y = lax.rem(self.me // 2, self.side), self.me // (2 * self.side)

    def each_colour(self, body):
        for kind in range(2):
            each(0, 2, lambda way: body((kind, way)))

    def device(self, colour, along, across, core):
        side = self.side
        kind, way = colour
        sign = 1 - 2 * way
        dx, dy = (along, across) if kind == 0 else (across, along)
        x = lax.rem(self.x - sign * dx + 2 * side, side)
        y = lax.rem(self.y - sign * dy + 2 * side, side)
        return (y * side + x) * 2 + core

    def within(self, colour):
        kind, way = colour
        return kind * 2 * self.rows[0] + way * self.rows[kind]

    def place(self, colour, s, h, core):
        return pl.ds(pl.multiple_of(self.device(colour, s, h, core) * self.tokens + self.within(colour), 8), self.rows[colour[0]])

    def piece(self, colour, s, h):
        return self.all.at[self.place(colour, s, h, self.core)]

    def own_piece(self, colour):
        return self.own.at[pl.ds(pl.multiple_of(self.within(colour), 8), self.rows[colour[0]])]

    def sem(self, sems, colour, s, h):
        return sems.at[colour[0] * 2 + colour[1], s * self.side + h]

    def ring_copy(self, colour, s, h, along, src=None):
        to = (s + along, h + 1 - along)
        dst = self.piece(colour, s, h)
        peer = self.device(colour, -along, along - 1, self.core)
        return remote(dst if src is None else src, dst, self.sem(self.ring_send, colour, *to), self.sem(self.ring_recv, colour, *to), peer)

    def core_copy(self, colour, s, h, src=None):
        dst = self.piece(colour, s, h)
        return remote(dst if src is None else src, dst, self.sem(self.core_send, colour, s, h), self.sem(self.core_recv, colour, s, h), self.me + 1 - 2 * self.core)

    def arrival(self, colour, s, h):
        dst = self.piece(colour, s, h)
        return remote(dst, dst, self.sem(self.ring_send, colour, s, h), self.sem(self.ring_recv, colour, s, h), self.me)

    def core_arrival(self, colour, s, h):
        dst = self.all.at[self.place(colour, s, h, 1 - self.core)]
        return remote(dst, dst, self.sem(self.core_send, colour, s, h), self.sem(self.core_recv, colour, s, h), self.me)

    def begin(self):
        def one(colour):
            self.ring_copy(colour, 0, 0, 1, self.own_piece(colour)).start()
            self.ring_copy(colour, 0, 0, 0, self.own_piece(colour)).start()

        self.each_colour(one)
        self.each_colour(lambda colour: self.core_copy(colour, 0, 0, self.own_piece(colour)).start())

    def pass_on(self, s, h):
        def one(colour):
            self.arrival(colour, s, h).wait_recv()

            @pl.when((h == 0) & (s < self.side - 1))
            def _():
                self.ring_copy(colour, s, h, 1).start()

            @pl.when(h < self.side - 1)
            def _():
                self.ring_copy(colour, s, h, 0).start()

            self.core_copy(colour, s, h).start()

        self.each_colour(one)

    def got_core(self, s, h):
        self.each_colour(lambda colour: self.core_arrival(colour, s, h).wait_recv())

    def end(self):
        def sent(number):
            s, h = number // self.side, lax.rem(number, self.side)

            def one(colour):
                @pl.when((s > 0) | (h > 0))
                def _():
                    self.arrival(colour, s, h).wait_send()

                self.core_copy(colour, s, h).wait_send()

            self.each_colour(one)

        each(0, self.side * self.side, sent)


def front_part(
    n_dev, n_group, x_ref, dy_ref, pos_ref, freq_ref, gain_ref, bias_ref, wo_ref, wq_ref, wk_ref, wv_ref,
    h_all, dy_all, q_ref, k_ref, v_ref, da_ref, cos_ref, sin_ref, x_hat_ref, inv_ref, pos_in,
    h_send, h_recv, h_core_send, h_core_recv, dy_send, dy_recv, dy_core_send, dy_core_recv, w_sem, h_sem, wo_sem, pos_send, pos_recv, local, da_send, da_recv,
    h_own, w_ref, pick_ref, w_buf, h_buf, wo_buf, da_buf, pos_own,
):
    me = lax.axis_index(AXIS)
    tokens, width = x_ref.shape
    head_dim = v_ref.shape[1]
    heads_tile = w_buf.shape[2]
    d_block = w_buf.shape[1]
    span = wo_buf.shape[1]
    n_wo = wo_ref.shape[0] // span
    per_wo = span // head_dim
    h_ring = Ring(n_dev, h_own, h_all, even_rows(tokens), h_send, h_recv, h_core_send, h_core_recv)
    dy_ring = Ring(n_dev, dy_ref, dy_all, lean_rows(tokens), dy_send, dy_recv, dy_core_send, dy_core_recv)
    rows_n = h_ring.rows[0]
    order = [(0, 0)] + ring_order(h_ring.side)
    n_event = len(order)
    where = Exchange(lambda peer: pos_own, lambda origin: pos_in.at[origin], lambda peer: pos_send.at[peer], lambda origin: pos_recv.at[origin])

    da_copy = Exchange(lambda peer: da_buf.at[peer], lambda origin: da_ref.at[rows_of(origin, tokens)], lambda peer: da_send.at[peer], lambda origin: da_recv.at[origin])

    n_d = width // d_block
    kv_head = me // n_group

    def w_load(t, which):
        ref, head = ((wq_ref, me), (wk_ref, kv_head), (wv_ref, kv_head))[which]
        slot = lax.rem(t, 2)
        return pltpu.make_async_copy(ref.at[rows_of(t, d_block), rows_of(head // heads_tile, heads_tile)], w_buf.at[slot], w_sem.at[slot])

    own_dy = pltpu.make_async_copy(dy_ref, dy_all.at[rows_of(me, tokens)], local.at[0])
    own_h = pltpu.make_async_copy(h_own, h_all.at[rows_of(me, tokens)], local.at[1])
    own_dy.start()
    w_load(0, 0).start()

    def wo_turn(t):
        return alternate(me // per_wo, t, n_wo)

    def wo_load(t):
        slot = lax.rem(t, 2)
        return pltpu.make_async_copy(wo_ref.at[rows_of(wo_turn(t), span)], wo_buf.at[slot], wo_sem.at[slot])

    wo_load(jnp.int32(0)).start()
    wo_load(jnp.int32(1)).start()
    pos_own[...] = jnp.broadcast_to(pos_ref[...], pos_own.shape)
    gain, bias = 1.0 + gain_ref[...], bias_ref[...]

    def norm(t):
        rows = rows_of(t, 16)
        x = x_ref[rows, :].astype(F32)
        centered = x - jnp.sum(x, axis=1, keepdims=True) * (1.0 / width)
        inv = lax.rsqrt(jnp.sum(centered * centered, axis=1, keepdims=True) * (1.0 / width) + EPS)
        x_hat = centered * inv
        x_hat_ref[rows, :] = x_hat
        inv_ref[rows, :] = inv
        h_own[rows, :] = (x_hat * gain + bias).astype(BF16)

    each(0, tokens // 16, norm)
    full_barrier(n_dev)

    def send_pos(step):
        peer = alternate(me, step, n_dev)
        where.start(peer, me, peer)

    h_ring.begin()
    each(0, n_dev, send_pos)
    own_h.start()

    for which in range(3):
        head = me if which == 0 else kv_head

        def pick(t):
            @pl.when(t + 1 < n_d)
            def _():
                w_load(t + 1, which).start()

            w_load(t, which).wait()
            pick_ref[...] = jnp.swapaxes(w_buf[lax.rem(t, 2)], 0, 1)
            w_ref[rows_of(t, d_block), which * head_dim : (which + 1) * head_dim] = pick_ref[lax.rem(head, heads_tile)]

        each(0, n_d, pick)
        if which < 2:
            w_load(0, which + 1).start()
        if which == 1:
            h_ring.pass_on(*(jnp.int32(v) for v in order[1]))
    own_dy.wait()
    own_h.wait()

    def tables(origin):
        where.got(origin)
        angles = freq_ref[...] * pos_in[origin, 0:1, :].astype(F32)
        cos_ref[:, rows_of(origin, tokens)] = jnp.cos(angles)
        sin_ref[:, rows_of(origin, tokens)] = jnp.sin(angles)

    def event(e):
        return lookup([p[0] for p in order], e), lookup([p[1] for p in order], e)

    def places_of(ring, s, h):
        return [ring.place((kind, way), s, h, core) for kind in range(2) for way in range(2) for core in range(2)]

    def fetch(ring, buf, sem, e):
        slot = lax.rem(e, 2)
        s, h = event(e)
        ring.got_core(s, h)
        for n, place in enumerate(places_of(ring, s, h)):
            pltpu.make_async_copy(ring.all.at[place], buf.at[slot, pl.ds(n * rows_n, rows_n)], sem.at[slot]).start()

    def fetched(ring, buf, sem, e):
        slot = lax.rem(e, 2)
        pltpu.make_async_copy(ring.all.at[pl.ds(0, 8 * rows_n)], buf.at[slot], sem.at[slot]).wait()
        return buf[slot]

    def send_da(t):
        def one(u):
            peer = wo_turn(t) * per_wo + lax.rem(u + me, per_wo)
            da_copy.start(peer, me, peer)

        each(0, per_wo, one)

    def make_da(t):
        @pl.when((t > 0) & (t <= n_wo))
        def _():
            send_da(t - 1)

        @pl.when((t >= 0) & (t < n_wo))
        def _():
            wo_load(t).wait()
            da = dot_t(dy_ref[...], wo_buf[lax.rem(t, 2)]).astype(BF16)
            for u in range(per_wo):
                da_buf[wo_turn(t) * per_wo + u] = da[:, u * head_dim : (u + 1) * head_dim]

            @pl.when(t + 2 < n_wo)
            def _():
                wo_load(t + 2).start()

    def project_rows(e):
        s, h = event(e)
        out = dot(fetched(h_ring, h_buf, h_sem, e), w_ref[...])
        for n, place in enumerate(places_of(h_ring, s, h)):
            part = out[n * rows_n : (n + 1) * rows_n]
            q_ref[place, :] = part[:, :head_dim]
            k_ref[place, :] = part[:, head_dim : 2 * head_dim]
            v_ref[place, :] = part[:, 2 * head_dim :].astype(BF16)

    def step(e):
        @pl.when((e > 1) & (e < n_event))
        def _():
            h_ring.pass_on(*event(e))

        @pl.when(e == max(n_event - 5, 1))
        def _():
            dy_ring.begin()

        for number in range(1, early_events(n_event) + 1):
            @pl.when(e == n_event - 3 + 2 * number)
            def _():
                dy_ring.pass_on(*(jnp.int32(v) for v in order[number]))

        @pl.when(e <= n_event)
        def _():
            fetch(h_ring, h_buf, h_sem, e - 1)

        make_da(e - 1)

        @pl.when((e > 1) & (e < n_event + 2))
        def _():
            project_rows(e - 2)

        @pl.when(e == 3)
        def _():
            each(0, n_dev, tables)

    each(1, max(n_event, n_wo) + 2, step)
    h_ring.end()

    def drain(index):
        where.sent(index, index)
        da_copy.sent(index, index)
        da_copy.got(index)

    each(0, n_dev, drain)


def causal(block):
    key = lax.broadcasted_iota(jnp.int32, (block, block), 0)
    query = lax.broadcasted_iota(jnp.int32, (block, block), 1)
    return key <= query


def part_sum(values):
    return jnp.sum(values.reshape(values.shape[0] // 8, 8, values.shape[1]), axis=0)


def main_part(
    ring_sems, n_dev, n_group, q_heads, kv_heads, n_buf, scale,
    q_raw, k_raw, v_ref, da_ref, cos_ref, sin_ref, x_ref, dy_own_ref, x_hat_ref, inv_ref, gain_ref, h_ref, dy_ref, wq_ref, wk_ref, wv_ref, wo_ref,
    out_ref, gx_ref, gwo_ref, gwq_ref, gwk_ref, gwv_ref, gain_out, bias_out,
    q_rows, kv_rows, sum_ref, at_ref, dqt_ref, a_head, dq_head, dkvt_ref, a_ref, g_ref, dkv_ref, land_one, land_two, kv_ref, kvt_ref, wq_out, wkv_out, dh_ref, part_ref, own_sum, sum_in, sum_mine,
    a_send, a_recv, dq_send, dq_recv, one_send, one_recv, two_send, two_recv, kv_send, kv_recv, near_send, near_recv,
    load_sem, q_send, q_recv, wkv_send, wkv_recv, s_send, s_recv, t_send, t_recv,
):
    me = lax.axis_index(AXIS)
    seq, head_dim = v_ref.shape
    tokens, width = x_ref.shape
    block = tokens * n_group
    n_block = seq // block
    half = block // 2
    fold = scale * math.log2(math.e)
    core, side = lax.rem(me, 2), lax.rem(me // 2, 2)
    member, group = lax.rem(me, n_group), me // n_group
    partner, across = me + 1 - 2 * core, me + 2 - 4 * side
    shift = lax.rem(group, max(2, n_block * 3 // 4))
    depth = width // n_dev
    span = math.lcm(depth, 128)
    n_col = width // span
    per_col = span // depth
    per_core = n_dev // 2
    n_sum = sum_mine.shape[0]
    q_cols = q_heads * head_dim

    def piece(index):
        return rows_of(index, tokens)

    def column(head):
        return rows_of(head, head_dim)

    def cols(j):
        return rows_of(j, span)

    a_copy = Exchange(lambda peer: a_head.at[piece(peer)], lambda head: a_ref.at[:, column(head)], lambda peer: a_send.at[peer], lambda head: a_recv.at[head])
    dq_copy = Exchange(lambda peer: dq_head.at[piece(peer)], lambda head: g_ref.at[:, column(head)], lambda peer: dq_send.at[peer], lambda head: dq_recv.at[head])
    kv_copy = Exchange(lambda n: kv_ref.at[n // 2, piece(lax.rem(n, 2))], lambda slot: g_ref.at[:, column(q_heads + slot)], lambda n: kv_send.at[n], lambda slot: kv_recv.at[slot])
    q_copy = Exchange(lambda peer: wq_out.at[rows_of(peer, depth)], lambda head: q_rows.at[head], lambda peer: q_send.at[peer], lambda head: q_recv.at[head])
    wkv_copy = Exchange(lambda i: wkv_out.at[rows_of(i, depth)], lambda head: kv_rows.at[head], lambda i: wkv_send.at[i], lambda head: wkv_recv.at[head])
    s_copy = Exchange(lambda peer: own_sum.at[pl.ds(peer * n_sum, n_sum)], lambda origin: sum_in.at[origin], lambda peer: s_send.at[peer], lambda origin: s_recv.at[origin])
    t_copy = Exchange(lambda peer: sum_mine, lambda origin: sum_ref.at[pl.ds(origin * n_sum, n_sum)], lambda peer: t_send.at[peer], lambda origin: t_recv.at[origin])


    def one_copy(i):
        return remote(dkv_ref.at[rows_of(i * 2 + 1 - core, half)], land_one.at[i], one_send.at[i], one_recv.at[i], partner)

    kind = side * kv_heads + group

    def half_of(i, which):
        return rows_of(i * 2 + which, half)

    def two_copy(i):
        return remote(dkv_ref.at[half_of(i, core), column(1 - side)], land_two.at[i], two_send.at[i], two_recv.at[i], across)

    def near_copy(i, which):
        return remote(kvt_ref.at[i], dkvt_ref.at[:, half_of(i, which)], near_send.at[i], near_recv.at[i], partner)

    def first(i):
        one_copy(i).start()

    def second(i):
        one_copy(i).wait_recv()
        for which in (1 - side, side):
            dkv_ref[half_of(i, core), column(which)] += land_one[i, :, column(which)]
        two_copy(i).start()

    def close(i):
        two_copy(i).wait_recv()
        rows = half_of(i, core)
        total = (dkv_ref[rows, column(side)] + land_two[i]).T

        def keep(values):
            values = values.astype(BF16)
            kvt_ref[i] = values
            dkvt_ref[:, rows] = values
            kv_ref[i] = values.T

        @pl.when(side == 0)
        def _():
            keep(rotate(total, cos_ref[:, rows], -sin_ref[:, rows]))

        @pl.when(side == 1)
        def _():
            keep(total)

    def spread(i):
        near_copy(i, core).start()
        for u in range(2):
            kv_copy.start(i * 2 + u, kind, i * n_group + core * 2 + u)

    steps = (first, second, close, spread)

    def block_at(t):
        return lax.rem(shift - 1 - t + 2 * n_block, n_block)

    def stages(t):
        for late in range(len(steps), 0, -1):
            n = t - late - shift

            @pl.when(n >= 0)
            def _():
                steps[late - 1](n_block - 1 - n)

    def stage_rest(late):
        each(jnp.maximum(n_block - late - shift, 0), n_block, lambda n: steps[late - 1](n_block - 1 - n))

    def send_pieces(i):
        def send(u):
            peer = i * n_group + lax.rem(u + me, n_group)
            a_copy.start(peer, me, peer)
            dq_copy.start(peer, me, peer)

        each(0, n_group, send)

    dy_ring = Ring(n_dev, dy_own_ref, dy_ref, lean_rows(tokens), *ring_sems)
    order = [(0, 0)] + ring_order(dy_ring.side)
    n_early = early_events(len(order))
    n_served = min(len(order) - 1, n_early + (n_block * (n_block + 1) - 1) // SERVE + 1)

    def serve(number):
        @pl.when(number < len(order))
        def _():
            dy_ring.pass_on(lookup([p[0] for p in order], number), lookup([p[1] for p in order], number))

    def tick(count):
        @pl.when(lax.rem(count, SERVE) == 0)
        def _():
            serve(count // SERVE + 1 + n_early)

    def attention(q_ref, k_ref, qt_ref, kt_ref, vt_ref, e_ref, dp_ref, peak_ref, dat_ref, mix_ref, acc_ref):
        def prepare(i):
            rows = rows_of(i, block)
            for raw, turned, plain in ((q_raw, qt_ref, q_ref), (k_raw, kt_ref, k_ref)):
                t = rotate(raw[rows, :].T, cos_ref[:, rows], sin_ref[:, rows]).astype(BF16)
                turned[:, rows] = t
                plain[rows, :] = t.T
            vt_ref[:, rows] = v_ref[rows, :].T
            dkv_ref[rows, :] = jnp.zeros((block, 2 * head_dim), F32)

        each(0, n_block, prepare)

        def compute(i, done):
            own = rows_of(i, block)
            dat_ref[...] = da_ref[own, :].T
            mix_ref[...] = jnp.zeros_like(mix_ref)
            acc_ref[...] = jnp.zeros_like(acc_ref)

            def scores(j, carry, diagonal):
                peak, total, mixed = carry
                tick(done + j)
                rows = rows_of(j, block)
                s = dot(k_ref[rows, :], qt_ref[:, own])
                if diagonal:
                    s = jnp.where(causal(block), s, -1e30)
                top = jnp.maximum(peak, jnp.max(s, axis=0, keepdims=True))
                e = jnp.exp2((s - top) * fold)
                dp = dot(v_ref[rows, :], dat_ref[...])
                fade = jnp.exp2((peak - top) * fold)
                e_ref[rows, :] = e
                dp_ref[rows, :] = dp
                peak_ref[j] = top
                return top, total * fade + part_sum(e), mixed * fade + part_sum(e * dp)

            start = (jnp.full((1, block), -jnp.inf, F32), jnp.zeros((8, block), F32), jnp.zeros((8, block), F32))
            carry = lax.fori_loop(0, i, functools.partial(scores, diagonal=False), start)
            peak, total, mixed = scores(i, carry, True)
            inv = 1.0 / jnp.sum(total, axis=0, keepdims=True)
            row_dot = jnp.sum(mixed, axis=0, keepdims=True) * inv
            q_own, da_own = q_ref[own, :], da_ref[own, :]

            def grads(j):
                tick(done + i + 1 + j)
                rows = rows_of(j, block)
                p = e_ref[rows, :] * (jnp.exp2((peak_ref[j] - peak) * fold) * inv)
                pb = p.astype(BF16)
                ds = ((dp_ref[rows, :] - row_dot) * (p * scale)).astype(BF16)
                dkv_ref[rows, :head_dim] += dot(ds, q_own)
                dkv_ref[rows, head_dim:] += dot(pb, da_own)
                mix_ref[...] += dot(vt_ref[:, rows], pb)
                acc_ref[...] += dot(kt_ref[:, rows], ds)

            each(0, i + 1, grads)
            at = mix_ref[...].astype(BF16)
            at_ref[:, own] = at
            a_head[own, :] = at.T
            dqt = rotate(acc_ref[...], cos_ref[:, own], -sin_ref[:, own]).astype(BF16)
            dqt_ref[:, own] = dqt
            dq_head[own, :] = dqt.T

        def iteration(t, done):
            stages(t)

            @pl.when(t > 0)
            def _():
                send_pieces(block_at(t - 1))

            i = block_at(t)
            compute(i, done)
            return done + 2 * (i + 1)

        lax.fori_loop(0, n_block, iteration, jnp.int32(0))

    pl.run_scoped(
        attention,
        pltpu.VMEM((seq, head_dim), BF16), pltpu.VMEM((seq, head_dim), BF16),
        pltpu.VMEM((head_dim, seq), BF16), pltpu.VMEM((head_dim, seq), BF16), pltpu.VMEM((head_dim, seq), BF16),
        pltpu.VMEM((seq, block), F32), pltpu.VMEM((seq, block), F32), pltpu.VMEM((n_block, 1, block), F32),
        pltpu.VMEM((head_dim, block), BF16), pltpu.VMEM((head_dim, block), F32), pltpu.VMEM((head_dim, block), F32),
    )

    def drain_sums():
        def one(i):
            one_copy(i).wait_send()
            two_copy(i).wait_send()
            near_copy(i, core).wait_send()
            near_copy(i, 1 - core).wait_recv()
            for u in range(2):
                kv_copy.sent(i * 2 + u, i * n_group + core * 2 + u)

        each(0, n_block, one)
        each(0, 2 * kv_heads, kv_copy.got)

    stage_rest(1)
    send_pieces(block_at(n_block - 1))

    def products(buf, w_buf):
        counts = (n_col, n_col, n_col, n_col // 2, n_col, n_col)
        starts = [sum(counts[:n]) for n in range(len(counts))]

        def loads(phase, j, slot):
            if phase == 1:
                return [pltpu.make_async_copy(wq_ref.at[cols(j)], w_buf.at[slot], load_sem.at[slot, 0])]
            if phase == 4:
                return [pltpu.make_async_copy(ref.at[cols(j)], w_buf.at[slot, :, pl.ds(n * kv_heads, kv_heads)], load_sem.at[slot, n]) for n, ref in enumerate((wk_ref, wv_ref))]
            ref = (h_ref, None, wo_ref, h_ref, None, dy_ref)[phase]
            col = core * (n_col // 2) + j if phase == 3 else j
            return [pltpu.make_async_copy(ref.at[:, cols(col)], buf.at[slot], load_sem.at[slot, 0])]

        def load(step):
            slot = lax.rem(step, n_buf)
            for phase, (begin, count) in enumerate(zip(starts, counts)):
                @pl.when((step >= begin) & (step < begin + count))
                def _():
                    for copy in loads(phase, step - begin, slot):
                        copy.start()

        def serve_late(number):
            for r in range(len(order) - 1 - n_served):
                @pl.when(number == 3 + 5 * r)
                def _():
                    serve(jnp.int32(n_served + 1 + r))

        last = len(counts) - 1

        def run(phase, body):
            def step(j):
                number = starts[phase] + j
                slot = lax.rem(number, n_buf)
                for copy in loads(phase, j, slot):
                    copy.wait()
                if phase < last:
                    serve_late(number)
                body(j, slot)

                @pl.when((number + n_buf < starts[last]) | (phase == last))
                def _():
                    load(number + n_buf)

            each(0, counts[phase], step)

        each(0, n_buf, load)

        def weight_columns(j, slot):
            @pl.when(j == n_col // 4)
            def _():
                stage_rest(2)

            wq_out[cols(j), :] = dot(dqt_ref[...], buf[slot]).T

        run(0, weight_columns)

        def send_rows(j):
            col = alternate(me // per_col, j, n_col)

            def send(u):
                peer = col * per_col + lax.rem(u + me, per_col)
                q_copy.start(peer, me, peer)

            each(0, per_col, send)

        def got_heads(head):
            a_copy.got(head)
            dq_copy.got(head)

        each(0, n_dev, got_heads)

        def flat(slot, n_head):
            rows = w_buf[slot, :, :n_head, :]
            return rows.reshape(rows.shape[0], n_head * head_dim)

        def back_query(j, slot):
            for late, at in ((3, n_col * 3 // 4), (4, n_col - 1)):
                @pl.when(j == at)
                def _():
                    stage_rest(late)

            @pl.when(j < n_col // 2)
            def _():
                send_rows(j)

            dh_ref[:, cols(j)] = dot_t(g_ref[:, :q_cols], flat(slot, q_heads))

        run(1, back_query)

        def output(j, slot):
            @pl.when(j < n_col // 2)
            def _():
                send_rows(n_col // 2 + j)

            out_ref[:, cols(j)] = (x_ref[:, cols(j)].astype(F32) + dot(a_ref[...], buf[slot])).astype(BF16)

        run(2, output)
        drain_sums()

        def weight_kv(j, slot):
            wkv_out[cols(j), :] = dot(dkvt_ref[...], buf[slot]).T

        run(3, weight_kv)

        def send_kv(step):
            index = alternate(lax.rem(me, per_core), step, per_core)
            wkv_copy.start(index, kind, core * per_core + index)

        def back_kv(j, slot):
            @pl.when(j == 0)
            def _():
                each(0, per_core, send_kv)

            dh_ref[:, cols(j)] += dot_t(g_ref[:, q_cols:], flat(slot, 2 * kv_heads))

        run(4, back_kv)

        part_ref[...] = jnp.zeros_like(part_ref)
        gain = 1.0 + gain_ref[...]

        def norm(t):
            rows = rows_of(t, 16)
            grad_h, x_hat = dh_ref[rows, :], x_hat_ref[rows, :]
            grad_hat = grad_h * gain
            one = jnp.sum(grad_hat, axis=1, keepdims=True) * (1.0 / width)
            two = jnp.sum(grad_hat * x_hat, axis=1, keepdims=True) * (1.0 / width)
            back = inv_ref[rows, :] * (grad_hat - one - x_hat * two)
            gx_ref[rows, :] = (dy_own_ref[rows, :].astype(F32) + back).astype(BF16)
            part_ref[0] += part_sum(grad_h * x_hat)
            part_ref[1] += part_sum(grad_h)

        each(0, tokens // 16, norm)
        own_sum[...] = jnp.zeros_like(own_sum)
        for which in range(2):
            total = jnp.sum(part_ref[which], axis=0, keepdims=True)
            for c in range(width // 128):
                own_sum[c, pl.ds(which, 1), :] = total[:, c * 128 : (c + 1) * 128]

        def to_all(copy):
            def send(step):
                peer = alternate(me, step, n_dev)
                copy.start(peer, me, peer)

            each(0, n_dev, send)

        def add(origin):
            sum_mine[...] += sum_in[origin]

        def weight_out(j, slot):
            @pl.when(j == 0)
            def _():
                to_all(s_copy)

            @pl.when(j == n_col // 2)
            def _():
                each(0, n_dev, s_copy.got)
                sum_mine[...] = jnp.zeros_like(sum_mine)
                each(0, n_dev, add)

            gwo_ref[:, cols(j)] = dot(at_ref[...], buf[slot])

            @pl.when(j == n_col // 2)
            def _():
                to_all(t_copy)

        for s, h in order:
            dy_ring.got_core(jnp.int32(s), jnp.int32(h))
        each(starts[last], starts[last] + n_buf, load)
        run(last, weight_out)

    pl.run_scoped(
        products,
        pltpu.VMEM((n_buf, seq, span), BF16),
        pltpu.VMEM((n_buf, span) + wq_ref.shape[1:], BF16),
    )

    dy_ring.end()

    def drain(index):
        for copy in (a_copy, dq_copy, s_copy, t_copy, q_copy):
            copy.sent(index, index)
        t_copy.got(index)
        q_copy.got(index)

    def drain_kv(index):
        wkv_copy.sent(index, core * per_core + index)

    each(0, n_dev, drain)
    each(0, per_core, drain_kv)
    each(0, 2 * kv_heads, wkv_copy.got)

    def settle(t):
        rows = rows_of(t, 8)
        gwq_ref[rows] = jnp.swapaxes(q_rows[:, rows, :], 0, 1)
        gwk_ref[rows] = jnp.swapaxes(kv_rows[:kv_heads, rows, :], 0, 1)
        gwv_ref[rows] = jnp.swapaxes(kv_rows[kv_heads:, rows, :], 0, 1)

    each(0, depth // 8, settle)
    for c in range(width // 128):
        gain_out[:, c * 128 : (c + 1) * 128] = sum_ref[c, 0:1, :]
        bias_out[:, c * 128 : (c + 1) * 128] = sum_ref[c, 1:2, :]


def block_kernel(n_dev, q_heads, kv_heads, n_buf, scale, *refs):
    x_ref, dy_ref, pos_ref, freq_ref, gain_ref, bias_ref, wo_ref, wq_ref, wk_ref, wv_ref = refs[:10]
    outs, (h_all, dy_all) = refs[10:18], refs[18:20]
    heads, pos_in, refs = refs[20:28], refs[28], refs[29:]
    front_sems, main_refs = refs[:16], refs[16:]
    tokens, width = x_ref.shape
    head_dim = wq_ref.shape[2]
    heads_tile = min(8, kv_heads)
    d_block = math.lcm(width // n_dev, 128)
    n_group = q_heads // kv_heads
    weights = (wo_ref, wq_ref, wk_ref, wv_ref)
    pl.run_scoped(
        functools.partial(front_part, n_dev, n_group, x_ref, dy_ref, pos_ref, freq_ref, gain_ref, bias_ref, *weights, h_all, dy_all, *heads, pos_in, *front_sems),
        pltpu.VMEM((tokens, width), BF16),
        pltpu.VMEM((width, 3 * head_dim), BF16),
        pltpu.VMEM((heads_tile, d_block, head_dim), BF16),
        pltpu.VMEM((2, d_block, heads_tile, head_dim), BF16),
        pltpu.VMEM((2, 2 * tokens, width), BF16),
        pltpu.VMEM((2, min(BLOCK, q_heads * head_dim // 2), width), BF16),
        pltpu.VMEM((n_dev, tokens, head_dim), BF16),
        pltpu.VMEM(pos_in.shape[1:], jnp.int32),
    )
    q, k, v, da, cos, sin, x_hat, inv = heads
    main_part(
        front_sems[4:8], n_dev, n_group, q_heads, kv_heads, n_buf, scale,
        q, k, v, da, cos, sin, x_ref, dy_ref, x_hat, inv, gain_ref, h_all, dy_all, wq_ref, wk_ref, wv_ref, wo_ref, *outs, *main_refs,
    )


def whole_block(n_dev, x_own, dy_own, positions, freq, gain, bias, wo, wq, wk, wv):
    tokens, width = x_own.shape
    q_heads, head_dim = wq.shape[1:]
    kv_heads = wk.shape[1]
    seq = tokens * n_dev
    n_group = q_heads // kv_heads
    n_block = n_dev // n_group
    depth = width // n_dev
    n_buf = 3
    n_sum = -(-width // (128 * n_dev))
    sums = (n_sum * n_dev, 8, 128)
    pieces = math.isqrt(n_dev // 2) ** 2
    whole, anywhere = pl.BlockSpec(memory_space=pltpu.VMEM), pl.BlockSpec(memory_space=pl.ANY)
    dma = pltpu.SemaphoreType.DMA
    return pl.pallas_call(
        functools.partial(block_kernel, n_dev, q_heads, kv_heads, n_buf, head_dim**-0.5),
        out_shape=[
            jax.ShapeDtypeStruct((tokens, width), BF16),
            jax.ShapeDtypeStruct((tokens, width), BF16),
            jax.ShapeDtypeStruct((head_dim, width), F32),
            jax.ShapeDtypeStruct((depth, q_heads, head_dim), F32),
            jax.ShapeDtypeStruct((depth, kv_heads, head_dim), F32),
            jax.ShapeDtypeStruct((depth, kv_heads, head_dim), F32),
            jax.ShapeDtypeStruct((1, width), F32),
            jax.ShapeDtypeStruct((1, width), F32),
            jax.ShapeDtypeStruct((seq, width), BF16),
            jax.ShapeDtypeStruct((seq, width), BF16),
        ],
        in_specs=[whole] * 6 + [anywhere] * 4,
        out_specs=[whole] * 8 + [anywhere] * 2,
        scratch_shapes=[
            pltpu.VMEM((seq, head_dim), F32),
            pltpu.VMEM((seq, head_dim), F32),
            pltpu.VMEM((seq, head_dim), BF16),
            pltpu.VMEM((seq, head_dim), BF16),
            pltpu.VMEM((head_dim // 4, seq), F32),
            pltpu.VMEM((head_dim // 4, seq), F32),
            pltpu.VMEM((tokens, width), F32),
            pltpu.VMEM((tokens, 1), F32),
            pltpu.VMEM((n_dev, 8, tokens), jnp.int32),
            dma((4, pieces)), dma((4, pieces)), dma((4, pieces)), dma((4, pieces)),
            dma((4, pieces)), dma((4, pieces)), dma((4, pieces)), dma((4, pieces)),
            dma((2,)), dma((2,)), dma((2,)), dma((n_dev,)), dma((n_dev,)), dma((3,)), dma((n_dev,)), dma((n_dev,)),
            pltpu.VMEM((q_heads, depth, head_dim), F32),
            pltpu.VMEM((2 * kv_heads, depth, head_dim), F32),
            pltpu.VMEM(sums, F32),
            pltpu.VMEM((head_dim, seq), BF16),
            pltpu.VMEM((head_dim, seq), BF16),
            pltpu.VMEM((seq, head_dim), BF16),
            pltpu.VMEM((seq, head_dim), BF16),
            pltpu.VMEM((head_dim, seq), BF16),
            pltpu.VMEM((tokens, q_heads * head_dim), BF16),
            pltpu.VMEM((tokens, (q_heads + 2 * kv_heads) * head_dim), BF16),
            pltpu.VMEM((seq, 2 * head_dim), F32),
            pltpu.VMEM((n_block, tokens * n_group // 2, 2 * head_dim), F32),
            pltpu.VMEM((n_block, tokens * n_group // 2, head_dim), F32),
            pltpu.VMEM((n_block, tokens * n_group // 2, head_dim), BF16),
            pltpu.VMEM((n_block, head_dim, tokens * n_group // 2), BF16),
            pltpu.VMEM((width, head_dim), F32),
            pltpu.VMEM((width // 2, head_dim), F32),
            pltpu.VMEM((tokens, width), F32),
            pltpu.VMEM((2, 8, width), F32),
            pltpu.VMEM(sums, F32),
            pltpu.VMEM((n_dev, n_sum, 8, 128), F32),
            pltpu.VMEM((n_sum, 8, 128), F32),
            dma((n_dev,)), dma((n_dev,)), dma((n_dev,)), dma((n_dev,)),
            dma((n_block,)), dma((n_block,)), dma((n_block,)), dma((n_block,)), dma((2 * n_block,)), dma((2 * kv_heads,)), dma((n_block,)), dma((n_block,)),
            dma((n_buf, 3)), dma((n_dev,)), dma((n_dev,)), dma((n_dev // 2,)), dma((2 * kv_heads,)), dma((n_dev,)), dma((n_dev,)), dma((n_dev,)), dma((n_dev,)),
        ],
        compiler_params=pltpu.CompilerParams(collective_id=1, has_side_effects=True, vmem_limit_bytes=VMEM_LIMIT, flags=FLAGS),
        cost_estimate=pl.CostEstimate(flops=6 * seq * seq * head_dim + 16 * seq * width * head_dim, bytes_accessed=16 * seq * width, transcendentals=seq * seq // 2),
        name="block",
    )(x_own, dy_own, positions, freq, gain, bias, wo, wq, wk, wv)


def solution(mesh):
    n_dev = mesh.shape[AXIS]

    def device_step(x_act, d_out, positions, ln_gain, ln_bias, w_query, w_key, w_value, w_out):
        n_batch, piece, width = x_act.shape
        head_dim = w_query.shape[2]
        tokens = n_batch * piece

        x_own, dy_own = x_act.reshape(tokens, width), d_out.reshape(tokens, width)
        gain, bias = ln_gain.reshape(1, width), ln_bias.reshape(1, width)
        block_out, grad_x, grad_wo, grad_wq, grad_wk, grad_wv, grad_gain, grad_bias, _, _ = whole_block(
            n_dev, x_own, dy_own, positions.reshape(1, tokens), frequencies(head_dim, tokens), gain, bias, w_out, w_query, w_key, w_value
        )
        return (block_out.reshape(x_act.shape), grad_x.reshape(x_act.shape), grad_wq, grad_wk, grad_wv, grad_wo, grad_gain.reshape(width), grad_bias.reshape(width))

    return jax.shard_map(device_step, mesh=mesh, in_specs=(P("dp", AXIS, None), P("dp", AXIS, None), P("dp", AXIS), P(None), P(None), P(None, None, None), P(None, None, None), P(None, None, None), P(None, None)), out_specs=(P("dp", AXIS, None), P("dp", AXIS, None), P(("dp", AXIS), None, None), P(("dp", AXIS), None, None), P(("dp", AXIS), None, None), P(("dp", AXIS), None), P("dp"), P("dp")), check_vma=False)
```
